16 devices in a mesh: rep: 2 (over y, z), dp: 8 (over x, core).
Axes of the slice: x: 4, y: 2, z: 1, core: 2. Of those that a mesh axis runs over, the one named last changes fastest.
The devices are a block of a 4x4x8 slice.
Arguments:
- x: bfloat16 [16, 2048, 1152], P(('rep', 'dp')), parts along dimension 0
- dy: bfloat16 [16, 2048, 1152], P(('rep', 'dp')), parts along dimension 0
- w_gate: bfloat16 [2, 1152, 4608], replicated
- w_up: bfloat16 [2, 1152, 4608], replicated
- w_down: bfloat16 [2, 4608, 1152], replicated
- m_w_gate: float32 [2, 1152, 4608], P(None, 'dp')
- m_w_up: float32 [2, 1152, 4608], P(None, 'dp')
- m_w_down: float32 [2, 4608, 1152], P(None, 'dp')
- v_w_gate: float32 [2, 1152, 4608], P(None, 'dp')
- v_w_up: float32 [2, 1152, 4608], P(None, 'dp')
- v_w_down: float32 [2, 4608, 1152], P(None, 'dp')
Outputs:
- output 1: bfloat16 [4, 1152, 4608], P('rep'), parts along dimension 0
- output 2: bfloat16 [4, 1152, 4608], P('rep'), parts along dimension 0
- output 3: bfloat16 [4, 4608, 1152], P('rep'), parts along dimension 0
- output 4: float32 [4, 1152, 4608], P('rep', 'dp'), parts along dimension 0
- output 5: float32 [4, 1152, 4608], P('rep', 'dp'), parts along dimension 0
- output 6: float32 [4, 4608, 1152], P('rep', 'dp'), parts along dimension 0
- output 7: float32 [4, 1152, 4608], P('rep', 'dp'), parts along dimension 0
- output 8: float32 [4, 1152, 4608], P('rep', 'dp'), parts along dimension 0
- output 9: float32 [4, 4608, 1152], P('rep', 'dp'), parts along dimension 0
There are 2 independent parts. The reference program is written for one: setup_inputs(seed, part) draws one part's arguments, and reference() takes and returns one part's arrays. A program takes and returns all parts, laid end to end along the dimension named above; an argument that names none is the same for every part.
All inputs are finite; a program needn't handle non-finite values.
Results may differ from the reference program's by a relative error of at most 0.022.
Values are sent between devices in bfloat16 or wider.
A program may use at most 768 MiB of HBM per device.

```python
import jax
import jax.numpy as jnp
from jax import lax

SEQUENCES = 8
TOKENS = 2048
D = 1152
FF = 4608
LAYERS = 2
NAMES = ("w_gate", "w_up", "w_down")
SHAPES = {"w_gate": (LAYERS, D, FF), "w_up": (LAYERS, D, FF), "w_down": (LAYERS, FF, D)}


def bump(key, n, height):
    away = (jnp.arange(n, dtype=jnp.int32) - jax.random.randint(key, (), 0, n, jnp.int32)) % n
    return jnp.where(away < n // 8, height, 1.0)


def together(key, own, strength):
    shared = jax.random.normal(key, own.shape[1:], jnp.float32)
    return (own + strength * shared) * lax.rsqrt(1 + strength * strength)


def setup_inputs(seed: int = 0, part: int = 0) -> dict:
    kx, kdy, ka, kb, kz, kf, kh, kl, *keys = jax.random.split(jax.random.key(seed), 8 + 3 * len(NAMES))
    kx, kdy, ka, kb = (jax.random.fold_in(k, part) for k in (kx, kdy, ka, kb))
    kw, km, kv = (keys[i::3] for i in range(3))
    shape = (SEQUENCES, TOKENS, D)
    much_x, much_dy = jax.random.uniform(kz, (2,), jnp.float32, 0.0, 1.0)
    loud = 2.0 ** jax.random.uniform(jax.random.fold_in(kz, 1), (), jnp.float32, -1.0, 2.0)
    layers = 2.0 ** jax.random.uniform(kl, (LAYERS, 1, 1), jnp.float32, -1.0, 1.0)
    x = together(ka, jax.random.normal(kx, shape, jnp.float32), much_x) * bump(kf, D, 4.0)
    dy = together(kb, jax.random.normal(kdy, shape, jnp.float32), much_dy)
    drawn = {"x": x.astype(jnp.bfloat16), "dy": (loud * dy * (SEQUENCES * TOKENS) ** -0.5).astype(jnp.bfloat16)}
    for key, name in zip(kw, NAMES, strict=True):
        w = jax.random.normal(key, SHAPES[name], jnp.float32) * SHAPES[name][1] ** -0.5
        drawn[name] = (w * {"w_gate": 1.0, "w_up": bump(kh, FF, 4.0), "w_down": layers}[name]).astype(jnp.bfloat16)
    for key, name in zip(km, NAMES, strict=True):
        drawn[f"m_{name}"] = 0.1 * jax.random.normal(key, SHAPES[name], jnp.float32)
    for key, name in zip(kv, NAMES, strict=True):
        drawn[f"v_{name}"] = jax.random.uniform(key, SHAPES[name], jnp.float32, 0.005, 0.015)
    return drawn


def matmul(a, w):
    return jnp.dot(a, w, preferred_element_type=jnp.float32).astype(jnp.bfloat16)


def normed(h):
    wide = h.astype(jnp.float32)
    scale = lax.rsqrt(jnp.mean(wide**2, -1, keepdims=True) + 1e-6)
    return (wide * scale).astype(jnp.bfloat16)


def layer(h, w):
    a = normed(h)
    gate = jnp.dot(a, w["w_gate"], preferred_element_type=jnp.float32)
    up = jnp.dot(a, w["w_up"], preferred_element_type=jnp.float32)
    return h + matmul((jax.nn.silu(gate) * up).astype(jnp.bfloat16), w["w_down"])


def adamw(w, m, v, g):
    m = 0.9 * m + 0.1 * g
    v = 0.95 * v + 0.05 * g * g
    step = m * lax.rsqrt(v + 1e-8) + 0.1 * w
    return (w - 0.02 * step).astype(jnp.bfloat16), m, v


def stack(weights, h):
    return lax.scan(lambda h, w: (layer(h, w), None), h, weights)[0]


def reference(x, dy, w_gate, w_up, w_down, m_w_gate, m_w_up, m_w_down, v_w_gate, v_w_up, v_w_down):
    weights = dict(zip(NAMES, (w_gate, w_up, w_down), strict=True))

    def take(so_far, sequence):
        h, by_y = sequence
        _, back = jax.vjp(lambda w: stack(w, h), weights)
        return jax.tree.map(lambda total, term: total + term.astype(jnp.float32), so_far, back(by_y)[0]), None

    none_yet = {name: jnp.zeros(w.shape, jnp.float32) for name, w in weights.items()}
    by_weights, _ = lax.scan(take, none_yet, (x, dy))
    gradients = [by_weights[name].astype(jnp.bfloat16).astype(jnp.float32) for name in NAMES]
    new = [
        adamw(w.astype(jnp.float32), m, v, g)
        for w, m, v, g in zip((w_gate, w_up, w_down), (m_w_gate, m_w_up, m_w_down), (v_w_gate, v_w_up, v_w_down), gradients, strict=True)
    ]
    return tuple(one[which] for which in range(3) for one in new)
```

```python
import jax
import jax.numpy as jnp
from jax import lax
from jax.sharding import PartitionSpec as P

NAMES = ("w_gate", "w_up", "w_down")
F32, BF16 = jnp.float32, jnp.bfloat16


def dot(a, b, dims):
    return lax.dot_general(a, b, (dims, ((), ())), preferred_element_type=F32)


def norm(h):
    wide = h.astype(F32)
    scale = lax.rsqrt(jnp.mean(wide**2, -1, keepdims=True) + 1e-6)
    return (wide * scale).astype(BF16)


def adamw(w, m, v, g):
    m = 0.9 * m + 0.1 * g
    v = 0.95 * v + 0.05 * g * g
    step = m * lax.rsqrt(v + 1e-8) + 0.1 * w
    return (w - 0.02 * step).astype(BF16), m, v


def hidden(gate, up):
    return (jax.nn.silu(gate) * up).astype(BF16)


def solution(mesh):
    def step(x, dy, wg, wu, wd, *moments):
        moments = {n: (moments[i], moments[i + 3]) for i, n in enumerate(NAMES)}
        weights = {"w_gate": wg, "w_up": wu, "w_down": wd}
        layers = wg.shape[0]
        me = lax.axis_index("dp")
        h, d = x[0], dy[0]

        kept = []
        for n in range(layers):
            a = norm(h)
            gate, up = dot(a, wg[n], ((1,), (0,))), dot(a, wu[n], ((1,), (0,)))
            z = hidden(gate, up)
            kept.append((h, a, gate, up, z))
            if n + 1 < layers:
                h = h + dot(z, wd[n], ((1,), (0,))).astype(BF16)

        new = {}
        def reduce(n, name, g):
            g = lax.psum_scatter(g, "dp", scatter_dimension=0, tiled=True).astype(F32)
            m, v = moments[name]
            rows = g.shape[0]
            w = lax.dynamic_slice_in_dim(weights[name][n], me * rows, rows, 0).astype(F32)
            w, m, v = adamw(w, m[n], v[n], g)
            new[name, n] = (lax.all_gather(w, "dp", axis=0, tiled=True), m, v)

        for n in reversed(range(layers)):
            h, a, gate, up, z = kept[n]
            reduce(n, "w_down", dot(z, d, ((0,), (0,))).astype(BF16))
            dz = dot(d, wd[n], ((1,), (1,))).astype(BF16)
            _, back = jax.vjp(lambda g, u: jax.nn.silu(g) * u, gate, up)
            dg, du = (t.astype(BF16) for t in back(dz.astype(F32)))
            reduce(n, "w_gate", dot(a, dg, ((0,), (0,))).astype(BF16))
            reduce(n, "w_up", dot(a, du, ((0,), (0,))).astype(BF16))
            if n:
                da = dot(dg, wg[n], ((1,), (1,))).astype(BF16) + dot(du, wu[n], ((1,), (1,))).astype(BF16)
                _, back = jax.vjp(norm, h)
                d = d + back(da)[0]
        return tuple(jnp.stack([new[name, n][i] for n in range(layers)]) for i in range(3) for name in NAMES)

    seq, whole, rows = P(("rep", "dp"), None, None), P(None, None, None), P(None, "dp", None)
    return jax.shard_map(
        step,
        mesh=mesh,
        in_specs=(seq, seq, whole, whole, whole) + (rows,) * 6,
        out_specs=(P("rep", None, None),) * 3 + (P("rep", "dp", None),) * 6,
        check_vma=False,
    )
```

```python
import functools

import jax
import jax.numpy as jnp
from jax import lax
from jax.experimental import pallas as pl
from jax.experimental.pallas import tpu as pltpu
from jax.sharding import PartitionSpec as P

NAMES = ("w_gate", "w_up", "w_down")
F32, BF16 = jnp.float32, jnp.bfloat16
NN, NT = (((1,), (0,)), ((), ())), (((1,), (1,)), ((), ()))
MESH = pl.DeviceIdType.MESH
ANY = pl.BlockSpec(memory_space=pl.ANY)
LANES = 128
CORES = 2
VMEM_BYTES = 62 << 20
VMEM_MOST = 67_043_328


def dot(a, b, dims=NN):
    return lax.dot_general(a, b, dims, preferred_element_type=F32)


def norm(h):
    wide = h.astype(F32)
    return (wide * lax.rsqrt(jnp.mean(wide**2, -1, keepdims=True) + 1e-6)).astype(BF16)


def strip(start, size):
    return pl.ds(pl.multiple_of(start, size), size)


def forward_kernel(tile, x_ref, wg_ref, wu_ref, wd_ref, a_ref, h_ref, total):
    block, blocks = pl.program_id(0), pl.num_programs(0)
    tiles = x_ref.shape[0] // tile

    @pl.when(block == 0)
    def _():
        def start(t, _):
            rows = strip(t * tile, tile)
            a_ref[0, rows, :] = norm(x_ref[rows, :])
            total[rows, :] = jnp.zeros((tile, total.shape[1]), F32)
            return 0

        lax.fori_loop(0, tiles, start, 0)

    def one(t, _):
        rows = strip(t * tile, tile)
        a = a_ref[0, rows, :]
        gate, up = dot(a, wg_ref[...]), dot(a, wu_ref[...])
        z = (jax.nn.sigmoid(gate) * gate * up).astype(BF16)
        total[rows, :] += dot(z, wd_ref[...])
        return 0

    lax.fori_loop(0, tiles, one, 0)

    @pl.when(block == blocks - 1)
    def _():
        def end(t, _):
            rows = strip(t * tile, tile)
            h = x_ref[rows, :] + total[rows, :].astype(BF16)
            h_ref[rows, :] = h
            a_ref[1, rows, :] = norm(h)
            return 0

        lax.fori_loop(0, tiles, end, 0)


def forward(x, wg, wu, wd, layer, width=512, tile=512):
    tokens, d = x.shape
    ff = wg.shape[2]
    whole = pl.BlockSpec((tokens, d), lambda i: (0, 0))
    return pl.pallas_call(
        functools.partial(forward_kernel, tile),
        grid=(ff // width,),
        out_shape=[jax.ShapeDtypeStruct((2, tokens, d), BF16), jax.ShapeDtypeStruct((tokens, d), BF16)],
        in_specs=[
            whole,
            pl.BlockSpec((None, d, width), lambda i: (layer, 0, i)),
            pl.BlockSpec((None, d, width), lambda i: (layer, 0, i)),
            pl.BlockSpec((None, width, d), lambda i: (layer, i, 0)),
        ],
        out_specs=[pl.BlockSpec((2, tokens, d), lambda i: (0, 0, 0)), whole],
        scratch_shapes=[pltpu.VMEM((tokens, d), F32)],
        compiler_params=pltpu.CompilerParams(dimension_semantics=("arbitrary",), vmem_limit_bytes=VMEM_BYTES),
        cost_estimate=pl.CostEstimate(flops=6 * tokens * d * ff, bytes_accessed=6 * d * ff + 8 * tokens * d, transcendentals=tokens * ff),
        name="forward",
    )(x, wg, wu, wd)


class Pool:
    def __init__(self, number, chips, core, chip, bufs, sems, gathered):
        self.number, self.chips, self.core, self.chip = number, chips, core, chip
        self.mine, self.other, self.cross, self.near, self.out1, self.out2, self.sum, self.new = bufs
        self.dma, self.credit, self.out_sem, self.ag_sem, self.own_sem = sems
        self.gathered = gathered
        self.slots, self.lanes, self.turns = self.mine.shape[0], self.cross.shape[0], self.ag_sem.shape[0]

    def index(self, chip, core):
        return lax.rem(chip + self.chips, self.chips) * CORES + core

    def device(self, hops, core=None):
        return {"dp": self.index(self.chip + hops, self.core if core is None else core)}

    def partner(self):
        return self.device(0, 1 - self.core)

    def hop(self, sems, src, dst, to):
        return pltpu.make_async_remote_copy(src_ref=src, dst_ref=dst, send_sem=sems.at[0], recv_sem=sems.at[1], device_id=to, device_id_type=MESH)

    def copies0(self, n, rows):
        slot = lax.rem(n, self.slots)
        src = self.mine.at[slot, 1 - self.core, :, pl.ds(0, rows), :]
        return [self.hop(self.dma.at[slot, 0], src, self.other.at[slot, :, pl.ds(0, rows), :], self.partner())]

    def copies1(self, n, rows):
        slot, sem, half = lax.rem(n, self.lanes), lax.rem(n, self.slots), pl.ds(0, rows // 2)
        return [
            self.hop(self.dma.at[sem, 1 + side], self.out1.at[slot, side, half, :], self.cross.at[slot, side, half, :], self.device(1 - 2 * side))
            for side in range(2)
        ]

    def copies2(self, n, rows):
        slot, sem, full = lax.rem(n, self.lanes), lax.rem(n, self.slots), pl.ds(0, rows)
        return [
            self.hop(self.dma.at[sem, 3 + side], self.out2.at[slot, side, full, :], self.near.at[slot, side, full, :], self.device(1 - 2 * side))
            for side in range(2)
        ]

    def both(self, n, hops, start, size):
        slot, chip = lax.rem(n, self.slots), lax.rem(self.chip + hops + self.chips, self.chips)
        rows = pl.ds(start, size)
        return self.mine[slot, self.core, chip, rows, :].astype(F32) + self.other[slot, chip, rows, :].astype(F32)

    def give(self, kind, to):
        pl.semaphore_signal(self.credit.at[kind], inc=1, device_id=to, device_id_type=MESH)

    def take(self, when, kinds):
        @pl.when(when)
        def _():
            for kind in kinds:
                pl.semaphore_wait(self.credit.at[kind], 1)

    def event0(self, n, rows):
        self.take(n >= self.slots, (0,))
        for copy in self.copies0(n, rows):
            copy.start()

    def event1(self, n, rows):
        slot, half = lax.rem(n, self.lanes), rows // 2
        for copy in self.copies0(n, rows):
            copy.wait()
        for side in range(2):
            self.out1[slot, side, pl.ds(0, half), :] = self.both(n, 2, side * half, half).astype(BF16)
        self.take(n >= self.lanes, (1, 2))
        for copy in self.copies1(n, rows):
            copy.start()

    def event2(self, n, rows):
        slot, half = lax.rem(n, self.lanes), rows // 2
        for copy in self.copies1(n, rows):
            copy.wait()
        for side in range(2):
            hops, there, here = 1 - 2 * side, pl.ds(side * half, half), pl.ds((1 - side) * half, half)
            passed = self.both(n, hops, side * half, half) + self.cross[slot, side, pl.ds(0, half), :].astype(F32)
            self.out2[slot, side, there, :] = passed.astype(BF16)
            self.out2[slot, side, here, :] = self.both(n, hops, (1 - side) * half, half).astype(BF16)

        @pl.when(n + self.lanes < self.number)
        def _():
            self.give(1, self.device(-1))
            self.give(2, self.device(1))

        self.take(n >= self.lanes, (3, 4))
        for copy in self.copies2(n, rows):
            copy.start()

    def event3(self, n, rows):
        slot = lax.rem(n, self.lanes)
        for copy in self.copies2(n, rows):
            copy.wait()
        total = self.both(n, 0, 0, rows)
        for side in range(2):
            total += self.near[slot, side, pl.ds(0, rows), :].astype(F32)

        @pl.when(n + self.slots < self.number)
        def _():
            self.give(0, self.partner())

        @pl.when(n + self.lanes < self.number)
        def _():
            self.give(3, self.device(-1))
            self.give(4, self.device(1))

        return total.astype(BF16).astype(F32)

    def block(self, n, hops, core, start, size):
        return self.gathered.at[n, self.index(self.chip + hops, core), pl.ds(start, size), :]

    def sems(self, n, kind):
        return self.ag_sem.at[lax.rem(n, self.turns), kind]

    def gathers1(self, n, rows):
        new, own = self.new.at[pl.ds(0, rows), :], self.block(n, 0, self.core, 0, rows)
        to = (self.device(1), self.device(-1), self.partner())
        return [self.hop(self.sems(n, kind), new, own, device) for kind, device in enumerate(to)] + [pltpu.make_async_copy(new, own, self.own_sem)]

    def gathers2(self, n, rows):
        copies = []
        for side in range(2):
            half = self.block(n, 2 * side - 1, self.core, side * (rows // 2), rows // 2)
            full = self.block(n, 2 * side - 1, self.core, 0, rows)
            copies.append(self.hop(self.sems(n, 3 + side), half, half, self.device(1 - 2 * side)))
            copies.append(self.hop(self.sems(n, 5 + side), full, full, self.partner()))
        return copies

    def gathers3(self, n, rows):
        opposite = self.block(n, 2, self.core, 0, rows)
        return [self.hop(self.sems(n, 7), opposite, opposite, self.partner())]

    def gather1(self, n, rows):
        for copy in self.gathers1(n, rows):
            copy.start()

    def gather2(self, n, rows):
        for copy in self.gathers1(n, rows):
            copy.wait()
        for copy in self.gathers2(n, rows):
            copy.start()

    def gather3(self, n, rows):
        for copy in self.gathers2(n, rows):
            copy.wait()
        for copy in self.gathers3(n, rows):
            copy.start()

    def gather4(self, n, rows):
        for copy in self.gathers3(n, rows):
            copy.wait()


def adam(w, m, v, g):
    m = 0.9 * m + 0.1 * g
    v = 0.95 * v + 0.05 * g * g
    w = w.astype(F32)
    return (w - 0.02 * (m * lax.rsqrt(v + 1e-8) + 0.1 * w)).astype(BF16)


def backward_kernel(chips, tile, *refs):
    a_hbm, dy_hbm, h_hbm, wg_hbm, wu_hbm, wd_hbm, mg_hbm, mu_hbm, md_hbm, vg_hbm, vu_hbm, vd_hbm, *refs = refs
    gg_hbm, gu_hbm, gd_hbm, whole_gu, whole_dn, dy0_hbm, *refs = refs
    a_tile, dy_tile, at_ref, dyt_ref, da_ref, wg_ref, wu_ref, wd_ref, z_ref, dgu_ref, m_ref, v_ref, w_ref, *refs = refs
    tile_sem, w_sem, state_sem, *pools = refs
    tokens, d = a_hbm.shape[1:]
    layers, _, ff = wg_hbm.shape
    width = chips * LANES
    blocks = ff // width
    pairs = blocks // 2
    rows = d // (CORES * chips)
    lane_blocks = d // LANES
    me = lax.axis_index("dp")
    chip, core = me // CORES, lax.rem(me, CORES)
    tiles = tokens // tile
    steps = layers * blocks
    full, small = d, d // 2

    gu = Pool(steps, chips, core, chip, pools[0:8], pools[8:13], whole_gu)
    dn = Pool(layers * (pairs + 1), chips, core, chip, pools[13:21], pools[21:26], whole_dn)

    def layer_of(j):
        return layers - 1 - j // blocks

    def block_of(j):
        j = lax.rem(j, blocks)
        return j // 2 + (pairs + 1) * lax.rem(j, 2)

    def columns(c, j):
        return strip(c * blocks * LANES + block_of(j) * LANES, LANES)

    def is_last(j):
        return lax.rem(j, blocks) == blocks - 1

    def gives_down(j):
        return (j >= 0) & (j < steps) & ((lax.rem(lax.rem(j, blocks), 2) == 1) | is_last(j))

    def down_of(j):
        return (j // blocks) * (pairs + 1) + lax.rem(j, blocks) // 2

    def for_down(j, act):
        @pl.when(gives_down(j) & ~is_last(j))
        def _():
            act(down_of(j), full)

        @pl.when(gives_down(j) & is_last(j))
        def _():
            act(down_of(j), small)

    def weight_copies(j):
        layer, slot = layer_of(j), lax.rem(j, 2)
        for c in range(chips):
            there, here = columns(c, j), pl.ds(c * LANES, LANES)
            yield pltpu.make_async_copy(wg_hbm.at[layer, :, there], wg_ref.at[slot, :, here], w_sem.at[slot, 3 * c])
            yield pltpu.make_async_copy(wu_hbm.at[layer, :, there], wu_ref.at[slot, :, here], w_sem.at[slot, 3 * c + 1])
            yield pltpu.make_async_copy(wd_hbm.at[layer, there, :], wd_ref.at[slot, here, :], w_sem.at[slot, 3 * c + 2])

    def load(src, buf, t, which):
        slot = lax.rem(t, 2)
        return pltpu.make_async_copy(src.at[strip(t * tile, tile), :], buf.at[slot], tile_sem.at[slot, which])

    def start_tile(j, t):
        load(a_hbm.at[layer_of(j)], a_tile, t, 0).start()

        @pl.when(layer_of(j) == layers - 1)
        def _():
            load(dy_hbm, dy_tile, t, 1).start()

        @pl.when(layer_of(j) < layers - 1)
        def _():
            load(dy0_hbm, dy_tile, t, 1).start()

    def wait_tile(t):
        load(dy_hbm, a_tile, t, 0).wait()
        load(dy_hbm, dy_tile, t, 1).wait()

    def gu_parts(n):
        for c in range(chips):
            for u in range(2):
                yield u * chips + c, u, pl.ds((u * chips + c) * rows, rows), columns(c, n)

    def gu_outs(n):
        for i, u, here, there in gu_parts(n):
            yield pltpu.make_async_copy(gu.sum.at[here, :], (gg_hbm, gu_hbm)[u].at[layer_of(n), :, there], gu.out_sem.at[i])

    def gu_state(n):
        layer = layer_of(n)
        for i, u, here, there in gu_parts(n):
            for k, (src, buf) in enumerate((((mg_hbm, mu_hbm)[u], m_ref), ((vg_hbm, vu_hbm)[u], v_ref))):
                yield pltpu.make_async_copy(src.at[layer, :, there], buf.at[here, :], state_sem.at[3 * i + k])
            src = (wg_hbm, wu_hbm)[u].at[layer, strip(me * rows, rows), there]
            yield pltpu.make_async_copy(src, w_ref.at[here, :], state_sem.at[3 * i + 2])

    def dn_parts(n, size):
        step = lax.rem(n, pairs + 1)
        start = step * LANES + core * (LANES // 2) if size == full else pairs * LANES * (1 - core)
        height = size // lane_blocks
        for b in range(lane_blocks):
            yield b, layers - 1 - n // (pairs + 1), start, height, pl.ds(b * height, height), pl.ds(b * LANES, LANES)

    def dn_outs(n, size):
        for b, layer, start, height, here, there in dn_parts(n, size):
            at = pl.ds(pl.multiple_of(start, LANES // 2), height)
            yield pltpu.make_async_copy(dn.sum.at[here, :], gd_hbm.at[layer, at, there], dn.out_sem.at[b])

    def dn_state(n, size):
        for b, layer, start, height, here, there in dn_parts(n, size):
            at = pl.ds(pl.multiple_of(start, LANES // 2), height)
            for k, (src, buf) in enumerate(((md_hbm, m_ref), (vd_hbm, v_ref))):
                yield pltpu.make_async_copy(src.at[layer, at, there], buf.at[here, :], state_sem.at[3 * b + k])
            at = pl.ds(pl.multiple_of(me * (d // 2) + start, LANES // 2), height)
            yield pltpu.make_async_copy(wd_hbm.at[layer, at, there], w_ref.at[here, :], state_sem.at[3 * b + 2])

    def start(copies):
        for copy in copies:
            copy.start()

    def wait(copies):
        for copy in copies:
            copy.wait()

    def gu_new(n):
        g = gu.event3(n, full)
        pl.when(n > 0)(lambda: wait(gu_outs(n - 1)))
        gu.sum[...] = g.astype(BF16)
        start(gu_outs(n))
        wait(gu_state(n))
        gu.new[...] = adam(w_ref[...], m_ref[...], v_ref[...], g)
        gu.gather1(n, full)

    def dn_new(n, size):
        g = dn.event3(n, size).T
        half, height = LANES // 2, size // lane_blocks
        if size == small:
            g = jnp.concatenate([g[:half], g[half:]], 1)
        if size == full:
            pl.when((n > 0) & (lax.rem(n, pairs + 1) > 0))(lambda: wait(dn_outs(n - 1, full)))
            pl.when((n > 0) & (lax.rem(n, pairs + 1) == 0))(lambda: wait(dn_outs(n - 1, small)))
        else:
            wait(dn_outs(n - 1, full))
        for b in range(lane_blocks):
            dn.sum[pl.ds(b * height, height), :] = g[:, b * LANES : (b + 1) * LANES].astype(BF16)
        start(dn_outs(n, size))
        wait(dn_state(n, size))
        for b in range(lane_blocks):
            here = pl.ds(b * height, height)
            dn.new[here, :] = adam(w_ref[here, :], m_ref[here, :], v_ref[here, :], g[:, b * LANES : (b + 1) * LANES])
        dn.gather1(n, size)

    def turn(buf, slot, into, part):
        for b in range(lane_blocks):
            into[pl.ds(b * LANES, LANES), part] = buf[slot, :, b * LANES : (b + 1) * LANES].T

    start_tile(0, 0)
    start(weight_copies(0))
    barrier = pltpu.get_barrier_semaphore()
    peers = (gu.partner(), gu.device(1), gu.device(-1))
    for peer in peers:
        pl.semaphore_signal(barrier, inc=1, device_id=peer, device_id_type=MESH)
    pl.semaphore_wait(barrier, len(peers))

    def first(t, _):
        part = strip(t * tile, tile)
        wait_tile(t)
        start_tile(0, lax.rem(t + 1, tiles))
        slot = lax.rem(t, 2)
        turn(a_tile, slot, at_ref, part)
        turn(dy_tile, slot, dyt_ref, part)
        da_ref[part, :] = jnp.zeros((tile, d), F32)
        return 0

    lax.fori_loop(0, tiles, first, 0)

    def compute_tile(j, t):
        slot, here = lax.rem(j, 2), lax.rem(t, 2)
        part = strip(t * tile, tile)
        wait_tile(t)
        pl.when(t + 1 < tiles)(lambda: start_tile(j, t + 1))
        a, dy = a_tile[here], dy_tile[here]
        gate = dot(a, wg_ref[slot])
        up = dot(a, wu_ref[slot])
        dz = dot(dy, wd_ref[slot], NT).astype(BF16).astype(F32)
        s = jax.nn.sigmoid(gate)
        act = s * gate
        z_ref[part, :] = (act * up).astype(BF16)
        dgu_ref[1, part, :] = (dz * act).astype(BF16)
        dgu_ref[0, part, :] = (dz * up * (s + act * (1 - s))).astype(BF16)

    def compute_down(j):
        slot = lax.rem(down_of(j), dn.slots)
        owner = lax.rem(lax.rem(j, blocks), 2)

        def part(h, _):
            g = dot(dyt_ref[...], z_ref[:, strip(h * 2 * LANES, 2 * LANES)]).astype(BF16)
            for c in range(2):
                dn.mine[slot, owner, 2 * h + c, :, :] = g[:, c * LANES : (c + 1) * LANES]
            return 0

        def last(h, _):
            g = dot(dyt_ref[...], z_ref[:, strip(h * 2 * LANES, 2 * LANES)])
            low = lax.broadcasted_iota(jnp.int32, (small, LANES), 1) < LANES // 2
            for c in range(2):
                top, bottom = g[:small, c * LANES : (c + 1) * LANES], g[small:, c * LANES : (c + 1) * LANES]
                dn.mine[slot, 0, 2 * h + c, pl.ds(0, small), :] = jnp.where(low, top, pltpu.roll(bottom, LANES // 2, 1)).astype(BF16)
                dn.mine[slot, 1, 2 * h + c, pl.ds(0, small), :] = jnp.where(low, pltpu.roll(top, LANES // 2, 1), bottom).astype(BF16)
            return 0

        @pl.when(~is_last(j))
        def _():
            lax.fori_loop(0, chips // 2, part, 0)

        @pl.when(is_last(j))
        def _():
            lax.fori_loop(0, chips // 2, last, 0)

    def compute_gate_up(j):
        slot = lax.rem(j, gu.slots)

        def part(s, _):
            u, h = s // (chips // 2), lax.rem(s, chips // 2)
            g = dot(at_ref[...], dgu_ref[u, :, strip(h * 2 * LANES, 2 * LANES)]).astype(BF16)
            for c in range(2):
                at = strip((u * chips + 2 * h + c) * rows, rows)
                for owner in range(CORES * chips):
                    gu.mine[slot, owner % CORES, owner // CORES, at, :] = g[owner * rows : (owner + 1) * rows, c * LANES : (c + 1) * LANES]
            return 0

        lax.fori_loop(0, chips, part, 0)

    def compute_da(j, t):
        slot = lax.rem(j, 2)
        part = strip(t * tile, tile)
        da_ref[part, :] += dot(dgu_ref[0, part, :], wg_ref[slot], NT) + dot(dgu_ref[1, part, :], wu_ref[slot], NT)

    def change_layer():
        size = tile // 4

        def keep(t):
            return pltpu.make_async_copy(dy_tile.at[lax.rem(t, 2)], dy0_hbm.at[strip(t * tile, tile), :], tile_sem.at[lax.rem(t, 2), 2])

        def begin(t):
            load(h_hbm, a_tile, t, 0).start()
            load(dy_hbm, dy_tile, t, 1).start()

        begin(0)

        def one(t, _):
            slot = lax.rem(t, 2)
            wait_tile(t)
            pl.when(t > 0)(lambda: keep(t - 1).wait())
            pl.when(t + 1 < tiles)(lambda: begin(t + 1))

            def piece(i, _):
                here, there = strip(i * size, size), strip(t * tile + i * size, size)
                wide = a_tile[slot, here, :].astype(F32)
                da = da_ref[there, :].astype(BF16).astype(F32)
                scale = lax.rsqrt(jnp.mean(wide * wide, -1, keepdims=True) + 1e-6)
                along = jnp.mean(da * wide, -1, keepdims=True)
                back = (da * scale - wide * (along * scale * scale * scale)).astype(BF16)
                dy_tile[slot, here, :] = dy_tile[slot, here, :] + back
                return 0

            lax.fori_loop(0, tile // size, piece, 0)
            keep(t).start()
            turn(dy_tile, slot, dyt_ref, strip(t * tile, tile))
            return 0

        lax.fori_loop(0, tiles, one, 0)
        keep(tiles - 1).wait()

    def on(j, act):
        pl.when((j >= 0) & (j < steps))(lambda: act(j))

    def step(j, _):
        busy = j < steps
        changes = is_last(j) & (layer_of(j) > 0) & busy

        @pl.when(busy)
        def _():
            wait(weight_copies(j))
            pl.when(j + 1 < steps)(lambda: start(weight_copies(j + 1)))

        def tile_step(t, _):
            pl.when(busy)(lambda: compute_tile(j, t))

            @pl.when(t == 0)
            def _():
                for_down(j - 1, dn.event2)
                for_down(j - 3, dn.gather2)

            @pl.when(t == 1)
            def _():
                on(j - 2, lambda n: gu.gather2(n, full))

            @pl.when(t == 2)
            def _():
                on(j - 1, lambda n: gu.event2(n, full))

            @pl.when(t == 3)
            def _():
                for_down(j - 2, dn_new)
                on(j - 1, lambda n: start(gu_state(n)))

            return 0

        lax.fori_loop(0, tiles, tile_step, 0)

        pl.when(busy)(lambda: compute_down(j))
        for_down(j, dn.event0)

        @pl.when(busy & (j + 1 < steps) & ~changes)
        def _():
            start_tile(j + 1, 0)

        on(j - 2, lambda n: gu.gather3(n, full))
        on(j - 3, lambda n: gu.gather4(n, full))

        @pl.when(busy)
        def _():
            compute_gate_up(j)
            gu.event0(j, full)

        for_down(j, dn.event1)
        on(j - 1, gu_new)
        for_down(j - 1, lambda n, size: start(dn_state(n, size)))

        @pl.when(busy & (layer_of(j) > 0))
        def _():
            def da_step(t, _):
                @pl.when(changes)
                def _():
                    pl.when(t == 0)(lambda: load(a_hbm.at[0], a_tile, 0, 0).start())
                    load(a_hbm.at[0], a_tile, t, 0).wait()
                    pl.when(t + 1 < tiles)(lambda: load(a_hbm.at[0], a_tile, t + 1, 0).start())

                compute_da(j, t)
                pl.when(changes)(lambda: turn(a_tile, lax.rem(t, 2), at_ref, strip(t * tile, tile)))
                return 0

            lax.fori_loop(0, tiles, da_step, 0)

        on(j, lambda n: gu.event1(n, full))
        for_down(j - 3, dn.gather3)
        for_down(j - 4, dn.gather4)

        @pl.when(changes)
        def _():
            change_layer()
            start_tile(j + 1, 0)

        return 0

    lax.fori_loop(0, steps + 4, step, 0)
    wait(gu_outs(steps - 1))
    wait(dn_outs(dn.number - 1, small))


def backward(mesh, a, dy, h, weights, m, v, tile=512):
    tokens, d = dy.shape
    layers, _, ff = weights[0].shape
    chips = mesh.shape["dp"] // CORES
    width = chips * LANES
    blocks = ff // width
    pairs = blocks // 2
    rows = d // (CORES * chips)
    assert layers == 2 and chips == 4 and blocks % 2 == 1 and blocks * width == ff and d % LANES == 0
    shape = lambda *s: jax.ShapeDtypeStruct(s, BF16)
    devices = CORES * chips
    outs = [
        shape(layers, rows, ff),
        shape(layers, rows, ff),
        shape(layers, ff // devices, d),
        shape(layers * blocks, devices, d, LANES),
        shape(layers * (pairs + 1), devices, d, LANES),
        shape(tokens, d),
    ]

    def pool(lanes, outputs):
        return [
            pltpu.VMEM((2, CORES, chips, d, LANES), BF16),
            pltpu.VMEM((2, chips, d, LANES), BF16),
            pltpu.VMEM((lanes, 2, d // 2, LANES), BF16),
            pltpu.VMEM((lanes, 2, d, LANES), BF16),
            pltpu.VMEM((lanes, 2, d // 2, LANES), BF16),
            pltpu.VMEM((lanes, 2, d, LANES), BF16),
            pltpu.VMEM((d, LANES), BF16),
            pltpu.VMEM((d, LANES), BF16),
            pltpu.SemaphoreType.DMA((2, 5, 2)),
            pltpu.SemaphoreType.REGULAR((5,)),
            pltpu.SemaphoreType.DMA((outputs,)),
            pltpu.SemaphoreType.DMA((4, 8, 2)),
            pltpu.SemaphoreType.DMA,
        ]

    return pl.pallas_call(
        functools.partial(backward_kernel, chips, tile),
        out_shape=outs,
        in_specs=[ANY] * 12,
        out_specs=[ANY] * len(outs),
        scratch_shapes=[
            pltpu.VMEM((2, tile, d), BF16),
            pltpu.VMEM((2, tile, d), BF16),
            pltpu.VMEM((d, tokens), BF16),
            pltpu.VMEM((d, tokens), BF16),
            pltpu.VMEM((tokens, d), F32),
            pltpu.VMEM((2, d, width), BF16),
            pltpu.VMEM((2, d, width), BF16),
            pltpu.VMEM((2, width, d), BF16),
            pltpu.VMEM((tokens, width), BF16),
            pltpu.VMEM((2, tokens, width), BF16),
            pltpu.VMEM((d, LANES), F32),
            pltpu.VMEM((d, LANES), F32),
            pltpu.VMEM((d, LANES), BF16),
            pltpu.SemaphoreType.DMA((2, 3)),
            pltpu.SemaphoreType.DMA((2, 3 * chips)),
            pltpu.SemaphoreType.DMA((max(6 * chips, 3 * (d // LANES)),)),
            *pool(1, 2 * chips),
            *pool(2, d // LANES),
        ],
        compiler_params=pltpu.CompilerParams(collective_id=1, has_side_effects=True, vmem_limit_bytes=VMEM_MOST),
        cost_estimate=pl.CostEstimate(flops=28 * tokens * d * ff, bytes_accessed=24 * d * ff, transcendentals=2 * tokens * ff),
        name="backward",
    )(a, dy, h, *weights, *m, *v)


def moments_kernel(m_ref, v_ref, g_ref, new_m, new_v):
    g = g_ref[...].astype(F32)
    new_m[...] = 0.9 * m_ref[...] + 0.1 * g
    new_v[...] = 0.95 * v_ref[...] + 0.05 * g * g


def moments(m, v, g, parts):
    layers, rows, cols = m.shape
    r, c = rows // parts[0], cols // parts[1]
    block = pl.BlockSpec((None, r, c), lambda l, i, j: (l, i, j))
    return pl.pallas_call(
        moments_kernel,
        grid=(layers, *parts),
        in_specs=[block] * 3,
        out_specs=[block] * 2,
        out_shape=[jax.ShapeDtypeStruct(m.shape, F32)] * 2,
        compiler_params=pltpu.CompilerParams(dimension_semantics=("arbitrary",) * 3, vmem_limit_bytes=VMEM_BYTES),
        cost_estimate=pl.CostEstimate(flops=8 * m.size, bytes_accessed=18 * m.size, transcendentals=0),
        name="moments",
    )(m, v, g)


def place_columns_kernel(x_ref, out_ref):
    blocks, devices, rows, _ = x_ref.shape
    for j in range(blocks):
        at = j // 2 + (blocks // 2 + 1) * (j % 2)
        for device in range(devices):
            out_ref[pl.ds(device * rows, rows), pl.ds(at * LANES, LANES)] = x_ref[j, device]


def place_columns(chunks, which, layers, d, ff):
    number, devices, height, _ = chunks.shape
    chips = devices // CORES
    blocks, rows = number // layers, d // devices
    x = chunks.reshape(layers, blocks, devices, 2, chips, rows, LANES)
    return pl.pallas_call(
        place_columns_kernel,
        grid=(layers, chips),
        in_specs=[pl.BlockSpec((None, blocks, devices, None, None, rows, LANES), lambda l, c: (layers - 1 - l, 0, 0, which, c, 0, 0))],
        out_specs=pl.BlockSpec((None, d, ff // chips), lambda l, c: (l, 0, c)),
        out_shape=jax.ShapeDtypeStruct((layers, d, ff), BF16),
        compiler_params=pltpu.CompilerParams(dimension_semantics=("arbitrary",) * 2, vmem_limit_bytes=VMEM_BYTES),
        cost_estimate=pl.CostEstimate(flops=0, bytes_accessed=4 * layers * d * ff, transcendentals=0),
        name="place_columns",
    )(x)


def place_rows_kernel(x_ref, out_ref):
    chunks, height, _ = x_ref.shape
    pairs, cols = chunks - 1, out_ref.shape[1]
    core = lax.rem(pl.program_id(1), CORES)
    half = LANES // 2
    for b in range(cols // LANES):
        there = pl.ds(b * LANES, LANES)
        for n in range(pairs):
            out_ref[pl.ds(pl.multiple_of(n * LANES + core * half, half), LANES), there] = x_ref[n, pl.ds(b * LANES, LANES), :]
        out_ref[pl.ds(pl.multiple_of(pairs * LANES * (1 - core), half), half), there] = x_ref[pairs, pl.ds(b * half, half), :]


def place_rows(chunks, layers, d, ff):
    number, devices, height, _ = chunks.shape
    x = chunks.reshape(layers, number // layers, devices, height, LANES)
    return pl.pallas_call(
        place_rows_kernel,
        grid=(layers, devices),
        in_specs=[pl.BlockSpec((None, number // layers, None, height, LANES), lambda l, i: (layers - 1 - l, 0, i, 0, 0))],
        out_specs=pl.BlockSpec((None, ff // devices, d), lambda l, i: (l, i, 0)),
        out_shape=jax.ShapeDtypeStruct((layers, ff, d), BF16),
        compiler_params=pltpu.CompilerParams(dimension_semantics=("arbitrary",) * 2, vmem_limit_bytes=VMEM_BYTES),
        cost_estimate=pl.CostEstimate(flops=0, bytes_accessed=4 * layers * d * ff, transcendentals=0),
        name="place_rows",
    )(x)


def solution(mesh):
    def step(x, dy, *arrays):
        weights, m, v = (arrays[i : i + 3] for i in (0, 3, 6))
        x, dy = x[0], dy[0]
        layers, d, ff = weights[0].shape
        a, h = forward(x, *weights, 0)
        *sums, columns, rows, _ = backward(mesh, a, dy, h, weights, m, v)
        new = [place_columns(columns, which, layers, d, ff) for which in range(2)] + [place_rows(rows, layers, d, ff)]
        states = [moments(*mvg, parts) for *mvg, parts in zip(m, v, sums, ((1, 3), (1, 3), (3, 1)))]
        return (*new, *(state[0] for state in states), *(state[1] for state in states))

    seq, whole, rows = P(("rep", "dp"), None, None), P(None, None, None), P(None, "dp", None)
    return jax.shard_map(
        step,
        mesh=mesh,
        in_specs=(seq, seq, whole, whole, whole) + (rows,) * 6,
        out_specs=(P("rep", None, None),) * 3 + (P("rep", "dp", None),) * 6,
        check_vma=False,
    )
```

```python
import functools

import jax
import jax.numpy as jnp
from jax import lax
from jax.experimental import pallas as pl
from jax.experimental.pallas import tpu as pltpu
from jax.sharding import PartitionSpec as P

NAMES = ("w_gate", "w_up", "w_down")
F32, BF16 = jnp.float32, jnp.bfloat16
NN, NT = (((1,), (0,)), ((), ())), (((1,), (1,)), ((), ()))
MESH = pl.DeviceIdType.MESH
ANY = pl.BlockSpec(memory_space=pl.ANY)
LANES = 128
CORES = 2
VMEM_BYTES = 62 << 20
VMEM_MOST = 67_043_328


def dot(a, b, dims=NN):
    return lax.dot_general(a, b, dims, preferred_element_type=F32)


def norm(h):
    wide = h.astype(F32)
    return (wide * lax.rsqrt(jnp.mean(wide**2, -1, keepdims=True) + 1e-6)).astype(BF16)


def strip(start, size):
    return pl.ds(pl.multiple_of(start, size), size)


def forward_kernel(tile, x_ref, wg_ref, wu_ref, wd_ref, a_hbm, h_hbm, a_ref, total, ends, a_sem, end_sem):
    block, blocks = pl.program_id(0), pl.num_programs(0)
    tiles = x_ref.shape[0] // tile

    def keep(t):
        rows = strip(t * tile, tile)
        return pltpu.make_async_copy(a_ref.at[rows, :], a_hbm.at[0, rows, :], a_sem.at[t])

    def finish(t):
        slot, rows = lax.rem(t, 2), strip(t * tile, tile)
        yield pltpu.make_async_copy(ends.at[slot, 0], h_hbm.at[rows, :], end_sem.at[slot, 0])
        yield pltpu.make_async_copy(ends.at[slot, 1], a_hbm.at[1, rows, :], end_sem.at[slot, 1])

    @pl.when(block == 0)
    def _():
        def start(t, _):
            rows = strip(t * tile, tile)
            a_ref[rows, :] = norm(x_ref[rows, :])
            total[rows, :] = jnp.zeros((tile, total.shape[1]), F32)
            keep(t).start()
            return 0

        lax.fori_loop(0, tiles, start, 0)

    def one(t, _):
        rows = strip(t * tile, tile)
        a = a_ref[rows, :]
        gate, up = dot(a, wg_ref[...]), dot(a, wu_ref[...])
        z = (jax.nn.sigmoid(gate) * gate * up).astype(BF16)
        total[rows, :] += dot(z, wd_ref[...])

        @pl.when(block == blocks - 1)
        def _():
            slot = lax.rem(t, 2)
            keep(t).wait()

            @pl.when(t >= 2)
            def _():
                for copy in finish(t - 2):
                    copy.wait()

            h = x_ref[rows, :] + total[rows, :].astype(BF16)
            ends[slot, 0] = h
            ends[slot, 1] = norm(h)
            for copy in finish(t):
                copy.start()

        return 0

    lax.fori_loop(0, tiles, one, 0)

    @pl.when(block == blocks - 1)
    def _():
        for t in (tiles - 2, tiles - 1):
            for copy in finish(t):
                copy.wait()


def forward(x, wg, wu, wd, layer, width=768, tile=512):
    tokens, d = x.shape
    ff = wg.shape[2]
    return pl.pallas_call(
        functools.partial(forward_kernel, tile),
        grid=(ff // width,),
        out_shape=[jax.ShapeDtypeStruct((2, tokens, d), BF16), jax.ShapeDtypeStruct((tokens, d), BF16)],
        in_specs=[
            pl.BlockSpec((tokens, d), lambda i: (0, 0)),
            pl.BlockSpec((None, d, width), lambda i: (layer, 0, i)),
            pl.BlockSpec((None, d, width), lambda i: (layer, 0, i)),
            pl.BlockSpec((None, width, d), lambda i: (layer, i, 0)),
        ],
        out_specs=[ANY, ANY],
        scratch_shapes=[
            pltpu.VMEM((tokens, d), BF16),
            pltpu.VMEM((tokens, d), F32),
            pltpu.VMEM((2, 2, tile, d), BF16),
            pltpu.SemaphoreType.DMA((tokens // tile,)),
            pltpu.SemaphoreType.DMA((2, 2)),
        ],
        compiler_params=pltpu.CompilerParams(dimension_semantics=("arbitrary",), vmem_limit_bytes=VMEM_BYTES),
        cost_estimate=pl.CostEstimate(flops=6 * tokens * d * ff, bytes_accessed=6 * d * ff + 8 * tokens * d, transcendentals=tokens * ff),
        name="forward",
    )(x, wg, wu, wd)


class Pool:
    def __init__(self, number, chips, core, chip, bufs, sems, gathered):
        self.number, self.chips, self.core, self.chip = number, chips, core, chip
        self.mine, self.other, self.cross, self.near, self.out1, self.out2, self.sum, self.new = bufs
        self.dma, self.credit, self.out_sem, self.ag_sem, self.own_sem = sems
        self.gathered = gathered
        self.slots, self.lanes, self.turns = self.mine.shape[0], self.cross.shape[0], self.ag_sem.shape[0]

    def index(self, chip, core):
        return lax.rem(chip + self.chips, self.chips) * CORES + core

    def device(self, hops, core=None):
        return {"dp": self.index(self.chip + hops, self.core if core is None else core)}

    def partner(self):
        return self.device(0, 1 - self.core)

    def hop(self, sems, src, dst, to):
        return pltpu.make_async_remote_copy(src_ref=src, dst_ref=dst, send_sem=sems.at[0], recv_sem=sems.at[1], device_id=to, device_id_type=MESH)

    def copies0(self, n, rows):
        slot = lax.rem(n, self.slots)
        src = self.mine.at[slot, 1 - self.core, :, pl.ds(0, rows), :]
        return [self.hop(self.dma.at[slot, 0], src, self.other.at[slot, :, pl.ds(0, rows), :], self.partner())]

    def copies1(self, n, rows):
        slot, sem, half = lax.rem(n, self.lanes), lax.rem(n, self.slots), pl.ds(0, rows // 2)
        return [
            self.hop(self.dma.at[sem, 1 + side], self.out1.at[slot, side, half, :], self.cross.at[slot, side, half, :], self.device(1 - 2 * side))
            for side in range(2)
        ]

    def copies2(self, n, rows):
        slot, sem, full = lax.rem(n, self.lanes), lax.rem(n, self.slots), pl.ds(0, rows)
        return [
            self.hop(self.dma.at[sem, 3 + side], self.out2.at[slot, side, full, :], self.near.at[slot, side, full, :], self.device(1 - 2 * side))
            for side in range(2)
        ]

    def both(self, n, hops, start, size):
        slot, chip = lax.rem(n, self.slots), lax.rem(self.chip + hops + self.chips, self.chips)
        rows = pl.ds(start, size)
        return self.mine[slot, self.core, chip, rows, :].astype(F32) + self.other[slot, chip, rows, :].astype(F32)

    def give(self, kind, to):
        pl.semaphore_signal(self.credit.at[kind], inc=1, device_id=to, device_id_type=MESH)

    def take(self, when, kinds):
        @pl.when(when)
        def _():
            for kind in kinds:
                pl.semaphore_wait(self.credit.at[kind], 1)

    def event0(self, n, rows):
        self.take(n >= self.slots, (0,))
        for copy in self.copies0(n, rows):
            copy.start()

    def event1(self, n, rows):
        slot, half = lax.rem(n, self.lanes), rows // 2
        for copy in self.copies0(n, rows):
            copy.wait()
        for side in range(2):
            self.out1[slot, side, pl.ds(0, half), :] = self.both(n, 2, side * half, half).astype(BF16)
        self.take(n >= self.lanes, (1, 2))
        for copy in self.copies1(n, rows):
            copy.start()

    def event2(self, n, rows):
        slot, half = lax.rem(n, self.lanes), rows // 2
        for copy in self.copies1(n, rows):
            copy.wait()
        for side in range(2):
            hops, there, here = 1 - 2 * side, pl.ds(side * half, half), pl.ds((1 - side) * half, half)
            passed = self.both(n, hops, side * half, half) + self.cross[slot, side, pl.ds(0, half), :].astype(F32)
            self.out2[slot, side, there, :] = passed.astype(BF16)
            self.out2[slot, side, here, :] = self.both(n, hops, (1 - side) * half, half).astype(BF16)

        @pl.when(n + self.lanes < self.number)
        def _():
            self.give(1, self.device(-1))
            self.give(2, self.device(1))

        self.take(n >= self.lanes, (3, 4))
        for copy in self.copies2(n, rows):
            copy.start()

    def event3(self, n, rows):
        slot = lax.rem(n, self.lanes)
        for copy in self.copies2(n, rows):
            copy.wait()
        total = self.both(n, 0, 0, rows)
        for side in range(2):
            total += self.near[slot, side, pl.ds(0, rows), :].astype(F32)

        @pl.when(n + self.slots < self.number)
        def _():
            self.give(0, self.partner())

        @pl.when(n + self.lanes < self.number)
        def _():
            self.give(3, self.device(-1))
            self.give(4, self.device(1))

        return total.astype(BF16).astype(F32)

    def block(self, n, hops, core, start, size):
        return self.gathered.at[n, self.index(self.chip + hops, core), pl.ds(start, size), :]

    def sems(self, n, kind):
        return self.ag_sem.at[lax.rem(n, self.turns), kind]

    def gathers1(self, n, rows):
        new, own = self.new.at[pl.ds(0, rows), :], self.block(n, 0, self.core, 0, rows)
        to = (self.device(1), self.device(-1), self.partner())
        return [self.hop(self.sems(n, kind), new, own, device) for kind, device in enumerate(to)] + [pltpu.make_async_copy(new, own, self.own_sem)]

    def gathers2(self, n, rows):
        copies = []
        for side in range(2):
            half = self.block(n, 2 * side - 1, self.core, side * (rows // 2), rows // 2)
            full = self.block(n, 2 * side - 1, self.core, 0, rows)
            copies.append(self.hop(self.sems(n, 3 + side), half, half, self.device(1 - 2 * side)))
            copies.append(self.hop(self.sems(n, 5 + side), full, full, self.partner()))
        return copies

    def gathers3(self, n, rows):
        opposite = self.block(n, 2, self.core, 0, rows)
        return [self.hop(self.sems(n, 7), opposite, opposite, self.partner())]

    def gather1(self, n, rows):
        for copy in self.gathers1(n, rows):
            copy.start()

    def gather2(self, n, rows):
        for copy in self.gathers1(n, rows):
            copy.wait()
        for copy in self.gathers2(n, rows):
            copy.start()

    def gather3(self, n, rows):
        for copy in self.gathers2(n, rows):
            copy.wait()
        for copy in self.gathers3(n, rows):
            copy.start()

    def gather4(self, n, rows):
        for copy in self.gathers3(n, rows):
            copy.wait()


def adam(w, m, v, g):
    m = 0.9 * m + 0.1 * g
    v = 0.95 * v + 0.05 * g * g
    w = w.astype(F32)
    return (w - 0.02 * (m * lax.rsqrt(v + 1e-8) + 0.1 * w)).astype(BF16)


def backward_kernel(chips, tile, *refs):
    a_hbm, dy_hbm, h_hbm, wg_hbm, wu_hbm, wd_hbm, mg_hbm, mu_hbm, md_hbm, vg_hbm, vu_hbm, vd_hbm, *refs = refs
    gg_hbm, gu_hbm, gd_hbm, whole_gu, whole_dn, dy0_hbm, *refs = refs
    a_tile, dy_tile, at_ref, dyt_ref, da_ref, wg_ref, wu_ref, wd_ref, z_ref, dgu_ref, m_ref, v_ref, w_ref, *refs = refs
    tile_sem, w_sem, state_sem, *pools = refs
    tokens, d = a_hbm.shape[1:]
    layers, _, ff = wg_hbm.shape
    width = chips * LANES
    blocks = ff // width
    pairs = blocks // 2
    rows = d // (CORES * chips)
    lane_blocks = d // LANES
    me = lax.axis_index("dp")
    chip, core = me // CORES, lax.rem(me, CORES)
    tiles = tokens // tile
    steps = layers * blocks
    full, small = d, d // 2

    gu = Pool(steps, chips, core, chip, pools[0:8], pools[8:13], whole_gu)
    dn = Pool(layers * (pairs + 1), chips, core, chip, pools[13:21], pools[21:26], whole_dn)

    def layer_of(j):
        return layers - 1 - j // blocks

    def block_of(j):
        j = lax.rem(j, blocks)
        return j // 2 + (pairs + 1) * lax.rem(j, 2)

    def columns(c, j):
        return strip(c * blocks * LANES + block_of(j) * LANES, LANES)

    def is_last(j):
        return lax.rem(j, blocks) == blocks - 1

    def gives_down(j):
        return (j >= 0) & (j < steps) & ((lax.rem(lax.rem(j, blocks), 2) == 1) | is_last(j))

    def down_of(j):
        return (j // blocks) * (pairs + 1) + lax.rem(j, blocks) // 2

    def for_down(j, act):
        @pl.when(gives_down(j) & ~is_last(j))
        def _():
            act(down_of(j), full)

        @pl.when(gives_down(j) & is_last(j))
        def _():
            act(down_of(j), small)

    def weight_copies(j):
        layer, slot = layer_of(j), lax.rem(j, 2)
        for c in range(chips):
            there, here = columns(c, j), pl.ds(c * LANES, LANES)
            yield pltpu.make_async_copy(wg_hbm.at[layer, :, there], wg_ref.at[slot, :, here], w_sem.at[slot, 3 * c])
            yield pltpu.make_async_copy(wu_hbm.at[layer, :, there], wu_ref.at[slot, :, here], w_sem.at[slot, 3 * c + 1])
            yield pltpu.make_async_copy(wd_hbm.at[layer, there, :], wd_ref.at[slot, here, :], w_sem.at[slot, 3 * c + 2])

    def load(src, buf, t, which):
        slot = lax.rem(t, 2)
        return pltpu.make_async_copy(src.at[strip(t * tile, tile), :], buf.at[slot], tile_sem.at[slot, which])

    def start_tile(j, t):
        load(a_hbm.at[layer_of(j)], a_tile, t, 0).start()

        @pl.when(layer_of(j) == layers - 1)
        def _():
            load(dy_hbm, dy_tile, t, 1).start()

        @pl.when(layer_of(j) < layers - 1)
        def _():
            load(dy0_hbm, dy_tile, t, 1).start()

    def wait_tile(t):
        load(dy_hbm, a_tile, t, 0).wait()
        load(dy_hbm, dy_tile, t, 1).wait()

    def gu_parts(n):
        for c in range(chips):
            for u in range(2):
                yield u * chips + c, u, pl.ds((u * chips + c) * rows, rows), columns(c, n)

    def gu_outs(n):
        for i, u, here, there in gu_parts(n):
            yield pltpu.make_async_copy(gu.sum.at[here, :], (gg_hbm, gu_hbm)[u].at[layer_of(n), :, there], gu.out_sem.at[i])

    def gu_state(n):
        layer = layer_of(n)
        for i, u, here, there in gu_parts(n):
            for k, (src, buf) in enumerate((((mg_hbm, mu_hbm)[u], m_ref), ((vg_hbm, vu_hbm)[u], v_ref))):
                yield pltpu.make_async_copy(src.at[layer, :, there], buf.at[here, :], state_sem.at[3 * i + k])
            src = (wg_hbm, wu_hbm)[u].at[layer, strip(me * rows, rows), there]
            yield pltpu.make_async_copy(src, w_ref.at[here, :], state_sem.at[3 * i + 2])

    def dn_parts(n, size):
        step = lax.rem(n, pairs + 1)
        start = step * LANES + core * (LANES // 2) if size == full else pairs * LANES * (1 - core)
        height = size // lane_blocks
        for b in range(lane_blocks):
            yield b, layers - 1 - n // (pairs + 1), start, height, pl.ds(b * height, height), pl.ds(b * LANES, LANES)

    def dn_outs(n, size):
        for b, layer, start, height, here, there in dn_parts(n, size):
            at = pl.ds(pl.multiple_of(start, LANES // 2), height)
            yield pltpu.make_async_copy(dn.sum.at[here, :], gd_hbm.at[layer, at, there], dn.out_sem.at[b])

    def dn_state(n, size):
        for b, layer, start, height, here, there in dn_parts(n, size):
            at = pl.ds(pl.multiple_of(start, LANES // 2), height)
            for k, (src, buf) in enumerate(((md_hbm, m_ref), (vd_hbm, v_ref))):
                yield pltpu.make_async_copy(src.at[layer, at, there], buf.at[here, :], state_sem.at[3 * b + k])
            at = pl.ds(pl.multiple_of(me * (d // 2) + start, LANES // 2), height)
            yield pltpu.make_async_copy(wd_hbm.at[layer, at, there], w_ref.at[here, :], state_sem.at[3 * b + 2])

    def start(copies):
        for copy in copies:
            copy.start()

    def wait(copies):
        for copy in copies:
            copy.wait()

    def gu_new(n, rows):
        g = gu.event3(n, rows)
        pl.when(n > 0)(lambda: wait(gu_outs(n - 1)))
        gu.sum[...] = g.astype(BF16)
        start(gu_outs(n))
        wait(gu_state(n))
        gu.new[...] = adam(w_ref[...], m_ref[...], v_ref[...], g)
        gu.gather1(n, rows)

    def dn_new(n, size):
        g = dn.event3(n, size).T
        half, height = LANES // 2, size // lane_blocks
        if size == small:
            g = jnp.concatenate([g[:half], g[half:]], 1)
        if size == full:
            pl.when((n > 0) & (lax.rem(n, pairs + 1) > 0))(lambda: wait(dn_outs(n - 1, full)))
            pl.when((n > 0) & (lax.rem(n, pairs + 1) == 0))(lambda: wait(dn_outs(n - 1, small)))
        else:
            wait(dn_outs(n - 1, full))
        for b in range(lane_blocks):
            dn.sum[pl.ds(b * height, height), :] = g[:, b * LANES : (b + 1) * LANES].astype(BF16)
        start(dn_outs(n, size))
        wait(dn_state(n, size))
        for b in range(lane_blocks):
            here = pl.ds(b * height, height)
            dn.new[here, :] = adam(w_ref[here, :], m_ref[here, :], v_ref[here, :], g[:, b * LANES : (b + 1) * LANES])
        dn.gather1(n, size)

    def turn(buf, slot, into, part):
        for b in range(lane_blocks):
            into[pl.ds(b * LANES, LANES), part] = buf[slot, :, b * LANES : (b + 1) * LANES].T

    start_tile(0, 0)
    start(weight_copies(0))
    barrier = pltpu.get_barrier_semaphore()
    peers = (gu.partner(), gu.device(1), gu.device(-1))
    for peer in peers:
        pl.semaphore_signal(barrier, inc=1, device_id=peer, device_id_type=MESH)
    pl.semaphore_wait(barrier, len(peers))

    def compute_tile(j, t):
        slot, here = lax.rem(j, 2), lax.rem(t, 2)
        part = strip(t * tile, tile)
        wait_tile(t)
        pl.when(t + 1 < tiles)(lambda: start_tile(j, t + 1))
        a, dy = a_tile[here], dy_tile[here]
        gate = dot(a, wg_ref[slot])
        up = dot(a, wu_ref[slot])
        dz = dot(dy, wd_ref[slot], NT).astype(BF16).astype(F32)
        s = jax.nn.sigmoid(gate)
        act = s * gate
        z_ref[part, :] = (act * up).astype(BF16)
        dgu_ref[1, part, :] = (dz * act).astype(BF16)
        dgu_ref[0, part, :] = (dz * up * (s + act * (1 - s))).astype(BF16)

        @pl.when(j == 0)
        def _():
            turn(a_tile, here, at_ref, part)
            turn(dy_tile, here, dyt_ref, part)
            da_ref[part, :] = jnp.zeros((tile, d), F32)

    def compute_gate_up(j, s):
        slot, u, h = lax.rem(j, gu.slots), s // (chips // 2), lax.rem(s, chips // 2)
        g = dot(at_ref[...], dgu_ref[u, :, strip(h * 2 * LANES, 2 * LANES)]).astype(BF16)
        for c in range(2):
            at = strip((u * chips + 2 * h + c) * rows, rows)
            for owner in range(CORES * chips):
                gu.mine[slot, owner % CORES, owner // CORES, at, :] = g[owner * rows : (owner + 1) * rows, c * LANES : (c + 1) * LANES]

    def compute_down(j, h):
        slot = lax.rem(down_of(j), dn.slots)
        owner = lax.rem(lax.rem(j, blocks), 2)

        @pl.when(~is_last(j))
        def _():
            g = dot(dyt_ref[...], z_ref[:, strip(h * 2 * LANES, 2 * LANES)]).astype(BF16)
            for c in range(2):
                dn.mine[slot, owner, 2 * h + c, :, :] = g[:, c * LANES : (c + 1) * LANES]

        @pl.when(is_last(j))
        def _():
            g = dot(dyt_ref[...], z_ref[:, strip(h * 2 * LANES, 2 * LANES)])
            low = lax.broadcasted_iota(jnp.int32, (small, LANES), 1) < LANES // 2
            for c in range(2):
                top, bottom = g[:small, c * LANES : (c + 1) * LANES], g[small:, c * LANES : (c + 1) * LANES]
                dn.mine[slot, 0, 2 * h + c, pl.ds(0, small), :] = jnp.where(low, top, pltpu.roll(bottom, LANES // 2, 1)).astype(BF16)
                dn.mine[slot, 1, 2 * h + c, pl.ds(0, small), :] = jnp.where(low, pltpu.roll(top, LANES // 2, 1), bottom).astype(BF16)

    def compute_da(j, t):
        slot = lax.rem(j, 2)
        part = strip(t * tile, tile)
        da_ref[part, :] += dot(dgu_ref[0, part, :], wg_ref[slot], NT) + dot(dgu_ref[1, part, :], wu_ref[slot], NT)

    def change_layer():
        size = tile // 4

        def keep(t):
            return pltpu.make_async_copy(dy_tile.at[lax.rem(t, 2)], dy0_hbm.at[strip(t * tile, tile), :], tile_sem.at[lax.rem(t, 2), 2])

        def begin(t):
            load(h_hbm, a_tile, t, 0).start()
            load(dy_hbm, dy_tile, t, 1).start()

        begin(0)

        def one(t, _):
            slot = lax.rem(t, 2)
            wait_tile(t)
            pl.when(t > 0)(lambda: keep(t - 1).wait())
            pl.when(t + 1 < tiles)(lambda: begin(t + 1))

            def piece(i, _):
                here, there = strip(i * size, size), strip(t * tile + i * size, size)
                wide = a_tile[slot, here, :].astype(F32)
                da = da_ref[there, :].astype(BF16).astype(F32)
                scale = lax.rsqrt(jnp.mean(wide * wide, -1, keepdims=True) + 1e-6)
                along = jnp.mean(da * wide, -1, keepdims=True)
                back = (da * scale - wide * (along * scale * scale * scale)).astype(BF16)
                dy_tile[slot, here, :] = dy_tile[slot, here, :] + back
                return 0

            lax.fori_loop(0, tile // size, piece, 0)
            keep(t).start()
            turn(dy_tile, slot, dyt_ref, strip(t * tile, tile))
            return 0

        lax.fori_loop(0, tiles, one, 0)
        keep(tiles - 1).wait()

    def on(j, act):
        pl.when((j >= 0) & (j < steps))(lambda: act(j, full))

    events = {
        "tile": {0: [(on, gu.event2, 1)], 1: [(for_down, dn.gather3, 3)], 3: [(on, gu.gather2, 2)]},
        "gate_up": {
            0: [(for_down, dn.event2, 1)],
            1: [(on, gu.gather4, 3), (for_down, dn.gather2, 2)],
            2: [(on, lambda n, _: start(gu_state(n)), 1)],
            3: [(on, gu.event0, 0)],
        },
        "down": {1: [(for_down, dn.event0, 0), (on, gu.event1, 0)]},
        "da": {
            0: [(for_down, dn.gather4, 3), (on, gu_new, 1), (for_down, lambda n, size: start(dn_state(n, size)), 1)],
            2: [(on, gu.gather3, 2), (for_down, dn.event1, 0)],
            3: [(for_down, dn_new, 1)],
        },
    }
    longest = max(ago for part in events.values() for these in part.values() for _, _, ago in these)

    def step(j, _):
        busy = j < steps
        lower = layer_of(j) > 0
        changes = is_last(j) & lower & busy

        @pl.when(busy)
        def _():
            wait(weight_copies(j))
            pl.when(j + 1 < steps)(lambda: start(weight_copies(j + 1)))

        def parts(name, number, active, compute):
            def one(t, _):
                pl.when(active)(lambda: compute(j, t))
                for at, these in events[name].items():

                    @pl.when(t == at)
                    def _():
                        for stream, act, ago in these:
                            stream(j - ago, act)

                return 0

            lax.fori_loop(0, number, one, 0)

        def da_tile(j, t):
            @pl.when(changes)
            def _():
                pl.when(t == 0)(lambda: load(a_hbm.at[0], a_tile, 0, 0).start())
                load(a_hbm.at[0], a_tile, t, 0).wait()
                pl.when(t + 1 < tiles)(lambda: load(a_hbm.at[0], a_tile, t + 1, 0).start())

            compute_da(j, t)
            pl.when(changes)(lambda: turn(a_tile, lax.rem(t, 2), at_ref, strip(t * tile, tile)))

        parts("tile", tiles, busy, compute_tile)
        pl.when(busy & (j + 1 < steps) & ~changes)(lambda: start_tile(j + 1, 0))
        parts("gate_up", chips, busy, compute_gate_up)
        parts("down", chips // 2, busy, compute_down)
        parts("da", tiles, busy & lower, da_tile)

        @pl.when(changes)
        def _():
            change_layer()
            start_tile(j + 1, 0)

        return 0

    lax.fori_loop(0, steps + longest, step, 0)
    wait(gu_outs(steps - 1))
    wait(dn_outs(dn.number - 1, small))


def backward(mesh, a, dy, h, weights, m, v, tile=512):
    tokens, d = dy.shape
    layers, _, ff = weights[0].shape
    chips = mesh.shape["dp"] // CORES
    width = chips * LANES
    blocks = ff // width
    pairs = blocks // 2
    rows = d // (CORES * chips)
    assert layers == 2 and chips == 4 and blocks % 2 == 1 and blocks * width == ff and d % LANES == 0
    shape = lambda *s: jax.ShapeDtypeStruct(s, BF16)
    devices = CORES * chips
    outs = [
        shape(layers, rows, ff),
        shape(layers, rows, ff),
        shape(layers, ff // devices, d),
        shape(layers * blocks, devices, d, LANES),
        shape(layers * (pairs + 1), devices, d, LANES),
        shape(tokens, d),
    ]

    def pool(lanes, outputs):
        return [
            pltpu.VMEM((2, CORES, chips, d, LANES), BF16),
            pltpu.VMEM((2, chips, d, LANES), BF16),
            pltpu.VMEM((lanes, 2, d // 2, LANES), BF16),
            pltpu.VMEM((lanes, 2, d, LANES), BF16),
            pltpu.VMEM((lanes, 2, d // 2, LANES), BF16),
            pltpu.VMEM((lanes, 2, d, LANES), BF16),
            pltpu.VMEM((d, LANES), BF16),
            pltpu.VMEM((d, LANES), BF16),
            pltpu.SemaphoreType.DMA((2, 5, 2)),
            pltpu.SemaphoreType.REGULAR((5,)),
            pltpu.SemaphoreType.DMA((outputs,)),
            pltpu.SemaphoreType.DMA((4, 8, 2)),
            pltpu.SemaphoreType.DMA,
        ]

    return pl.pallas_call(
        functools.partial(backward_kernel, chips, tile),
        out_shape=outs,
        in_specs=[ANY] * 12,
        out_specs=[ANY] * len(outs),
        scratch_shapes=[
            pltpu.VMEM((2, tile, d), BF16),
            pltpu.VMEM((2, tile, d), BF16),
            pltpu.VMEM((d, tokens), BF16),
            pltpu.VMEM((d, tokens), BF16),
            pltpu.VMEM((tokens, d), F32),
            pltpu.VMEM((2, d, width), BF16),
            pltpu.VMEM((2, d, width), BF16),
            pltpu.VMEM((2, width, d), BF16),
            pltpu.VMEM((tokens, width), BF16),
            pltpu.VMEM((2, tokens, width), BF16),
            pltpu.VMEM((d, LANES), F32),
            pltpu.VMEM((d, LANES), F32),
            pltpu.VMEM((d, LANES), BF16),
            pltpu.SemaphoreType.DMA((2, 3)),
            pltpu.SemaphoreType.DMA((2, 3 * chips)),
            pltpu.SemaphoreType.DMA((max(6 * chips, 3 * (d // LANES)),)),
            *pool(1, 2 * chips),
            *pool(2, d // LANES),
        ],
        compiler_params=pltpu.CompilerParams(collective_id=1, has_side_effects=True, vmem_limit_bytes=VMEM_MOST),
        cost_estimate=pl.CostEstimate(flops=28 * tokens * d * ff, bytes_accessed=24 * d * ff, transcendentals=2 * tokens * ff),
        name="backward",
    )(a, dy, h, *weights, *m, *v)


def moments_kernel(*refs):
    number = len(refs) // 5
    for i in range(number):
        m_ref, v_ref, g_ref, new_m, new_v = refs[i::number]
        g = g_ref[...].astype(F32)
        new_m[...] = 0.9 * m_ref[...] + 0.1 * g
        new_v[...] = 0.95 * v_ref[...] + 0.05 * g * g


def moments(m, v, g, parts):
    blocks = []
    for one, (r, c) in zip(m, parts):
        blocks.append(pl.BlockSpec((None, one.shape[1] // r, one.shape[2] // c), (lambda l, i: (l, i, 0)) if r > 1 else (lambda l, i: (l, 0, i))))
    size = sum(one.size for one in m)
    new = pl.pallas_call(
        moments_kernel,
        grid=(m[0].shape[0], max(parts[0])),
        in_specs=blocks * 3,
        out_specs=blocks * 2,
        out_shape=[jax.ShapeDtypeStruct(one.shape, F32) for one in m] * 2,
        compiler_params=pltpu.CompilerParams(dimension_semantics=("arbitrary",) * 2, vmem_limit_bytes=VMEM_BYTES),
        cost_estimate=pl.CostEstimate(flops=8 * size, bytes_accessed=18 * size, transcendentals=0),
        name="moments",
    )(*m, *v, *g)
    return new


def place_columns_kernel(x_ref, gate_ref, up_ref):
    blocks, devices, _, rows, _ = x_ref.shape
    for j in range(blocks):
        at = j // 2 + (blocks // 2 + 1) * (j % 2)
        for device in range(devices):
            for u, out_ref in enumerate((gate_ref, up_ref)):
                out_ref[pl.ds(device * rows, rows), pl.ds(at * LANES, LANES)] = x_ref[j, device, u]


def place_columns(chunks, layers, d, ff):
    number, devices, height, _ = chunks.shape
    chips = devices // CORES
    blocks, rows = number // layers, d // devices
    x = chunks.reshape(layers, blocks, devices, 2, chips, rows, LANES)
    out = pl.BlockSpec((None, d // 2, ff // chips), lambda l, c, h: (l, h, c))
    return pl.pallas_call(
        place_columns_kernel,
        grid=(layers, chips, 2),
        in_specs=[pl.BlockSpec((None, blocks, devices // 2, 2, None, rows, LANES), lambda l, c, h: (layers - 1 - l, 0, h, 0, c, 0, 0))],
        out_specs=[out, out],
        out_shape=[jax.ShapeDtypeStruct((layers, d, ff), BF16)] * 2,
        compiler_params=pltpu.CompilerParams(dimension_semantics=("arbitrary",) * 3, vmem_limit_bytes=VMEM_BYTES),
        cost_estimate=pl.CostEstimate(flops=0, bytes_accessed=8 * layers * d * ff, transcendentals=0),
        name="place_columns",
    )(x)


def place_rows_kernel(x_ref, out_ref):
    chunks, height, _ = x_ref.shape
    pairs, cols = chunks - 1, out_ref.shape[1]
    core = lax.rem(pl.program_id(1), CORES)
    half = LANES // 2
    for b in range(cols // LANES):
        there = pl.ds(b * LANES, LANES)
        for n in range(pairs):
            out_ref[pl.ds(pl.multiple_of(n * LANES + core * half, half), LANES), there] = x_ref[n, pl.ds(b * LANES, LANES), :]
        out_ref[pl.ds(pl.multiple_of(pairs * LANES * (1 - core), half), half), there] = x_ref[pairs, pl.ds(b * half, half), :]


def place_rows(chunks, layers, d, ff):
    number, devices, height, _ = chunks.shape
    x = chunks.reshape(layers, number // layers, devices, height, LANES)
    return pl.pallas_call(
        place_rows_kernel,
        grid=(layers, devices),
        in_specs=[pl.BlockSpec((None, number // layers, None, height, LANES), lambda l, i: (layers - 1 - l, 0, i, 0, 0))],
        out_specs=pl.BlockSpec((None, ff // devices, d), lambda l, i: (l, i, 0)),
        out_shape=jax.ShapeDtypeStruct((layers, ff, d), BF16),
        compiler_params=pltpu.CompilerParams(dimension_semantics=("arbitrary",) * 2, vmem_limit_bytes=VMEM_BYTES),
        cost_estimate=pl.CostEstimate(flops=0, bytes_accessed=4 * layers * d * ff, transcendentals=0),
        name="place_rows",
    )(x)


def solution(mesh):
    def step(x, dy, *arrays):
        weights, m, v = (arrays[i : i + 3] for i in (0, 3, 6))
        x, dy = x[0], dy[0]
        layers, d, ff = weights[0].shape
        a, h = forward(x, *weights, 0)
        *sums, columns, rows, _ = backward(mesh, a, dy, h, weights, m, v)
        new = (*place_columns(columns, layers, d, ff), place_rows(rows, layers, d, ff))
        states = moments(m, v, sums, ((1, 9), (1, 9), (9, 1)))
        return (*new, *states)

    seq, whole, rows = P(("rep", "dp"), None, None), P(None, None, None), P(None, "dp", None)
    return jax.shard_map(
        step,
        mesh=mesh,
        in_specs=(seq, seq, whole, whole, whole) + (rows,) * 6,
        out_specs=(P("rep", None, None),) * 3 + (P("rep", "dp", None),) * 6,
        check_vma=False,
    )
```

```python
import functools

import jax
import jax.numpy as jnp
from jax import lax
from jax.experimental import pallas as pl
from jax.experimental.pallas import tpu as pltpu
from jax.sharding import PartitionSpec as P

NAMES = ("w_gate", "w_up", "w_down")
F32, BF16 = jnp.float32, jnp.bfloat16
NN, NT = (((1,), (0,)), ((), ())), (((1,), (1,)), ((), ()))
MESH = pl.DeviceIdType.MESH
ANY = pl.BlockSpec(memory_space=pl.ANY)
LANES = 128
CORES = 2
VMEM_BYTES = 62 << 20
VMEM_MOST = 67_043_328
COPY_FLOPS = 64


def dot(a, b, dims=NN):
    return lax.dot_general(a, b, dims, preferred_element_type=F32)


def norm(h):
    wide = h.astype(F32)
    return (wide * lax.rsqrt(jnp.mean(wide**2, -1, keepdims=True) + 1e-6)).astype(BF16)


def strip(start, size):
    return pl.ds(pl.multiple_of(start, size), size)


def forward_kernel(tile, x_ref, wg_ref, wu_ref, wd_ref, a_hbm, h_hbm, a_ref, total, ends, a_sem, end_sem):
    block, blocks = pl.program_id(0), pl.num_programs(0)
    tiles = x_ref.shape[0] // tile

    def keep(t):
        rows = strip(t * tile, tile)
        return pltpu.make_async_copy(a_ref.at[rows, :], a_hbm.at[0, rows, :], a_sem.at[t])

    def finish(t):
        slot, rows = lax.rem(t, 2), strip(t * tile, tile)
        yield pltpu.make_async_copy(ends.at[slot, 0], h_hbm.at[rows, :], end_sem.at[slot, 0])
        yield pltpu.make_async_copy(ends.at[slot, 1], a_hbm.at[1, rows, :], end_sem.at[slot, 1])

    @pl.when(block == 0)
    def _():
        def start(t, _):
            rows = strip(t * tile, tile)
            a_ref[rows, :] = norm(x_ref[rows, :])
            total[rows, :] = jnp.zeros((tile, total.shape[1]), F32)
            keep(t).start()
            return 0

        lax.fori_loop(0, tiles, start, 0)

    def one(t, _):
        rows = strip(t * tile, tile)
        a = a_ref[rows, :]
        gate, up = dot(a, wg_ref[...]), dot(a, wu_ref[...])
        z = (jax.nn.sigmoid(gate) * gate * up).astype(BF16)
        total[rows, :] += dot(z, wd_ref[...])

        @pl.when(block == blocks - 1)
        def _():
            slot = lax.rem(t, 2)
            keep(t).wait()

            @pl.when(t >= 2)
            def _():
                for copy in finish(t - 2):
                    copy.wait()

            h = x_ref[rows, :] + total[rows, :].astype(BF16)
            ends[slot, 0] = h
            ends[slot, 1] = norm(h)
            for copy in finish(t):
                copy.start()

        return 0

    lax.fori_loop(0, tiles, one, 0)

    @pl.when(block == blocks - 1)
    def _():
        for t in (tiles - 2, tiles - 1):
            for copy in finish(t):
                copy.wait()


def forward(x, wg, wu, wd, layer, width=768, tile=512):
    tokens, d = x.shape
    ff = wg.shape[2]
    return pl.pallas_call(
        functools.partial(forward_kernel, tile),
        grid=(ff // width,),
        out_shape=[jax.ShapeDtypeStruct((2, tokens, d), BF16), jax.ShapeDtypeStruct((tokens, d), BF16)],
        in_specs=[
            pl.BlockSpec((tokens, d), lambda i: (0, 0)),
            pl.BlockSpec((None, d, width), lambda i: (layer, 0, i)),
            pl.BlockSpec((None, d, width), lambda i: (layer, 0, i)),
            pl.BlockSpec((None, width, d), lambda i: (layer, i, 0)),
        ],
        out_specs=[ANY, ANY],
        scratch_shapes=[
            pltpu.VMEM((tokens, d), BF16),
            pltpu.VMEM((tokens, d), F32),
            pltpu.VMEM((2, 2, tile, d), BF16),
            pltpu.SemaphoreType.DMA((tokens // tile,)),
            pltpu.SemaphoreType.DMA((2, 2)),
        ],
        compiler_params=pltpu.CompilerParams(dimension_semantics=("arbitrary",), vmem_limit_bytes=VMEM_BYTES),
        cost_estimate=pl.CostEstimate(flops=6 * tokens * d * ff, bytes_accessed=6 * d * ff + 8 * tokens * d, transcendentals=tokens * ff),
        name="forward",
    )(x, wg, wu, wd)


class Pool:
    def __init__(self, number, chips, core, chip, bufs, sems, gathered):
        self.number, self.chips, self.core, self.chip = number, chips, core, chip
        self.mine, self.other, self.cross, self.near, self.out1, self.out2, self.sum, self.new = bufs
        self.dma, self.credit, self.out_sem, self.ag_sem, self.own_sem = sems
        self.gathered = gathered
        self.slots, self.lanes, self.turns = self.mine.shape[0], self.cross.shape[0], self.ag_sem.shape[0]

    def index(self, chip, core):
        return lax.rem(chip + self.chips, self.chips) * CORES + core

    def device(self, hops, core=None):
        return {"dp": self.index(self.chip + hops, self.core if core is None else core)}

    def partner(self):
        return self.device(0, 1 - self.core)

    def hop(self, sems, src, dst, to):
        return pltpu.make_async_remote_copy(src_ref=src, dst_ref=dst, send_sem=sems.at[0], recv_sem=sems.at[1], device_id=to, device_id_type=MESH)

    def copies0(self, n, rows):
        slot = lax.rem(n, self.slots)
        src = self.mine.at[slot, 1 - self.core, :, pl.ds(0, rows), :]
        return [self.hop(self.dma.at[slot, 0], src, self.other.at[slot, :, pl.ds(0, rows), :], self.partner())]

    def copies1(self, n, rows):
        slot, sem, half = lax.rem(n, self.lanes), lax.rem(n, self.slots), pl.ds(0, rows // 2)
        return [
            self.hop(self.dma.at[sem, 1 + side], self.out1.at[slot, side, half, :], self.cross.at[slot, side, half, :], self.device(1 - 2 * side))
            for side in range(2)
        ]

    def copies2(self, n, rows):
        slot, sem, full = lax.rem(n, self.lanes), lax.rem(n, self.slots), pl.ds(0, rows)
        return [
            self.hop(self.dma.at[sem, 3 + side], self.out2.at[slot, side, full, :], self.near.at[slot, side, full, :], self.device(1 - 2 * side))
            for side in range(2)
        ]

    def both(self, n, hops, start, size):
        slot, chip = lax.rem(n, self.slots), lax.rem(self.chip + hops + self.chips, self.chips)
        rows = pl.ds(start, size)
        return self.mine[slot, self.core, chip, rows, :].astype(F32) + self.other[slot, chip, rows, :].astype(F32)

    def give(self, kind, to):
        pl.semaphore_signal(self.credit.at[kind], inc=1, device_id=to, device_id_type=MESH)

    def take(self, when, kinds):
        @pl.when(when)
        def _():
            for kind in kinds:
                pl.semaphore_wait(self.credit.at[kind], 1)

    def event0(self, n, rows):
        self.take(n >= self.slots, (0,))
        for copy in self.copies0(n, rows):
            copy.start()

    def event1(self, n, rows):
        slot, half = lax.rem(n, self.lanes), rows // 2
        for copy in self.copies0(n, rows):
            copy.wait()
        for side in range(2):
            self.out1[slot, side, pl.ds(0, half), :] = self.both(n, 2, side * half, half).astype(BF16)
        self.take(n >= self.lanes, (1, 2))
        for copy in self.copies1(n, rows):
            copy.start()

    def event2(self, n, rows):
        slot, half = lax.rem(n, self.lanes), rows // 2
        for copy in self.copies1(n, rows):
            copy.wait()
        for side in range(2):
            hops, there, here = 1 - 2 * side, pl.ds(side * half, half), pl.ds((1 - side) * half, half)
            passed = self.both(n, hops, side * half, half) + self.cross[slot, side, pl.ds(0, half), :].astype(F32)
            self.out2[slot, side, there, :] = passed.astype(BF16)
            self.out2[slot, side, here, :] = self.both(n, hops, (1 - side) * half, half).astype(BF16)

        @pl.when(n + self.lanes < self.number)
        def _():
            self.give(1, self.device(-1))
            self.give(2, self.device(1))

        self.take(n >= self.lanes, (3, 4))
        for copy in self.copies2(n, rows):
            copy.start()

    def event3(self, n, rows):
        slot = lax.rem(n, self.lanes)
        for copy in self.copies2(n, rows):
            copy.wait()
        total = self.both(n, 0, 0, rows)
        for side in range(2):
            total += self.near[slot, side, pl.ds(0, rows), :].astype(F32)

        @pl.when(n + self.slots < self.number)
        def _():
            self.give(0, self.partner())

        @pl.when(n + self.lanes < self.number)
        def _():
            self.give(3, self.device(-1))
            self.give(4, self.device(1))

        return total.astype(BF16).astype(F32)

    def block(self, n, hops, core, start, size):
        return self.gathered.at[n, self.index(self.chip + hops, core), pl.ds(start, size), :]

    def sems(self, n, kind):
        return self.ag_sem.at[lax.rem(n, self.turns), kind]

    def gathers1(self, n, rows):
        new, own = self.new.at[pl.ds(0, rows), :], self.block(n, 0, self.core, 0, rows)
        to = (self.device(1), self.device(-1), self.partner())
        return [self.hop(self.sems(n, kind), new, own, device) for kind, device in enumerate(to)] + [pltpu.make_async_copy(new, own, self.own_sem)]

    def gathers2(self, n, rows):
        copies = []
        for side in range(2):
            half = self.block(n, 2 * side - 1, self.core, side * (rows // 2), rows // 2)
            full = self.block(n, 2 * side - 1, self.core, 0, rows)
            copies.append(self.hop(self.sems(n, 3 + side), half, half, self.device(1 - 2 * side)))
            copies.append(self.hop(self.sems(n, 5 + side), full, full, self.partner()))
        return copies

    def gathers3(self, n, rows):
        opposite = self.block(n, 2, self.core, 0, rows)
        return [self.hop(self.sems(n, 7), opposite, opposite, self.partner())]

    def gather1(self, n, rows):
        for copy in self.gathers1(n, rows):
            copy.start()

    def gather2(self, n, rows):
        for copy in self.gathers1(n, rows):
            copy.wait()
        for copy in self.gathers2(n, rows):
            copy.start()

    def gather3(self, n, rows):
        for copy in self.gathers2(n, rows):
            copy.wait()
        for copy in self.gathers3(n, rows):
            copy.start()

    def gather4(self, n, rows):
        for copy in self.gathers3(n, rows):
            copy.wait()


def adam(w, m, v, g):
    m = 0.9 * m + 0.1 * g
    v = 0.95 * v + 0.05 * g * g
    w = w.astype(F32)
    return (w - 0.02 * (m * lax.rsqrt(v + 1e-8) + 0.1 * w)).astype(BF16)


def backward_kernel(chips, tile, *refs):
    a_hbm, dy_hbm, h_hbm, wg_hbm, wu_hbm, wd_hbm, mg_hbm, mu_hbm, md_hbm, vg_hbm, vu_hbm, vd_hbm, *refs = refs
    gg_hbm, gu_hbm, gd_hbm, whole_gu, whole_dn, own_hbm, dy0_hbm, *refs = refs
    a_tile, dy_tile, at_ref, dyt_ref, da_ref, wg_ref, wu_ref, wd_ref, z_ref, dgu_ref, m_ref, v_ref, w_ref, *refs = refs
    tile_sem, w_sem, state_sem, rows_sem, *pools = refs
    tokens, d = a_hbm.shape[1:]
    layers, _, ff = wg_hbm.shape
    width = chips * LANES
    blocks = ff // width
    pairs = blocks // 2
    rows = d // (CORES * chips)
    lane_blocks = d // LANES
    me = lax.axis_index("dp")
    chip, core = me // CORES, lax.rem(me, CORES)
    tiles = tokens // tile
    steps = layers * blocks
    full, small = d, d // 2

    gu = Pool(steps, chips, core, chip, pools[0:8], pools[8:13], whole_gu)
    dn = Pool(layers * (pairs + 1), chips, core, chip, pools[13:21], pools[21:26], whole_dn)

    def layer_of(j):
        return layers - 1 - j // blocks

    def block_of(j):
        j = lax.rem(j, blocks)
        return j // 2 + (pairs + 1) * lax.rem(j, 2)

    def columns(c, j):
        return strip(c * blocks * LANES + block_of(j) * LANES, LANES)

    def is_last(j):
        return lax.rem(j, blocks) == blocks - 1

    def gives_down(j):
        return (j >= 0) & (j < steps) & ((lax.rem(lax.rem(j, blocks), 2) == 1) | is_last(j))

    def down_of(j):
        return (j // blocks) * (pairs + 1) + lax.rem(j, blocks) // 2

    def for_down(j, act):
        @pl.when(gives_down(j) & ~is_last(j))
        def _():
            act(down_of(j), full)

        @pl.when(gives_down(j) & is_last(j))
        def _():
            act(down_of(j), small)

    def weight_copies(j):
        layer, slot = layer_of(j), lax.rem(j, 2)
        for c in range(chips):
            there, here = columns(c, j), pl.ds(c * LANES, LANES)
            yield pltpu.make_async_copy(wg_hbm.at[layer, :, there], wg_ref.at[slot, :, here], w_sem.at[slot, 3 * c])
            yield pltpu.make_async_copy(wu_hbm.at[layer, :, there], wu_ref.at[slot, :, here], w_sem.at[slot, 3 * c + 1])
            yield pltpu.make_async_copy(wd_hbm.at[layer, there, :], wd_ref.at[slot, here, :], w_sem.at[slot, 3 * c + 2])

    def load(src, buf, t, which):
        slot = lax.rem(t, 2)
        return pltpu.make_async_copy(src.at[strip(t * tile, tile), :], buf.at[slot], tile_sem.at[slot, which])

    def start_tile(j, t):
        load(a_hbm.at[layer_of(j)], a_tile, t, 0).start()

        @pl.when(layer_of(j) == layers - 1)
        def _():
            load(dy_hbm, dy_tile, t, 1).start()

        @pl.when(layer_of(j) < layers - 1)
        def _():
            load(dy0_hbm, dy_tile, t, 1).start()

    def wait_tile(t):
        load(dy_hbm, a_tile, t, 0).wait()
        load(dy_hbm, dy_tile, t, 1).wait()

    def gu_parts(n):
        for c in range(chips):
            for u in range(2):
                yield u * chips + c, u, pl.ds((u * chips + c) * rows, rows), columns(c, n)

    def gu_outs(n):
        for i, u, here, there in gu_parts(n):
            yield pltpu.make_async_copy(gu.sum.at[here, :], (gg_hbm, gu_hbm)[u].at[layer_of(n), :, there], gu.out_sem.at[i])

    def gu_state(n):
        layer = layer_of(n)
        for i, u, here, there in gu_parts(n):
            for k, (src, buf) in enumerate((((mg_hbm, mu_hbm)[u], m_ref), ((vg_hbm, vu_hbm)[u], v_ref))):
                yield pltpu.make_async_copy(src.at[layer, :, there], buf.at[here, :], state_sem.at[3 * i + k])
            src = (wg_hbm, wu_hbm)[u].at[layer, strip(me * rows, rows), there]
            yield pltpu.make_async_copy(src, w_ref.at[here, :], state_sem.at[3 * i + 2])

    def dn_parts(n, size):
        step = lax.rem(n, pairs + 1)
        start = step * LANES + core * (LANES // 2) if size == full else pairs * LANES * (1 - core)
        height = size // lane_blocks
        for b in range(lane_blocks):
            yield b, layers - 1 - n // (pairs + 1), start, height, pl.ds(b * height, height), pl.ds(b * LANES, LANES)

    def dn_outs(n, size):
        for b, layer, start, height, here, there in dn_parts(n, size):
            at = pl.ds(pl.multiple_of(start, LANES // 2), height)
            yield pltpu.make_async_copy(dn.sum.at[here, :], gd_hbm.at[layer, at, there], dn.out_sem.at[b])

    def own_outs(n, size):
        for b, _, start, height, here, there in dn_parts(n, size):
            at = pl.ds(pl.multiple_of(start, LANES // 2), height)
            yield pltpu.make_async_copy(dn.new.at[here, :], own_hbm.at[at, there], rows_sem.at[b])

    def dn_state(n, size):
        for b, layer, start, height, here, there in dn_parts(n, size):
            at = pl.ds(pl.multiple_of(start, LANES // 2), height)
            for k, (src, buf) in enumerate(((md_hbm, m_ref), (vd_hbm, v_ref))):
                yield pltpu.make_async_copy(src.at[layer, at, there], buf.at[here, :], state_sem.at[3 * b + k])
            at = pl.ds(pl.multiple_of(me * (d // 2) + start, LANES // 2), height)
            yield pltpu.make_async_copy(wd_hbm.at[layer, at, there], w_ref.at[here, :], state_sem.at[3 * b + 2])

    def start(copies):
        for copy in copies:
            copy.start()

    def wait(copies):
        for copy in copies:
            copy.wait()

    def gu_new(n, rows):
        g = gu.event3(n, rows)
        pl.when(n > 0)(lambda: wait(gu_outs(n - 1)))
        gu.sum[...] = g.astype(BF16)
        start(gu_outs(n))
        wait(gu_state(n))
        gu.new[...] = adam(w_ref[...], m_ref[...], v_ref[...], g)
        gu.gather1(n, rows)

    def dn_new(n, size):
        g = dn.event3(n, size).T
        half, height = LANES // 2, size // lane_blocks
        if size == small:
            g = jnp.concatenate([g[:half], g[half:]], 1)
        if size == full:
            pl.when((n > 0) & (lax.rem(n, pairs + 1) > 0))(lambda: wait(dn_outs(n - 1, full)))
            pl.when((n > 0) & (lax.rem(n, pairs + 1) == 0))(lambda: wait(dn_outs(n - 1, small)))
        else:
            wait(dn_outs(n - 1, full))
        for b in range(lane_blocks):
            dn.sum[pl.ds(b * height, height), :] = g[:, b * LANES : (b + 1) * LANES].astype(BF16)
        start(dn_outs(n, size))
        wait(dn_state(n, size))
        upper = n < (layers - 1) * (pairs + 1)
        pl.when(n > (layers - 1) * (pairs + 1))(lambda: wait(own_outs(n - 1, full)))
        for b in range(lane_blocks):
            here = pl.ds(b * height, height)
            dn.new[here, :] = adam(w_ref[here, :], m_ref[here, :], v_ref[here, :], g[:, b * LANES : (b + 1) * LANES])
        pl.when(upper)(lambda: dn.gather1(n, size))
        pl.when(~upper)(lambda: start(own_outs(n, size)))

    def turn(buf, slot, into, part):
        for b in range(lane_blocks):
            into[pl.ds(b * LANES, LANES), part] = buf[slot, :, b * LANES : (b + 1) * LANES].T

    start_tile(0, 0)
    start(weight_copies(0))
    barrier = pltpu.get_barrier_semaphore()
    peers = (gu.partner(), gu.device(1), gu.device(-1))
    for peer in peers:
        pl.semaphore_signal(barrier, inc=1, device_id=peer, device_id_type=MESH)
    pl.semaphore_wait(barrier, len(peers))

    def compute_tile(j, t):
        slot, here = lax.rem(j, 2), lax.rem(t, 2)
        part = strip(t * tile, tile)
        wait_tile(t)
        pl.when(t + 1 < tiles)(lambda: start_tile(j, t + 1))
        a, dy = a_tile[here], dy_tile[here]
        gate = dot(a, wg_ref[slot])
        up = dot(a, wu_ref[slot])
        dz = dot(dy, wd_ref[slot], NT).astype(BF16).astype(F32)
        s = jax.nn.sigmoid(gate)
        act = s * gate
        z_ref[part, :] = (act * up).astype(BF16)
        dgu_ref[1, part, :] = (dz * act).astype(BF16)
        dgu_ref[0, part, :] = (dz * up * (s + act * (1 - s))).astype(BF16)

        @pl.when(j == 0)
        def _():
            turn(a_tile, here, at_ref, part)
            turn(dy_tile, here, dyt_ref, part)
            da_ref[part, :] = jnp.zeros((tile, d), F32)

    def compute_gate_up(j, s):
        slot, u, h = lax.rem(j, gu.slots), s // (chips // 2), lax.rem(s, chips // 2)
        g = dot(at_ref[...], dgu_ref[u, :, strip(h * 2 * LANES, 2 * LANES)]).astype(BF16)
        for c in range(2):
            at = strip((u * chips + 2 * h + c) * rows, rows)
            for owner in range(CORES * chips):
                gu.mine[slot, owner % CORES, owner // CORES, at, :] = g[owner * rows : (owner + 1) * rows, c * LANES : (c + 1) * LANES]

    def compute_down(j, h):
        slot = lax.rem(down_of(j), dn.slots)
        owner = lax.rem(lax.rem(j, blocks), 2)

        @pl.when(~is_last(j))
        def _():
            g = dot(dyt_ref[...], z_ref[:, strip(h * 2 * LANES, 2 * LANES)]).astype(BF16)
            for c in range(2):
                dn.mine[slot, owner, 2 * h + c, :, :] = g[:, c * LANES : (c + 1) * LANES]

        @pl.when(is_last(j))
        def _():
            g = dot(dyt_ref[...], z_ref[:, strip(h * 2 * LANES, 2 * LANES)])
            low = lax.broadcasted_iota(jnp.int32, (small, LANES), 1) < LANES // 2
            for c in range(2):
                top, bottom = g[:small, c * LANES : (c + 1) * LANES], g[small:, c * LANES : (c + 1) * LANES]
                dn.mine[slot, 0, 2 * h + c, pl.ds(0, small), :] = jnp.where(low, top, pltpu.roll(bottom, LANES // 2, 1)).astype(BF16)
                dn.mine[slot, 1, 2 * h + c, pl.ds(0, small), :] = jnp.where(low, pltpu.roll(top, LANES // 2, 1), bottom).astype(BF16)

    def compute_da(j, t):
        slot = lax.rem(j, 2)
        part = strip(t * tile, tile)
        da_ref[part, :] += dot(dgu_ref[0, part, :], wg_ref[slot], NT) + dot(dgu_ref[1, part, :], wu_ref[slot], NT)

    def change_layer():
        size = tile // 4

        def keep(t):
            return pltpu.make_async_copy(dy_tile.at[lax.rem(t, 2)], dy0_hbm.at[strip(t * tile, tile), :], tile_sem.at[lax.rem(t, 2), 2])

        def begin(t):
            load(h_hbm, a_tile, t, 0).start()
            load(dy_hbm, dy_tile, t, 1).start()

        begin(0)

        def one(t, _):
            slot = lax.rem(t, 2)
            wait_tile(t)
            pl.when(t > 0)(lambda: keep(t - 1).wait())
            pl.when(t + 1 < tiles)(lambda: begin(t + 1))

            def piece(i, _):
                here, there = strip(i * size, size), strip(t * tile + i * size, size)
                wide = a_tile[slot, here, :].astype(F32)
                da = da_ref[there, :].astype(BF16).astype(F32)
                scale = lax.rsqrt(jnp.mean(wide * wide, -1, keepdims=True) + 1e-6)
                along = jnp.mean(da * wide, -1, keepdims=True)
                back = (da * scale - wide * (along * scale * scale * scale)).astype(BF16)
                dy_tile[slot, here, :] = dy_tile[slot, here, :] + back
                return 0

            lax.fori_loop(0, tile // size, piece, 0)
            keep(t).start()
            turn(dy_tile, slot, dyt_ref, strip(t * tile, tile))
            return 0

        lax.fori_loop(0, tiles, one, 0)
        keep(tiles - 1).wait()

    def on(j, act):
        pl.when((j >= 0) & (j < steps))(lambda: act(j, full))

    def upper_down(j, act):
        pl.when(j < (layers - 1) * blocks)(lambda: for_down(j, act))

    events = {
        "tile": {
            0: [(on, gu.gather4, 4), (upper_down, dn.gather2, 3)],
            1: [(on, gu.event2, 1)],
            2: [(for_down, dn.event1, 1)],
        },
        "gate_up": {
            0: [(on, gu.gather2, 2)],
            2: [(for_down, dn_new, 2)],
            3: [(on, gu.event0, 0), (on, lambda n, _: start(gu_state(n)), 1)],
        },
        "down": {1: [(for_down, dn.event0, 0), (upper_down, dn.gather3, 3), (on, gu.event1, 0)]},
        "da": {
            0: [(on, gu.gather3, 3), (on, gu_new, 1)],
            1: [(upper_down, dn.gather4, 3), (for_down, lambda n, size: start(dn_state(n, size)), 1)],
            2: [(for_down, dn.event2, 1)],
        },
    }
    longest = max(ago for part in events.values() for these in part.values() for _, _, ago in these)

    def step(j, _):
        busy = j < steps
        lower = layer_of(j) > 0
        changes = is_last(j) & lower & busy

        @pl.when(busy)
        def _():
            wait(weight_copies(j))
            pl.when(j + 1 < steps)(lambda: start(weight_copies(j + 1)))

        def parts(name, number, active, compute):
            def one(t, _):
                pl.when(active)(lambda: compute(j, t))
                for at, these in events[name].items():

                    @pl.when(t == at)
                    def _():
                        for stream, act, ago in these:
                            stream(j - ago, act)

                return 0

            lax.fori_loop(0, number, one, 0)

        def da_tile(j, t):
            @pl.when(changes)
            def _():
                pl.when(t == 0)(lambda: load(a_hbm.at[0], a_tile, 0, 0).start())
                load(a_hbm.at[0], a_tile, t, 0).wait()
                pl.when(t + 1 < tiles)(lambda: load(a_hbm.at[0], a_tile, t + 1, 0).start())

            compute_da(j, t)
            pl.when(changes)(lambda: turn(a_tile, lax.rem(t, 2), at_ref, strip(t * tile, tile)))

        parts("tile", tiles, busy, compute_tile)
        pl.when(busy & (j + 1 < steps) & ~changes)(lambda: start_tile(j + 1, 0))
        parts("gate_up", chips, busy, compute_gate_up)
        parts("down", chips // 2, busy, compute_down)
        parts("da", tiles, busy & lower, da_tile)

        @pl.when(changes)
        def _():
            change_layer()
            start_tile(j + 1, 0)

        return 0

    lax.fori_loop(0, steps + longest, step, 0)
    wait(gu_outs(steps - 1))
    wait(dn_outs(dn.number - 1, small))
    wait(own_outs(dn.number - 1, small))


def backward(mesh, a, dy, h, weights, m, v, tile=512):
    tokens, d = dy.shape
    layers, _, ff = weights[0].shape
    chips = mesh.shape["dp"] // CORES
    width = chips * LANES
    blocks = ff // width
    pairs = blocks // 2
    rows = d // (CORES * chips)
    assert layers == 2 and chips == 4 and blocks % 2 == 1 and blocks * width == ff and d % LANES == 0
    shape = lambda *s: jax.ShapeDtypeStruct(s, BF16)
    devices = CORES * chips
    outs = [
        shape(layers, rows, ff),
        shape(layers, rows, ff),
        shape(layers, ff // devices, d),
        shape(layers * blocks, devices, d, LANES),
        shape((layers - 1) * (pairs + 1), devices, d, LANES),
        shape(ff // devices, d),
        shape(tokens, d),
    ]

    def pool(lanes, outputs):
        return [
            pltpu.VMEM((2, CORES, chips, d, LANES), BF16),
            pltpu.VMEM((2, chips, d, LANES), BF16),
            pltpu.VMEM((lanes, 2, d // 2, LANES), BF16),
            pltpu.VMEM((lanes, 2, d, LANES), BF16),
            pltpu.VMEM((lanes, 2, d // 2, LANES), BF16),
            pltpu.VMEM((lanes, 2, d, LANES), BF16),
            pltpu.VMEM((d, LANES), BF16),
            pltpu.VMEM((d, LANES), BF16),
            pltpu.SemaphoreType.DMA((2, 5, 2)),
            pltpu.SemaphoreType.REGULAR((5,)),
            pltpu.SemaphoreType.DMA((outputs,)),
            pltpu.SemaphoreType.DMA((4, 8, 2)),
            pltpu.SemaphoreType.DMA,
        ]

    return pl.pallas_call(
        functools.partial(backward_kernel, chips, tile),
        out_shape=outs,
        in_specs=[ANY] * 12,
        out_specs=[ANY] * len(outs),
        scratch_shapes=[
            pltpu.VMEM((2, tile, d), BF16),
            pltpu.VMEM((2, tile, d), BF16),
            pltpu.VMEM((d, tokens), BF16),
            pltpu.VMEM((d, tokens), BF16),
            pltpu.VMEM((tokens, d), F32),
            pltpu.VMEM((2, d, width), BF16),
            pltpu.VMEM((2, d, width), BF16),
            pltpu.VMEM((2, width, d), BF16),
            pltpu.VMEM((tokens, width), BF16),
            pltpu.VMEM((2, tokens, width), BF16),
            pltpu.VMEM((d, LANES), F32),
            pltpu.VMEM((d, LANES), F32),
            pltpu.VMEM((d, LANES), BF16),
            pltpu.SemaphoreType.DMA((2, 3)),
            pltpu.SemaphoreType.DMA((2, 3 * chips)),
            pltpu.SemaphoreType.DMA((max(6 * chips, 3 * (d // LANES)),)),
            pltpu.SemaphoreType.DMA((d // LANES,)),
            *pool(1, 2 * chips),
            *pool(2, d // LANES),
        ],
        compiler_params=pltpu.CompilerParams(collective_id=1, has_side_effects=True, vmem_limit_bytes=VMEM_MOST),
        cost_estimate=pl.CostEstimate(flops=28 * tokens * d * ff, bytes_accessed=24 * d * ff, transcendentals=2 * tokens * ff),
        name="backward",
    )(a, dy, h, *weights, *m, *v)


class Ring:
    def __init__(self, units, slots, loads, stores, work):
        self.units, self.slots, self.loads, self.stores, self.work = units, slots, loads, stores, work

    def begin(self):
        for unit in range(self.slots):
            for copy in self.loads(unit, unit):
                copy.start()

    def run(self):
        def one(unit, _):
            slot = lax.rem(unit, self.slots)
            for copy in self.loads(unit, slot):
                copy.wait()

            @pl.when(unit >= self.slots)
            def _():
                for copy in self.stores(unit - self.slots, slot):
                    copy.wait()

            self.work(unit, slot)
            for copy in self.stores(unit, slot):
                copy.start()

            @pl.when(unit + self.slots < self.units)
            def _():
                for copy in self.loads(unit + self.slots, slot):
                    copy.start()

            return 0

        lax.fori_loop(0, self.units, one, 0)

    def end(self):
        for unit in range(self.units - self.slots, self.units):
            for copy in self.stores(unit, unit % self.slots):
                copy.wait()


def place_columns_kernel(layers, slots, x_hbm, gate_hbm, up_hbm, c_in, c_out, sem):
    _, blocks, devices, _, chips, rows, _ = x_hbm.shape
    wide, some = blocks * LANES, c_in.shape[2]
    turns = devices // some

    def place(unit):
        return unit // (chips * turns), lax.rem(unit, chips * turns) // turns, lax.rem(unit, turns) * some

    def loads(unit, slot):
        layer, chip, owners = place(unit)
        return [pltpu.make_async_copy(x_hbm.at[layers - 1 - layer, :, pl.ds(owners, some), :, chip], c_in.at[slot], sem.at[slot, 0])]

    def stores(unit, slot):
        layer, chip, owners = place(unit)
        at = layer, strip(owners * rows, some * rows), strip(chip * wide, wide)
        return [pltpu.make_async_copy(c_out.at[slot, u], out.at[at], sem.at[slot, 1 + u]) for u, out in enumerate((gate_hbm, up_hbm))]

    def work(unit, slot):
        for j in range(blocks):
            at = pl.ds((j // 2 + (blocks // 2 + 1) * (j % 2)) * LANES, LANES)
            for owner in range(some):
                for u in range(2):
                    c_out[slot, u, pl.ds(owner * rows, rows), at] = c_in[slot, j, owner, u]

    ring = Ring(layers * chips * turns, slots, loads, stores, work)
    ring.begin()
    ring.run()
    ring.end()


def place_columns(chunks, layers, d, ff, slots=4, some=2):
    devices = chunks.shape[1]
    chips, rows = devices // CORES, d // devices
    x = chunks.reshape(layers, -1, devices, 2, chips, rows, LANES)
    return pl.pallas_call(
        functools.partial(place_columns_kernel, layers, slots),
        in_specs=[ANY],
        out_specs=[ANY] * 2,
        out_shape=[jax.ShapeDtypeStruct((layers, d, ff), BF16)] * 2,
        scratch_shapes=[
            pltpu.VMEM((slots, x.shape[1], some, 2, rows, LANES), BF16),
            pltpu.VMEM((slots, 2, some * rows, ff // chips), BF16),
            pltpu.SemaphoreType.DMA((slots, 3)),
        ],
        compiler_params=pltpu.CompilerParams(vmem_limit_bytes=VMEM_BYTES),
        cost_estimate=pl.CostEstimate(flops=COPY_FLOPS * 8 * layers * d * ff, bytes_accessed=8 * layers * d * ff, transcendentals=0),
        name="place_columns",
    )(x)


def moments_kernel(layers, parts, slots, *refs):
    states, news, s_in, g_in, s_out, sem = refs[:9], refs[9:15], refs[15:18], refs[18:21], refs[21:24], refs[24]

    def at(i, unit):
        layer, part = unit // parts, lax.rem(unit, parts)
        _, r, c = states[i].shape
        return (layer, strip(part * (r // parts), r // parts), slice(None)) if i == 2 else (layer, slice(None), strip(part * (c // parts), c // parts))

    def loads(unit, slot):
        copies = []
        for i in range(3):
            for k in range(2):
                copies.append(pltpu.make_async_copy(states[3 * k + i].at[at(i, unit)], s_in[i].at[slot, k], sem.at[slot, 5 * i + k]))
            copies.append(pltpu.make_async_copy(states[6 + i].at[at(i, unit)], g_in[i].at[slot], sem.at[slot, 5 * i + 2]))
        return copies

    def stores(unit, slot):
        return [
            pltpu.make_async_copy(s_out[i].at[slot, k], news[3 * k + i].at[at(i, unit)], sem.at[slot, 5 * i + 3 + k]) for i in range(3) for k in range(2)
        ]

    def work(unit, slot):
        for i in range(3):
            g = g_in[i][slot].astype(F32)
            s_out[i][slot, 0] = 0.9 * s_in[i][slot, 0] + 0.1 * g
            s_out[i][slot, 1] = 0.95 * s_in[i][slot, 1] + 0.05 * g * g

    ring = Ring(layers * parts, slots, loads, stores, work)
    ring.begin()
    ring.run()
    ring.end()


def moments(m, v, g, parts=9, slots=4):
    layers = m[0].shape[0]
    shapes = [(one.shape[1], one.shape[2] // parts) for one in m[:2]] + [(m[2].shape[1] // parts, m[2].shape[2])]
    size = sum(one.size for one in m)
    return pl.pallas_call(
        functools.partial(moments_kernel, layers, parts, slots),
        in_specs=[ANY] * 9,
        out_specs=[ANY] * 6,
        out_shape=[jax.ShapeDtypeStruct(one.shape, F32) for one in m] * 2,
        scratch_shapes=[
            *(pltpu.VMEM((slots, 2, *shape), F32) for shape in shapes),
            *(pltpu.VMEM((slots, *shape), BF16) for shape in shapes),
            *(pltpu.VMEM((slots, 2, *shape), F32) for shape in shapes),
            pltpu.SemaphoreType.DMA((slots, 15)),
        ],
        compiler_params=pltpu.CompilerParams(vmem_limit_bytes=VMEM_BYTES),
        cost_estimate=pl.CostEstimate(flops=COPY_FLOPS * 18 * size, bytes_accessed=18 * size, transcendentals=0),
        name="moments",
    )(*m, *v, *g)


def place_rows_kernel(layers, slots, me_ref, x_hbm, *refs):
    pieces, down_hbm, (r_in, r_out, held, sem, held_sem) = refs[:-6], refs[-6], refs[-5:]
    devices = x_hbm.shape[2]
    pairs = x_hbm.shape[1] - 1
    height, d = r_out.shape[1:]
    chips = devices // CORES
    half = LANES // 2
    chip, core = me_ref[0] // CORES, lax.rem(me_ref[0], CORES)

    def owner(hops, flip):
        return lax.rem(chip + hops + chips, chips) * CORES + (1 - core if flip else core)

    starts = [owner(hops, flip) * height for flip in (0, 1) for hops in (0, -1, 1)] + [owner(2, 0) * height + part * (height // 2) for part in (0, 1)]
    fetch, put = [], []
    for i, (piece, start) in enumerate(zip(pieces, starts)):
        size = piece.shape[0]
        fetch.append(pltpu.make_async_copy(piece, held.at[i, pl.ds(0, size)], held_sem.at[i, 0]))
        put.append(pltpu.make_async_copy(held.at[i, pl.ds(0, size)], down_hbm.at[0, pl.ds(pl.multiple_of(start, 32), size), :], held_sem.at[i, 1]))

    def loads(unit, slot):
        layer, device = layers - 2 - unit // devices, lax.rem(unit, devices)
        return [
            pltpu.make_async_copy(x_hbm.at[layer, pl.ds(0, pairs), device], r_in.at[slot, pl.ds(0, pairs)], sem.at[slot, 0]),
            pltpu.make_async_copy(x_hbm.at[layer, pairs, device, pl.ds(0, d // 2)], r_in.at[slot, pairs, pl.ds(0, d // 2)], sem.at[slot, 1]),
        ]

    def stores(unit, slot):
        layer, device = unit // devices + 1, lax.rem(unit, devices)
        return [pltpu.make_async_copy(r_out.at[slot], down_hbm.at[layer, strip(device * height, height), :], sem.at[slot, 2])]

    def work(unit, slot):
        low = lax.rem(unit, CORES)
        for b in range(d // LANES):
            there = pl.ds(b * LANES, LANES)
            for n in range(pairs):
                r_out[slot, pl.ds(pl.multiple_of(n * LANES + low * half, half), LANES), there] = r_in[slot, n, pl.ds(b * LANES, LANES), :]
            r_out[slot, pl.ds(pl.multiple_of(pairs * LANES * (1 - low), half), half), there] = r_in[slot, pairs, pl.ds(b * half, half), :]

    for copy in fetch:
        copy.start()
    ring = Ring((layers - 1) * devices, slots, loads, stores, work)
    ring.begin()
    for one, other in zip(fetch, put):
        one.wait()
        other.start()
    ring.run()
    ring.end()
    for copy in put:
        copy.wait()


def place_rows(me, chunks, pieces, layers, d, ff, slots=4):
    number, devices, _, _ = chunks.shape
    x = chunks.reshape(layers - 1, -1, devices, d, LANES)
    height = ff // devices
    return pl.pallas_call(
        functools.partial(place_rows_kernel, layers, slots),
        in_specs=[pl.BlockSpec(memory_space=pltpu.SMEM)] + [ANY] * (1 + len(pieces)),
        out_specs=ANY,
        out_shape=jax.ShapeDtypeStruct((layers, ff, d), BF16),
        scratch_shapes=[
            pltpu.VMEM((slots, x.shape[1], d, LANES), BF16),
            pltpu.VMEM((slots, height, d), BF16),
            pltpu.VMEM((len(pieces), height, d), BF16),
            pltpu.SemaphoreType.DMA((slots, 3)),
            pltpu.SemaphoreType.DMA((len(pieces), 2)),
        ],
        compiler_params=pltpu.CompilerParams(vmem_limit_bytes=VMEM_BYTES),
        cost_estimate=pl.CostEstimate(flops=COPY_FLOPS * 4 * layers * d * ff, bytes_accessed=4 * layers * d * ff, transcendentals=0),
        name="place_rows",
    )(me, x, *pieces)


def place_last_kernel(me_ref, top_hbm, bottom_hbm, _, down_hbm, held, sem):
    half = top_hbm.shape[0]
    chips = down_hbm.shape[1] // (2 * half * CORES)
    owner = lax.rem(me_ref[0] // CORES + 2, chips) * CORES + 1 - lax.rem(me_ref[0], CORES)
    fetch, put = [], []
    for i, piece in enumerate((top_hbm, bottom_hbm)):
        fetch.append(pltpu.make_async_copy(piece, held.at[i], sem.at[i, 0]))
        put.append(pltpu.make_async_copy(held.at[i], down_hbm.at[0, pl.ds(pl.multiple_of((2 * owner + i) * half, 32), half), :], sem.at[i, 1]))
    for copy in fetch:
        copy.start()
    for one, other in zip(fetch, put):
        one.wait()
        other.start()
    for copy in put:
        copy.wait()


def place_last(me, top, bottom, down):
    return pl.pallas_call(
        place_last_kernel,
        in_specs=[pl.BlockSpec(memory_space=pltpu.SMEM)] + [ANY] * 3,
        out_specs=ANY,
        out_shape=jax.ShapeDtypeStruct(down.shape, BF16),
        input_output_aliases={3: 0},
        scratch_shapes=[pltpu.VMEM((2, *top.shape), BF16), pltpu.SemaphoreType.DMA((2, 2))],
        cost_estimate=pl.CostEstimate(flops=COPY_FLOPS * 4 * top.size, bytes_accessed=8 * top.size, transcendentals=0),
        name="place_last",
    )(me, top, bottom, down)


def solution(mesh):
    group = mesh.shape["dp"]
    swap = [(i, i ^ 1) for i in range(group)]
    right = [(i, (i + CORES) % group) for i in range(group)]
    left = [(i, (i - CORES) % group) for i in range(group)]

    def step(x, dy, *arrays):
        weights, m, v = (arrays[i : i + 3] for i in (0, 3, 6))
        layers, d, ff = weights[0].shape
        x, dy = x[0], dy[0]
        me = lax.axis_index("dp").reshape(1)
        a, h = forward(x, *weights, 0)
        *sums, columns, rows, own, _ = backward(mesh, a, dy, h, weights, m, v)

        def send(block, to):
            return lax.ppermute(block, "dp", to)

        near = [own, send(own, right), send(own, left)]
        gate, up = place_columns(columns, layers, d, ff)
        gate, *near[1:] = lax.optimization_barrier((gate, *near[1:]))
        half = own.shape[0] // 2
        far = [send(near[1][:half], right), send(near[2][half:], left)]
        other = [send(block, swap) for block in near]
        first, *states = moments(m, v, sums)
        first, *far = lax.optimization_barrier((first, *far))
        last = [send(block, swap) for block in far]
        down = place_rows(me, rows, near + other + far, layers, d, ff)
        return (gate, up, place_last(me, *last, down), first, *states)

    seq, whole, rows = P(("rep", "dp"), None, None), P(None, None, None), P(None, "dp", None)
    return jax.shard_map(
        step,
        mesh=mesh,
        in_specs=(seq, seq, whole, whole, whole) + (rows,) * 6,
        out_specs=(P("rep", None, None),) * 3 + (P("rep", "dp", None),) * 6,
        check_vma=False,
    )
```

```python
import functools

import jax
import jax.numpy as jnp
from jax import lax
from jax.experimental import pallas as pl
from jax.experimental.pallas import tpu as pltpu
from jax.sharding import PartitionSpec as P

F32, BF16 = jnp.float32, jnp.bfloat16
NN, NT = (((1,), (0,)), ((), ())), (((1,), (1,)), ((), ()))
MESH = pl.DeviceIdType.MESH
ANY = pl.BlockSpec(memory_space=pl.ANY)
LANES = 128
CORES = 2
VMEM_BYTES = 67_043_328
COPY_FLOPS = 64
SIDES = (0, 1), (1, -1)


def dot(a, b, dims=NN):
    return lax.dot_general(a, b, dims, preferred_element_type=F32)


def norm(h):
    wide = h.astype(F32)
    return (wide * lax.rsqrt(jnp.mean(wide**2, -1, keepdims=True) + 1e-6)).astype(BF16)


def strip(start, size):
    return pl.ds(pl.multiple_of(start, size), size)


def head(size):
    return pl.ds(0, size)


def parity(n):
    return lax.rem(n, 2)


def lanes(n):
    return pl.ds(n * LANES, LANES)


def start(copies):
    for copy in copies:
        copy.start()


def wait(copies):
    for copy in copies:
        copy.wait()


def cost(flops, moved):
    return pl.CostEstimate(flops=flops, bytes_accessed=moved, transcendentals=moved)


def forward_kernel(tile, x_ref, wg_ref, wu_ref, wd_ref, a_hbm, h_hbm, a_ref, total, ends, a_sem, end_sem):
    block = pl.program_id(0)
    first, last = block == 0, block == pl.num_programs(0) - 1
    tiles = x_ref.shape[0] // tile

    def keep(t):
        rows = strip(t * tile, tile)
        return pltpu.make_async_copy(a_ref.at[rows], a_hbm.at[0, rows], a_sem.at[t])

    def finish(t):
        rows = strip(t * tile, tile)
        for i, out in enumerate((h_hbm, a_hbm.at[1])):
            yield pltpu.make_async_copy(ends.at[parity(t), i], out.at[rows], end_sem.at[parity(t), i])

    @pl.when(first)
    def _():
        def begin(t, _):
            rows = strip(t * tile, tile)
            a_ref[rows, :] = norm(x_ref[rows, :])
            total[rows, :] = jnp.zeros((tile, total.shape[1]), F32)
            keep(t).start()
            return t

        lax.fori_loop(0, tiles, begin, 0)

    def one(t, _):
        rows = strip(t * tile, tile)
        a = a_ref[rows, :]
        gate, up = dot(a, wg_ref[...]), dot(a, wu_ref[...])
        z = (jax.nn.sigmoid(gate) * gate * up).astype(BF16)
        total[rows, :] += dot(z, wd_ref[...])

        @pl.when(last)
        def _():
            keep(t).wait()
            pl.when(t >= 2)(lambda: wait(finish(t - 2)))
            h = x_ref[rows, :] + total[rows, :].astype(BF16)
            for i, end in enumerate((h, norm(h))):
                ends[parity(t), i] = end
            start(finish(t))

        return t

    lax.fori_loop(0, tiles, one, 0)

    @pl.when(last)
    def _():
        for t in range(tiles - 2, tiles):
            wait(finish(t))


def forward(x, wg, wu, wd, layer, width=768, tile=512):
    tokens, d = x.shape
    ff = wg.shape[2]
    state = jax.ShapeDtypeStruct((tokens, d), BF16)
    columns = pl.BlockSpec((None, d, width), lambda i: (layer, 0, i))
    return pl.pallas_call(
        functools.partial(forward_kernel, tile),
        grid=(ff // width,),
        out_shape=[jax.ShapeDtypeStruct((2, tokens, d), BF16), state],
        in_specs=[pl.BlockSpec(x.shape, lambda i: (0, 0)), columns, columns, pl.BlockSpec((None, width, d), lambda i: (layer, i, 0))],
        out_specs=[ANY] * 2,
        scratch_shapes=[
            pltpu.VMEM(x.shape, BF16),
            pltpu.VMEM(x.shape, F32),
            pltpu.VMEM((2, 2, tile, d), BF16),
            pltpu.SemaphoreType.DMA((tokens // tile,)),
            pltpu.SemaphoreType.DMA((2, 2)),
        ],
        compiler_params=pltpu.CompilerParams(vmem_limit_bytes=VMEM_BYTES),
        cost_estimate=cost(6 * tokens * d * ff, 6 * d * ff),
        name="forward",
    )(x, wg, wu, wd)


class Pool:
    def __init__(self, number, chips, core, chip, bufs, sems, gathered):
        self.number, self.chips, self.core, self.chip = number, chips, core, chip
        self.mine, self.other, self.cross, self.near, self.out1, self.out2, self.sum, self.new = bufs
        self.dma, self.credit, self.out_sem, self.ag_sem, self.own_sem = sems
        self.gathered = gathered
        self.slots, self.lanes, self.turns = self.mine.shape[0], self.cross.shape[0], self.ag_sem.shape[0]

    def index(self, chip, core):
        return lax.rem(chip + self.chips, self.chips) * CORES + core

    def device(self, hops, core=None):
        return {"dp": self.index(self.chip + hops, self.core if core is None else core)}

    def partner(self):
        return self.device(0, 1 - self.core)

    def hop(self, sems, src, dst, to):
        return pltpu.make_async_remote_copy(src_ref=src, dst_ref=dst, send_sem=sems.at[0], recv_sem=sems.at[1], device_id=to, device_id_type=MESH)

    def copies0(self, n, rows):
        slot = lax.rem(n, self.slots)
        src = self.mine.at[slot, 1 - self.core, :, head(rows), :]
        return [self.hop(self.dma.at[slot, 0], src, self.other.at[slot, :, head(rows), :], self.partner())]

    def copies1(self, n, rows):
        slot, sem, half = lax.rem(n, self.lanes), lax.rem(n, self.slots), head(rows // 2)
        return [self.hop(self.dma.at[sem, 1 + side], self.out1.at[slot, side, half], self.cross.at[slot, side, half], self.device(hop)) for side, hop in SIDES]

    def copies2(self, n, rows):
        slot, sem, full = lax.rem(n, self.lanes), lax.rem(n, self.slots), head(rows)
        return [self.hop(self.dma.at[sem, 3 + side], self.out2.at[slot, side, full], self.near.at[slot, side, full], self.device(hop)) for side, hop in SIDES]

    def both(self, n, hops, start, size):
        slot, chip = lax.rem(n, self.slots), lax.rem(self.chip + hops + self.chips, self.chips)
        rows = pl.ds(start, size)
        return self.mine[slot, self.core, chip, rows, :].astype(F32) + self.other[slot, chip, rows, :].astype(F32)

    def give(self, kind, to):
        pl.semaphore_signal(self.credit.at[kind], inc=1, device_id=to, device_id_type=MESH)

    def take(self, when, kinds):
        @pl.when(when)
        def _():
            for kind in kinds:
                pl.semaphore_wait(self.credit.at[kind], 1)

    def event0(self, n, rows):
        self.take(n >= self.slots, (0,))
        start(self.copies0(n, rows))

    def event1(self, n, rows):
        slot, half = lax.rem(n, self.lanes), rows // 2
        wait(self.copies0(n, rows))
        for side, _ in SIDES:
            self.out1[slot, side, head(half)] = self.both(n, 2, side * half, half).astype(BF16)
        self.take(n >= self.lanes, (1, 2))
        start(self.copies1(n, rows))

    def event2(self, n, rows):
        slot, half = lax.rem(n, self.lanes), rows // 2
        wait(self.copies1(n, rows))
        for side, hop in SIDES:
            passed = self.both(n, hop, side * half, half) + self.cross[slot, side, head(half)].astype(F32)
            self.out2[slot, side, pl.ds(side * half, half), :] = passed.astype(BF16)
            self.out2[slot, side, pl.ds(half - side * half, half), :] = self.both(n, hop, half - side * half, half).astype(BF16)

        @pl.when(n + self.lanes < self.number)
        def _():
            for side, hop in SIDES:
                self.give(1 + side, self.device(-hop))

        self.take(n >= self.lanes, (3, 4))
        start(self.copies2(n, rows))

    def event3(self, n, rows):
        slot = lax.rem(n, self.lanes)
        wait(self.copies2(n, rows))
        total = self.both(n, 0, 0, rows)
        for side, _ in SIDES:
            total += self.near[slot, side, head(rows)].astype(F32)
        pl.when(n + self.slots < self.number)(lambda: self.give(0, self.partner()))

        @pl.when(n + self.lanes < self.number)
        def _():
            for side, hop in SIDES:
                self.give(3 + side, self.device(-hop))

        return total.astype(BF16).astype(F32)

    def block(self, n, hops, core, start, size):
        return self.gathered.at[n, self.index(self.chip + hops, core), pl.ds(start, size), :]

    def sems(self, n, kind):
        return self.ag_sem.at[lax.rem(n, self.turns), kind]

    def gathers1(self, n, rows):
        new, own = self.new.at[head(rows)], self.block(n, 0, self.core, 0, rows)
        copies = [self.hop(self.sems(n, side), new, own, self.device(hop)) for side, hop in SIDES]
        return [*copies, self.hop(self.sems(n, 7), new, own, self.partner()), pltpu.make_async_copy(new, own, self.own_sem)]

    def gathers2(self, n, rows):
        copies, half = [], rows // 2
        for side, hop in SIDES:
            part, full = (self.block(n, -hop, self.core, *which) for which in ((side * half, half), (0, rows)))
            copies.append(self.hop(self.sems(n, 2 + side), part, part, self.device(hop)))
            copies.append(self.hop(self.sems(n, 4 + side), full, full, self.partner()))
        return copies

    def gathers3(self, n, rows):
        opposite = self.block(n, 2, self.core, 0, rows)
        return [self.hop(self.sems(n, 6), opposite, opposite, self.partner())]

    def gather1(self, n, rows):
        start(self.gathers1(n, rows))

    def gather2(self, n, rows):
        wait(self.gathers1(n, rows))
        start(self.gathers2(n, rows))

    def gather3(self, n, rows):
        wait(self.gathers2(n, rows))
        start(self.gathers3(n, rows))

    def gather4(self, n, rows):
        wait(self.gathers3(n, rows))


def moment(m, v, g):
    return 0.9 * m + 0.1 * g, 0.95 * v + 0.05 * g * g


def adam(w, m, v, g):
    m, v = moment(m, v, g)
    w = w.astype(F32)
    return (w - 0.02 * (m * lax.rsqrt(v + 1e-8) + 0.1 * w)).astype(BF16)


def backward_kernel(chips, tile, *refs):
    a_hbm, h_hbm, dy_hbm, wg_hbm, wu_hbm, wd_hbm, mg_hbm, mu_hbm, md_hbm, vg_hbm, vu_hbm, vd_hbm, *refs = refs
    gg_hbm, gu_hbm, gd_hbm, whole_gu, whole_dn, own_hbm, dy0_hbm, *refs = refs
    a_tile, dy_tile, at_ref, dyt_ref, da_ref, wg_ref, wu_ref, wd_ref, z_ref, dgu_ref, m_ref, v_ref, w_ref, *refs = refs
    tile_sem, w_sem, state_sem, rows_sem, *pools = refs
    tokens, d = dy_hbm.shape
    layers, _, ff = wg_hbm.shape
    width = chips * LANES
    blocks = ff // width
    pairs = blocks // 2
    rows = d // (CORES * chips)
    lane_blocks = d // LANES
    me = lax.axis_index("dp")
    chip, core = me // CORES, lax.rem(me, CORES)
    tiles = tokens // tile
    steps = layers * blocks
    full, small, small_tile = d, d // 2, tile // 4

    gu = Pool(steps, chips, core, chip, pools[0:8], pools[8:13], whole_gu)
    dn = Pool(layers * (pairs + 1), chips, core, chip, pools[13:21], pools[21:26], whole_dn)

    def layer_of(j):
        return layers - 1 - j // blocks

    def block_of(j):
        j = lax.rem(j, blocks)
        return j // 2 + (pairs + 1) * parity(j)

    def columns(c, j):
        return strip(c * blocks * LANES + block_of(j) * LANES, LANES)

    def is_last(j):
        return lax.rem(j, blocks) == blocks - 1

    def gives_down(j):
        return (j >= 0) & (j < steps) & ((parity(lax.rem(j, blocks)) == 1) | is_last(j))

    def down_of(j):
        return (j // blocks) * (pairs + 1) + lax.rem(j, blocks) // 2

    def for_down(j, act):
        @pl.when(gives_down(j) & ~is_last(j))
        def _():
            act(down_of(j), full)

        @pl.when(gives_down(j) & is_last(j))
        def _():
            act(down_of(j), small)

    def weight_copies(j):
        layer, slot = layer_of(j), parity(j)
        for c in range(chips):
            there, here = columns(c, j), lanes(c)
            yield pltpu.make_async_copy(wg_hbm.at[layer, :, there], wg_ref.at[slot, :, here], w_sem.at[slot, 3 * c])
            yield pltpu.make_async_copy(wu_hbm.at[layer, :, there], wu_ref.at[slot, :, here], w_sem.at[slot, 3 * c + 1])
            yield pltpu.make_async_copy(wd_hbm.at[layer, there, :], wd_ref.at[slot, here, :], w_sem.at[slot, 3 * c + 2])

    def load(src, buf, t, which):
        slot = parity(t)
        return pltpu.make_async_copy(src.at[strip(t * tile, tile), :], buf.at[slot], tile_sem.at[slot, which])

    def start_tile(j, t):
        load(a_hbm.at[layer_of(j)], a_tile, t, 0).start()

        @pl.when(layer_of(j) == layers - 1)
        def _():
            load(dy_hbm, dy_tile, t, 1).start()

        @pl.when(layer_of(j) < layers - 1)
        def _():
            load(dy0_hbm, dy_tile, t, 1).start()

    def wait_tile(t):
        load(dy_hbm, a_tile, t, 0).wait()
        load(dy_hbm, dy_tile, t, 1).wait()

    def gu_parts(n):
        for c in range(chips):
            for u in range(2):
                yield u * chips + c, u, pl.ds((u * chips + c) * rows, rows), columns(c, n)

    def gu_outs(n):
        for i, u, here, there in gu_parts(n):
            yield pltpu.make_async_copy(gu.sum.at[here, :], (gg_hbm, gu_hbm)[u].at[layer_of(n), :, there], gu.out_sem.at[i])

    def gu_state(n):
        layer = layer_of(n)
        for i, u, here, there in gu_parts(n):
            for k, (src, buf) in enumerate((((mg_hbm, mu_hbm)[u], m_ref), ((vg_hbm, vu_hbm)[u], v_ref))):
                yield pltpu.make_async_copy(src.at[layer, :, there], buf.at[here, :], state_sem.at[3 * i + k])
            src = (wg_hbm, wu_hbm)[u].at[layer, strip(me * rows, rows), there]
            yield pltpu.make_async_copy(src, w_ref.at[here, :], state_sem.at[3 * i + 2])

    def dn_parts(n, size):
        step = lax.rem(n, pairs + 1)
        start = step * LANES + core * (LANES // 2) if size == full else pairs * LANES * (1 - core)
        height = size // lane_blocks
        for b in range(lane_blocks):
            yield b, layers - 1 - n // (pairs + 1), start, height, pl.ds(b * height, height), lanes(b)

    def dn_outs(n, size):
        for b, layer, start, height, here, there in dn_parts(n, size):
            at = pl.ds(pl.multiple_of(start, LANES // 2), height)
            yield pltpu.make_async_copy(dn.sum.at[here, :], gd_hbm.at[layer, at, there], dn.out_sem.at[b])

    def own_outs(n, size):
        for b, _, start, height, here, there in dn_parts(n, size):
            at = pl.ds(pl.multiple_of(start, LANES // 2), height)
            yield pltpu.make_async_copy(dn.new.at[here, :], own_hbm.at[at, there], rows_sem.at[b])

    def dn_state(n, size):
        for b, layer, start, height, here, there in dn_parts(n, size):
            at = pl.ds(pl.multiple_of(start, LANES // 2), height)
            for k, (src, buf) in enumerate(((md_hbm, m_ref), (vd_hbm, v_ref))):
                yield pltpu.make_async_copy(src.at[layer, at, there], buf.at[here, :], state_sem.at[3 * b + k])
            at = pl.ds(pl.multiple_of(me * (d // 2) + start, LANES // 2), height)
            yield pltpu.make_async_copy(wd_hbm.at[layer, at, there], w_ref.at[here, :], state_sem.at[3 * b + 2])

    def gu_new(n, rows):
        g = gu.event3(n, rows)
        pl.when(n > 0)(lambda: wait(gu_outs(n - 1)))
        gu.sum[...] = g.astype(BF16)
        start(gu_outs(n))
        wait(gu_state(n))
        gu.new[...] = adam(w_ref[...], m_ref[...], v_ref[...], g)
        gu.gather1(n, rows)

    def dn_new(n, size):
        g = dn.event3(n, size).T
        half, height = LANES // 2, size // lane_blocks
        if size == small:
            g = jnp.concatenate([g[:half], g[half:]], 1)
        if size == full:
            pl.when((n > 0) & (lax.rem(n, pairs + 1) > 0))(lambda: wait(dn_outs(n - 1, full)))
            pl.when((n > 0) & (lax.rem(n, pairs + 1) == 0))(lambda: wait(dn_outs(n - 1, small)))
        else:
            wait(dn_outs(n - 1, full))
        for b in range(lane_blocks):
            dn.sum[pl.ds(b * height, height), :] = g[:, b * LANES : (b + 1) * LANES].astype(BF16)
        start(dn_outs(n, size))
        wait(dn_state(n, size))
        upper = n < (layers - 1) * (pairs + 1)
        pl.when(n > (layers - 1) * (pairs + 1))(lambda: wait(own_outs(n - 1, full)))
        for b in range(lane_blocks):
            here = pl.ds(b * height, height)
            dn.new[here, :] = adam(w_ref[here, :], m_ref[here, :], v_ref[here, :], g[:, b * LANES : (b + 1) * LANES])
        pl.when(upper)(lambda: dn.gather1(n, size))
        pl.when(~upper)(lambda: start(own_outs(n, size)))

    def turn(buf, slot, into, part):
        for b in range(lane_blocks):
            into[lanes(b), part] = buf[slot, :, b * LANES : (b + 1) * LANES].T

    start_tile(0, 0)
    start(weight_copies(0))
    barrier = pltpu.get_barrier_semaphore()
    peers = (gu.partner(), gu.device(1), gu.device(-1))
    for peer in peers:
        pl.semaphore_signal(barrier, inc=1, device_id=peer, device_id_type=MESH)
    pl.semaphore_wait(barrier, len(peers))

    def keep(t):
        slot = parity(t)
        return pltpu.make_async_copy(dy_tile.at[slot], dy0_hbm.at[strip(t * tile, tile)], tile_sem.at[slot, 2])

    def compute_tile(j, t):
        slot, here = parity(j), parity(t)
        part = strip(t * tile, tile)
        wait_tile(t)
        pl.when(t + 1 < tiles)(lambda: start_tile(j, t + 1))
        a, dy = a_tile[here], dy_tile[here]
        gate = dot(a, wg_ref[slot])
        up = dot(a, wu_ref[slot])
        dz = dot(dy, wd_ref[slot], NT).astype(BF16).astype(F32)
        s = jax.nn.sigmoid(gate)
        act = s * gate
        z_ref[part, :] = (act * up).astype(BF16)
        dgu_ref[1, part, :] = (dz * act).astype(BF16)
        dgu_ref[0, part, :] = (dz * up * (s + act * (1 - s))).astype(BF16)

        @pl.when(j == 0)
        def _():
            turn(a_tile, here, at_ref, part)
            turn(dy_tile, here, dyt_ref, part)
            da_ref[part, :] = jnp.zeros((tile, d), F32)

    def compute_gate_up(j, u):
        slot = lax.rem(j, gu.slots)
        g = dot(at_ref[...], dgu_ref[u]).astype(BF16)
        for c in range(chips):
            at = strip((u * chips + c) * rows, rows)
            for owner in range(CORES * chips):
                gu.mine[slot, owner % CORES, owner // CORES, at, :] = g[owner * rows : (owner + 1) * rows, c * LANES : (c + 1) * LANES]

    def compute_down(j, h):
        slot = lax.rem(down_of(j), dn.slots)
        owner = parity(lax.rem(j, blocks))
        chips_here = [2 * h, 2 * h + 1]
        z = strip(chips_here[0] * LANES, 2 * LANES)

        @pl.when(~is_last(j))
        def _():
            g = dot(dyt_ref[...], z_ref[:, z]).astype(BF16)
            for c, at in enumerate(chips_here):
                dn.mine[slot, owner, at, :, :] = g[:, c * LANES : (c + 1) * LANES]

        @pl.when(is_last(j))
        def _():
            g = dot(dyt_ref[...], z_ref[:, z])
            half = LANES // 2
            low = lax.broadcasted_iota(jnp.int32, (small, LANES), 1) < half
            for c, at in enumerate(chips_here):
                both = g[:, c * LANES : (c + 1) * LANES]
                turned = pltpu.roll(both, half, 1)
                dn.mine[slot, 0, at, head(small), :] = jnp.where(low, both[:small], turned[small:]).astype(BF16)
                dn.mine[slot, 1, at, head(small), :] = jnp.where(low, turned[:small], both[small:]).astype(BF16)

    def compute_da(j, t):
        slot, part = parity(j), strip(t * tile, tile)
        da_ref[part, :] += dot(dgu_ref[0, part, :], wg_ref[slot], NT) + dot(dgu_ref[1, part, :], wu_ref[slot], NT)

    def change_layer():
        def begin(t):
            load(h_hbm, a_tile, t, 0).start()
            load(dy_hbm, dy_tile, t, 1).start()

        begin(0)

        def one(t, _):
            slot = parity(t)
            wait_tile(t)
            pl.when(t > 0)(lambda: keep(t - 1).wait())
            pl.when(t + 1 < tiles)(lambda: begin(t + 1))

            def piece(i, _):
                here, there = strip(i * small_tile, small_tile), strip(t * tile + i * small_tile, small_tile)
                wide = a_tile[slot, here, :].astype(F32)
                da = da_ref[there, :].astype(BF16).astype(F32)
                scale = lax.rsqrt(jnp.mean(wide * wide, -1, keepdims=True) + 1e-6)
                along = jnp.mean(da * wide, -1, keepdims=True)
                back = (da * scale - wide * (along * scale * scale * scale)).astype(BF16)
                dy_tile[slot, here, :] = dy_tile[slot, here, :] + back
                return 0

            lax.fori_loop(0, tile // small_tile, piece, 0)
            keep(t).start()
            turn(dy_tile, slot, dyt_ref, strip(t * tile, tile))
            return 0

        lax.fori_loop(0, tiles, one, 0)
        keep(tiles - 1).wait()

    def on(j, act):
        pl.when((j >= 0) & (j < steps))(lambda: act(j, full))

    def upper_down(j, act):
        pl.when(j < (layers - 1) * blocks)(lambda: for_down(j, act))

    def gu_load(n, rows):
        start(gu_state(n))

    def dn_load(n, rows):
        start(dn_state(n, rows))

    events = {
        "tile0": [(on, gu.gather4, 4)],
        "tile1": [(for_down, dn_new, 2)],
        "tile2": [(on, gu.event2, 1)],
        "gate0": [(for_down, dn.event2, 1), (on, gu_load, 1)],
        "gate1": [(on, gu.event0), (upper_down, dn.gather3, 3)],
        "down1": [(for_down, dn.event0), (upper_down, dn.gather2, 2)],
        "back0": [(on, gu.event1)],
        "back2": [(upper_down, dn.gather4, 3), (on, gu.gather3, 3), (on, gu.gather2, 2), (for_down, dn.event1)],
        "back3": [(on, gu_new, 1), (for_down, dn_load, 1)],
    }
    longest = max(sum(ago) for these in events.values() for _, _, *ago in these)

    def step(j, _):
        busy = j < steps
        lower = layer_of(j) > 0
        changes = is_last(j) & lower & busy

        @pl.when(busy)
        def _():
            wait(weight_copies(j))
            pl.when(j + 1 < steps)(lambda: start(weight_copies(j + 1)))

        def parts(name, number, active, compute):
            def one(t, _):
                pl.when(active)(lambda: compute(j, t))
                for at in range(number):

                    @pl.when(t == at)
                    def _():
                        for stream, act, *ago in events.get(f"{name}{at}", ()):
                            stream(j - sum(ago), act)

                return 0

            lax.fori_loop(0, number, one, 0)

        def da_tile(j, t):
            fetch = load(a_hbm.at[0], a_tile, t, 0)
            pl.when(changes)(fetch.start)
            compute_da(j, t)

            @pl.when(changes)
            def _():
                fetch.wait()
                turn(a_tile, parity(t), at_ref, strip(t * tile, tile))

        parts("tile", tiles, busy, compute_tile)
        pl.when(busy & (j + 1 < steps) & ~changes)(lambda: start_tile(j + 1, 0))
        parts("gate", 2, busy, compute_gate_up)
        parts("down", chips // 2, busy, compute_down)
        parts("back", tiles, busy & lower, da_tile)

        @pl.when(changes)
        def _():
            change_layer()
            start_tile(j + 1, 0)

        return 0

    lax.fori_loop(0, steps + longest, step, 0)
    wait(gu_outs(steps - 1))
    wait(dn_outs(dn.number - 1, small))
    wait(own_outs(dn.number - 1, small))


def backward(mesh, a, h, dy, weights, m, v, tile=512):
    tokens, d = dy.shape
    layers, _, ff = weights[0].shape
    chips = mesh.shape["dp"] // CORES
    width = chips * LANES
    blocks = ff // width
    pairs = blocks // 2
    rows = d // (CORES * chips)
    assert layers == 2 and chips == 4 and blocks % 2 == 1 and blocks * width == ff and d % LANES == 0
    shape = lambda *s: jax.ShapeDtypeStruct(s, BF16)
    devices = CORES * chips
    outs = [
        shape(layers, rows, ff),
        shape(layers, rows, ff),
        shape(layers, ff // devices, d),
        shape(layers * blocks, devices, d, LANES),
        shape((layers - 1) * (pairs + 1), devices, d, LANES),
        shape(ff // devices, d),
        shape(tokens, d),
    ]

    def pool(lanes, outputs):
        return [
            pltpu.VMEM((2, CORES, chips, d, LANES), BF16),
            pltpu.VMEM((2, chips, d, LANES), BF16),
            pltpu.VMEM((lanes, 2, d // 2, LANES), BF16),
            pltpu.VMEM((lanes, 2, d, LANES), BF16),
            pltpu.VMEM((lanes, 2, d // 2, LANES), BF16),
            pltpu.VMEM((lanes, 2, d, LANES), BF16),
            pltpu.VMEM((d, LANES), BF16),
            pltpu.VMEM((d, LANES), BF16),
            pltpu.SemaphoreType.DMA((2, 5, 2)),
            pltpu.SemaphoreType.REGULAR((5,)),
            pltpu.SemaphoreType.DMA((outputs,)),
            pltpu.SemaphoreType.DMA((4, 8, 2)),
            pltpu.SemaphoreType.DMA,
        ]

    return pl.pallas_call(
        functools.partial(backward_kernel, chips, tile),
        out_shape=outs,
        in_specs=[ANY] * 12,
        out_specs=[ANY] * len(outs),
        scratch_shapes=[
            pltpu.VMEM((2, tile, d), BF16),
            pltpu.VMEM((2, tile, d), BF16),
            pltpu.VMEM((d, tokens), BF16),
            pltpu.VMEM((d, tokens), BF16),
            pltpu.VMEM((tokens, d), F32),
            pltpu.VMEM((2, d, width), BF16),
            pltpu.VMEM((2, d, width), BF16),
            pltpu.VMEM((2, width, d), BF16),
            pltpu.VMEM((tokens, width), BF16),
            pltpu.VMEM((2, tokens, width), BF16),
            pltpu.VMEM((d, LANES), F32),
            pltpu.VMEM((d, LANES), F32),
            pltpu.VMEM((d, LANES), BF16),
            pltpu.SemaphoreType.DMA((2, 3)),
            pltpu.SemaphoreType.DMA((2, 3 * chips)),
            pltpu.SemaphoreType.DMA((max(6 * chips, 3 * (d // LANES)),)),
            pltpu.SemaphoreType.DMA((d // LANES,)),
            *pool(1, 2 * chips),
            *pool(2, d // LANES),
        ],
        compiler_params=pltpu.CompilerParams(collective_id=1, has_side_effects=True, vmem_limit_bytes=VMEM_BYTES),
        cost_estimate=cost(28 * tokens * d * ff, 24 * d * ff),
        name="backward",
    )(a, h, dy, *weights, *m, *v)


class Ring:
    def __init__(self, units, slots, loads, stores, work):
        self.units, self.slots, self.loads, self.stores, self.work = units, slots, loads, stores, work

    def begin(self):
        for unit in range(self.slots):
            for copy in self.loads(unit, unit):
                copy.start()

    def run(self):
        def one(unit, _):
            slot = lax.rem(unit, self.slots)
            for copy in self.loads(unit, slot):
                copy.wait()

            @pl.when(unit >= self.slots)
            def _():
                for copy in self.stores(unit - self.slots, slot):
                    copy.wait()

            self.work(unit, slot)
            for copy in self.stores(unit, slot):
                copy.start()

            @pl.when(unit + self.slots < self.units)
            def _():
                for copy in self.loads(unit + self.slots, slot):
                    copy.start()

            return 0

        lax.fori_loop(0, self.units, one, 0)

    def end(self):
        for unit in range(self.units - self.slots, self.units):
            for copy in self.stores(unit, unit % self.slots):
                copy.wait()


def place_columns_kernel(layers, slots, x_hbm, gate_hbm, up_hbm, c_in, c_out, sem):
    _, blocks, devices, _, chips, rows, _ = x_hbm.shape
    wide, some = blocks * LANES, c_in.shape[2]
    turns = devices // some

    def place(unit):
        return unit // (chips * turns), lax.rem(unit, chips * turns) // turns, lax.rem(unit, turns) * some

    def loads(unit, slot):
        layer, chip, owners = place(unit)
        return [pltpu.make_async_copy(x_hbm.at[layers - 1 - layer, :, pl.ds(owners, some), :, chip], c_in.at[slot], sem.at[slot, 0])]

    def stores(unit, slot):
        layer, chip, owners = place(unit)
        at = layer, strip(owners * rows, some * rows), strip(chip * wide, wide)
        return [pltpu.make_async_copy(c_out.at[slot, u], out.at[at], sem.at[slot, 1 + u]) for u, out in enumerate((gate_hbm, up_hbm))]

    def work(unit, slot):
        for j in range(blocks):
            at = pl.ds((j // 2 + (blocks // 2 + 1) * (j % 2)) * LANES, LANES)
            for owner in range(some):
                for u in range(2):
                    c_out[slot, u, pl.ds(owner * rows, rows), at] = c_in[slot, j, owner, u]

    ring = Ring(layers * chips * turns, slots, loads, stores, work)
    ring.begin()
    ring.run()
    ring.end()


def place_columns(chunks, layers, d, ff, slots=4, some=2):
    devices = chunks.shape[1]
    chips, rows = devices // CORES, d // devices
    x = chunks.reshape(layers, -1, devices, 2, chips, rows, LANES)
    return pl.pallas_call(
        functools.partial(place_columns_kernel, layers, slots),
        in_specs=[ANY],
        out_specs=[ANY] * 2,
        out_shape=[jax.ShapeDtypeStruct((layers, d, ff), BF16)] * 2,
        scratch_shapes=[
            pltpu.VMEM((slots, x.shape[1], some, 2, rows, LANES), BF16),
            pltpu.VMEM((slots, 2, some * rows, ff // chips), BF16),
            pltpu.SemaphoreType.DMA((slots, 3)),
        ],
        compiler_params=pltpu.CompilerParams(vmem_limit_bytes=VMEM_BYTES),
        cost_estimate=cost(COPY_FLOPS * 8 * layers * d * ff, 8 * layers * d * ff),
        name="place_columns",
    )(x)


def moments_kernel(layers, parts, slots, *refs):
    states, news, s_in, g_in, s_out, sem = refs[:9], refs[9:15], refs[15:18], refs[18:21], refs[21:24], refs[24]

    def at(i, unit):
        layer, part = unit // parts, lax.rem(unit, parts)
        _, r, c = states[i].shape
        return (layer, strip(part * (r // parts), r // parts), slice(None)) if i == 2 else (layer, slice(None), strip(part * (c // parts), c // parts))

    def loads(unit, slot):
        copies = []
        for i in range(3):
            for k in range(2):
                copies.append(pltpu.make_async_copy(states[3 * k + i].at[at(i, unit)], s_in[i].at[slot, k], sem.at[slot, 5 * i + k]))
            copies.append(pltpu.make_async_copy(states[6 + i].at[at(i, unit)], g_in[i].at[slot], sem.at[slot, 5 * i + 2]))
        return copies

    def stores(unit, slot):
        return [
            pltpu.make_async_copy(s_out[i].at[slot, k], news[3 * k + i].at[at(i, unit)], sem.at[slot, 5 * i + 3 + k]) for i in range(3) for k in range(2)
        ]

    def work(unit, slot):
        for i in range(3):
            g = g_in[i][slot].astype(F32)
            s_out[i][slot, 0], s_out[i][slot, 1] = moment(s_in[i][slot, 0], s_in[i][slot, 1], g)

    ring = Ring(layers * parts, slots, loads, stores, work)
    ring.begin()
    ring.run()
    ring.end()


def moments(m, v, g, parts=9, slots=4):
    layers = m[0].shape[0]
    shapes = [(one.shape[1], one.shape[2] // parts) for one in m[:2]] + [(m[2].shape[1] // parts, m[2].shape[2])]
    size = sum(one.size for one in m)
    return pl.pallas_call(
        functools.partial(moments_kernel, layers, parts, slots),
        in_specs=[ANY] * 9,
        out_specs=[ANY] * 6,
        out_shape=[jax.ShapeDtypeStruct(one.shape, F32) for one in m] * 2,
        scratch_shapes=[
            *(pltpu.VMEM((slots, 2, *shape), F32) for shape in shapes),
            *(pltpu.VMEM((slots, *shape), BF16) for shape in shapes),
            *(pltpu.VMEM((slots, 2, *shape), F32) for shape in shapes),
            pltpu.SemaphoreType.DMA((slots, 15)),
        ],
        compiler_params=pltpu.CompilerParams(vmem_limit_bytes=VMEM_BYTES),
        cost_estimate=cost(COPY_FLOPS * 18 * size, 18 * size),
        name="moments",
    )(*m, *v, *g)


def place_rows_kernel(layers, slots, me_ref, x_hbm, *refs):
    pieces, down_hbm, (r_in, r_out, held, sem, held_sem) = refs[:-6], refs[-6], refs[-5:]
    devices = x_hbm.shape[2]
    pairs = x_hbm.shape[1] - 1
    height, d = r_out.shape[1:]
    chips = devices // CORES
    half = LANES // 2
    chip, core = me_ref[0] // CORES, lax.rem(me_ref[0], CORES)

    owners = [lax.rem(chip + hops + chips, chips) * CORES + (1 - core if flip else core) for flip in range(2) for hops in (0, -1, 1)]
    owners.append(lax.rem(chip + 2, chips) * CORES + core)
    fetch = [pltpu.make_async_copy(piece, held.at[i], held_sem.at[i, 0]) for i, piece in enumerate(pieces)]
    put = [pltpu.make_async_copy(held.at[i], down_hbm.at[0, strip(owner * height, height), :], held_sem.at[i, 1]) for i, owner in enumerate(owners)]

    def loads(unit, slot):
        layer, device = layers - 2 - unit // devices, lax.rem(unit, devices)
        return [
            pltpu.make_async_copy(x_hbm.at[layer, head(pairs), device], r_in.at[slot, head(pairs)], sem.at[slot, 0]),
            pltpu.make_async_copy(x_hbm.at[layer, pairs, device, head(d // 2)], r_in.at[slot, pairs, head(d // 2)], sem.at[slot, 1]),
        ]

    def stores(unit, slot):
        layer, device = unit // devices + 1, lax.rem(unit, devices)
        return [pltpu.make_async_copy(r_out.at[slot], down_hbm.at[layer, strip(device * height, height), :], sem.at[slot, 2])]

    def work(unit, slot):
        low = lax.rem(unit, CORES)
        for b in range(d // LANES):
            there = lanes(b)
            for n in range(pairs):
                r_out[slot, pl.ds(pl.multiple_of(n * LANES + low * half, half), LANES), there] = r_in[slot, n, lanes(b), :]
            r_out[slot, pl.ds(pl.multiple_of(pairs * LANES * (1 - low), half), half), there] = r_in[slot, pairs, pl.ds(b * half, half), :]

    both = fetch[len(owners) - 1 :]
    start(fetch[: len(owners) - 1])
    for k in range(CORES):
        pl.when(core == k)(both[k].start)
    ring = Ring((layers - 1) * devices, slots, loads, stores, work)
    ring.begin()
    for one, other in zip(fetch, put[:-1]):
        one.wait()
        other.start()
    for k in range(CORES):

        @pl.when(core == k)
        def _():
            both[k].wait()
            pltpu.make_async_copy(held.at[len(owners) - 1 + k], put[-1].dst_ref, held_sem.at[len(owners) - 1, 1]).start()

    ring.run()
    ring.end()
    wait(put)


def place_rows(me, chunks, pieces, layers, d, ff, slots=4):
    number, devices, _, _ = chunks.shape
    x = chunks.reshape(layers - 1, -1, devices, d, LANES)
    height = ff // devices
    return pl.pallas_call(
        functools.partial(place_rows_kernel, layers, slots),
        in_specs=[pl.BlockSpec(memory_space=pltpu.SMEM)] + [ANY] * (1 + len(pieces)),
        out_specs=ANY,
        out_shape=jax.ShapeDtypeStruct((layers, ff, d), BF16),
        scratch_shapes=[
            pltpu.VMEM((slots, x.shape[1], d, LANES), BF16),
            pltpu.VMEM((slots, height, d), BF16),
            pltpu.VMEM((len(pieces), height, d), BF16),
            pltpu.SemaphoreType.DMA((slots, 3)),
            pltpu.SemaphoreType.DMA((len(pieces), 2)),
        ],
        compiler_params=pltpu.CompilerParams(vmem_limit_bytes=VMEM_BYTES),
        cost_estimate=cost(COPY_FLOPS * 4 * layers * d * ff, 4 * layers * d * ff),
        name="place_rows",
    )(me, x, *pieces)


def place_last_kernel(me_ref, even_hbm, odd_hbm, _, down_hbm, held, sem):
    height = even_hbm.shape[0]
    chips = down_hbm.shape[1] // (height * CORES)
    core = lax.rem(me_ref[0], CORES)
    owner = lax.rem(me_ref[0] // CORES + 2, chips) * CORES + 1 - core
    for k, piece in enumerate((odd_hbm, even_hbm)):

        @pl.when(core == k)
        def _():
            fetch = pltpu.make_async_copy(piece, held, sem)
            fetch.start()
            fetch.wait()

    put = pltpu.make_async_copy(held, down_hbm.at[0, strip(owner * height, height), :], sem)
    put.start()
    put.wait()


def place_last(me, even, odd, down):
    return pl.pallas_call(
        place_last_kernel,
        in_specs=[pl.BlockSpec(memory_space=pltpu.SMEM)] + [ANY] * 3,
        out_specs=ANY,
        out_shape=jax.ShapeDtypeStruct(down.shape, BF16),
        input_output_aliases={3: 0},
        scratch_shapes=[pltpu.VMEM(even.shape, BF16), pltpu.SemaphoreType.DMA],
        cost_estimate=cost(COPY_FLOPS * 4 * even.size, 4 * even.size),
        name="place_last",
    )(me, even, odd, down)


def solution(mesh):
    group = mesh.shape["dp"]
    swap = [(i, i ^ 1) for i in range(group)]
    right = [(i, (i + CORES) % group) for i in range(group)]
    left = [(i, (i - CORES) % group) for i in range(group)]

    def step(x, dy, *arrays):
        weights, m, v = (arrays[i : i + 3] for i in (0, 3, 6))
        layers, d, ff = weights[0].shape
        me = lax.axis_index("dp").reshape(1)
        *sums, columns, rows, own, _ = backward(mesh, *forward(x[0], *weights, 0), dy[0], weights, m, v)

        def send(block, to):
            return lax.ppermute(block, "dp", to)

        near = [own, send(own, right), send(own, left)]
        gate, up = place_columns(columns, layers, d, ff)
        gate, *near[1:] = lax.optimization_barrier((gate, *near[1:]))
        far = [send(near[1], right[::CORES]), send(near[2], left[1::CORES])]
        other = [send(block, swap) for block in near]
        first, *states = moments(m, v, sums)
        first, *far = lax.optimization_barrier((first, *far))
        last = [send(block, swap[k::CORES]) for k, block in enumerate(far)]
        down = place_rows(me, rows, near + other + far, layers, d, ff)
        return (gate, up, place_last(me, *last, down), first, *states)

    seq, whole, rows = P(("rep", "dp"), None, None), P(None, None, None), P(None, "dp", None)
    return jax.shard_map(
        step,
        mesh=mesh,
        in_specs=(seq, seq, whole, whole, whole) + (rows,) * 6,
        out_specs=(P("rep", None, None),) * 3 + (P("rep", "dp", None),) * 6,
        check_vma=False,
    )
```

```python
import functools

import jax
import jax.numpy as jnp
from jax import lax
from jax.experimental import pallas as pl
from jax.experimental.pallas import tpu as pltpu
from jax.sharding import PartitionSpec as P

F32, BF16 = jnp.float32, jnp.bfloat16
NN, NT = (((1,), (0,)), ((), ())), (((1,), (1,)), ((), ()))
MESH = pl.DeviceIdType.MESH
ANY = pl.BlockSpec(memory_space=pl.ANY)
LANES = 128
CORES = 2
VMEM_BYTES = 67_043_328
COPY_FLOPS = 64
SIDES = (0, 1), (1, -1)


def dot(a, b, dims=NN):
    return lax.dot_general(a, b, dims, preferred_element_type=F32)


def norm(h):
    wide = h.astype(F32)
    return (wide * lax.rsqrt(jnp.mean(wide**2, -1, keepdims=True) + 1e-6)).astype(BF16)


def strip(start, size):
    return pl.ds(pl.multiple_of(start, size), size)


def head(size):
    return pl.ds(0, size)


def parity(n):
    return lax.rem(n, 2)


def lanes(n):
    return pl.ds(n * LANES, LANES)


def start(copies):
    for copy in copies:
        copy.start()


def wait(copies):
    for copy in copies:
        copy.wait()


def cost(flops, moved):
    return pl.CostEstimate(flops=flops, bytes_accessed=moved, transcendentals=moved)


def forward_kernel(tile, x_ref, wg_ref, wu_ref, wd_ref, a_hbm, h_hbm, a_ref, total, ends, a_sem, end_sem):
    block = pl.program_id(0)
    first, last = block == 0, block == pl.num_programs(0) - 1
    tiles = x_ref.shape[0] // tile

    def keep(t):
        rows = strip(t * tile, tile)
        return pltpu.make_async_copy(a_ref.at[rows], a_hbm.at[0, rows], a_sem.at[t])

    def finish(t):
        rows = strip(t * tile, tile)
        for i, out in enumerate((h_hbm, a_hbm.at[1])):
            yield pltpu.make_async_copy(ends.at[parity(t), i], out.at[rows], end_sem.at[parity(t), i])

    @pl.when(first)
    def _():
        def begin(t, _):
            rows = strip(t * tile, tile)
            a_ref[rows, :] = norm(x_ref[rows, :])
            total[rows, :] = jnp.zeros((tile, total.shape[1]), F32)
            keep(t).start()
            return t

        lax.fori_loop(0, tiles, begin, 0)

    def one(t, _):
        rows = strip(t * tile, tile)
        a = a_ref[rows, :]
        gate, up = dot(a, wg_ref[...]), dot(a, wu_ref[...])
        z = (jax.nn.sigmoid(gate) * gate * up).astype(BF16)
        total[rows, :] += dot(z, wd_ref[...])

        @pl.when(last)
        def _():
            keep(t).wait()
            pl.when(t >= 2)(lambda: wait(finish(t - 2)))
            h = x_ref[rows, :] + total[rows, :].astype(BF16)
            for i, end in enumerate((h, norm(h))):
                ends[parity(t), i] = end
            start(finish(t))

        return t

    lax.fori_loop(0, tiles, one, 0)

    @pl.when(last)
    def _():
        for t in range(tiles - 2, tiles):
            wait(finish(t))


def forward(x, wg, wu, wd, layer, width=768, tile=512):
    tokens, d = x.shape
    ff = wg.shape[2]
    state = jax.ShapeDtypeStruct((tokens, d), BF16)
    columns = pl.BlockSpec((None, d, width), lambda i: (layer, 0, i))
    return pl.pallas_call(
        functools.partial(forward_kernel, tile),
        grid=(ff // width,),
        out_shape=[jax.ShapeDtypeStruct((2, tokens, d), BF16), state],
        in_specs=[pl.BlockSpec(x.shape, lambda i: (0, 0)), columns, columns, pl.BlockSpec((None, width, d), lambda i: (layer, i, 0))],
        out_specs=[ANY] * 2,
        scratch_shapes=[
            pltpu.VMEM(x.shape, BF16),
            pltpu.VMEM(x.shape, F32),
            pltpu.VMEM((2, 2, tile, d), BF16),
            pltpu.SemaphoreType.DMA((tokens // tile,)),
            pltpu.SemaphoreType.DMA((2, 2)),
        ],
        compiler_params=pltpu.CompilerParams(vmem_limit_bytes=VMEM_BYTES),
        cost_estimate=cost(6 * tokens * d * ff, 6 * d * ff),
        name="forward",
    )(x, wg, wu, wd)


class Pool:
    def __init__(self, number, chips, core, chip, bufs, sems, gathered):
        self.number, self.chips, self.core, self.chip = number, chips, core, chip
        self.mine, self.other, self.cross, self.near, self.out1, self.out2, self.sum, self.new = bufs
        self.dma, self.credit, self.out_sem, self.ag_sem, self.own_sem = sems
        self.gathered = gathered
        self.slots, self.lanes, self.turns = self.mine.shape[0], self.cross.shape[0], self.ag_sem.shape[0]

    def index(self, chip, core):
        return lax.rem(chip + self.chips, self.chips) * CORES + core

    def device(self, hops, core=None):
        return {"dp": self.index(self.chip + hops, self.core if core is None else core)}

    def partner(self):
        return self.device(0, 1 - self.core)

    def hop(self, sems, src, dst, to):
        return pltpu.make_async_remote_copy(src_ref=src, dst_ref=dst, send_sem=sems.at[0], recv_sem=sems.at[1], device_id=to, device_id_type=MESH)

    def copies0(self, n, rows):
        slot = lax.rem(n, self.slots)
        src = self.mine.at[slot, 1 - self.core, :, head(rows), :]
        return [self.hop(self.dma.at[slot, 0], src, self.other.at[slot, :, head(rows), :], self.partner())]

    def copies1(self, n, rows):
        slot, sem, half = lax.rem(n, self.lanes), lax.rem(n, self.slots), head(rows // 2)
        return [self.hop(self.dma.at[sem, 1 + side], self.out1.at[slot, side, half], self.cross.at[slot, side, half], self.device(hop)) for side, hop in SIDES]

    def copies2(self, n, rows):
        slot, sem, full = lax.rem(n, self.lanes), lax.rem(n, self.slots), head(rows)
        return [self.hop(self.dma.at[sem, 3 + side], self.out2.at[slot, side, full], self.near.at[slot, side, full], self.device(hop)) for side, hop in SIDES]

    def both(self, n, hops, start, size):
        slot, chip = lax.rem(n, self.slots), lax.rem(self.chip + hops + self.chips, self.chips)
        rows = pl.ds(start, size)
        return self.mine[slot, self.core, chip, rows, :].astype(F32) + self.other[slot, chip, rows, :].astype(F32)

    def give(self, kind, to):
        pl.semaphore_signal(self.credit.at[kind], inc=1, device_id=to, device_id_type=MESH)

    def take(self, when, kinds):
        @pl.when(when)
        def _():
            for kind in kinds:
                pl.semaphore_wait(self.credit.at[kind], 1)

    def event0(self, n, rows):
        self.take(n >= self.slots, (0,))
        start(self.copies0(n, rows))

    def event1(self, n, rows):
        slot, half = lax.rem(n, self.lanes), rows // 2
        wait(self.copies0(n, rows))
        for side, _ in SIDES:
            self.out1[slot, side, head(half)] = self.both(n, 2, side * half, half).astype(BF16)
        self.take(n >= self.lanes, (1, 2))
        start(self.copies1(n, rows))

    def event2(self, n, rows):
        slot, half = lax.rem(n, self.lanes), rows // 2
        wait(self.copies1(n, rows))
        for side, hop in SIDES:
            passed = self.both(n, hop, side * half, half) + self.cross[slot, side, head(half)].astype(F32)
            self.out2[slot, side, pl.ds(side * half, half), :] = passed.astype(BF16)
            self.out2[slot, side, pl.ds(half - side * half, half), :] = self.both(n, hop, half - side * half, half).astype(BF16)

        @pl.when(n + self.lanes < self.number)
        def _():
            for side, hop in SIDES:
                self.give(1 + side, self.device(-hop))

        self.take(n >= self.lanes, (3, 4))
        start(self.copies2(n, rows))

    def total(self, n, start, size):
        total = self.both(n, 0, start, size)
        for side, _ in SIDES:
            total += self.near[lax.rem(n, self.lanes), side, pl.ds(start, size), :].astype(F32)
        return total.astype(BF16).astype(F32)

    def event3(self, n, rows):
        wait(self.copies2(n, rows))

    def after3(self, n):
        pl.when(n + self.slots < self.number)(lambda: self.give(0, self.partner()))

        @pl.when(n + self.lanes < self.number)
        def _():
            for side, hop in SIDES:
                self.give(3 + side, self.device(-hop))

    def block(self, n, hops, core, start, size):
        return self.gathered.at[n, self.index(self.chip + hops, core), pl.ds(start, size), :]

    def sems(self, n, kind):
        return self.ag_sem.at[lax.rem(n, self.turns), kind]

    def gathers1(self, n, rows):
        new, own = self.new.at[head(rows)], self.block(n, 0, self.core, 0, rows)
        copies = [self.hop(self.sems(n, side), new, own, self.device(hop)) for side, hop in SIDES]
        return [*copies, self.hop(self.sems(n, 7), new, own, self.partner()), pltpu.make_async_copy(new, own, self.own_sem)]

    def gathers2(self, n, rows):
        copies, half = [], rows // 2
        for side, hop in SIDES:
            part, full = (self.block(n, -hop, self.core, *which) for which in ((side * half, half), (0, rows)))
            copies.append(self.hop(self.sems(n, 2 + side), part, part, self.device(hop)))
            copies.append(self.hop(self.sems(n, 4 + side), full, full, self.partner()))
        return copies

    def gathers3(self, n, rows):
        opposite = self.block(n, 2, self.core, 0, rows)
        return [self.hop(self.sems(n, 6), opposite, opposite, self.partner())]

    def gather1(self, n, rows):
        start(self.gathers1(n, rows))

    def gather2(self, n, rows):
        wait(self.gathers1(n, rows))
        start(self.gathers2(n, rows))

    def gather3(self, n, rows):
        wait(self.gathers2(n, rows))
        start(self.gathers3(n, rows))

    def gather4(self, n, rows):
        wait(self.gathers3(n, rows))


def moment(m, v, g):
    return 0.9 * m + 0.1 * g, 0.95 * v + 0.05 * g * g


def adam(w, m, v, g):
    m, v = moment(m, v, g)
    w = w.astype(F32)
    return (w - 0.02 * (m * lax.rsqrt(v + 1e-8) + 0.1 * w)).astype(BF16)


def backward_kernel(chips, tile, *refs):
    a_hbm, h_hbm, dy_hbm, wg_hbm, wu_hbm, wd_hbm, mg_hbm, mu_hbm, md_hbm, vg_hbm, vu_hbm, vd_hbm, *refs = refs
    gg_hbm, gu_hbm, gd_hbm, whole_gu, whole_dn, own_hbm, dy0_hbm, *refs = refs
    a_tile, dy_tile, at_ref, dyt_ref, da_ref, wg_ref, wu_ref, wd_ref, z_ref, dgu_ref, m_ref, v_ref, w_ref, *refs = refs
    tile_sem, w_sem, state_sem, rows_sem, *pools = refs
    tokens, d = dy_hbm.shape
    layers, _, ff = wg_hbm.shape
    width = chips * LANES
    blocks = ff // width
    pairs = blocks // 2
    rows = d // (CORES * chips)
    lane_blocks = d // LANES
    me = lax.axis_index("dp")
    chip, core = me // CORES, lax.rem(me, CORES)
    tiles = tokens // tile
    steps = layers * blocks
    full, small, small_tile = d, d // 2, tile // 4

    gu = Pool(steps, chips, core, chip, pools[0:8], pools[8:13], whole_gu)
    dn = Pool(layers * (pairs + 1), chips, core, chip, pools[13:21], pools[21:26], whole_dn)

    def layer_of(j):
        return layers - 1 - j // blocks

    def block_of(j):
        j = lax.rem(j, blocks)
        return j // 2 + (pairs + 1) * parity(j)

    def columns(c, j):
        return strip(c * blocks * LANES + block_of(j) * LANES, LANES)

    def is_last(j):
        return lax.rem(j, blocks) == blocks - 1

    def gives_down(j):
        return (j >= 0) & (j < steps) & ((parity(lax.rem(j, blocks)) == 1) | is_last(j))

    def down_of(j):
        return (j // blocks) * (pairs + 1) + lax.rem(j, blocks) // 2

    def for_down(j, act):
        @pl.when(gives_down(j) & ~is_last(j))
        def _():
            act(down_of(j), full)

        @pl.when(gives_down(j) & is_last(j))
        def _():
            act(down_of(j), small)

    def weight_copies(j):
        layer, slot = layer_of(j), parity(j)
        for c in range(chips):
            there, here = columns(c, j), lanes(c)
            yield pltpu.make_async_copy(wg_hbm.at[layer, :, there], wg_ref.at[slot, :, here], w_sem.at[slot, 3 * c])
            yield pltpu.make_async_copy(wu_hbm.at[layer, :, there], wu_ref.at[slot, :, here], w_sem.at[slot, 3 * c + 1])
            yield pltpu.make_async_copy(wd_hbm.at[layer, there, :], wd_ref.at[slot, here, :], w_sem.at[slot, 3 * c + 2])

    def load(src, buf, t, which):
        slot = parity(t)
        return pltpu.make_async_copy(src.at[strip(t * tile, tile), :], buf.at[slot], tile_sem.at[slot, which])

    def start_tile(j, t):
        load(a_hbm.at[layer_of(j)], a_tile, t, 0).start()

        @pl.when(layer_of(j) == layers - 1)
        def _():
            load(dy_hbm, dy_tile, t, 1).start()

        @pl.when(layer_of(j) < layers - 1)
        def _():
            load(dy0_hbm, dy_tile, t, 1).start()

    def wait_tile(t):
        load(dy_hbm, a_tile, t, 0).wait()
        load(dy_hbm, dy_tile, t, 1).wait()

    def gu_parts(n):
        for c in range(chips):
            for u in range(2):
                yield u * chips + c, u, pl.ds((u * chips + c) * rows, rows), columns(c, n)

    def gu_outs(n):
        for i, u, here, there in gu_parts(n):
            yield pltpu.make_async_copy(gu.sum.at[here, :], (gg_hbm, gu_hbm)[u].at[layer_of(n), :, there], gu.out_sem.at[i])

    def gu_state(n):
        layer = layer_of(n)
        for i, u, here, there in gu_parts(n):
            for k, (src, buf) in enumerate((((mg_hbm, mu_hbm)[u], m_ref), ((vg_hbm, vu_hbm)[u], v_ref))):
                yield pltpu.make_async_copy(src.at[layer, :, there], buf.at[here, :], state_sem.at[3 * i + k])
            src = (wg_hbm, wu_hbm)[u].at[layer, strip(me * rows, rows), there]
            yield pltpu.make_async_copy(src, w_ref.at[here, :], state_sem.at[3 * i + 2])

    def dn_parts(n, size):
        step = lax.rem(n, pairs + 1)
        start = step * LANES + core * (LANES // 2) if size == full else pairs * LANES * (1 - core)
        height = size // lane_blocks
        for b in range(lane_blocks):
            yield b, layers - 1 - n // (pairs + 1), start, height, pl.ds(b * height, height), lanes(b)

    def dn_outs(n, size):
        for b, layer, start, height, here, there in dn_parts(n, size):
            at = pl.ds(pl.multiple_of(start, LANES // 2), height)
            yield pltpu.make_async_copy(dn.sum.at[here, :], gd_hbm.at[layer, at, there], dn.out_sem.at[b])

    def own_outs(n, size):
        for b, _, start, height, here, there in dn_parts(n, size):
            at = pl.ds(pl.multiple_of(start, LANES // 2), height)
            yield pltpu.make_async_copy(dn.new.at[here, :], own_hbm.at[at, there], rows_sem.at[b])

    def dn_state(n, size):
        for b, layer, start, height, here, there in dn_parts(n, size):
            at = pl.ds(pl.multiple_of(start, LANES // 2), height)
            for k, (src, buf) in enumerate(((md_hbm, m_ref), (vd_hbm, v_ref))):
                yield pltpu.make_async_copy(src.at[layer, at, there], buf.at[here, :], state_sem.at[3 * b + k])
            at = pl.ds(pl.multiple_of(me * (d // 2) + start, LANES // 2), height)
            yield pltpu.make_async_copy(wd_hbm.at[layer, at, there], w_ref.at[here, :], state_sem.at[3 * b + 2])

    some = d // 3

    def gu_new(n, size):
        gu.event3(n, size)
        pl.when(n > 0)(lambda: wait(gu_outs(n - 1)))
        wait(gu_state(n))

        def piece(i, _):
            at = strip(i * some, some)
            g = gu.total(n, i * some, some)
            gu.sum[at, :] = g.astype(BF16)
            gu.new[at, :] = adam(w_ref[at, :], m_ref[at, :], v_ref[at, :], g)
            return i

        lax.fori_loop(0, size // some, piece, 0)
        gu.after3(n)
        start(gu_outs(n))
        gu.gather1(n, size)

    def dn_new(n, size):
        half, height = LANES // 2, size // lane_blocks
        dn.event3(n, size)
        if size == full:
            begins = lax.rem(n, pairs + 1) == 0
            pl.when((n > 0) & ~begins)(lambda: wait(dn_outs(n - 1, full)))
            pl.when((n > 0) & begins)(lambda: wait(dn_outs(n - 1, small)))
        else:
            wait(dn_outs(n - 1, full))
        wait(dn_state(n, size))
        upper = n < (layers - 1) * (pairs + 1)
        pl.when(n > (layers - 1) * (pairs + 1))(lambda: wait(own_outs(n - 1, full)))

        def finish(at, g):
            dn.sum[at, :] = g.astype(BF16)
            dn.new[at, :] = adam(w_ref[at, :], m_ref[at, :], v_ref[at, :], g)

        if size == full:

            def piece(i, _):
                for start in range(0, some, LANES):
                    finish(strip(i * some + start, LANES), dn.total(n, i * some + start, LANES).T)
                return i

            lax.fori_loop(0, size // some, piece, 0)
        else:
            g = dn.total(n, 0, size).T
            g = jnp.concatenate([g[:half], g[half:]], 1)
            for b in range(lane_blocks):
                finish(pl.ds(b * height, height), g[:, b * LANES : (b + 1) * LANES])
        dn.after3(n)
        start(dn_outs(n, size))
        pl.when(upper)(lambda: dn.gather1(n, size))
        pl.when(~upper)(lambda: start(own_outs(n, size)))

    def turn(buf, slot, into, part):
        for b in range(lane_blocks):
            into[lanes(b), part] = buf[slot, :, b * LANES : (b + 1) * LANES].T

    start_tile(0, 0)
    start(weight_copies(0))
    barrier = pltpu.get_barrier_semaphore()
    peers = (gu.partner(), gu.device(1), gu.device(-1))
    for peer in peers:
        pl.semaphore_signal(barrier, inc=1, device_id=peer, device_id_type=MESH)
    pl.semaphore_wait(barrier, len(peers))

    def keep(t):
        slot = parity(t)
        return pltpu.make_async_copy(dy_tile.at[slot], dy0_hbm.at[strip(t * tile, tile)], tile_sem.at[slot, 2])

    def compute_tile(j, t):
        slot, here = parity(j), parity(t)
        part = strip(t * tile, tile)
        wait_tile(t)
        pl.when(t + 1 < tiles)(lambda: start_tile(j, t + 1))
        a, dy = a_tile[here], dy_tile[here]
        gate = dot(a, wg_ref[slot])
        up = dot(a, wu_ref[slot])
        dz = dot(dy, wd_ref[slot], NT).astype(BF16).astype(F32)
        s = jax.nn.sigmoid(gate)
        act = s * gate
        z_ref[part, :] = (act * up).astype(BF16)
        dgu_ref[1, part, :] = (dz * act).astype(BF16)
        dgu_ref[0, part, :] = (dz * up * (s + act * (1 - s))).astype(BF16)

        @pl.when(j == 0)
        def _():
            turn(a_tile, here, at_ref, part)
            turn(dy_tile, here, dyt_ref, part)
            da_ref[part, :] = jnp.zeros((tile, d), F32)

    def compute_gate_up(j, s):
        slot, u, h = lax.rem(j, gu.slots), s // (chips // 2), 2 * lax.rem(s, chips // 2)
        g = dot(at_ref[...], dgu_ref[u, :, strip(h * LANES, 2 * LANES)]).astype(BF16)
        for c in range(2):
            at = strip((u * chips + h + c) * rows, rows)
            for owner in range(CORES * chips):
                gu.mine[slot, owner % CORES, owner // CORES, at, :] = g[owner * rows : (owner + 1) * rows, c * LANES : (c + 1) * LANES]

    def compute_down(j, h):
        slot = lax.rem(down_of(j), dn.slots)
        owner = parity(lax.rem(j, blocks))
        chips_here = [2 * h, 2 * h + 1]
        z = strip(chips_here[0] * LANES, 2 * LANES)

        @pl.when(~is_last(j))
        def _():
            g = dot(dyt_ref[...], z_ref[:, z]).astype(BF16)
            for c, at in enumerate(chips_here):
                dn.mine[slot, owner, at, :, :] = g[:, c * LANES : (c + 1) * LANES]

        @pl.when(is_last(j))
        def _():
            g = dot(dyt_ref[...], z_ref[:, z])
            half = LANES // 2
            low = lax.broadcasted_iota(jnp.int32, (small, LANES), 1) < half
            for c, at in enumerate(chips_here):
                both = g[:, c * LANES : (c + 1) * LANES]
                turned = pltpu.roll(both, half, 1)
                dn.mine[slot, 0, at, head(small), :] = jnp.where(low, both[:small], turned[small:]).astype(BF16)
                dn.mine[slot, 1, at, head(small), :] = jnp.where(low, turned[:small], both[small:]).astype(BF16)

    def compute_da(j, t):
        slot, part = parity(j), strip(t * tile, tile)
        da_ref[part, :] += dot(dgu_ref[0, part, :], wg_ref[slot], NT) + dot(dgu_ref[1, part, :], wu_ref[slot], NT)

    def change_layer():
        def begin(t):
            load(h_hbm, a_tile, t, 0).start()
            load(dy_hbm, dy_tile, t, 1).start()

        begin(0)

        def one(t, _):
            slot = parity(t)
            wait_tile(t)
            pl.when(t > 0)(lambda: keep(t - 1).wait())
            pl.when(t + 1 < tiles)(lambda: begin(t + 1))

            def piece(i, _):
                here, there = strip(i * small_tile, small_tile), strip(t * tile + i * small_tile, small_tile)
                wide = a_tile[slot, here, :].astype(F32)
                da = da_ref[there, :].astype(BF16).astype(F32)
                scale = lax.rsqrt(jnp.mean(wide * wide, -1, keepdims=True) + 1e-6)
                along = jnp.mean(da * wide, -1, keepdims=True)
                back = (da * scale - wide * (along * scale * scale * scale)).astype(BF16)
                dy_tile[slot, here, :] = dy_tile[slot, here, :] + back
                return 0

            lax.fori_loop(0, tile // small_tile, piece, 0)
            keep(t).start()
            turn(dy_tile, slot, dyt_ref, strip(t * tile, tile))
            return 0

        lax.fori_loop(0, tiles, one, 0)
        keep(tiles - 1).wait()

    def on(j, act):
        pl.when((j >= 0) & (j < steps))(lambda: act(j, full))

    def upper_down(j, act):
        pl.when(j < (layers - 1) * blocks)(lambda: for_down(j, act))

    def gu_load(n, rows):
        start(gu_state(n))

    def dn_load(n, rows):
        start(dn_state(n, rows))

    events = {
        "tile1": [(for_down, dn_new, 2)],
        "tile3": [(on, gu.gather3, 3), (on, gu.event2, 1)],
        "gate0": [(on, gu_load, 1)],
        "gate3": [(on, gu.event0), (for_down, dn.event2, 1)],
        "down0": [(on, gu.gather4, 3)],
        "down1": [(for_down, dn.event0), (upper_down, dn.gather3, 3)],
        "back0": [(on, gu.gather2, 2)],
        "back1": [(upper_down, dn.gather2, 2)],
        "back2": [(on, gu.event1), (for_down, dn.event1)],
        "back3": [(upper_down, dn.gather4, 3), (on, gu_new, 1), (for_down, dn_load, 1)],
    }
    longest = max(sum(ago) for these in events.values() for _, _, *ago in these)

    def step(j, _):
        busy = j < steps
        lower = layer_of(j) > 0
        changes = is_last(j) & lower & busy

        @pl.when(busy)
        def _():
            wait(weight_copies(j))
            pl.when(j + 1 < steps)(lambda: start(weight_copies(j + 1)))

        def parts(name, number, active, compute):
            def one(t, _):
                pl.when(active)(lambda: compute(j, t))
                for at in range(number):

                    @pl.when(t == at)
                    def _():
                        for stream, act, *ago in events.get(f"{name}{at}", ()):
                            stream(j - sum(ago), act)

                return 0

            lax.fori_loop(0, number, one, 0)

        def da_tile(j, t):
            fetch = load(a_hbm.at[0], a_tile, t, 0)
            pl.when(changes)(fetch.start)
            compute_da(j, t)

            @pl.when(changes)
            def _():
                fetch.wait()
                turn(a_tile, parity(t), at_ref, strip(t * tile, tile))

        parts("tile", tiles, busy, compute_tile)
        pl.when(busy & (j + 1 < steps) & ~changes)(lambda: start_tile(j + 1, 0))
        parts("gate", chips, busy, compute_gate_up)
        parts("down", chips // 2, busy, compute_down)
        parts("back", tiles, busy & lower, da_tile)

        @pl.when(changes)
        def _():
            change_layer()
            start_tile(j + 1, 0)

        return 0

    lax.fori_loop(0, steps + longest, step, 0)
    wait(gu_outs(steps - 1))
    wait(dn_outs(dn.number - 1, small))
    wait(own_outs(dn.number - 1, small))


def backward(mesh, a, h, dy, weights, m, v, tile=512):
    tokens, d = dy.shape
    layers, _, ff = weights[0].shape
    chips = mesh.shape["dp"] // CORES
    width = chips * LANES
    blocks = ff // width
    pairs = blocks // 2
    rows = d // (CORES * chips)
    assert layers == 2 and chips == 4 and blocks % 2 == 1 and blocks * width == ff and d % LANES == 0
    shape = lambda *s: jax.ShapeDtypeStruct(s, BF16)
    devices = CORES * chips
    outs = [
        shape(layers, rows, ff),
        shape(layers, rows, ff),
        shape(layers, ff // devices, d),
        shape(layers * blocks, devices, d, LANES),
        shape((layers - 1) * (pairs + 1), devices, d, LANES),
        shape(ff // devices, d),
        shape(tokens, d),
    ]

    def pool(lanes, outputs):
        return [
            pltpu.VMEM((2, CORES, chips, d, LANES), BF16),
            pltpu.VMEM((2, chips, d, LANES), BF16),
            pltpu.VMEM((lanes, 2, d // 2, LANES), BF16),
            pltpu.VMEM((lanes, 2, d, LANES), BF16),
            pltpu.VMEM((lanes, 2, d // 2, LANES), BF16),
            pltpu.VMEM((lanes, 2, d, LANES), BF16),
            pltpu.VMEM((d, LANES), BF16),
            pltpu.VMEM((d, LANES), BF16),
            pltpu.SemaphoreType.DMA((2, 5, 2)),
            pltpu.SemaphoreType.REGULAR((5,)),
            pltpu.SemaphoreType.DMA((outputs,)),
            pltpu.SemaphoreType.DMA((4, 8, 2)),
            pltpu.SemaphoreType.DMA,
        ]

    return pl.pallas_call(
        functools.partial(backward_kernel, chips, tile),
        out_shape=outs,
        in_specs=[ANY] * 12,
        out_specs=[ANY] * len(outs),
        scratch_shapes=[
            pltpu.VMEM((2, tile, d), BF16),
            pltpu.VMEM((2, tile, d), BF16),
            pltpu.VMEM((d, tokens), BF16),
            pltpu.VMEM((d, tokens), BF16),
            pltpu.VMEM((tokens, d), F32),
            pltpu.VMEM((2, d, width), BF16),
            pltpu.VMEM((2, d, width), BF16),
            pltpu.VMEM((2, width, d), BF16),
            pltpu.VMEM((tokens, width), BF16),
            pltpu.VMEM((2, tokens, width), BF16),
            pltpu.VMEM((d, LANES), F32),
            pltpu.VMEM((d, LANES), F32),
            pltpu.VMEM((d, LANES), BF16),
            pltpu.SemaphoreType.DMA((2, 3)),
            pltpu.SemaphoreType.DMA((2, 3 * chips)),
            pltpu.SemaphoreType.DMA((max(6 * chips, 3 * (d // LANES)),)),
            pltpu.SemaphoreType.DMA((d // LANES,)),
            *pool(1, 2 * chips),
            *pool(2, d // LANES),
        ],
        compiler_params=pltpu.CompilerParams(collective_id=1, has_side_effects=True, vmem_limit_bytes=VMEM_BYTES),
        cost_estimate=cost(28 * tokens * d * ff, 24 * d * ff),
        name="backward",
    )(a, h, dy, *weights, *m, *v)


class Ring:
    def __init__(self, units, slots, loads, stores, work):
        self.units, self.slots, self.loads, self.stores, self.work = units, slots, loads, stores, work

    def begin(self):
        for unit in range(self.slots):
            for copy in self.loads(unit, unit):
                copy.start()

    def run(self):
        def one(unit, _):
            slot = lax.rem(unit, self.slots)
            for copy in self.loads(unit, slot):
                copy.wait()

            @pl.when(unit >= self.slots)
            def _():
                for copy in self.stores(unit - self.slots, slot):
                    copy.wait()

            self.work(unit, slot)
            for copy in self.stores(unit, slot):
                copy.start()

            @pl.when(unit + self.slots < self.units)
            def _():
                for copy in self.loads(unit + self.slots, slot):
                    copy.start()

            return 0

        lax.fori_loop(0, self.units, one, 0)

    def end(self):
        for unit in range(self.units - self.slots, self.units):
            for copy in self.stores(unit, unit % self.slots):
                copy.wait()


def place_columns_kernel(layers, slots, x_hbm, gate_hbm, up_hbm, c_in, c_out, sem):
    _, blocks, devices, _, chips, rows, _ = x_hbm.shape
    wide, some = blocks * LANES, c_in.shape[2]
    turns = devices // some

    def place(unit):
        return unit // (chips * turns), lax.rem(unit, chips * turns) // turns, lax.rem(unit, turns) * some

    def loads(unit, slot):
        layer, chip, owners = place(unit)
        return [pltpu.make_async_copy(x_hbm.at[layers - 1 - layer, :, pl.ds(owners, some), :, chip], c_in.at[slot], sem.at[slot, 0])]

    def stores(unit, slot):
        layer, chip, owners = place(unit)
        at = layer, strip(owners * rows, some * rows), strip(chip * wide, wide)
        return [pltpu.make_async_copy(c_out.at[slot, u], out.at[at], sem.at[slot, 1 + u]) for u, out in enumerate((gate_hbm, up_hbm))]

    def work(unit, slot):
        for j in range(blocks):
            at = pl.ds((j // 2 + (blocks // 2 + 1) * (j % 2)) * LANES, LANES)
            for owner in range(some):
                for u in range(2):
                    c_out[slot, u, pl.ds(owner * rows, rows), at] = c_in[slot, j, owner, u]

    ring = Ring(layers * chips * turns, slots, loads, stores, work)
    ring.begin()
    ring.run()
    ring.end()


def place_columns(chunks, layers, d, ff, slots=8, some=2):
    devices = chunks.shape[1]
    chips, rows = devices // CORES, d // devices
    x = chunks.reshape(layers, -1, devices, 2, chips, rows, LANES)
    return pl.pallas_call(
        functools.partial(place_columns_kernel, layers, slots),
        in_specs=[ANY],
        out_specs=[ANY] * 2,
        out_shape=[jax.ShapeDtypeStruct((layers, d, ff), BF16)] * 2,
        scratch_shapes=[
            pltpu.VMEM((slots, x.shape[1], some, 2, rows, LANES), BF16),
            pltpu.VMEM((slots, 2, some * rows, ff // chips), BF16),
            pltpu.SemaphoreType.DMA((slots, 3)),
        ],
        compiler_params=pltpu.CompilerParams(vmem_limit_bytes=VMEM_BYTES),
        cost_estimate=cost(COPY_FLOPS * 8 * layers * d * ff, 8 * layers * d * ff),
        name="place_columns",
    )(x)


def moments_kernel(layers, parts, slots, *refs):
    states, news, s_in, g_in, s_out, sem = refs[:9], refs[9:15], refs[15:18], refs[18:21], refs[21:24], refs[24]

    def at(i, unit):
        layer, part = unit // parts, lax.rem(unit, parts)
        _, r, c = states[i].shape
        return (layer, strip(part * (r // parts), r // parts), slice(None)) if i == 2 else (layer, slice(None), strip(part * (c // parts), c // parts))

    def loads(unit, slot):
        copies = []
        for i in range(3):
            for k in range(2):
                copies.append(pltpu.make_async_copy(states[3 * k + i].at[at(i, unit)], s_in[i].at[slot, k], sem.at[slot, 5 * i + k]))
            copies.append(pltpu.make_async_copy(states[6 + i].at[at(i, unit)], g_in[i].at[slot], sem.at[slot, 5 * i + 2]))
        return copies

    def stores(unit, slot):
        return [
            pltpu.make_async_copy(s_out[i].at[slot, k], news[3 * k + i].at[at(i, unit)], sem.at[slot, 5 * i + 3 + k]) for i in range(3) for k in range(2)
        ]

    def work(unit, slot):
        for i in range(3):
            g = g_in[i][slot].astype(F32)
            s_out[i][slot, 0], s_out[i][slot, 1] = moment(s_in[i][slot, 0], s_in[i][slot, 1], g)

    ring = Ring(layers * parts, slots, loads, stores, work)
    ring.begin()
    ring.run()
    ring.end()


def moments(m, v, g, parts=9, slots=8):
    layers = m[0].shape[0]
    shapes = [(one.shape[1], one.shape[2] // parts) for one in m[:2]] + [(m[2].shape[1] // parts, m[2].shape[2])]
    size = sum(one.size for one in m)
    return pl.pallas_call(
        functools.partial(moments_kernel, layers, parts, slots),
        in_specs=[ANY] * 9,
        out_specs=[ANY] * 6,
        out_shape=[jax.ShapeDtypeStruct(one.shape, F32) for one in m] * 2,
        scratch_shapes=[
            *(pltpu.VMEM((slots, 2, *shape), F32) for shape in shapes),
            *(pltpu.VMEM((slots, *shape), BF16) for shape in shapes),
            *(pltpu.VMEM((slots, 2, *shape), F32) for shape in shapes),
            pltpu.SemaphoreType.DMA((slots, 15)),
        ],
        compiler_params=pltpu.CompilerParams(vmem_limit_bytes=VMEM_BYTES),
        cost_estimate=cost(COPY_FLOPS * 18 * size, 18 * size),
        name="moments",
    )(*m, *v, *g)


def place_rows_kernel(layers, slots, x_hbm, down_hbm, r_in, r_out, sem):
    devices = x_hbm.shape[2]
    pairs = x_hbm.shape[1] - 1
    height, d = r_out.shape[1:]
    half = LANES // 2

    def loads(unit, slot):
        layer, device = layers - 2 - unit // devices, lax.rem(unit, devices)
        return [
            pltpu.make_async_copy(x_hbm.at[layer, head(pairs), device], r_in.at[slot, head(pairs)], sem.at[slot, 0]),
            pltpu.make_async_copy(x_hbm.at[layer, pairs, device, head(d // 2)], r_in.at[slot, pairs, head(d // 2)], sem.at[slot, 1]),
        ]

    def stores(unit, slot):
        layer, device = unit // devices + 1, lax.rem(unit, devices)
        return [pltpu.make_async_copy(r_out.at[slot], down_hbm.at[layer, strip(device * height, height)], sem.at[slot, 2])]

    def work(unit, slot):
        low = lax.rem(unit, CORES)
        for b in range(d // LANES):
            for n in range(pairs):
                r_out[slot, pl.ds(pl.multiple_of(n * LANES + low * half, half), LANES), lanes(b)] = r_in[slot, n, lanes(b), :]
            r_out[slot, pl.ds(pl.multiple_of(pairs * LANES * (1 - low), half), half), lanes(b)] = r_in[slot, pairs, pl.ds(b * half, half), :]

    ring = Ring((layers - 1) * devices, slots, loads, stores, work)
    ring.begin()
    ring.run()
    ring.end()


def place_rows(chunks, layers, d, ff, slots=8):
    devices = chunks.shape[1]
    x = chunks.reshape(layers - 1, -1, devices, d, LANES)
    height = ff // devices
    return pl.pallas_call(
        functools.partial(place_rows_kernel, layers, slots),
        in_specs=[ANY],
        out_specs=ANY,
        out_shape=jax.ShapeDtypeStruct((layers, ff, d), BF16),
        scratch_shapes=[
            pltpu.VMEM((slots, x.shape[1], d, LANES), BF16),
            pltpu.VMEM((slots, height, d), BF16),
            pltpu.SemaphoreType.DMA((slots, 3)),
        ],
        compiler_params=pltpu.CompilerParams(vmem_limit_bytes=VMEM_BYTES),
        cost_estimate=cost(COPY_FLOPS * 4 * d * ff, 4 * d * ff),
        name="place_rows",
    )(x)


def place_blocks_kernel(wheres, me_ref, *refs):
    blocks, (down_hbm, held, sem) = refs[:-4], refs[-3:]
    height = held.shape[1]
    chips = down_hbm.shape[1] // (height * CORES)
    chip, core = me_ref[0] // CORES, lax.rem(me_ref[0], CORES)
    fetch, put = [], []
    for i, (block, (hops, flip)) in enumerate(zip(blocks, wheres)):
        owner = lax.rem(chip + hops + chips, chips) * CORES + (1 - core if flip else core)
        fetch.append(pltpu.make_async_copy(block, held.at[i], sem.at[i, 0]))
        put.append(pltpu.make_async_copy(held.at[i], down_hbm.at[0, strip(owner * height, height)], sem.at[i, 1]))
    start(fetch)
    for one, other in zip(fetch, put):
        one.wait()
        other.start()
    wait(put)


def place_blocks(me, blocks, down):
    wheres, blocks = tuple(blocks), list(blocks.values())
    size = blocks[0].size * len(blocks)
    return pl.pallas_call(
        functools.partial(place_blocks_kernel, wheres),
        in_specs=[pl.BlockSpec(memory_space=pltpu.SMEM)] + [ANY] * (len(blocks) + 1),
        out_specs=ANY,
        out_shape=jax.ShapeDtypeStruct(down.shape, BF16),
        input_output_aliases={len(blocks) + 1: 0},
        scratch_shapes=[pltpu.VMEM((len(blocks), *blocks[0].shape), BF16), pltpu.SemaphoreType.DMA((len(blocks), 2))],
        compiler_params=pltpu.CompilerParams(vmem_limit_bytes=VMEM_BYTES),
        cost_estimate=cost(COPY_FLOPS * 4 * size, 4 * size),
        name="place_blocks",
    )(me, *blocks, down)


def solution(mesh):
    group = mesh.shape["dp"]
    swap = [(i, i ^ 1) for i in range(group)]
    right = [(i, (i + CORES) % group) for i in range(group)]
    left = [(i, (i - CORES) % group) for i in range(group)]

    def step(x, dy, *arrays):
        weights, m, v = (arrays[i : i + 3] for i in (0, 3, 6))
        layers, d, ff = weights[0].shape
        me = lax.axis_index("dp").reshape(1)
        *sums, columns, rows, own, _ = backward(mesh, *forward(x[0], *weights, 0), dy[0], weights, m, v)

        def send(block, to):
            return lax.ppermute(block, "dp", to)

        from_left, from_right = send(own, right), send(own, left)
        gate, up = place_columns(columns, layers, d, ff)
        gate, from_left, from_right = lax.optimization_barrier((gate, from_left, from_right))
        opposite = send(from_left, right)
        near = {(0, 0): own, (-1, 0): from_left, (1, 0): from_right}
        other = {(hops, 1): send(block, swap) for (hops, _), block in near.items()}
        first, *states = moments(m, v, sums)
        first, rows = lax.optimization_barrier((first, rows))
        down = place_rows(rows, layers, d, ff)
        down, opposite = lax.optimization_barrier((down, opposite))
        last = {(2, 1): send(opposite, swap)}
        down = place_blocks(me, {**near, **other, (2, 0): opposite}, down)
        return (gate, up, place_blocks(me, last, down), first, *states)

    seq, whole, rows = P(("rep", "dp"), None, None), P(None, None, None), P(None, "dp", None)
    return jax.shard_map(
        step,
        mesh=mesh,
        in_specs=(seq, seq, whole, whole, whole) + (rows,) * 6,
        out_specs=(P("rep", None, None),) * 3 + (P("rep", "dp", None),) * 6,
        check_vma=False,
    )
```

```python
import functools

import jax
import jax.numpy as jnp
from jax import lax
from jax.experimental import pallas as pl
from jax.experimental.pallas import tpu as pltpu
from jax.sharding import PartitionSpec as P

F32, BF16 = jnp.float32, jnp.bfloat16
NN, NT = (((1,), (0,)), ((), ())), (((1,), (1,)), ((), ()))
MESH = pl.DeviceIdType.MESH
ANY = pl.BlockSpec(memory_space=pl.ANY)
LANES = 128
CORES = 2
VMEM_BYTES = 67_043_328
COPY_FLOPS = 64
LATE = 2
SIDES = (0, 1), (1, -1)


def dot(a, b, dims=NN):
    return lax.dot_general(a, b, dims, preferred_element_type=F32)


def norm(h):
    wide = h.astype(F32)
    return (wide * lax.rsqrt(jnp.mean(wide**2, -1, keepdims=True) + 1e-6)).astype(BF16)


def strip(start, size):
    return pl.ds(pl.multiple_of(start, size), size)


def head(size):
    return pl.ds(0, size)


def parity(n):
    return lax.rem(n, 2)


def lanes(n):
    return pl.ds(n * LANES, LANES)


def start(copies):
    for copy in copies:
        copy.start()


def wait(copies):
    for copy in copies:
        copy.wait()


def cost(flops, moved):
    return pl.CostEstimate(flops=flops, bytes_accessed=moved, transcendentals=moved)


def forward_kernel(tile, x_ref, wg_ref, wu_ref, wd_ref, a_hbm, h_hbm, a_ref, total, ends, a_sem, end_sem):
    block = pl.program_id(0)
    first, last = block == 0, block == pl.num_programs(0) - 1
    tiles = x_ref.shape[0] // tile

    def keep(t):
        rows = strip(t * tile, tile)
        return pltpu.make_async_copy(a_ref.at[rows], a_hbm.at[0, rows], a_sem.at[t])

    def finish(t):
        rows = strip(t * tile, tile)
        for i, out in enumerate((h_hbm, a_hbm.at[1])):
            yield pltpu.make_async_copy(ends.at[parity(t), i], out.at[rows], end_sem.at[parity(t), i])

    @pl.when(first)
    def _():
        def begin(t, _):
            rows = strip(t * tile, tile)
            a_ref[rows, :] = norm(x_ref[rows, :])
            total[rows, :] = jnp.zeros((tile, total.shape[1]), F32)
            keep(t).start()
            return t

        lax.fori_loop(0, tiles, begin, 0)

    def one(t, _):
        rows = strip(t * tile, tile)
        a = a_ref[rows, :]
        gate, up = dot(a, wg_ref[...]), dot(a, wu_ref[...])
        z = (jax.nn.sigmoid(gate) * gate * up).astype(BF16)
        total[rows, :] += dot(z, wd_ref[...])

        @pl.when(last)
        def _():
            keep(t).wait()
            pl.when(t >= 2)(lambda: wait(finish(t - 2)))
            h = x_ref[rows, :] + total[rows, :].astype(BF16)
            for i, end in enumerate((h, norm(h))):
                ends[parity(t), i] = end
            start(finish(t))

        return t

    lax.fori_loop(0, tiles, one, 0)

    @pl.when(last)
    def _():
        for t in range(tiles - 2, tiles):
            wait(finish(t))


def forward(x, wg, wu, wd, layer, width=768, tile=512):
    tokens, d = x.shape
    ff = wg.shape[2]
    state = jax.ShapeDtypeStruct((tokens, d), BF16)
    columns = pl.BlockSpec((None, d, width), lambda i: (layer, 0, i))
    return pl.pallas_call(
        functools.partial(forward_kernel, tile),
        grid=(ff // width,),
        out_shape=[jax.ShapeDtypeStruct((2, tokens, d), BF16), state],
        in_specs=[pl.BlockSpec(x.shape, lambda i: (0, 0)), columns, columns, pl.BlockSpec((None, width, d), lambda i: (layer, i, 0))],
        out_specs=[ANY] * 2,
        scratch_shapes=[
            pltpu.VMEM(x.shape, BF16),
            pltpu.VMEM(x.shape, F32),
            pltpu.VMEM((2, 2, tile, d), BF16),
            pltpu.SemaphoreType.DMA((tokens // tile,)),
            pltpu.SemaphoreType.DMA((2, 2)),
        ],
        compiler_params=pltpu.CompilerParams(vmem_limit_bytes=VMEM_BYTES),
        cost_estimate=cost(6 * tokens * d * ff, 6 * d * ff),
        name="forward",
    )(x, wg, wu, wd)


class Pool:
    def __init__(self, number, chips, core, chip, bufs, sems, gathered):
        self.number, self.chips, self.core, self.chip = number, chips, core, chip
        self.mine, self.other, self.cross, self.near, self.out1, self.out2, self.sum, self.new = bufs
        self.dma, self.credit, self.out_sem, self.ag_sem, self.own_sem = sems
        self.gathered = gathered
        self.slots, self.lanes, self.turns = self.mine.shape[0], self.cross.shape[0], self.ag_sem.shape[0]

    def index(self, chip, core):
        return lax.rem(chip + self.chips, self.chips) * CORES + core

    def device(self, hops, core=None):
        return {"dp": self.index(self.chip + hops, self.core if core is None else core)}

    def partner(self):
        return self.device(0, 1 - self.core)

    def hop(self, sems, src, dst, to):
        return pltpu.make_async_remote_copy(src_ref=src, dst_ref=dst, send_sem=sems.at[0], recv_sem=sems.at[1], device_id=to, device_id_type=MESH)

    def copies0(self, n, rows):
        slot = lax.rem(n, self.slots)
        src = self.mine.at[slot, 1 - self.core, :, head(rows), :]
        return [self.hop(self.dma.at[slot, 0], src, self.other.at[slot, :, head(rows), :], self.partner())]

    def copies1(self, n, rows):
        slot, sem, half = lax.rem(n, self.lanes), lax.rem(n, self.slots), head(rows // 2)
        return [self.hop(self.dma.at[sem, 1 + side], self.out1.at[slot, side, half], self.cross.at[slot, side, half], self.device(hop)) for side, hop in SIDES]

    def copies2(self, n, rows):
        slot, sem, full = lax.rem(n, self.lanes), lax.rem(n, self.slots), head(rows)
        return [self.hop(self.dma.at[sem, 3 + side], self.out2.at[slot, side, full], self.near.at[slot, side, full], self.device(hop)) for side, hop in SIDES]

    def both(self, n, hops, start, size):
        slot, chip = lax.rem(n, self.slots), lax.rem(self.chip + hops + self.chips, self.chips)
        rows = pl.ds(start, size)
        return self.mine[slot, self.core, chip, rows, :].astype(F32) + self.other[slot, chip, rows, :].astype(F32)

    def give(self, kind, to):
        pl.semaphore_signal(self.credit.at[kind], inc=1, device_id=to, device_id_type=MESH)

    def take(self, when, kinds):
        @pl.when(when)
        def _():
            for kind in kinds:
                pl.semaphore_wait(self.credit.at[kind], 1)

    def event0(self, n, rows):
        self.take(n >= self.slots, (0,))
        start(self.copies0(n, rows))

    def event1(self, n, rows):
        slot, half = lax.rem(n, self.lanes), rows // 2
        wait(self.copies0(n, rows))
        for side, _ in SIDES:
            self.out1[slot, side, head(half)] = self.both(n, 2, side * half, half).astype(BF16)
        self.take(n >= self.lanes, (1, 2))
        start(self.copies1(n, rows))

    def event2(self, n, rows):
        slot, half = lax.rem(n, self.lanes), rows // 2
        wait(self.copies1(n, rows))
        for side, hop in SIDES:
            passed = self.both(n, hop, side * half, half) + self.cross[slot, side, head(half)].astype(F32)
            self.out2[slot, side, pl.ds(side * half, half), :] = passed.astype(BF16)
            self.out2[slot, side, pl.ds(half - side * half, half), :] = self.both(n, hop, half - side * half, half).astype(BF16)

        @pl.when(n + self.lanes < self.number)
        def _():
            for side, hop in SIDES:
                self.give(1 + side, self.device(-hop))

        self.take(n >= self.lanes, (3, 4))
        start(self.copies2(n, rows))

    def total(self, n, start, size):
        total = self.both(n, 0, start, size)
        for side, _ in SIDES:
            total += self.near[lax.rem(n, self.lanes), side, pl.ds(start, size), :].astype(F32)
        return total.astype(BF16).astype(F32)

    def event3(self, n, rows):
        wait(self.copies2(n, rows))

    def after3(self, n):
        pl.when(n + self.slots < self.number)(lambda: self.give(0, self.partner()))

        @pl.when(n + self.lanes < self.number)
        def _():
            for side, hop in SIDES:
                self.give(3 + side, self.device(-hop))

    def block(self, n, hops, core, start, size):
        return self.gathered.at[n, self.index(self.chip + hops, core), pl.ds(start, size), :]

    def sems(self, n, kind):
        return self.ag_sem.at[lax.rem(n, self.turns), kind]

    def gathers1(self, n, rows):
        new, own = self.new.at[head(rows)], self.block(n, 0, self.core, 0, rows)
        copies = [self.hop(self.sems(n, side), new, own, self.device(hop)) for side, hop in SIDES]
        return [*copies, self.hop(self.sems(n, 7), new, own, self.partner()), pltpu.make_async_copy(new, own, self.own_sem)]

    def gathers2(self, n, rows):
        copies, half = [], rows // 2
        for side, hop in SIDES:
            part, full = (self.block(n, -hop, self.core, *which) for which in ((side * half, half), (0, rows)))
            copies.append(self.hop(self.sems(n, 2 + side), part, part, self.device(hop)))
            copies.append(self.hop(self.sems(n, 4 + side), full, full, self.partner()))
        return copies

    def gathers3(self, n, rows):
        opposite = self.block(n, 2, self.core, 0, rows)
        return [self.hop(self.sems(n, 6), opposite, opposite, self.partner())]

    def gather1(self, n, rows):
        start(self.gathers1(n, rows))

    def gather2(self, n, rows):
        wait(self.gathers1(n, rows))
        start(self.gathers2(n, rows))

    def gather3(self, n, rows):
        wait(self.gathers2(n, rows))
        start(self.gathers3(n, rows))

    def gather4(self, n, rows):
        wait(self.gathers3(n, rows))


def moment(m, v, g):
    return 0.9 * m + 0.1 * g, 0.95 * v + 0.05 * g * g


def adam(w, m, v, g):
    m, v = moment(m, v, g)
    w = w.astype(F32)
    return (w - 0.02 * (m * lax.rsqrt(v + 1e-8) + 0.1 * w)).astype(BF16)


def backward_kernel(chips, tile, *refs):
    a_hbm, h_hbm, dy_hbm, wg_hbm, wu_hbm, wd_hbm, mg_hbm, mu_hbm, md_hbm, vg_hbm, vu_hbm, vd_hbm, *refs = refs
    gg_hbm, gu_hbm, gd_hbm, whole_gu, whole_dn, own_hbm, dy0_hbm, *refs = refs
    a_tile, dy_tile, at_ref, dyt_ref, da_ref, wg_ref, wu_ref, wd_ref, z_ref, dgu_ref, m_ref, v_ref, w_ref, *refs = refs
    tile_sem, w_sem, state_sem, own_sem, *pools = refs
    tokens, d = dy_hbm.shape
    layers, _, ff = wg_hbm.shape
    width = chips * LANES
    blocks = ff // width
    pairs = blocks // 2
    rows = d // (CORES * chips)
    lane_blocks = d // LANES
    me = lax.axis_index("dp")
    chip, core = me // CORES, lax.rem(me, CORES)
    tiles = tokens // tile
    steps = layers * blocks
    full, small, small_tile = d, d // 2, tile // 4

    gu = Pool(steps, chips, core, chip, pools[0:8], pools[8:13], whole_gu)
    dn = Pool(layers * (pairs + 1), chips, core, chip, pools[13:21], pools[21:26], whole_dn)

    def layer_of(j):
        return layers - 1 - j // blocks

    def block_of(j):
        j = lax.rem(j, blocks)
        return j // 2 + (pairs + 1) * parity(j)

    def columns(c, j):
        return strip(c * blocks * LANES + block_of(j) * LANES, LANES)

    def is_last(j):
        return lax.rem(j, blocks) == blocks - 1

    def gives_down(j):
        return (j >= 0) & (j < steps) & ((parity(lax.rem(j, blocks)) == 1) | is_last(j))

    def down_of(j):
        return (j // blocks) * (pairs + 1) + lax.rem(j, blocks) // 2

    def for_down(j, act):
        @pl.when(gives_down(j) & ~is_last(j))
        def _():
            act(down_of(j), full)

        @pl.when(gives_down(j) & is_last(j))
        def _():
            act(down_of(j), small)

    def weight_copies(j):
        layer, slot = layer_of(j), parity(j)
        for c in range(chips):
            there, here = columns(c, j), lanes(c)
            yield pltpu.make_async_copy(wg_hbm.at[layer, :, there], wg_ref.at[slot, :, here], w_sem.at[slot, 3 * c])
            yield pltpu.make_async_copy(wu_hbm.at[layer, :, there], wu_ref.at[slot, :, here], w_sem.at[slot, 3 * c + 1])
            yield pltpu.make_async_copy(wd_hbm.at[layer, there, :], wd_ref.at[slot, here, :], w_sem.at[slot, 3 * c + 2])

    def load(src, buf, t, which):
        slot = parity(t)
        return pltpu.make_async_copy(src.at[strip(t * tile, tile), :], buf.at[slot], tile_sem.at[slot, which])

    def start_tile(j, t):
        load(a_hbm.at[layer_of(j)], a_tile, t, 0).start()

        @pl.when(layer_of(j) == layers - 1)
        def _():
            load(dy_hbm, dy_tile, t, 1).start()

        @pl.when(layer_of(j) < layers - 1)
        def _():
            load(dy0_hbm, dy_tile, t, 1).start()

    def wait_tile(t):
        load(dy_hbm, a_tile, t, 0).wait()
        load(dy_hbm, dy_tile, t, 1).wait()

    def gu_parts(n):
        for c in range(chips):
            for u in range(2):
                yield u * chips + c, u, pl.ds((u * chips + c) * rows, rows), columns(c, n)

    def gu_outs(n):
        for i, u, here, there in gu_parts(n):
            yield pltpu.make_async_copy(gu.sum.at[here, :], (gg_hbm, gu_hbm)[u].at[layer_of(n), :, there], gu.out_sem.at[i])

    def gu_state(n):
        layer = layer_of(n)
        for i, u, here, there in gu_parts(n):
            for k, (src, buf) in enumerate((((mg_hbm, mu_hbm)[u], m_ref), ((vg_hbm, vu_hbm)[u], v_ref))):
                yield pltpu.make_async_copy(src.at[layer, :, there], buf.at[here, :], state_sem.at[3 * i + k])
            src = (wg_hbm, wu_hbm)[u].at[layer, strip(me * rows, rows), there]
            yield pltpu.make_async_copy(src, w_ref.at[here, :], state_sem.at[3 * i + 2])

    def dn_parts(n, size):
        step = lax.rem(n, pairs + 1)
        start = step * LANES + core * (LANES // 2) if size == full else pairs * LANES * (1 - core)
        height = size // lane_blocks
        for b in range(lane_blocks):
            yield b, layers - 1 - n // (pairs + 1), start, height, pl.ds(b * height, height), lanes(b)

    def dn_outs(n, size):
        for b, layer, start, height, here, there in dn_parts(n, size):
            at = pl.ds(pl.multiple_of(start, LANES // 2), height)
            yield pltpu.make_async_copy(dn.sum.at[here, :], gd_hbm.at[layer, at, there], dn.out_sem.at[b])

    def own_out(pool, at, size, sem):
        return [pltpu.make_async_copy(pool.new.at[head(size)], own_hbm.at[pl.ds(pl.multiple_of(at, LANES // 2), size)], own_sem.at[sem])]

    def dn_own(n, size):
        return own_out(dn, (n - (layers - 1) * (pairs + 1)) * full, size, 0)

    def gu_own(n):
        return own_out(gu, pairs * full + small + (n - steps + LATE) * full, full, 1)

    def dn_state(n, size):
        for b, layer, start, height, here, there in dn_parts(n, size):
            at = pl.ds(pl.multiple_of(start, LANES // 2), height)
            for k, (src, buf) in enumerate(((md_hbm, m_ref), (vd_hbm, v_ref))):
                yield pltpu.make_async_copy(src.at[layer, at, there], buf.at[here, :], state_sem.at[3 * b + k])
            at = pl.ds(pl.multiple_of(me * (d // 2) + start, LANES // 2), height)
            yield pltpu.make_async_copy(wd_hbm.at[layer, at, there], w_ref.at[here, :], state_sem.at[3 * b + 2])

    some = d // 3

    def gu_new(n, size):
        gu.event3(n, size)
        pl.when(n > 0)(lambda: wait(gu_outs(n - 1)))
        wait(gu_state(n))
        late = n >= steps - LATE
        pl.when(n > steps - LATE)(lambda: wait(gu_own(n - 1)))

        def piece(i, _):
            at = strip(i * some, some)
            g = gu.total(n, i * some, some)
            gu.sum[at, :] = g.astype(BF16)
            gu.new[at, :] = adam(w_ref[at, :], m_ref[at, :], v_ref[at, :], g)
            return i

        lax.fori_loop(0, size // some, piece, 0)
        gu.after3(n)
        start(gu_outs(n))
        pl.when(~late)(lambda: gu.gather1(n, size))
        pl.when(late)(lambda: start(gu_own(n)))

    def dn_new(n, size):
        half, height = LANES // 2, size // lane_blocks
        dn.event3(n, size)
        if size == full:
            begins = lax.rem(n, pairs + 1) == 0
            pl.when((n > 0) & ~begins)(lambda: wait(dn_outs(n - 1, full)))
            pl.when((n > 0) & begins)(lambda: wait(dn_outs(n - 1, small)))
        else:
            wait(dn_outs(n - 1, full))
        wait(dn_state(n, size))
        upper = n < (layers - 1) * (pairs + 1)
        pl.when(n > (layers - 1) * (pairs + 1))(lambda: wait(dn_own(n - 1, full)))

        def finish(at, g):
            dn.sum[at, :] = g.astype(BF16)
            dn.new[at, :] = adam(w_ref[at, :], m_ref[at, :], v_ref[at, :], g)

        if size == full:

            def piece(i, _):
                for start in range(0, some, LANES):
                    finish(strip(i * some + start, LANES), dn.total(n, i * some + start, LANES).T)
                return i

            lax.fori_loop(0, size // some, piece, 0)
        else:
            g = dn.total(n, 0, size).T
            g = jnp.concatenate([g[:half], g[half:]], 1)
            for b in range(lane_blocks):
                finish(pl.ds(b * height, height), g[:, b * LANES : (b + 1) * LANES])
        dn.after3(n)
        start(dn_outs(n, size))
        pl.when(upper)(lambda: dn.gather1(n, size))
        pl.when(~upper)(lambda: start(dn_own(n, size)))

    def turn(buf, slot, into, part):
        for b in range(lane_blocks):
            into[lanes(b), part] = buf[slot, :, b * LANES : (b + 1) * LANES].T

    start_tile(0, 0)
    start(weight_copies(0))
    barrier = pltpu.get_barrier_semaphore()
    peers = (gu.partner(), gu.device(1), gu.device(-1))
    for peer in peers:
        pl.semaphore_signal(barrier, inc=1, device_id=peer, device_id_type=MESH)
    pl.semaphore_wait(barrier, len(peers))

    def keep(t):
        slot = parity(t)
        return pltpu.make_async_copy(dy_tile.at[slot], dy0_hbm.at[strip(t * tile, tile)], tile_sem.at[slot, 2])

    def compute_tile(j, t):
        slot, here = parity(j), parity(t)
        part = strip(t * tile, tile)
        wait_tile(t)
        pl.when(t + 1 < tiles)(lambda: start_tile(j, t + 1))
        a, dy = a_tile[here], dy_tile[here]
        gate = dot(a, wg_ref[slot])
        up = dot(a, wu_ref[slot])
        dz = dot(dy, wd_ref[slot], NT).astype(BF16).astype(F32)
        s = jax.nn.sigmoid(gate)
        act = s * gate
        z_ref[part, :] = (act * up).astype(BF16)
        dgu_ref[1, part, :] = (dz * act).astype(BF16)
        dgu_ref[0, part, :] = (dz * up * (s + act * (1 - s))).astype(BF16)

        @pl.when(j == 0)
        def _():
            turn(a_tile, here, at_ref, part)
            turn(dy_tile, here, dyt_ref, part)
            da_ref[part, :] = jnp.zeros((tile, d), F32)

    def compute_gate_up(j, s):
        slot, u, h = lax.rem(j, gu.slots), s // (chips // 2), 2 * lax.rem(s, chips // 2)
        g = dot(at_ref[...], dgu_ref[u, :, strip(h * LANES, 2 * LANES)]).astype(BF16)
        for c in range(2):
            at = strip((u * chips + h + c) * rows, rows)
            for owner in range(CORES * chips):
                gu.mine[slot, owner % CORES, owner // CORES, at, :] = g[owner * rows : (owner + 1) * rows, c * LANES : (c + 1) * LANES]

    def compute_down(j, h):
        slot = lax.rem(down_of(j), dn.slots)
        owner = parity(lax.rem(j, blocks))
        chips_here = [2 * h, 2 * h + 1]
        z = strip(chips_here[0] * LANES, 2 * LANES)

        @pl.when(~is_last(j))
        def _():
            g = dot(dyt_ref[...], z_ref[:, z]).astype(BF16)
            for c, at in enumerate(chips_here):
                dn.mine[slot, owner, at, :, :] = g[:, c * LANES : (c + 1) * LANES]

        @pl.when(is_last(j))
        def _():
            g = dot(dyt_ref[...], z_ref[:, z])
            half = LANES // 2
            low = lax.broadcasted_iota(jnp.int32, (small, LANES), 1) < half
            for c, at in enumerate(chips_here):
                both = g[:, c * LANES : (c + 1) * LANES]
                turned = pltpu.roll(both, half, 1)
                dn.mine[slot, 0, at, head(small), :] = jnp.where(low, both[:small], turned[small:]).astype(BF16)
                dn.mine[slot, 1, at, head(small), :] = jnp.where(low, turned[:small], both[small:]).astype(BF16)

    def compute_da(j, t):
        slot, part = parity(j), strip(t * tile, tile)
        da_ref[part, :] += dot(dgu_ref[0, part, :], wg_ref[slot], NT) + dot(dgu_ref[1, part, :], wu_ref[slot], NT)

    def change_layer():
        def begin(t):
            load(h_hbm, a_tile, t, 0).start()
            load(dy_hbm, dy_tile, t, 1).start()

        begin(0)

        def one(t, _):
            slot = parity(t)
            wait_tile(t)
            pl.when(t > 0)(lambda: keep(t - 1).wait())
            pl.when(t + 1 < tiles)(lambda: begin(t + 1))

            def piece(i, _):
                here, there = strip(i * small_tile, small_tile), strip(t * tile + i * small_tile, small_tile)
                wide = a_tile[slot, here, :].astype(F32)
                da = da_ref[there, :].astype(BF16).astype(F32)
                scale = lax.rsqrt(jnp.mean(wide * wide, -1, keepdims=True) + 1e-6)
                along = jnp.mean(da * wide, -1, keepdims=True)
                back = (da * scale - wide * (along * scale * scale * scale)).astype(BF16)
                dy_tile[slot, here, :] = dy_tile[slot, here, :] + back
                return 0

            lax.fori_loop(0, tile // small_tile, piece, 0)
            keep(t).start()
            turn(dy_tile, slot, dyt_ref, strip(t * tile, tile))
            return 0

        lax.fori_loop(0, tiles, one, 0)
        keep(tiles - 1).wait()

    def on(j, act):
        pl.when((j >= 0) & (j < steps))(lambda: act(j, full))

    def early(j, act):
        pl.when(j < steps - LATE)(lambda: on(j, act))

    def upper_down(j, act):
        pl.when(j < (layers - 1) * blocks)(lambda: for_down(j, act))

    def gu_load(n, rows):
        start(gu_state(n))

    def dn_load(n, rows):
        start(dn_state(n, rows))

    events = {
        "tile0": [(early, gu.gather4, 4), (for_down, dn_new, 2)],
        "tile2": [(on, gu.event2, 1)],
        "tile3": [(on, gu_load, 1)],
        "gate1": [(early, gu.gather3, 3), (for_down, dn.event2, 1)],
        "gate3": [(on, gu.event0), (upper_down, dn.gather3, 3), (early, gu.gather2, 2)],
        "down0": [(upper_down, dn.gather2, 2)],
        "down1": [(for_down, dn.event0)],
        "back0": [(on, gu.event1)],
        "back1": [(upper_down, dn.gather4, 3), (for_down, dn.event1)],
        "back2": [(on, gu_new, 1)],
        "back3": [(for_down, dn_load, 1)],
    }
    longest = max(sum(ago) for these in events.values() for _, _, *ago in these)

    def step(j, _):
        busy = j < steps
        lower = layer_of(j) > 0
        changes = is_last(j) & lower & busy

        @pl.when(busy)
        def _():
            wait(weight_copies(j))
            pl.when(j + 1 < steps)(lambda: start(weight_copies(j + 1)))

        def parts(name, number, active, compute):
            def one(t, _):
                pl.when(active)(lambda: compute(j, t))
                for at in range(number):

                    @pl.when(t == at)
                    def _():
                        for stream, act, *ago in events.get(f"{name}{at}", ()):
                            stream(j - sum(ago), act)

                return 0

            lax.fori_loop(0, number, one, 0)

        def da_tile(j, t):
            fetch = load(a_hbm.at[0], a_tile, t, 0)
            pl.when(changes)(fetch.start)
            compute_da(j, t)

            @pl.when(changes)
            def _():
                fetch.wait()
                turn(a_tile, parity(t), at_ref, strip(t * tile, tile))

        parts("tile", tiles, busy, compute_tile)
        pl.when(busy & (j + 1 < steps) & ~changes)(lambda: start_tile(j + 1, 0))
        parts("gate", chips, busy, compute_gate_up)
        parts("down", chips // 2, busy, compute_down)
        parts("back", tiles, busy & lower, da_tile)

        @pl.when(changes)
        def _():
            change_layer()
            start_tile(j + 1, 0)

        return 0

    lax.fori_loop(0, steps + longest, step, 0)
    wait(gu_outs(steps - 1))
    wait(dn_outs(dn.number - 1, small))
    wait(dn_own(dn.number - 1, small))
    wait(gu_own(steps - 1))


def backward(mesh, a, h, dy, weights, m, v, tile=512):
    tokens, d = dy.shape
    layers, _, ff = weights[0].shape
    chips = mesh.shape["dp"] // CORES
    width = chips * LANES
    blocks = ff // width
    pairs = blocks // 2
    rows = d // (CORES * chips)
    assert layers == 2 and chips == 4 and blocks % 2 == 1 and blocks * width == ff and d % LANES == 0
    shape = lambda *s: jax.ShapeDtypeStruct(s, BF16)
    devices = CORES * chips
    outs = [
        shape(layers, rows, ff),
        shape(layers, rows, ff),
        shape(layers, ff // devices, d),
        shape(layers * blocks, devices, d, LANES),
        shape((layers - 1) * (pairs + 1), devices, d, LANES),
        shape(pairs * d + d // 2 + LATE * d, LANES),
        shape(tokens, d),
    ]

    def pool(lanes, outputs):
        return [
            pltpu.VMEM((2, CORES, chips, d, LANES), BF16),
            pltpu.VMEM((2, chips, d, LANES), BF16),
            pltpu.VMEM((lanes, 2, d // 2, LANES), BF16),
            pltpu.VMEM((lanes, 2, d, LANES), BF16),
            pltpu.VMEM((lanes, 2, d // 2, LANES), BF16),
            pltpu.VMEM((lanes, 2, d, LANES), BF16),
            pltpu.VMEM((d, LANES), BF16),
            pltpu.VMEM((d, LANES), BF16),
            pltpu.SemaphoreType.DMA((2, 5, 2)),
            pltpu.SemaphoreType.REGULAR((5,)),
            pltpu.SemaphoreType.DMA((outputs,)),
            pltpu.SemaphoreType.DMA((4, 8, 2)),
            pltpu.SemaphoreType.DMA,
        ]

    return pl.pallas_call(
        functools.partial(backward_kernel, chips, tile),
        out_shape=outs,
        in_specs=[ANY] * 12,
        out_specs=[ANY] * len(outs),
        scratch_shapes=[
            pltpu.VMEM((2, tile, d), BF16),
            pltpu.VMEM((2, tile, d), BF16),
            pltpu.VMEM((d, tokens), BF16),
            pltpu.VMEM((d, tokens), BF16),
            pltpu.VMEM((tokens, d), F32),
            pltpu.VMEM((2, d, width), BF16),
            pltpu.VMEM((2, d, width), BF16),
            pltpu.VMEM((2, width, d), BF16),
            pltpu.VMEM((tokens, width), BF16),
            pltpu.VMEM((2, tokens, width), BF16),
            pltpu.VMEM((d, LANES), F32),
            pltpu.VMEM((d, LANES), F32),
            pltpu.VMEM((d, LANES), BF16),
            pltpu.SemaphoreType.DMA((2, 3)),
            pltpu.SemaphoreType.DMA((2, 3 * chips)),
            pltpu.SemaphoreType.DMA((max(6 * chips, 3 * (d // LANES)),)),
            pltpu.SemaphoreType.DMA((2,)),
            *pool(1, 2 * chips),
            *pool(2, d // LANES),
        ],
        compiler_params=pltpu.CompilerParams(collective_id=1, has_side_effects=True, vmem_limit_bytes=VMEM_BYTES),
        cost_estimate=cost(28 * tokens * d * ff, 24 * d * ff),
        name="backward",
    )(a, h, dy, *weights, *m, *v)


class Ring:
    def __init__(self, units, slots, loads, stores, work):
        self.units, self.slots, self.loads, self.stores, self.work = units, slots, loads, stores, work

    def begin(self):
        for unit in range(self.slots):
            for copy in self.loads(unit, unit):
                copy.start()

    def run(self):
        def one(unit, _):
            slot = lax.rem(unit, self.slots)
            for copy in self.loads(unit, slot):
                copy.wait()

            @pl.when(unit >= self.slots)
            def _():
                for copy in self.stores(unit - self.slots, slot):
                    copy.wait()

            self.work(unit, slot)
            for copy in self.stores(unit, slot):
                copy.start()

            @pl.when(unit + self.slots < self.units)
            def _():
                for copy in self.loads(unit + self.slots, slot):
                    copy.start()

            return 0

        lax.fori_loop(0, self.units, one, 0)

    def end(self):
        for unit in range(self.units - self.slots, self.units):
            for copy in self.stores(unit, unit % self.slots):
                copy.wait()


def place_columns_kernel(layer, slots, x_hbm, *refs):
    gate_hbm, up_hbm, c_in, c_out, sem = refs[-5:]
    _, blocks, devices, _, chips, rows, _ = x_hbm.shape
    wide, some = blocks * LANES, c_in.shape[2]
    turns = devices // some

    def place(unit):
        return unit // turns, lax.rem(unit, turns) * some

    def loads(unit, slot):
        chip, owners = place(unit)
        return [pltpu.make_async_copy(x_hbm.at[x_hbm.shape[0] - 1 - layer, :, pl.ds(owners, some), :, chip], c_in.at[slot], sem.at[slot, 0])]

    def stores(unit, slot):
        chip, owners = place(unit)
        at = layer, strip(owners * rows, some * rows), strip(chip * wide, wide)
        return [pltpu.make_async_copy(c_out.at[slot, u], out.at[at], sem.at[slot, 1 + u]) for u, out in enumerate((gate_hbm, up_hbm))]

    def work(unit, slot):
        for j in range(blocks):
            at = pl.ds((j // 2 + (blocks // 2 + 1) * (j % 2)) * LANES, LANES)
            for owner in range(some):
                for u in range(2):
                    c_out[slot, u, pl.ds(owner * rows, rows), at] = c_in[slot, j, owner, u]

    ring = Ring(chips * turns, slots, loads, stores, work)
    ring.begin()
    ring.run()
    ring.end()


def place_columns(chunks, layer, layers, d, ff, into=(), slots=4, some=2):
    devices = chunks.shape[1]
    chips, rows = devices // CORES, d // devices
    x = chunks.reshape(layers, -1, devices, 2, chips, rows, LANES)
    return pl.pallas_call(
        functools.partial(place_columns_kernel, layer, slots),
        in_specs=[ANY] * (1 + len(into)),
        out_specs=[ANY] * 2,
        input_output_aliases={1 + i: i for i in range(len(into))},
        out_shape=[jax.ShapeDtypeStruct((layers, d, ff), BF16)] * 2,
        scratch_shapes=[
            pltpu.VMEM((slots, x.shape[1], some, 2, rows, LANES), BF16),
            pltpu.VMEM((slots, 2, some * rows, ff // chips), BF16),
            pltpu.SemaphoreType.DMA((slots, 3)),
        ],
        compiler_params=pltpu.CompilerParams(vmem_limit_bytes=VMEM_BYTES),
        cost_estimate=cost(COPY_FLOPS * 8 * d * ff, 8 * d * ff),
        name="place_columns",
    )(x, *into)


def moments_kernel(layers, parts, slots, *refs):
    states, news, s_in, g_in, s_out, sem = refs[:9], refs[9:15], refs[15:18], refs[18:21], refs[21:24], refs[24]

    def at(i, unit):
        layer, part = unit // parts, lax.rem(unit, parts)
        _, r, c = states[i].shape
        return (layer, strip(part * (r // parts), r // parts), slice(None)) if i == 2 else (layer, slice(None), strip(part * (c // parts), c // parts))

    def loads(unit, slot):
        copies = []
        for i in range(3):
            for k in range(2):
                copies.append(pltpu.make_async_copy(states[3 * k + i].at[at(i, unit)], s_in[i].at[slot, k], sem.at[slot, 5 * i + k]))
            copies.append(pltpu.make_async_copy(states[6 + i].at[at(i, unit)], g_in[i].at[slot], sem.at[slot, 5 * i + 2]))
        return copies

    def stores(unit, slot):
        return [
            pltpu.make_async_copy(s_out[i].at[slot, k], news[3 * k + i].at[at(i, unit)], sem.at[slot, 5 * i + 3 + k]) for i in range(3) for k in range(2)
        ]

    def work(unit, slot):
        for i in range(3):
            g = g_in[i][slot].astype(F32)
            s_out[i][slot, 0], s_out[i][slot, 1] = moment(s_in[i][slot, 0], s_in[i][slot, 1], g)

    ring = Ring(layers * parts, slots, loads, stores, work)
    ring.begin()
    ring.run()
    ring.end()


def moments(m, v, g, parts=9, slots=4):
    layers = m[0].shape[0]
    shapes = [(one.shape[1], one.shape[2] // parts) for one in m[:2]] + [(m[2].shape[1] // parts, m[2].shape[2])]
    size = sum(one.size for one in m)
    return pl.pallas_call(
        functools.partial(moments_kernel, layers, parts, slots),
        in_specs=[ANY] * 9,
        out_specs=[ANY] * 6,
        out_shape=[jax.ShapeDtypeStruct(one.shape, F32) for one in m] * 2,
        scratch_shapes=[
            *(pltpu.VMEM((slots, 2, *shape), F32) for shape in shapes),
            *(pltpu.VMEM((slots, *shape), BF16) for shape in shapes),
            *(pltpu.VMEM((slots, 2, *shape), F32) for shape in shapes),
            pltpu.SemaphoreType.DMA((slots, 15)),
        ],
        compiler_params=pltpu.CompilerParams(vmem_limit_bytes=VMEM_BYTES),
        cost_estimate=cost(COPY_FLOPS * 18 * size, 18 * size),
        name="moments",
    )(*m, *v, *g)


def unfold(chunks, out, core):
    pairs, half = chunks.shape[0] - 1, LANES // 2
    for b in range(out.shape[1] // LANES):
        for n in range(pairs):
            out[pl.ds(pl.multiple_of(n * LANES + core * half, half), LANES), lanes(b)] = chunks[n, lanes(b), :]
        out[pl.ds(pl.multiple_of(pairs * LANES * (1 - core), half), half), lanes(b)] = chunks[pairs, pl.ds(b * half, half), :]


def place_rows_kernel(layers, slots, x_hbm, down_hbm, r_in, r_out, sem):
    devices = x_hbm.shape[2]
    pairs = x_hbm.shape[1] - 1
    height, d = r_out.shape[1:]

    def loads(unit, slot):
        layer, device = layers - 2 - unit // devices, lax.rem(unit, devices)
        return [
            pltpu.make_async_copy(x_hbm.at[layer, head(pairs), device], r_in.at[slot, head(pairs)], sem.at[slot, 0]),
            pltpu.make_async_copy(x_hbm.at[layer, pairs, device, head(d // 2)], r_in.at[slot, pairs, head(d // 2)], sem.at[slot, 1]),
        ]

    def stores(unit, slot):
        layer, device = unit // devices + 1, lax.rem(unit, devices)
        return [pltpu.make_async_copy(r_out.at[slot], down_hbm.at[layer, strip(device * height, height)], sem.at[slot, 2])]

    def work(unit, slot):
        unfold(r_in.at[slot], r_out.at[slot], lax.rem(unit, CORES))

    ring = Ring((layers - 1) * devices, slots, loads, stores, work)
    ring.begin()
    ring.run()
    ring.end()


def place_rows(chunks, layers, d, ff, slots=4):
    devices = chunks.shape[1]
    x = chunks.reshape(layers - 1, -1, devices, d, LANES)
    height = ff // devices
    return pl.pallas_call(
        functools.partial(place_rows_kernel, layers, slots),
        in_specs=[ANY],
        out_specs=ANY,
        out_shape=jax.ShapeDtypeStruct((layers, ff, d), BF16),
        scratch_shapes=[
            pltpu.VMEM((slots, x.shape[1], d, LANES), BF16),
            pltpu.VMEM((slots, height, d), BF16),
            pltpu.SemaphoreType.DMA((slots, 3)),
        ],
        compiler_params=pltpu.CompilerParams(vmem_limit_bytes=VMEM_BYTES),
        cost_estimate=cost(COPY_FLOPS * 4 * d * ff, 4 * d * ff),
        name="place_rows",
    )(x)


def place_blocks_kernel(wheres, pieces, me_ref, *refs):
    blocks, (gate_hbm, up_hbm, down_hbm, held, down, sem) = refs[: pieces * len(wheres)], refs[-6:]
    layers, d, ff = gate_hbm.shape
    height = down.shape[1]
    devices = ff // height
    chips, rows = devices // CORES, d // devices
    wide, size = ff // chips, blocks[0].shape[0]
    pairs = wide // LANES // 2
    chip, core = me_ref[0] // CORES, lax.rem(me_ref[0], CORES)

    def fetch(i):
        for k in range(pieces):
            yield pltpu.make_async_copy(blocks[pieces * i + k], held.at[i, pl.ds(k * size, size)], sem.at[i, k])

    def put(i):
        hops, flip = wheres[i]
        side = 1 - core if flip else core
        owner = lax.rem(chip + hops + chips, chips) * CORES + side
        copies = [pltpu.make_async_copy(down.at[i], down_hbm.at[0, strip(owner * height, height)], sem.at[i, 2])]
        for n in range(LATE):
            step = 2 * pairs + 1 - LATE + n
            column = (step // 2 + (pairs + 1) * (step % 2)) * LANES
            for u, out in enumerate((gate_hbm, up_hbm)):
                for c in range(chips):
                    here = pl.ds(pairs * d + d // 2 + n * d + (u * chips + c) * rows, rows)
                    to = out.at[0, strip(owner * rows, rows), pl.ds(c * wide + column, LANES)]
                    copies.append(pltpu.make_async_copy(held.at[i, here], to, sem.at[i, 2 + len(copies)]))
        return side, copies

    number = len(wheres)
    for i in range(number):
        start(fetch(i))
    for i in range(number):
        wait(fetch(i))
        side, copies = put(i)
        start(copies[1:])
        for n in range(pairs + 1):
            size_n = d if n < pairs else d // 2
            for b in range(d // LANES):
                part = size_n // (d // LANES)
                at = n * LANES + side * (LANES // 2) if n < pairs else pairs * LANES * (1 - side)
                down[i, pl.ds(pl.multiple_of(at, LANES // 2), part), lanes(b)] = held[i, pl.ds(n * d + b * part, part), :]
        copies[0].start()
    for i in range(number):
        wait(put(i)[1])


def place_blocks(me, blocks, weights):
    wheres, blocks = tuple(blocks), list(blocks.values())
    number, pieces = len(blocks), len(blocks[0])
    rows = pieces * blocks[0][0].shape[0]
    layers, ff, d = weights[2].shape
    height = rows * LANES // d - LATE * LANES
    return pl.pallas_call(
        functools.partial(place_blocks_kernel, wheres, pieces),
        in_specs=[pl.BlockSpec(memory_space=pltpu.SMEM)] + [ANY] * (number * pieces + 3),
        out_specs=[ANY] * 3,
        out_shape=[jax.ShapeDtypeStruct(one.shape, BF16) for one in weights],
        input_output_aliases={number * pieces + 1 + i: i for i in range(3)},
        scratch_shapes=[
            pltpu.VMEM((number, rows, LANES), BF16),
            pltpu.VMEM((number, height, d), BF16),
            pltpu.SemaphoreType.DMA((number, 3 + LATE * ff // height)),
        ],
        compiler_params=pltpu.CompilerParams(vmem_limit_bytes=VMEM_BYTES),
        cost_estimate=cost(COPY_FLOPS * 4 * number * rows * LANES, 4 * number * rows * LANES),
        name="place_blocks",
    )(me, *(piece for block in blocks for piece in block), *weights)


def solution(mesh):
    group = mesh.shape["dp"]
    swap = [(i, i ^ 1) for i in range(group)]
    right = [(i, (i + CORES) % group) for i in range(group)]
    left = [(i, (i - CORES) % group) for i in range(group)]

    def step(x, dy, *arrays):
        weights, m, v = (arrays[i : i + 3] for i in (0, 3, 6))
        layers, d, ff = weights[0].shape
        me = lax.axis_index("dp").reshape(1)
        *sums, columns, rows, own, _ = backward(mesh, *forward(x[0], *weights, 0), dy[0], weights, m, v)

        def send(block, to):
            return [lax.ppermute(piece, "dp", to) for piece in block]

        half = own.shape[0] // 2
        (from_left,), (from_right,) = send([own], right), send([own], left)
        gate, up = place_columns(columns, 1, layers, d, ff)
        first, *states = moments(m, v, sums)
        gate, first, from_left, from_right = lax.optimization_barrier((gate, first, from_left, from_right))
        opposite = send([from_left[:half]], right) + send([from_right[half:]], left)
        near = {(0, 0): [own], (-1, 0): [from_left], (1, 0): [from_right]}
        other = {(hops, 1): send(block, swap) for (hops, _), block in near.items()}
        gate, up = place_columns(columns, 0, layers, d, ff, (gate, up))
        up, rows = lax.optimization_barrier((up, rows))
        down = place_rows(rows, layers, d, ff)
        down, *opposite = lax.optimization_barrier((down, *opposite))
        last = send(opposite, swap)
        weights = place_blocks(me, {**near, **other}, (gate, up, down))
        weights = place_blocks(me, {(2, 0): opposite, (2, 1): last}, weights)
        return (*weights, first, *states)

    seq, whole, rows = P(("rep", "dp"), None, None), P(None, None, None), P(None, "dp", None)
    return jax.shard_map(
        step,
        mesh=mesh,
        in_specs=(seq, seq, whole, whole, whole) + (rows,) * 6,
        out_specs=(P("rep", None, None),) * 3 + (P("rep", "dp", None),) * 6,
        check_vma=False,
    )
```

```python
import functools

import jax
import jax.numpy as jnp
from jax import lax
from jax.experimental import pallas as pl
from jax.experimental.pallas import tpu as pltpu
from jax.sharding import PartitionSpec as P

F32, BF16 = jnp.float32, jnp.bfloat16
NN, NT = (((1,), (0,)), ((), ())), (((1,), (1,)), ((), ()))
MESH = pl.DeviceIdType.MESH
ANY = pl.BlockSpec(memory_space=pl.ANY)
LANES = 128
CORES = 2
VMEM_BYTES = 67_043_328
COPY_FLOPS = 64
LATE = 2
SIDES = (0, 1), (1, -1)


def dot(a, b, dims=NN):
    return lax.dot_general(a, b, dims, preferred_element_type=F32)


def norm(h):
    wide = h.astype(F32)
    return (wide * lax.rsqrt(jnp.mean(wide**2, -1, keepdims=True) + 1e-6)).astype(BF16)


def strip(start, size):
    return pl.ds(pl.multiple_of(start, size), size)


def head(size):
    return pl.ds(0, size)


def parity(n):
    return lax.rem(n, 2)


def lanes(n):
    return pl.ds(n * LANES, LANES)


def start(copies):
    for copy in copies:
        copy.start()


def wait(copies):
    for copy in copies:
        copy.wait()


def cost(flops, moved):
    return pl.CostEstimate(flops=flops, bytes_accessed=moved, transcendentals=moved)


def forward_kernel(tile, x_ref, wg_ref, wu_ref, wd_ref, a_hbm, h_hbm, a_ref, total, ends, a_sem, end_sem):
    block = pl.program_id(0)
    first, last = block == 0, block == pl.num_programs(0) - 1
    tiles = x_ref.shape[0] // tile

    def keep(t):
        rows = strip(t * tile, tile)
        return pltpu.make_async_copy(a_ref.at[rows], a_hbm.at[0, rows], a_sem.at[t])

    def finish(t):
        rows = strip(t * tile, tile)
        for i, out in enumerate((h_hbm, a_hbm.at[1])):
            yield pltpu.make_async_copy(ends.at[parity(t), i], out.at[rows], end_sem.at[parity(t), i])

    @pl.when(first)
    def _():
        def begin(t, _):
            rows = strip(t * tile, tile)
            a_ref[rows, :] = norm(x_ref[rows, :])
            total[rows, :] = jnp.zeros((tile, total.shape[1]), F32)
            keep(t).start()
            return t

        lax.fori_loop(0, tiles, begin, 0)

    def one(t, _):
        rows = strip(t * tile, tile)
        a = a_ref[rows, :]
        gate, up = dot(a, wg_ref[...]), dot(a, wu_ref[...])
        z = (jax.nn.sigmoid(gate) * gate * up).astype(BF16)
        total[rows, :] += dot(z, wd_ref[...])

        @pl.when(last)
        def _():
            keep(t).wait()
            pl.when(t >= 2)(lambda: wait(finish(t - 2)))
            h = x_ref[rows, :] + total[rows, :].astype(BF16)
            for i, end in enumerate((h, norm(h))):
                ends[parity(t), i] = end
            start(finish(t))

        return t

    lax.fori_loop(0, tiles, one, 0)

    @pl.when(last)
    def _():
        for t in range(tiles - 2, tiles):
            wait(finish(t))


def forward(x, wg, wu, wd, layer, width=768, tile=512):
    tokens, d = x.shape
    ff = wg.shape[2]
    state = jax.ShapeDtypeStruct((tokens, d), BF16)
    columns = pl.BlockSpec((None, d, width), lambda i: (layer, 0, i))
    return pl.pallas_call(
        functools.partial(forward_kernel, tile),
        grid=(ff // width,),
        out_shape=[jax.ShapeDtypeStruct((2, tokens, d), BF16), state],
        in_specs=[pl.BlockSpec(x.shape, lambda i: (0, 0)), columns, columns, pl.BlockSpec((None, width, d), lambda i: (layer, i, 0))],
        out_specs=[ANY] * 2,
        scratch_shapes=[
            pltpu.VMEM(x.shape, BF16),
            pltpu.VMEM(x.shape, F32),
            pltpu.VMEM((2, 2, tile, d), BF16),
            pltpu.SemaphoreType.DMA((tokens // tile,)),
            pltpu.SemaphoreType.DMA((2, 2)),
        ],
        compiler_params=pltpu.CompilerParams(vmem_limit_bytes=VMEM_BYTES),
        cost_estimate=cost(6 * tokens * d * ff, 6 * d * ff),
        name="forward",
    )(x, wg, wu, wd)


class Pool:
    def __init__(self, number, chips, core, chip, bufs, sems, gathered):
        self.number, self.chips, self.core, self.chip = number, chips, core, chip
        self.mine, self.other, self.cross, self.near, self.out1, self.out2, self.sum, self.new = bufs
        self.dma, self.credit, self.out_sem, self.ag_sem, self.own_sem = sems
        self.gathered = gathered
        self.slots, self.lanes, self.turns = self.mine.shape[0], self.cross.shape[0], self.ag_sem.shape[0]

    def index(self, chip, core):
        return lax.rem(chip + self.chips, self.chips) * CORES + core

    def device(self, hops, core=None):
        return {"dp": self.index(self.chip + hops, self.core if core is None else core)}

    def partner(self):
        return self.device(0, 1 - self.core)

    def hop(self, sems, src, dst, to):
        return pltpu.make_async_remote_copy(src_ref=src, dst_ref=dst, send_sem=sems.at[0], recv_sem=sems.at[1], device_id=to, device_id_type=MESH)

    def copies0(self, n, rows):
        slot = lax.rem(n, self.slots)
        src = self.mine.at[slot, 1 - self.core, :, head(rows), :]
        return [self.hop(self.dma.at[slot, 0], src, self.other.at[slot, :, head(rows), :], self.partner())]

    def copies1(self, n, rows):
        slot, sem, half = lax.rem(n, self.lanes), lax.rem(n, self.slots), head(rows // 2)
        return [self.hop(self.dma.at[sem, 1 + side], self.out1.at[slot, side, half], self.cross.at[slot, side, half], self.device(hop)) for side, hop in SIDES]

    def copies2(self, n, rows):
        slot, sem, full = lax.rem(n, self.lanes), lax.rem(n, self.slots), head(rows)
        return [self.hop(self.dma.at[sem, 3 + side], self.out2.at[slot, side, full], self.near.at[slot, side, full], self.device(hop)) for side, hop in SIDES]

    def both(self, n, hops, start, size):
        slot, chip = lax.rem(n, self.slots), lax.rem(self.chip + hops + self.chips, self.chips)
        rows = pl.ds(start, size)
        return self.mine[slot, self.core, chip, rows, :].astype(F32) + self.other[slot, chip, rows, :].astype(F32)

    def give(self, kind, to):
        pl.semaphore_signal(self.credit.at[kind], inc=1, device_id=to, device_id_type=MESH)

    def take(self, when, kinds):
        @pl.when(when)
        def _():
            for kind in kinds:
                pl.semaphore_wait(self.credit.at[kind], 1)

    def event0(self, n, rows):
        self.take(n >= self.slots, (0,))
        start(self.copies0(n, rows))

    def event1(self, n, rows):
        slot, half = lax.rem(n, self.lanes), rows // 2
        wait(self.copies0(n, rows))
        for side, _ in SIDES:
            self.out1[slot, side, head(half)] = self.both(n, 2, side * half, half).astype(BF16)
        self.take(n >= self.lanes, (1, 2))
        start(self.copies1(n, rows))

    def event2(self, n, rows):
        slot, half = lax.rem(n, self.lanes), rows // 2
        wait(self.copies1(n, rows))
        for side, hop in SIDES:
            passed = self.both(n, hop, side * half, half) + self.cross[slot, side, head(half)].astype(F32)
            self.out2[slot, side, pl.ds(side * half, half), :] = passed.astype(BF16)
            self.out2[slot, side, pl.ds(half - side * half, half), :] = self.both(n, hop, half - side * half, half).astype(BF16)

        @pl.when(n + self.lanes < self.number)
        def _():
            for side, hop in SIDES:
                self.give(1 + side, self.device(-hop))

        self.take(n >= self.lanes, (3, 4))
        start(self.copies2(n, rows))

    def total(self, n, start, size):
        total = self.both(n, 0, start, size)
        for side, _ in SIDES:
            total += self.near[lax.rem(n, self.lanes), side, pl.ds(start, size), :].astype(F32)
        return total.astype(BF16).astype(F32)

    def event3(self, n, rows):
        wait(self.copies2(n, rows))

    def after3(self, n):
        pl.when(n + self.slots < self.number)(lambda: self.give(0, self.partner()))

        @pl.when(n + self.lanes < self.number)
        def _():
            for side, hop in SIDES:
                self.give(3 + side, self.device(-hop))

    def block(self, n, hops, core, start, size):
        return self.gathered.at[n, self.index(self.chip + hops, core), pl.ds(start, size), :]

    def sems(self, n, kind):
        return self.ag_sem.at[lax.rem(n, self.turns), kind]

    def gathers1(self, n, rows):
        new, own = self.new.at[head(rows)], self.block(n, 0, self.core, 0, rows)
        copies = [self.hop(self.sems(n, side), new, own, self.device(hop)) for side, hop in SIDES]
        return [*copies, self.hop(self.sems(n, 7), new, own, self.partner()), pltpu.make_async_copy(new, own, self.own_sem)]

    def gathers2(self, n, rows):
        copies, half = [], rows // 2
        for side, hop in SIDES:
            part, full = (self.block(n, -hop, self.core, *which) for which in ((side * half, half), (0, rows)))
            copies.append(self.hop(self.sems(n, 2 + side), part, part, self.device(hop)))
            copies.append(self.hop(self.sems(n, 4 + side), full, full, self.partner()))
        return copies

    def gathers3(self, n, rows):
        opposite = self.block(n, 2, self.core, 0, rows)
        return [self.hop(self.sems(n, 6), opposite, opposite, self.partner())]

    def gather1(self, n, rows):
        start(self.gathers1(n, rows))

    def gather2(self, n, rows):
        wait(self.gathers1(n, rows))
        start(self.gathers2(n, rows))

    def gather3(self, n, rows):
        wait(self.gathers2(n, rows))
        start(self.gathers3(n, rows))

    def gather4(self, n, rows):
        wait(self.gathers3(n, rows))


def moment(m, v, g):
    return 0.9 * m + 0.1 * g, 0.95 * v + 0.05 * g * g


def adam(w, m, v, g):
    m, v = moment(m, v, g)
    w = w.astype(F32)
    return (w - 0.02 * (m * lax.rsqrt(v + 1e-8) + 0.1 * w)).astype(BF16)


def backward_kernel(chips, tile, *refs):
    a_hbm, h_hbm, dy_hbm, wg_hbm, wu_hbm, wd_hbm, mg_hbm, mu_hbm, md_hbm, vg_hbm, vu_hbm, vd_hbm, *refs = refs
    gg_hbm, gu_hbm, gd_hbm, whole_gu, whole_dn, own_hbm, dy0_hbm, *refs = refs
    a_tile, dy_tile, at_ref, dyt_ref, da_ref, wg_ref, wu_ref, wd_ref, z_ref, dgu_ref, m_ref, v_ref, w_ref, *refs = refs
    tile_sem, w_sem, state_sem, own_sem, *pools = refs
    tokens, d = dy_hbm.shape
    layers, _, ff = wg_hbm.shape
    width = chips * LANES
    blocks = ff // width
    pairs = blocks // 2
    rows = d // (CORES * chips)
    lane_blocks = d // LANES
    me = lax.axis_index("dp")
    chip, core = me // CORES, lax.rem(me, CORES)
    tiles = tokens // tile
    steps = layers * blocks
    full, small, small_tile = d, d // 2, tile // 4

    gu = Pool(steps, chips, core, chip, pools[0:8], pools[8:13], whole_gu)
    dn = Pool(layers * (pairs + 1), chips, core, chip, pools[13:21], pools[21:26], whole_dn)

    def layer_of(j):
        return layers - 1 - j // blocks

    def block_of(j):
        j = lax.rem(j, blocks)
        return j // 2 + (pairs + 1) * parity(j)

    def columns(c, j):
        return strip(c * blocks * LANES + block_of(j) * LANES, LANES)

    def is_last(j):
        return lax.rem(j, blocks) == blocks - 1

    def gives_down(j):
        return (j >= 0) & (j < steps) & ((parity(lax.rem(j, blocks)) == 1) | is_last(j))

    def down_of(j):
        return (j // blocks) * (pairs + 1) + lax.rem(j, blocks) // 2

    def for_down(j, act):
        @pl.when(gives_down(j) & ~is_last(j))
        def _():
            act(down_of(j), full)

        @pl.when(gives_down(j) & is_last(j))
        def _():
            act(down_of(j), small)

    def weight_copies(j):
        layer, slot = layer_of(j), parity(j)
        for c in range(chips):
            there, here = columns(c, j), lanes(c)
            yield pltpu.make_async_copy(wg_hbm.at[layer, :, there], wg_ref.at[slot, :, here], w_sem.at[slot, 3 * c])
            yield pltpu.make_async_copy(wu_hbm.at[layer, :, there], wu_ref.at[slot, :, here], w_sem.at[slot, 3 * c + 1])
            yield pltpu.make_async_copy(wd_hbm.at[layer, there, :], wd_ref.at[slot, here, :], w_sem.at[slot, 3 * c + 2])

    def load(src, buf, t, which):
        slot = parity(t)
        return pltpu.make_async_copy(src.at[strip(t * tile, tile), :], buf.at[slot], tile_sem.at[slot, which])

    def start_tile(j, t):
        load(a_hbm.at[layer_of(j)], a_tile, t, 0).start()

        @pl.when(layer_of(j) == layers - 1)
        def _():
            load(dy_hbm, dy_tile, t, 1).start()

        @pl.when(layer_of(j) < layers - 1)
        def _():
            load(dy0_hbm, dy_tile, t, 1).start()

    def wait_tile(t):
        load(dy_hbm, a_tile, t, 0).wait()
        load(dy_hbm, dy_tile, t, 1).wait()

    def gu_parts(n):
        for c in range(chips):
            for u in range(2):
                yield u * chips + c, u, pl.ds((u * chips + c) * rows, rows), columns(c, n)

    def gu_outs(n):
        for i, u, here, there in gu_parts(n):
            yield pltpu.make_async_copy(gu.sum.at[here, :], (gg_hbm, gu_hbm)[u].at[layer_of(n), :, there], gu.out_sem.at[i])

    def gu_state(n):
        layer = layer_of(n)
        for i, u, here, there in gu_parts(n):
            for k, (src, buf) in enumerate((((mg_hbm, mu_hbm)[u], m_ref), ((vg_hbm, vu_hbm)[u], v_ref))):
                yield pltpu.make_async_copy(src.at[layer, :, there], buf.at[here, :], state_sem.at[3 * i + k])
            src = (wg_hbm, wu_hbm)[u].at[layer, strip(me * rows, rows), there]
            yield pltpu.make_async_copy(src, w_ref.at[here, :], state_sem.at[3 * i + 2])

    def dn_parts(n, size):
        step = lax.rem(n, pairs + 1)
        start = step * LANES + core * (LANES // 2) if size == full else pairs * LANES * (1 - core)
        height = size // lane_blocks
        for b in range(lane_blocks):
            yield b, layers - 1 - n // (pairs + 1), start, height, pl.ds(b * height, height), lanes(b)

    def dn_outs(n, size):
        for b, layer, start, height, here, there in dn_parts(n, size):
            at = pl.ds(pl.multiple_of(start, LANES // 2), height)
            yield pltpu.make_async_copy(dn.sum.at[here, :], gd_hbm.at[layer, at, there], dn.out_sem.at[b])

    def own_out(pool, at, size, sem):
        return [pltpu.make_async_copy(pool.new.at[head(size)], own_hbm.at[pl.ds(pl.multiple_of(at, LANES // 2), size)], own_sem.at[sem])]

    def dn_own(n, size):
        return own_out(dn, (n - (layers - 1) * (pairs + 1)) * full, size, 0)

    def gu_own(n):
        return own_out(gu, pairs * full + small + (n - steps + LATE) * full, full, 1)

    def dn_state(n, size):
        for b, layer, start, height, here, there in dn_parts(n, size):
            at = pl.ds(pl.multiple_of(start, LANES // 2), height)
            for k, (src, buf) in enumerate(((md_hbm, m_ref), (vd_hbm, v_ref))):
                yield pltpu.make_async_copy(src.at[layer, at, there], buf.at[here, :], state_sem.at[3 * b + k])
            at = pl.ds(pl.multiple_of(me * (d // 2) + start, LANES // 2), height)
            yield pltpu.make_async_copy(wd_hbm.at[layer, at, there], w_ref.at[here, :], state_sem.at[3 * b + 2])

    some = d // 3

    def gu_new(n, size):
        gu.event3(n, size)
        pl.when(n > 0)(lambda: wait(gu_outs(n - 1)))
        wait(gu_state(n))
        late = n >= steps - LATE
        pl.when(n > steps - LATE)(lambda: wait(gu_own(n - 1)))

        def piece(i, _):
            at = strip(i * some, some)
            g = gu.total(n, i * some, some)
            gu.sum[at, :] = g.astype(BF16)
            gu.new[at, :] = adam(w_ref[at, :], m_ref[at, :], v_ref[at, :], g)
            return i

        lax.fori_loop(0, size // some, piece, 0)
        gu.after3(n)
        start(gu_outs(n))
        pl.when(~late)(lambda: gu.gather1(n, size))
        pl.when(late)(lambda: start(gu_own(n)))

    def dn_new(n, size):
        half, height = LANES // 2, size // lane_blocks
        dn.event3(n, size)
        if size == full:
            begins = lax.rem(n, pairs + 1) == 0
            pl.when((n > 0) & ~begins)(lambda: wait(dn_outs(n - 1, full)))
            pl.when((n > 0) & begins)(lambda: wait(dn_outs(n - 1, small)))
        else:
            wait(dn_outs(n - 1, full))
        wait(dn_state(n, size))
        upper = n < (layers - 1) * (pairs + 1)
        pl.when(n > (layers - 1) * (pairs + 1))(lambda: wait(dn_own(n - 1, full)))

        def finish(at, g):
            dn.sum[at, :] = g.astype(BF16)
            dn.new[at, :] = adam(w_ref[at, :], m_ref[at, :], v_ref[at, :], g)

        if size == full:

            def piece(i, _):
                for start in range(0, some, LANES):
                    finish(strip(i * some + start, LANES), dn.total(n, i * some + start, LANES).T)
                return i

            lax.fori_loop(0, size // some, piece, 0)
        else:
            g = dn.total(n, 0, size).T
            g = jnp.concatenate([g[:half], g[half:]], 1)
            for b in range(lane_blocks):
                finish(pl.ds(b * height, height), g[:, b * LANES : (b + 1) * LANES])
        dn.after3(n)
        start(dn_outs(n, size))
        pl.when(upper)(lambda: dn.gather1(n, size))
        pl.when(~upper)(lambda: start(dn_own(n, size)))

    def turn(buf, slot, into, part):
        for b in range(lane_blocks):
            into[lanes(b), part] = buf[slot, :, b * LANES : (b + 1) * LANES].T

    start_tile(0, 0)
    start(weight_copies(0))
    barrier = pltpu.get_barrier_semaphore()
    peers = (gu.partner(), gu.device(1), gu.device(-1))
    for peer in peers:
        pl.semaphore_signal(barrier, inc=1, device_id=peer, device_id_type=MESH)
    pl.semaphore_wait(barrier, len(peers))

    def keep(t):
        slot = parity(t)
        return pltpu.make_async_copy(dy_tile.at[slot], dy0_hbm.at[strip(t * tile, tile)], tile_sem.at[slot, 2])

    def compute_tile(j, t):
        slot, here = parity(j), parity(t)
        part = strip(t * tile, tile)
        wait_tile(t)
        pl.when(t + 1 < tiles)(lambda: start_tile(j, t + 1))
        a, dy = a_tile[here], dy_tile[here]
        for c in range(0, chips, 2):
            some = pl.ds(c * LANES, 2 * LANES)
            gate = dot(a, wg_ref[slot, :, some])
            up = dot(a, wu_ref[slot, :, some])
            dz = dot(dy, wd_ref[slot, some, :], NT).astype(BF16).astype(F32)
            s = jax.nn.sigmoid(gate)
            act = s * gate
            z_ref[part, some] = (act * up).astype(BF16)
            dgu_ref[1, part, some] = (dz * act).astype(BF16)
            dgu_ref[0, part, some] = (dz * up * (s + act * (1 - s))).astype(BF16)

        @pl.when(j == 0)
        def _():
            turn(a_tile, here, at_ref, part)
            turn(dy_tile, here, dyt_ref, part)
            da_ref[part, :] = jnp.zeros((tile, d), F32)

    def compute_gate_up(j, u):
        slot = lax.rem(j, gu.slots)
        g = dot(at_ref[...], dgu_ref[u]).astype(BF16)
        for c in range(chips):
            at = strip((u * chips + c) * rows, rows)
            for owner in range(CORES * chips):
                gu.mine[slot, owner % CORES, owner // CORES, at, :] = g[owner * rows : (owner + 1) * rows, c * LANES : (c + 1) * LANES]

    def compute_down(j, h):
        slot = lax.rem(down_of(j), dn.slots)
        owner = parity(lax.rem(j, blocks))
        chips_here = [2 * h, 2 * h + 1]
        z = strip(chips_here[0] * LANES, 2 * LANES)

        @pl.when(~is_last(j))
        def _():
            g = dot(dyt_ref[...], z_ref[:, z]).astype(BF16)
            for c, at in enumerate(chips_here):
                dn.mine[slot, owner, at, :, :] = g[:, c * LANES : (c + 1) * LANES]

        @pl.when(is_last(j))
        def _():
            g = dot(dyt_ref[...], z_ref[:, z])
            half = LANES // 2
            low = lax.broadcasted_iota(jnp.int32, (small, LANES), 1) < half
            for c, at in enumerate(chips_here):
                both = g[:, c * LANES : (c + 1) * LANES]
                turned = pltpu.roll(both, half, 1)
                dn.mine[slot, 0, at, head(small), :] = jnp.where(low, both[:small], turned[small:]).astype(BF16)
                dn.mine[slot, 1, at, head(small), :] = jnp.where(low, turned[:small], both[small:]).astype(BF16)

    def compute_da(j, t):
        slot, part = parity(j), strip(t * tile, tile)
        da_ref[part, :] += dot(dgu_ref[0, part, :], wg_ref[slot], NT) + dot(dgu_ref[1, part, :], wu_ref[slot], NT)

    def begin_change(t):
        load(h_hbm, a_tile, t, 0).start()
        load(dy_hbm, dy_tile, t, 1).start()

    def change_layer():
        def one(t, _):
            slot = parity(t)
            wait_tile(t)
            pl.when(t > 0)(lambda: keep(t - 1).wait())
            pl.when(t + 1 < tiles)(lambda: begin_change(t + 1))
            pl.when(t + 1 == tiles)(lambda: start_tile(blocks, 0))

            def piece(i, _):
                here, there = strip(i * small_tile, small_tile), strip(t * tile + i * small_tile, small_tile)
                wide = a_tile[slot, here, :].astype(F32)
                da = da_ref[there, :].astype(BF16).astype(F32)
                scale = lax.rsqrt(jnp.mean(wide * wide, -1, keepdims=True) + 1e-6)
                along = jnp.mean(da * wide, -1, keepdims=True)
                back = (da * scale - wide * (along * scale * scale * scale)).astype(BF16)
                dy_tile[slot, here, :] = dy_tile[slot, here, :] + back
                return 0

            lax.fori_loop(0, tile // small_tile, piece, 0)
            keep(t).start()
            turn(dy_tile, slot, dyt_ref, strip(t * tile, tile))
            return 0

        lax.fori_loop(0, tiles, one, 0)
        keep(tiles - 1).wait()

    def on(j, act):
        pl.when((j >= 0) & (j < steps))(lambda: act(j, full))

    def early(j, act):
        pl.when(j < steps - LATE)(lambda: on(j, act))

    def upper_down(j, act):
        pl.when(j < (layers - 1) * blocks)(lambda: for_down(j, act))

    def gu_load(n, rows):
        start(gu_state(n))

    def dn_load(n, rows):
        start(dn_state(n, rows))

    events = {
        "tile1": [(for_down, dn_new, 2)],
        "tile2": [(on, gu.event2, 1)],
        "tile3": [(upper_down, dn.gather3, 3), (for_down, dn.event2, 1)],
        "gate0": [(on, gu_load, 1)],
        "gate1": [(on, gu.event0), (early, gu.gather3, 3)],
        "down0": [(upper_down, dn.gather2, 2)],
        "down1": [(for_down, dn.event0), (upper_down, dn.gather4, 3), (on, gu.event1)],
        "back0": [(early, gu.gather4, 3)],
        "back1": [(early, gu.gather2, 2), (for_down, dn.event1)],
        "back2": [(on, gu_new, 1)],
        "back3": [(for_down, dn_load, 1)],
    }
    longest = max(sum(ago) for these in events.values() for _, _, *ago in these)

    def step(j, _):
        busy = j < steps
        lower = layer_of(j) > 0
        changes = is_last(j) & lower & busy

        @pl.when(busy)
        def _():
            wait(weight_copies(j))
            pl.when(j + 1 < steps)(lambda: start(weight_copies(j + 1)))

        def parts(name, number, active, compute):
            def one(t, _):
                pl.when(active)(lambda: compute(j, t))
                for at in range(number):

                    @pl.when(t == at)
                    def _():
                        for stream, act, *ago in events.get(f"{name}{at}", ()):
                            stream(j - sum(ago), act)

                return 0

            lax.fori_loop(0, number, one, 0)

        def da_tile(j, t):
            fetch = load(a_hbm.at[0], a_tile, t, 0)
            pl.when(changes)(fetch.start)
            pl.when(changes & (t + 1 == tiles))(lambda: begin_change(0))
            compute_da(j, t)

            @pl.when(changes)
            def _():
                fetch.wait()
                turn(a_tile, parity(t), at_ref, strip(t * tile, tile))

        parts("tile", tiles, busy, compute_tile)
        pl.when(busy & (j + 1 < steps) & ~changes)(lambda: start_tile(j + 1, 0))
        parts("gate", 2, busy, compute_gate_up)
        parts("down", chips // 2, busy, compute_down)
        parts("back", tiles, busy & lower, da_tile)

        pl.when(changes)(change_layer)

        return 0

    lax.fori_loop(0, steps + longest, step, 0)
    wait(gu_outs(steps - 1))
    wait(dn_outs(dn.number - 1, small))
    wait(dn_own(dn.number - 1, small))
    wait(gu_own(steps - 1))


def backward(mesh, a, h, dy, weights, m, v, tile=512):
    tokens, d = dy.shape
    layers, _, ff = weights[0].shape
    chips = mesh.shape["dp"] // CORES
    width = chips * LANES
    blocks = ff // width
    pairs = blocks // 2
    rows = d // (CORES * chips)
    assert layers == 2 and chips == 4 and blocks % 2 == 1 and blocks * width == ff and d % LANES == 0
    shape = lambda *s: jax.ShapeDtypeStruct(s, BF16)
    devices = CORES * chips
    outs = [
        shape(layers, rows, ff),
        shape(layers, rows, ff),
        shape(layers, ff // devices, d),
        shape(layers * blocks, devices, d, LANES),
        shape((layers - 1) * (pairs + 1), devices, d, LANES),
        shape(pairs * d + d // 2 + LATE * d, LANES),
        shape(tokens, d),
    ]

    def pool(lanes, outputs):
        return [
            pltpu.VMEM((2, CORES, chips, d, LANES), BF16),
            pltpu.VMEM((2, chips, d, LANES), BF16),
            pltpu.VMEM((lanes, 2, d // 2, LANES), BF16),
            pltpu.VMEM((lanes, 2, d, LANES), BF16),
            pltpu.VMEM((lanes, 2, d // 2, LANES), BF16),
            pltpu.VMEM((lanes, 2, d, LANES), BF16),
            pltpu.VMEM((d, LANES), BF16),
            pltpu.VMEM((d, LANES), BF16),
            pltpu.SemaphoreType.DMA((2, 5, 2)),
            pltpu.SemaphoreType.REGULAR((5,)),
            pltpu.SemaphoreType.DMA((outputs,)),
            pltpu.SemaphoreType.DMA((4, 8, 2)),
            pltpu.SemaphoreType.DMA,
        ]

    return pl.pallas_call(
        functools.partial(backward_kernel, chips, tile),
        out_shape=outs,
        in_specs=[ANY] * 12,
        out_specs=[ANY] * len(outs),
        scratch_shapes=[
            pltpu.VMEM((2, tile, d), BF16),
            pltpu.VMEM((2, tile, d), BF16),
            pltpu.VMEM((d, tokens), BF16),
            pltpu.VMEM((d, tokens), BF16),
            pltpu.VMEM((tokens, d), F32),
            pltpu.VMEM((2, d, width), BF16),
            pltpu.VMEM((2, d, width), BF16),
            pltpu.VMEM((2, width, d), BF16),
            pltpu.VMEM((tokens, width), BF16),
            pltpu.VMEM((2, tokens, width), BF16),
            pltpu.VMEM((d, LANES), F32),
            pltpu.VMEM((d, LANES), F32),
            pltpu.VMEM((d, LANES), BF16),
            pltpu.SemaphoreType.DMA((2, 3)),
            pltpu.SemaphoreType.DMA((2, 3 * chips)),
            pltpu.SemaphoreType.DMA((max(6 * chips, 3 * (d // LANES)),)),
            pltpu.SemaphoreType.DMA((2,)),
            *pool(1, 2 * chips),
            *pool(2, d // LANES),
        ],
        compiler_params=pltpu.CompilerParams(collective_id=1, has_side_effects=True, vmem_limit_bytes=VMEM_BYTES),
        cost_estimate=cost(28 * tokens * d * ff, 24 * d * ff),
        name="backward",
    )(a, h, dy, *weights, *m, *v)


class Ring:
    def __init__(self, units, slots, loads, stores, work):
        self.units, self.slots, self.loads, self.stores, self.work = units, slots, loads, stores, work

    def begin(self):
        for unit in range(self.slots):
            for copy in self.loads(unit, unit):
                copy.start()

    def run(self):
        def one(unit, _):
            slot = lax.rem(unit, self.slots)
            for copy in self.loads(unit, slot):
                copy.wait()

            @pl.when(unit >= self.slots)
            def _():
                for copy in self.stores(unit - self.slots, slot):
                    copy.wait()

            self.work(unit, slot)
            for copy in self.stores(unit, slot):
                copy.start()

            @pl.when(unit + self.slots < self.units)
            def _():
                for copy in self.loads(unit + self.slots, slot):
                    copy.start()

            return 0

        lax.fori_loop(0, self.units, one, 0)

    def end(self):
        for unit in range(self.units - self.slots, self.units):
            for copy in self.stores(unit, unit % self.slots):
                copy.wait()


def place_columns_kernel(layer, slots, x_hbm, *refs):
    gate_hbm, up_hbm, c_in, c_out, sem = refs[-5:]
    _, blocks, devices, _, chips, rows, _ = x_hbm.shape
    wide, some = blocks * LANES, c_in.shape[2]
    turns = devices // some

    def place(unit):
        return unit // turns, lax.rem(unit, turns) * some

    def loads(unit, slot):
        chip, owners = place(unit)
        return [pltpu.make_async_copy(x_hbm.at[x_hbm.shape[0] - 1 - layer, :, pl.ds(owners, some), :, chip], c_in.at[slot], sem.at[slot, 0])]

    def stores(unit, slot):
        chip, owners = place(unit)
        at = layer, strip(owners * rows, some * rows), strip(chip * wide, wide)
        return [pltpu.make_async_copy(c_out.at[slot, u], out.at[at], sem.at[slot, 1 + u]) for u, out in enumerate((gate_hbm, up_hbm))]

    def work(unit, slot):
        for j in range(blocks):
            at = pl.ds((j // 2 + (blocks // 2 + 1) * (j % 2)) * LANES, LANES)
            for owner in range(some):
                for u in range(2):
                    c_out[slot, u, pl.ds(owner * rows, rows), at] = c_in[slot, j, owner, u]

    ring = Ring(chips * turns, slots, loads, stores, work)
    ring.begin()
    ring.run()
    ring.end()


def place_columns(chunks, layer, layers, d, ff, into=(), slots=4, some=2):
    devices = chunks.shape[1]
    chips, rows = devices // CORES, d // devices
    x = chunks.reshape(layers, -1, devices, 2, chips, rows, LANES)
    return pl.pallas_call(
        functools.partial(place_columns_kernel, layer, slots),
        in_specs=[ANY] * (1 + len(into)),
        out_specs=[ANY] * 2,
        input_output_aliases={1 + i: i for i in range(len(into))},
        out_shape=[jax.ShapeDtypeStruct((layers, d, ff), BF16)] * 2,
        scratch_shapes=[
            pltpu.VMEM((slots, x.shape[1], some, 2, rows, LANES), BF16),
            pltpu.VMEM((slots, 2, some * rows, ff // chips), BF16),
            pltpu.SemaphoreType.DMA((slots, 3)),
        ],
        compiler_params=pltpu.CompilerParams(vmem_limit_bytes=VMEM_BYTES),
        cost_estimate=cost(COPY_FLOPS * 8 * d * ff, 8 * d * ff),
        name="place_columns",
    )(x, *into)


def moments_kernel(layers, parts, slots, *refs):
    states, news, s_in, g_in, s_out, sem = refs[:9], refs[9:15], refs[15:18], refs[18:21], refs[21:24], refs[24]

    def at(i, unit):
        layer, part = unit // parts, lax.rem(unit, parts)
        _, r, c = states[i].shape
        return (layer, strip(part * (r // parts), r // parts), slice(None)) if i == 2 else (layer, slice(None), strip(part * (c // parts), c // parts))

    def loads(unit, slot):
        copies = []
        for i in range(3):
            for k in range(2):
                copies.append(pltpu.make_async_copy(states[3 * k + i].at[at(i, unit)], s_in[i].at[slot, k], sem.at[slot, 5 * i + k]))
            copies.append(pltpu.make_async_copy(states[6 + i].at[at(i, unit)], g_in[i].at[slot], sem.at[slot, 5 * i + 2]))
        return copies

    def stores(unit, slot):
        return [
            pltpu.make_async_copy(s_out[i].at[slot, k], news[3 * k + i].at[at(i, unit)], sem.at[slot, 5 * i + 3 + k]) for i in range(3) for k in range(2)
        ]

    def work(unit, slot):
        for i in range(3):
            g = g_in[i][slot].astype(F32)
            s_out[i][slot, 0], s_out[i][slot, 1] = moment(s_in[i][slot, 0], s_in[i][slot, 1], g)

    ring = Ring(layers * parts, slots, loads, stores, work)
    ring.begin()
    ring.run()
    ring.end()


def moments(m, v, g, parts=9, slots=4):
    layers = m[0].shape[0]
    shapes = [(one.shape[1], one.shape[2] // parts) for one in m[:2]] + [(m[2].shape[1] // parts, m[2].shape[2])]
    size = sum(one.size for one in m)
    return pl.pallas_call(
        functools.partial(moments_kernel, layers, parts, slots),
        in_specs=[ANY] * 9,
        out_specs=[ANY] * 6,
        out_shape=[jax.ShapeDtypeStruct(one.shape, F32) for one in m] * 2,
        scratch_shapes=[
            *(pltpu.VMEM((slots, 2, *shape), F32) for shape in shapes),
            *(pltpu.VMEM((slots, *shape), BF16) for shape in shapes),
            *(pltpu.VMEM((slots, 2, *shape), F32) for shape in shapes),
            pltpu.SemaphoreType.DMA((slots, 15)),
        ],
        compiler_params=pltpu.CompilerParams(vmem_limit_bytes=VMEM_BYTES),
        cost_estimate=cost(COPY_FLOPS * 18 * size, 18 * size),
        name="moments",
    )(*m, *v, *g)


def unfold(chunks, out, core):
    pairs, half = chunks.shape[0] - 1, LANES // 2
    for b in range(out.shape[1] // LANES):
        for n in range(pairs):
            out[pl.ds(pl.multiple_of(n * LANES + core * half, half), LANES), lanes(b)] = chunks[n, lanes(b), :]
        out[pl.ds(pl.multiple_of(pairs * LANES * (1 - core), half), half), lanes(b)] = chunks[pairs, pl.ds(b * half, half), :]


def place_rows_kernel(layers, slots, x_hbm, down_hbm, r_in, r_out, sem):
    devices = x_hbm.shape[2]
    pairs = x_hbm.shape[1] - 1
    height, d = r_out.shape[1:]

    def loads(unit, slot):
        layer, device = layers - 2 - unit // devices, lax.rem(unit, devices)
        return [
            pltpu.make_async_copy(x_hbm.at[layer, head(pairs), device], r_in.at[slot, head(pairs)], sem.at[slot, 0]),
            pltpu.make_async_copy(x_hbm.at[layer, pairs, device, head(d // 2)], r_in.at[slot, pairs, head(d // 2)], sem.at[slot, 1]),
        ]

    def stores(unit, slot):
        layer, device = unit // devices + 1, lax.rem(unit, devices)
        return [pltpu.make_async_copy(r_out.at[slot], down_hbm.at[layer, strip(device * height, height)], sem.at[slot, 2])]

    def work(unit, slot):
        unfold(r_in.at[slot], r_out.at[slot], lax.rem(unit, CORES))

    ring = Ring((layers - 1) * devices, slots, loads, stores, work)
    ring.begin()
    ring.run()
    ring.end()


def place_rows(chunks, layers, d, ff, slots=4):
    devices = chunks.shape[1]
    x = chunks.reshape(layers - 1, -1, devices, d, LANES)
    height = ff // devices
    return pl.pallas_call(
        functools.partial(place_rows_kernel, layers, slots),
        in_specs=[ANY],
        out_specs=ANY,
        out_shape=jax.ShapeDtypeStruct((layers, ff, d), BF16),
        scratch_shapes=[
            pltpu.VMEM((slots, x.shape[1], d, LANES), BF16),
            pltpu.VMEM((slots, height, d), BF16),
            pltpu.SemaphoreType.DMA((slots, 3)),
        ],
        compiler_params=pltpu.CompilerParams(vmem_limit_bytes=VMEM_BYTES),
        cost_estimate=cost(COPY_FLOPS * 4 * d * ff, 4 * d * ff),
        name="place_rows",
    )(x)


def place_blocks_kernel(wheres, me_ref, *refs):
    blocks, (gate_hbm, up_hbm, down_hbm, held, down, sem) = refs[: len(wheres)], refs[-6:]
    layers, d, ff = gate_hbm.shape
    height = down.shape[1]
    devices = ff // height
    chips, rows = devices // CORES, d // devices
    wide = ff // chips
    pairs = wide // LANES // 2
    chip, core = me_ref[0] // CORES, lax.rem(me_ref[0], CORES)

    def fetch(i):
        return pltpu.make_async_copy(blocks[i], held.at[i], sem.at[i, 0])

    def put(i):
        hops, flip = wheres[i]
        side = 1 - core if flip else core
        owner = lax.rem(chip + hops + chips, chips) * CORES + side
        copies = [pltpu.make_async_copy(down.at[i], down_hbm.at[0, strip(owner * height, height)], sem.at[i, 1])]
        for n in range(LATE):
            step = 2 * pairs + 1 - LATE + n
            column = (step // 2 + (pairs + 1) * (step % 2)) * LANES
            for u, out in enumerate((gate_hbm, up_hbm)):
                for c in range(chips):
                    here = pl.ds(pairs * d + d // 2 + n * d + (u * chips + c) * rows, rows)
                    to = out.at[0, strip(owner * rows, rows), pl.ds(c * wide + column, LANES)]
                    copies.append(pltpu.make_async_copy(held.at[i, here], to, sem.at[i, 1 + len(copies)]))
        return side, copies

    number = len(wheres)
    for i in range(number):
        fetch(i).start()
    for i in range(number):
        fetch(i).wait()
        side, copies = put(i)
        start(copies[1:])
        for n in range(pairs + 1):
            size_n = d if n < pairs else d // 2
            for b in range(d // LANES):
                part = size_n // (d // LANES)
                at = n * LANES + side * (LANES // 2) if n < pairs else pairs * LANES * (1 - side)
                down[i, pl.ds(pl.multiple_of(at, LANES // 2), part), lanes(b)] = held[i, pl.ds(n * d + b * part, part), :]
        copies[0].start()
    for i in range(number):
        wait(put(i)[1])


def place_blocks(me, blocks, weights):
    wheres, blocks = tuple(blocks), list(blocks.values())
    number, rows = len(blocks), blocks[0].shape[0]
    layers, ff, d = weights[2].shape
    height = rows * LANES // d - LATE * LANES
    return pl.pallas_call(
        functools.partial(place_blocks_kernel, wheres),
        in_specs=[pl.BlockSpec(memory_space=pltpu.SMEM)] + [ANY] * (number + 3),
        out_specs=[ANY] * 3,
        out_shape=[jax.ShapeDtypeStruct(one.shape, BF16) for one in weights],
        input_output_aliases={number + 1 + i: i for i in range(3)},
        scratch_shapes=[
            pltpu.VMEM((number, rows, LANES), BF16),
            pltpu.VMEM((number, height, d), BF16),
            pltpu.SemaphoreType.DMA((number, 2 + LATE * ff // height)),
        ],
        compiler_params=pltpu.CompilerParams(vmem_limit_bytes=VMEM_BYTES),
        cost_estimate=cost(COPY_FLOPS * 4 * number * rows * LANES, 4 * number * rows * LANES),
        name="place_blocks",
    )(me, *blocks, *weights)


def solution(mesh):
    group = mesh.shape["dp"]
    swap = [(i, i ^ 1) for i in range(group)]
    right = [(i, (i + CORES) % group) for i in range(group)]
    left = [(i, (i - CORES) % group) for i in range(group)]

    def step(x, dy, *arrays):
        weights, m, v = (arrays[i : i + 3] for i in (0, 3, 6))
        layers, d, ff = weights[0].shape
        me = lax.axis_index("dp").reshape(1)
        *sums, columns, rows, own, _ = backward(mesh, *forward(x[0], *weights, 0), dy[0], weights, m, v)

        def send(block, to):
            return lax.ppermute(block, "dp", to)

        from_left, from_right = send(own, right), send(own, left)
        gate, up = place_columns(columns, 1, layers, d, ff)
        first, *states = moments(m, v, sums)
        gate, first, from_left, from_right = lax.optimization_barrier((gate, first, from_left, from_right))
        opposite = send(jnp.where(lax.rem(lax.axis_index("dp"), CORES) == 0, from_left, from_right), [(right, left)[i % CORES][i] for i in range(group)])
        near = {(0, 0): own, (-1, 0): from_left, (1, 0): from_right}
        other = {(hops, 1): send(block, swap) for (hops, _), block in near.items()}
        gate, up = place_columns(columns, 0, layers, d, ff, (gate, up))
        up, rows = lax.optimization_barrier((up, rows))
        down = place_rows(rows, layers, d, ff)
        down, opposite = lax.optimization_barrier((down, opposite))
        last = send(opposite, swap)
        weights = place_blocks(me, {**near, **other}, (gate, up, down))
        weights = place_blocks(me, {(2, 0): opposite, (2, 1): last}, weights)
        return (*weights, first, *states)

    seq, whole, rows = P(("rep", "dp"), None, None), P(None, None, None), P(None, "dp", None)
    return jax.shard_map(
        step,
        mesh=mesh,
        in_specs=(seq, seq, whole, whole, whole) + (rows,) * 6,
        out_specs=(P("rep", None, None),) * 3 + (P("rep", "dp", None),) * 6,
        check_vma=False,
    )
```

```python
import functools

import jax
import jax.numpy as jnp
from jax import lax
from jax.experimental import pallas as pl
from jax.experimental.pallas import tpu as pltpu
from jax.sharding import PartitionSpec as P

F32, BF16 = jnp.float32, jnp.bfloat16
NN, NT = (((1,), (0,)), ((), ())), (((1,), (1,)), ((), ()))
MESH = pl.DeviceIdType.MESH
ANY = pl.BlockSpec(memory_space=pl.ANY)
LANES = 128
CORES = 2
VMEM_BYTES = 67_043_328
COPY_FLOPS = 64
LATE = 2
SIDES = (0, 1), (1, -1)


def dot(a, b, dims=NN):
    return lax.dot_general(a, b, dims, preferred_element_type=F32)


def norm(h):
    wide = h.astype(F32)
    return (wide * lax.rsqrt(jnp.mean(wide**2, -1, keepdims=True) + 1e-6)).astype(BF16)


def strip(start, size):
    return pl.ds(pl.multiple_of(start, size), size)


def head(size):
    return pl.ds(0, size)


def parity(n):
    return lax.rem(n, 2)


def lanes(n):
    return pl.ds(n * LANES, LANES)


def start(copies):
    for copy in copies:
        copy.start()


def wait(copies):
    for copy in copies:
        copy.wait()


def moves(moved):
    return cost(COPY_FLOPS * moved, moved)


def cost(flops, moved):
    return pl.CostEstimate(flops=flops, bytes_accessed=moved, transcendentals=moved)


def forward_kernel(tile, x_ref, wg_ref, wu_ref, wd_ref, a_hbm, h_hbm, a_ref, total, ends, a_sem, end_sem):
    block = pl.program_id(0)
    first, last = block == 0, block == pl.num_programs(0) - 1
    tiles = x_ref.shape[0] // tile

    def keep(t):
        rows = strip(t * tile, tile)
        return pltpu.make_async_copy(a_ref.at[rows], a_hbm.at[0, rows], a_sem.at[t])

    def finish(t):
        rows = strip(t * tile, tile)
        for i, out in enumerate((h_hbm, a_hbm.at[1])):
            yield pltpu.make_async_copy(ends.at[parity(t), i], out.at[rows], end_sem.at[parity(t), i])

    @pl.when(first)
    def _():
        def begin(t, _):
            rows = strip(t * tile, tile)
            a_ref[rows, :] = norm(x_ref[rows, :])
            total[rows, :] = jnp.zeros((tile, total.shape[1]), F32)
            keep(t).start()
            return t

        lax.fori_loop(0, tiles, begin, 0)

    def one(t, _):
        rows = strip(t * tile, tile)
        a = a_ref[rows, :]
        gate, up = dot(a, wg_ref[...]), dot(a, wu_ref[...])
        z = (jax.nn.sigmoid(gate) * gate * up).astype(BF16)
        total[rows, :] += dot(z, wd_ref[...])

        @pl.when(last)
        def _():
            keep(t).wait()
            pl.when(t >= 2)(lambda: wait(finish(t - 2)))
            h = x_ref[rows, :] + total[rows, :].astype(BF16)
            for i, end in enumerate((h, norm(h))):
                ends[parity(t), i] = end
            start(finish(t))

        return t

    lax.fori_loop(0, tiles, one, 0)

    @pl.when(last)
    def _():
        for t in range(tiles - 2, tiles):
            wait(finish(t))


def forward(x, wg, wu, wd, layer, width=768, tile=512):
    tokens, d = x.shape
    ff = wg.shape[2]
    state = jax.ShapeDtypeStruct((tokens, d), BF16)
    columns = pl.BlockSpec((None, d, width), lambda i: (layer, 0, i))
    return pl.pallas_call(
        functools.partial(forward_kernel, tile),
        grid=(ff // width,),
        out_shape=[jax.ShapeDtypeStruct((2, tokens, d), BF16), state],
        in_specs=[pl.BlockSpec(x.shape, lambda i: (0, 0)), columns, columns, pl.BlockSpec((None, width, d), lambda i: (layer, i, 0))],
        out_specs=[ANY] * 2,
        scratch_shapes=[
            pltpu.VMEM(x.shape, BF16),
            pltpu.VMEM(x.shape, F32),
            pltpu.VMEM((2, 2, tile, d), BF16),
            pltpu.SemaphoreType.DMA((tokens // tile,)),
            pltpu.SemaphoreType.DMA((2, 2)),
        ],
        compiler_params=pltpu.CompilerParams(vmem_limit_bytes=VMEM_BYTES),
        cost_estimate=cost(6 * tokens * d * ff, 6 * d * ff),
        name="forward",
    )(x, wg, wu, wd)


class Pool:
    def __init__(self, number, chips, core, chip, bufs, sems, gathered):
        self.number, self.chips, self.core, self.chip = number, chips, core, chip
        self.mine, self.other, self.cross, self.near, self.out1, self.out2, self.sum, self.new = bufs
        self.dma, self.credit, self.out_sem, self.ag_sem, self.own_sem = sems
        self.gathered = gathered
        self.slots, self.lanes, self.turns = self.mine.shape[0], self.cross.shape[0], self.ag_sem.shape[0]

    def index(self, chip, core):
        return lax.rem(chip + self.chips, self.chips) * CORES + core

    def device(self, hops, core=None):
        return {"dp": self.index(self.chip + hops, self.core if core is None else core)}

    def partner(self):
        return self.device(0, 1 - self.core)

    def hop(self, sems, src, dst, to):
        return pltpu.make_async_remote_copy(src_ref=src, dst_ref=dst, send_sem=sems.at[0], recv_sem=sems.at[1], device_id=to, device_id_type=MESH)

    def copies0(self, n, rows):
        slot = lax.rem(n, self.slots)
        src = self.mine.at[slot, 1 - self.core, :, head(rows), :]
        return [self.hop(self.dma.at[slot, 0], src, self.other.at[slot, :, head(rows), :], self.partner())]

    def copies1(self, n, rows):
        slot, sem, half = lax.rem(n, self.lanes), lax.rem(n, self.slots), head(rows // 2)
        return [self.hop(self.dma.at[sem, 1 + side], self.out1.at[slot, side, half], self.cross.at[slot, side, half], self.device(hop)) for side, hop in SIDES]

    def copies2(self, n, rows):
        slot, sem, full = lax.rem(n, self.lanes), lax.rem(n, self.slots), head(rows)
        return [self.hop(self.dma.at[sem, 3 + side], self.out2.at[slot, side, full], self.near.at[slot, side, full], self.device(hop)) for side, hop in SIDES]

    def both(self, n, hops, start, size):
        slot, chip = lax.rem(n, self.slots), lax.rem(self.chip + hops + self.chips, self.chips)
        rows = pl.ds(start, size)
        return self.mine[slot, self.core, chip, rows, :].astype(F32) + self.other[slot, chip, rows, :].astype(F32)

    def give(self, kind, to):
        pl.semaphore_signal(self.credit.at[kind], inc=1, device_id=to, device_id_type=MESH)

    def take(self, when, kinds):
        @pl.when(when)
        def _():
            for kind in kinds:
                pl.semaphore_wait(self.credit.at[kind], 1)

    def event0(self, n, rows):
        self.take(n >= self.slots, (0,))
        start(self.copies0(n, rows))

    def event1(self, n, rows):
        slot, half = lax.rem(n, self.lanes), rows // 2
        wait(self.copies0(n, rows))
        for side, _ in SIDES:
            self.out1[slot, side, head(half)] = self.both(n, 2, side * half, half).astype(BF16)
        self.take(n >= self.lanes, (1, 2))
        start(self.copies1(n, rows))

    def event2(self, n, rows):
        slot, half = lax.rem(n, self.lanes), rows // 2
        wait(self.copies1(n, rows))
        for side, hop in SIDES:
            passed = self.both(n, hop, side * half, half) + self.cross[slot, side, head(half)].astype(F32)
            self.out2[slot, side, pl.ds(side * half, half), :] = passed.astype(BF16)
            self.out2[slot, side, pl.ds(half - side * half, half), :] = self.both(n, hop, half - side * half, half).astype(BF16)

        @pl.when(n + self.lanes < self.number)
        def _():
            for side, hop in SIDES:
                self.give(1 + side, self.device(-hop))

        self.take(n >= self.lanes, (3, 4))
        start(self.copies2(n, rows))

    def total(self, n, start, size):
        total = self.both(n, 0, start, size)
        for side, _ in SIDES:
            total += self.near[lax.rem(n, self.lanes), side, pl.ds(start, size), :].astype(F32)
        return total.astype(BF16).astype(F32)

    def event3(self, n, rows):
        wait(self.copies2(n, rows))

    def after3(self, n):
        pl.when(n + self.slots < self.number)(lambda: self.give(0, self.partner()))

        @pl.when(n + self.lanes < self.number)
        def _():
            for side, hop in SIDES:
                self.give(3 + side, self.device(-hop))

    def block(self, n, hops, core, start, size):
        return self.gathered.at[n, self.index(self.chip + hops, core), pl.ds(start, size), :]

    def sems(self, n, kind):
        return self.ag_sem.at[lax.rem(n, self.turns), kind]

    def gathers1(self, n, rows):
        new, own = self.new.at[head(rows)], self.block(n, 0, self.core, 0, rows)
        copies = [self.hop(self.sems(n, side), new, own, self.device(hop)) for side, hop in SIDES]
        return [*copies, self.hop(self.sems(n, 7), new, own, self.partner()), pltpu.make_async_copy(new, own, self.own_sem)]

    def gathers2(self, n, rows):
        copies, half = [], rows // 2
        for side, hop in SIDES:
            part, full = (self.block(n, -hop, self.core, *which) for which in ((side * half, half), (0, rows)))
            copies.append(self.hop(self.sems(n, 2 + side), part, part, self.device(hop)))
            copies.append(self.hop(self.sems(n, 4 + side), full, full, self.partner()))
        return copies

    def gathers3(self, n, rows):
        opposite = self.block(n, 2, self.core, 0, rows)
        return [self.hop(self.sems(n, 6), opposite, opposite, self.partner())]

    def gather1(self, n, rows):
        start(self.gathers1(n, rows))

    def gather2(self, n, rows):
        wait(self.gathers1(n, rows))
        start(self.gathers2(n, rows))

    def gather3(self, n, rows):
        wait(self.gathers2(n, rows))
        start(self.gathers3(n, rows))

    def gather4(self, n, rows):
        wait(self.gathers3(n, rows))


def moment(m, v, g):
    return 0.9 * m + 0.1 * g, 0.95 * v + 0.05 * g * g


def adam(w, m, v, g):
    m, v = moment(m, v, g)
    w = w.astype(F32)
    return (w - 0.02 * (m * lax.rsqrt(v + 1e-8) + 0.1 * w)).astype(BF16)


def backward_kernel(chips, tile, *refs):
    a_hbm, h_hbm, dy_hbm, wg_hbm, wu_hbm, wd_hbm, mg_hbm, mu_hbm, md_hbm, vg_hbm, vu_hbm, vd_hbm, *refs = refs
    gg_hbm, gu_hbm, gd_hbm, whole_gu, whole_dn, own_hbm, dy0_hbm, *refs = refs
    a_tile, dy_tile, at_ref, dyt_ref, da_ref, wg_ref, wu_ref, wd_ref, z_ref, dgu_ref, m_ref, v_ref, w_ref, *refs = refs
    tile_sem, w_sem, state_sem, own_sem, *pools = refs
    tokens, d = dy_hbm.shape
    layers, _, ff = wg_hbm.shape
    width = chips * LANES
    blocks = ff // width
    pairs = blocks // 2
    rows = d // (CORES * chips)
    lane_blocks = d // LANES
    me = lax.axis_index("dp")
    chip, core = me // CORES, lax.rem(me, CORES)
    tiles = tokens // tile
    steps = layers * blocks
    full, small, small_tile = d, d // 2, tile // 4

    gu = Pool(steps, chips, core, chip, pools[0:8], pools[8:13], whole_gu)
    dn = Pool(layers * (pairs + 1), chips, core, chip, pools[13:21], pools[21:26], whole_dn)

    def layer_of(j):
        return layers - 1 - j // blocks

    def block_of(j):
        j = lax.rem(j, blocks)
        return j // 2 + (pairs + 1) * parity(j)

    def columns(c, j):
        return strip(c * blocks * LANES + block_of(j) * LANES, LANES)

    def is_last(j):
        return lax.rem(j, blocks) == blocks - 1

    def gives_down(j):
        return (j >= 0) & (j < steps) & ((parity(lax.rem(j, blocks)) == 1) | is_last(j))

    def down_of(j):
        return (j // blocks) * (pairs + 1) + lax.rem(j, blocks) // 2

    def for_down(j, act):
        @pl.when(gives_down(j) & ~is_last(j))
        def _():
            act(down_of(j), full)

        @pl.when(gives_down(j) & is_last(j))
        def _():
            act(down_of(j), small)

    def weight_copies(j):
        layer, slot = layer_of(j), parity(j)
        for c in range(chips):
            there, here = columns(c, j), lanes(c)
            yield pltpu.make_async_copy(wg_hbm.at[layer, :, there], wg_ref.at[slot, :, here], w_sem.at[slot, 3 * c])
            yield pltpu.make_async_copy(wu_hbm.at[layer, :, there], wu_ref.at[slot, :, here], w_sem.at[slot, 3 * c + 1])
            yield pltpu.make_async_copy(wd_hbm.at[layer, there, :], wd_ref.at[slot, here, :], w_sem.at[slot, 3 * c + 2])

    def load(src, buf, t, which):
        slot = parity(t)
        return pltpu.make_async_copy(src.at[strip(t * tile, tile), :], buf.at[slot], tile_sem.at[slot, which])

    def start_tile(j, t):
        load(a_hbm.at[layer_of(j)], a_tile, t, 0).start()

        @pl.when(layer_of(j) == layers - 1)
        def _():
            load(dy_hbm, dy_tile, t, 1).start()

        @pl.when(layer_of(j) < layers - 1)
        def _():
            load(dy0_hbm, dy_tile, t, 1).start()

    def wait_tile(t):
        load(dy_hbm, a_tile, t, 0).wait()
        load(dy_hbm, dy_tile, t, 1).wait()

    def gu_parts(n):
        for c in range(chips):
            for u in range(2):
                yield u * chips + c, u, pl.ds((u * chips + c) * rows, rows), columns(c, n)

    def gu_outs(n):
        for i, u, here, there in gu_parts(n):
            yield pltpu.make_async_copy(gu.sum.at[here, :], (gg_hbm, gu_hbm)[u].at[layer_of(n), :, there], gu.out_sem.at[i])

    def gu_state(n):
        layer = layer_of(n)
        for i, u, here, there in gu_parts(n):
            for k, (src, buf) in enumerate((((mg_hbm, mu_hbm)[u], m_ref), ((vg_hbm, vu_hbm)[u], v_ref))):
                yield pltpu.make_async_copy(src.at[layer, :, there], buf.at[here, :], state_sem.at[3 * i + k])
            src = (wg_hbm, wu_hbm)[u].at[layer, strip(me * rows, rows), there]
            yield pltpu.make_async_copy(src, w_ref.at[here, :], state_sem.at[3 * i + 2])

    def dn_parts(n, size):
        step = lax.rem(n, pairs + 1)
        start = step * LANES + core * (LANES // 2) if size == full else pairs * LANES * (1 - core)
        height = size // lane_blocks
        for b in range(lane_blocks):
            yield b, layers - 1 - n // (pairs + 1), start, height, pl.ds(b * height, height), lanes(b)

    def dn_outs(n, size):
        for b, layer, start, height, here, there in dn_parts(n, size):
            at = pl.ds(pl.multiple_of(start, LANES // 2), height)
            yield pltpu.make_async_copy(dn.sum.at[here, :], gd_hbm.at[layer, at, there], dn.out_sem.at[b])

    def own_out(pool, at, size, sem):
        return [pltpu.make_async_copy(pool.new.at[head(size)], own_hbm.at[pl.ds(pl.multiple_of(at, LANES // 2), size)], own_sem.at[sem])]

    def dn_own(n, size):
        return own_out(dn, (n - (layers - 1) * (pairs + 1)) * full, size, 0)

    def gu_own(n):
        return own_out(gu, pairs * full + small + (n - steps + LATE) * full, full, 1)

    def dn_state(n, size):
        for b, layer, start, height, here, there in dn_parts(n, size):
            at = pl.ds(pl.multiple_of(start, LANES // 2), height)
            for k, (src, buf) in enumerate(((md_hbm, m_ref), (vd_hbm, v_ref))):
                yield pltpu.make_async_copy(src.at[layer, at, there], buf.at[here, :], state_sem.at[3 * b + k])
            at = pl.ds(pl.multiple_of(me * (d // 2) + start, LANES // 2), height)
            yield pltpu.make_async_copy(wd_hbm.at[layer, at, there], w_ref.at[here, :], state_sem.at[3 * b + 2])

    some = d // 3

    def gu_new(n, size):
        gu.event3(n, size)
        pl.when(n > 0)(lambda: wait(gu_outs(n - 1)))
        wait(gu_state(n))
        late = n >= steps - LATE
        pl.when(n > steps - LATE)(lambda: wait(gu_own(n - 1)))

        def piece(i, _):
            at = strip(i * some, some)
            g = gu.total(n, i * some, some)
            gu.sum[at, :] = g.astype(BF16)
            gu.new[at, :] = adam(w_ref[at, :], m_ref[at, :], v_ref[at, :], g)
            return i

        lax.fori_loop(0, size // some, piece, 0)
        gu.after3(n)
        start(gu_outs(n))
        pl.when(~late)(lambda: gu.gather1(n, size))
        pl.when(late)(lambda: start(gu_own(n)))

    def dn_new(n, size):
        half, height = LANES // 2, size // lane_blocks
        dn.event3(n, size)
        if size == full:
            begins = lax.rem(n, pairs + 1) == 0
            pl.when((n > 0) & ~begins)(lambda: wait(dn_outs(n - 1, full)))
            pl.when((n > 0) & begins)(lambda: wait(dn_outs(n - 1, small)))
        else:
            wait(dn_outs(n - 1, full))
        wait(dn_state(n, size))
        upper = n < (layers - 1) * (pairs + 1)
        pl.when(n > (layers - 1) * (pairs + 1))(lambda: wait(dn_own(n - 1, full)))

        def finish(at, g):
            dn.sum[at, :] = g.astype(BF16)
            dn.new[at, :] = adam(w_ref[at, :], m_ref[at, :], v_ref[at, :], g)

        if size == full:

            def piece(i, _):
                for start in range(0, some, LANES):
                    finish(strip(i * some + start, LANES), dn.total(n, i * some + start, LANES).T)
                return i

            lax.fori_loop(0, size // some, piece, 0)
        else:
            g = dn.total(n, 0, size).T
            g = jnp.concatenate([g[:half], g[half:]], 1)
            for b in range(lane_blocks):
                finish(pl.ds(b * height, height), g[:, b * LANES : (b + 1) * LANES])
        dn.after3(n)
        start(dn_outs(n, size))
        pl.when(upper)(lambda: dn.gather1(n, size))
        pl.when(~upper)(lambda: start(dn_own(n, size)))

    def turn(buf, slot, into, part):
        for b in range(lane_blocks):
            into[lanes(b), part] = buf[slot, :, b * LANES : (b + 1) * LANES].T

    start_tile(0, 0)
    start(weight_copies(0))
    barrier = pltpu.get_barrier_semaphore()
    peers = (gu.partner(), gu.device(1), gu.device(-1))
    for peer in peers:
        pl.semaphore_signal(barrier, inc=1, device_id=peer, device_id_type=MESH)
    pl.semaphore_wait(barrier, len(peers))

    def keep(t):
        slot = parity(t)
        return pltpu.make_async_copy(dy_tile.at[slot], dy0_hbm.at[strip(t * tile, tile)], tile_sem.at[slot, 2])

    def compute_tile(j, t):
        slot, here = parity(j), parity(t)
        part = strip(t * tile, tile)
        wait_tile(t)
        pl.when(t + 1 < tiles)(lambda: start_tile(j, t + 1))
        a, dy = a_tile[here], dy_tile[here]
        for c in range(0, chips, 2):
            some = pl.ds(c * LANES, 2 * LANES)
            gate = dot(a, wg_ref[slot, :, some])
            up = dot(a, wu_ref[slot, :, some])
            dz = dot(dy, wd_ref[slot, some, :], NT).astype(BF16).astype(F32)
            s = jax.nn.sigmoid(gate)
            act = s * gate
            z_ref[part, some] = (act * up).astype(BF16)
            dgu_ref[1, part, some] = (dz * act).astype(BF16)
            dgu_ref[0, part, some] = (dz * up * (s + act * (1 - s))).astype(BF16)

        @pl.when(j == 0)
        def _():
            turn(a_tile, here, at_ref, part)
            turn(dy_tile, here, dyt_ref, part)
            da_ref[part, :] = jnp.zeros((tile, d), F32)

    def compute_gate_up(j, u):
        slot = lax.rem(j, gu.slots)
        g = dot(at_ref[...], dgu_ref[u]).astype(BF16)
        for c in range(chips):
            at = strip((u * chips + c) * rows, rows)
            for owner in range(CORES * chips):
                gu.mine[slot, owner % CORES, owner // CORES, at, :] = g[owner * rows : (owner + 1) * rows, c * LANES : (c + 1) * LANES]

    def compute_down(j, _):
        slot, owner = lax.rem(down_of(j), dn.slots), parity(lax.rem(j, blocks))

        @pl.when(~is_last(j))
        def _():
            g = dot(dyt_ref[...], z_ref[...]).astype(BF16)
            for c in range(chips):
                dn.mine[slot, owner, c, :, :] = g[:, c * LANES : (c + 1) * LANES]

        @pl.when(is_last(j))
        def _():
            half = LANES // 2
            low = lax.broadcasted_iota(jnp.int32, (small, LANES), 1) < half

            def one(h, _):
                both = dot(dyt_ref[...], z_ref[:, strip(h * 2 * LANES, 2 * LANES)])
                for c in range(2):
                    straight = both[:, c * LANES : (c + 1) * LANES]
                    turned = pltpu.roll(straight, half, 1)
                    dn.mine[slot, 0, 2 * h + c, head(small), :] = jnp.where(low, straight[:small], turned[small:]).astype(BF16)
                    dn.mine[slot, 1, 2 * h + c, head(small), :] = jnp.where(low, turned[:small], straight[small:]).astype(BF16)
                return h

            lax.fori_loop(0, chips // 2, one, 0)

    def compute_da(j, t):
        slot, part = parity(j), strip(t * 2 * tile, 2 * tile)
        middle = lane_blocks // 2 * LANES
        for begin, end in ((0, middle), (middle, d)):
            some = pl.ds(begin, end - begin)
            da_ref[part, some] += dot(dgu_ref[0, part, :], wg_ref[slot, some, :], NT) + dot(dgu_ref[1, part, :], wu_ref[slot, some, :], NT)

    def begin_change(t):
        load(h_hbm, a_tile, t, 0).start()
        load(dy_hbm, dy_tile, t, 1).start()

    def change_layer():
        def one(t, _):
            slot = parity(t)
            wait_tile(t)
            pl.when(t > 0)(lambda: keep(t - 1).wait())
            pl.when(t + 1 < tiles)(lambda: begin_change(t + 1))
            pl.when(t + 1 == tiles)(lambda: start_tile(blocks, 0))

            def piece(i, _):
                here, there = strip(i * small_tile, small_tile), strip(t * tile + i * small_tile, small_tile)
                wide = a_tile[slot, here, :].astype(F32)
                da = da_ref[there, :].astype(BF16).astype(F32)
                scale = lax.rsqrt(jnp.mean(wide * wide, -1, keepdims=True) + 1e-6)
                along = jnp.mean(da * wide, -1, keepdims=True)
                back = (da * scale - wide * (along * scale * scale * scale)).astype(BF16)
                dy_tile[slot, here, :] = dy_tile[slot, here, :] + back
                return 0

            lax.fori_loop(0, tile // small_tile, piece, 0)
            keep(t).start()
            turn(dy_tile, slot, dyt_ref, strip(t * tile, tile))
            return 0

        lax.fori_loop(0, tiles, one, 0)
        keep(tiles - 1).wait()

    def on(j, act):
        pl.when((j >= 0) & (j < steps))(lambda: act(j, full))

    def early(j, act):
        pl.when(j < steps - LATE)(lambda: on(j, act))

    def upper_down(j, act):
        pl.when(j < (layers - 1) * blocks)(lambda: for_down(j, act))

    def gu_load(n, rows):
        start(gu_state(n))

    def dn_load(n, rows):
        start(dn_state(n, rows))

    events = {
        "tile0": [(on, gu_new, 2)],
        "tile1": [(upper_down, dn.gather2, 2), (for_down, dn_load, 1)],
        "tile3": [(upper_down, dn.gather3, 3), (on, gu.event2, 1)],
        "down0": [(for_down, dn.event0)],
        "gate0": [(early, gu.gather3, 3), (for_down, dn.event1)],
        "gate1": [(on, gu.event0), (early, gu.gather4, 3), (early, gu.gather2, 2), (for_down, dn_new, 1)],
        "back0": [(upper_down, dn.gather4, 3), (on, gu.event1), (on, gu_load, 1)],
        "back1": [(for_down, dn.event2)],
    }
    longest = max(sum(ago) for these in events.values() for _, _, *ago in these)

    def step(j, _):
        busy = j < steps
        lower = layer_of(j) > 0
        changes = is_last(j) & lower & busy

        @pl.when(busy)
        def _():
            wait(weight_copies(j))
            pl.when(j + 1 < steps)(lambda: start(weight_copies(j + 1)))

        def parts(name, number, active, compute):
            def one(t, _):
                pl.when(active)(lambda: compute(j, t))
                for at in range(number):

                    @pl.when(t == at)
                    def _():
                        for stream, act, *ago in events.get(f"{name}{at}", ()):
                            stream(j - sum(ago), act)

                return 0

            lax.fori_loop(0, number, one, 0)

        def da_tiles(j, t):
            fetch = [load(a_hbm.at[0], a_tile, 2 * t + i, 0) for i in range(2)]
            pl.when(changes)(lambda: start(fetch))
            compute_da(j, t)

            @pl.when(changes)
            def _():
                for i, one in enumerate(fetch):
                    one.wait()
                    turn(a_tile, i, at_ref, strip((2 * t + i) * tile, tile))
                pl.when(t > 0)(lambda: begin_change(0))

        parts("tile", tiles, busy, compute_tile)
        pl.when(busy & (j + 1 < steps) & ~changes)(lambda: start_tile(j + 1, 0))
        parts("down", 1, busy, compute_down)
        parts("gate", 2, busy, compute_gate_up)
        parts("back", tiles // 2, busy & lower, da_tiles)

        pl.when(changes)(change_layer)

        return 0

    lax.fori_loop(0, steps + longest, step, 0)
    wait(gu_outs(steps - 1))
    wait(dn_outs(dn.number - 1, small))
    wait(dn_own(dn.number - 1, small))
    wait(gu_own(steps - 1))


def backward(mesh, a, h, dy, weights, m, v, tile=512):
    tokens, d = dy.shape
    layers, _, ff = weights[0].shape
    chips = mesh.shape["dp"] // CORES
    width = chips * LANES
    blocks = ff // width
    pairs = blocks // 2
    rows = d // (CORES * chips)
    assert layers == 2 and chips == 4 and blocks % 2 == 1 and blocks * width == ff and d % LANES == 0
    shape = lambda *s: jax.ShapeDtypeStruct(s, BF16)
    devices = CORES * chips
    outs = [
        shape(layers, rows, ff),
        shape(layers, rows, ff),
        shape(layers, ff // devices, d),
        shape(layers * blocks, devices, d, LANES),
        shape((layers - 1) * (pairs + 1), devices, d, LANES),
        shape(pairs * d + d // 2 + LATE * d, LANES),
        shape(tokens, d),
    ]

    def pool(lanes, outputs):
        return [
            pltpu.VMEM((2, CORES, chips, d, LANES), BF16),
            pltpu.VMEM((2, chips, d, LANES), BF16),
            pltpu.VMEM((lanes, 2, d // 2, LANES), BF16),
            pltpu.VMEM((lanes, 2, d, LANES), BF16),
            pltpu.VMEM((lanes, 2, d // 2, LANES), BF16),
            pltpu.VMEM((lanes, 2, d, LANES), BF16),
            pltpu.VMEM((d, LANES), BF16),
            pltpu.VMEM((d, LANES), BF16),
            pltpu.SemaphoreType.DMA((2, 5, 2)),
            pltpu.SemaphoreType.REGULAR((5,)),
            pltpu.SemaphoreType.DMA((outputs,)),
            pltpu.SemaphoreType.DMA((4, 8, 2)),
            pltpu.SemaphoreType.DMA,
        ]

    return pl.pallas_call(
        functools.partial(backward_kernel, chips, tile),
        out_shape=outs,
        in_specs=[ANY] * 12,
        out_specs=[ANY] * len(outs),
        scratch_shapes=[
            pltpu.VMEM((2, tile, d), BF16),
            pltpu.VMEM((2, tile, d), BF16),
            pltpu.VMEM((d, tokens), BF16),
            pltpu.VMEM((d, tokens), BF16),
            pltpu.VMEM((tokens, d), F32),
            pltpu.VMEM((2, d, width), BF16),
            pltpu.VMEM((2, d, width), BF16),
            pltpu.VMEM((2, width, d), BF16),
            pltpu.VMEM((tokens, width), BF16),
            pltpu.VMEM((2, tokens, width), BF16),
            pltpu.VMEM((d, LANES), F32),
            pltpu.VMEM((d, LANES), F32),
            pltpu.VMEM((d, LANES), BF16),
            pltpu.SemaphoreType.DMA((2, 3)),
            pltpu.SemaphoreType.DMA((2, 3 * chips)),
            pltpu.SemaphoreType.DMA((max(6 * chips, 3 * (d // LANES)),)),
            pltpu.SemaphoreType.DMA((2,)),
            *pool(1, 2 * chips),
            *pool(2, d // LANES),
        ],
        compiler_params=pltpu.CompilerParams(collective_id=1, has_side_effects=True, vmem_limit_bytes=VMEM_BYTES),
        cost_estimate=cost(28 * tokens * d * ff, 24 * d * ff),
        name="backward",
    )(a, h, dy, *weights, *m, *v)


class Ring:
    def __init__(self, units, slots, loads, stores, work):
        self.units, self.slots, self.loads, self.stores, self.work = units, slots, loads, stores, work

    def begin(self):
        for unit in range(self.slots):
            for copy in self.loads(unit, unit):
                copy.start()

    def run(self):
        def one(unit, _):
            slot = lax.rem(unit, self.slots)
            for copy in self.loads(unit, slot):
                copy.wait()

            @pl.when(unit >= self.slots)
            def _():
                for copy in self.stores(unit - self.slots, slot):
                    copy.wait()

            self.work(unit, slot)
            for copy in self.stores(unit, slot):
                copy.start()

            @pl.when(unit + self.slots < self.units)
            def _():
                for copy in self.loads(unit + self.slots, slot):
                    copy.start()

            return 0

        lax.fori_loop(0, self.units, one, 0)

    def end(self):
        for unit in range(self.units - self.slots, self.units):
            for copy in self.stores(unit, unit % self.slots):
                copy.wait()


def place_columns_kernel(layer, slots, x_hbm, *refs):
    gate_hbm, up_hbm, c_in, c_out, sem = refs[-5:]
    _, blocks, devices, _, chips, rows, _ = x_hbm.shape
    wide, there, some = blocks * LANES, *c_in.shape[1:3]
    spots = [j // 2 + (blocks // 2 + 1) * (j % 2) for j in range(there)]
    begins = [at for at in spots if at - 1 not in spots]
    ends = [at + 1 for at in spots if at + 1 not in spots]
    spans = list(zip(sorted(begins), sorted(ends)))
    turns = devices // some

    def place(unit):
        return unit // turns, lax.rem(unit, turns) * some

    def loads(unit, slot):
        chip, owners = place(unit)
        return [pltpu.make_async_copy(x_hbm.at[x_hbm.shape[0] - 1 - layer, head(there), pl.ds(owners, some), :, chip], c_in.at[slot], sem.at[slot, 0])]

    def stores(unit, slot):
        chip, owners = place(unit)
        copies = []
        for begin, end in spans:
            size = (end - begin) * LANES
            to = layer, strip(owners * rows, some * rows), pl.ds(pl.multiple_of(chip * wide + begin * LANES, LANES), size)
            for u, out in enumerate((gate_hbm, up_hbm)):
                copies.append(pltpu.make_async_copy(c_out.at[slot, u, :, pl.ds(begin * LANES, size)], out.at[to], sem.at[slot, 1 + len(copies)]))
        return copies

    def work(unit, slot):
        for j, at in enumerate(spots):
            for owner in range(some):
                for u in range(2):
                    c_out[slot, u, pl.ds(owner * rows, rows), lanes(at)] = c_in[slot, j, owner, u]

    ring = Ring(chips * turns, slots, loads, stores, work)
    ring.begin()
    ring.run()
    ring.end()


def place_columns(chunks, layer, layers, d, ff, into=(), slots=4, some=2):
    devices = chunks.shape[1]
    chips, rows = devices // CORES, d // devices
    x = chunks.reshape(layers, -1, devices, 2, chips, rows, LANES)
    there = x.shape[1] - LATE * (layer == 0)
    return pl.pallas_call(
        functools.partial(place_columns_kernel, layer, slots),
        in_specs=[ANY] * (1 + len(into)),
        out_specs=[ANY] * 2,
        input_output_aliases={1 + i: i for i in range(len(into))},
        out_shape=[jax.ShapeDtypeStruct((layers, d, ff), BF16)] * 2,
        scratch_shapes=[
            pltpu.VMEM((slots, there, some, 2, rows, LANES), BF16),
            pltpu.VMEM((slots, 2, some * rows, ff // chips), BF16),
            pltpu.SemaphoreType.DMA((slots, devices)),
        ],
        compiler_params=pltpu.CompilerParams(vmem_limit_bytes=VMEM_BYTES),
        cost_estimate=moves(8 * d * ff),
        name="place_columns",
    )(x, *into)


def moments_kernel(layers, parts, slots, *refs):
    states, news, s_in, g_in, s_out, sem = refs[:9], refs[9:15], refs[15:18], refs[18:21], refs[21:24], refs[24]

    def at(i, unit):
        layer, part = unit // parts, lax.rem(unit, parts)
        _, r, c = states[i].shape
        return (layer, strip(part * (r // parts), r // parts), slice(None)) if i == 2 else (layer, slice(None), strip(part * (c // parts), c // parts))

    def loads(unit, slot):
        copies = []
        for i in range(3):
            for k in range(2):
                copies.append(pltpu.make_async_copy(states[3 * k + i].at[at(i, unit)], s_in[i].at[slot, k], sem.at[slot, 5 * i + k]))
            copies.append(pltpu.make_async_copy(states[6 + i].at[at(i, unit)], g_in[i].at[slot], sem.at[slot, 5 * i + 2]))
        return copies

    def stores(unit, slot):
        return [
            pltpu.make_async_copy(s_out[i].at[slot, k], news[3 * k + i].at[at(i, unit)], sem.at[slot, 5 * i + 3 + k]) for i in range(3) for k in range(2)
        ]

    def work(unit, slot):
        for i in range(3):
            g = g_in[i][slot].astype(F32)
            s_out[i][slot, 0], s_out[i][slot, 1] = moment(s_in[i][slot, 0], s_in[i][slot, 1], g)

    ring = Ring(layers * parts, slots, loads, stores, work)
    ring.begin()
    ring.run()
    ring.end()


def moments(m, v, g, parts=9, slots=4):
    layers = m[0].shape[0]
    shapes = [(one.shape[1], one.shape[2] // parts) for one in m[:2]] + [(m[2].shape[1] // parts, m[2].shape[2])]
    size = sum(one.size for one in m)
    return pl.pallas_call(
        functools.partial(moments_kernel, layers, parts, slots),
        in_specs=[ANY] * 9,
        out_specs=[ANY] * 6,
        out_shape=[jax.ShapeDtypeStruct(one.shape, F32) for one in m] * 2,
        scratch_shapes=[
            *(pltpu.VMEM((slots, 2, *shape), F32) for shape in shapes),
            *(pltpu.VMEM((slots, *shape), BF16) for shape in shapes),
            *(pltpu.VMEM((slots, 2, *shape), F32) for shape in shapes),
            pltpu.SemaphoreType.DMA((slots, 15)),
        ],
        compiler_params=pltpu.CompilerParams(vmem_limit_bytes=VMEM_BYTES),
        cost_estimate=moves(18 * size),
        name="moments",
    )(*m, *v, *g)


def unfold(chunks, out, core):
    pairs, half = chunks.shape[0] - 1, LANES // 2
    for b in range(out.shape[1] // LANES):
        for n in range(pairs):
            out[pl.ds(pl.multiple_of(n * LANES + core * half, half), LANES), lanes(b)] = chunks[n, lanes(b), :]
        out[pl.ds(pl.multiple_of(pairs * LANES * (1 - core), half), half), lanes(b)] = chunks[pairs, pl.ds(b * half, half), :]


def place_rows_kernel(layers, slots, x_hbm, down_hbm, r_in, r_out, sem):
    devices = x_hbm.shape[2]
    pairs = x_hbm.shape[1] - 1
    height, d = r_out.shape[1:]

    def loads(unit, slot):
        layer, device = layers - 2 - unit // devices, lax.rem(unit, devices)
        return [
            pltpu.make_async_copy(x_hbm.at[layer, head(pairs), device], r_in.at[slot, head(pairs)], sem.at[slot, 0]),
            pltpu.make_async_copy(x_hbm.at[layer, pairs, device, head(d // 2)], r_in.at[slot, pairs, head(d // 2)], sem.at[slot, 1]),
        ]

    def stores(unit, slot):
        layer, device = unit // devices + 1, lax.rem(unit, devices)
        return [pltpu.make_async_copy(r_out.at[slot], down_hbm.at[layer, strip(device * height, height)], sem.at[slot, 2])]

    def work(unit, slot):
        unfold(r_in.at[slot], r_out.at[slot], lax.rem(unit, CORES))

    ring = Ring((layers - 1) * devices, slots, loads, stores, work)
    ring.begin()
    ring.run()
    ring.end()


def place_rows(chunks, layers, d, ff, slots=4):
    devices = chunks.shape[1]
    x = chunks.reshape(layers - 1, -1, devices, d, LANES)
    height = ff // devices
    return pl.pallas_call(
        functools.partial(place_rows_kernel, layers, slots),
        in_specs=[ANY],
        out_specs=ANY,
        out_shape=jax.ShapeDtypeStruct((layers, ff, d), BF16),
        scratch_shapes=[
            pltpu.VMEM((slots, x.shape[1], d, LANES), BF16),
            pltpu.VMEM((slots, height, d), BF16),
            pltpu.SemaphoreType.DMA((slots, 3)),
        ],
        compiler_params=pltpu.CompilerParams(vmem_limit_bytes=VMEM_BYTES),
        cost_estimate=moves(4 * d * ff),
        name="place_rows",
    )(x)


def place_blocks_kernel(wheres, me_ref, *refs):
    blocks, (gate_hbm, up_hbm, down_hbm, held, down, sem) = refs[: len(wheres)], refs[-6:]
    layers, d, ff = gate_hbm.shape
    height = down.shape[1]
    devices = ff // height
    chips, rows = devices // CORES, d // devices
    wide = ff // chips
    pairs = wide // LANES // 2
    chip, core = me_ref[0] // CORES, lax.rem(me_ref[0], CORES)

    def fetch(i):
        return pltpu.make_async_copy(blocks[i], held.at[i], sem.at[i, 0])

    def put(i):
        hops, flip = wheres[i]
        side = 1 - core if flip else core
        owner = lax.rem(chip + hops + chips, chips) * CORES + side
        copies = [pltpu.make_async_copy(down.at[i], down_hbm.at[0, strip(owner * height, height)], sem.at[i, 1])]
        for n in range(LATE):
            step = 2 * pairs + 1 - LATE + n
            column = (step // 2 + (pairs + 1) * (step % 2)) * LANES
            for u, out in enumerate((gate_hbm, up_hbm)):
                for c in range(chips):
                    here = pl.ds(pairs * d + d // 2 + n * d + (u * chips + c) * rows, rows)
                    to = out.at[0, strip(owner * rows, rows), pl.ds(c * wide + column, LANES)]
                    copies.append(pltpu.make_async_copy(held.at[i, here], to, sem.at[i, 1 + len(copies)]))
        return side, copies

    number = len(wheres)
    for i in range(number):
        fetch(i).start()
    for i in range(number):
        fetch(i).wait()
        side, copies = put(i)
        start(copies[1:])
        for n in range(pairs + 1):
            size_n = d if n < pairs else d // 2
            for b in range(d // LANES):
                part = size_n // (d // LANES)
                at = n * LANES + side * (LANES // 2) if n < pairs else pairs * LANES * (1 - side)
                down[i, pl.ds(pl.multiple_of(at, LANES // 2), part), lanes(b)] = held[i, pl.ds(n * d + b * part, part), :]
        copies[0].start()
    for i in range(number):
        wait(put(i)[1])


def place_blocks(me, blocks, weights):
    wheres, blocks = tuple(blocks), list(blocks.values())
    number, rows = len(blocks), blocks[0].shape[0]
    layers, ff, d = weights[2].shape
    height = rows * LANES // d - LATE * LANES
    return pl.pallas_call(
        functools.partial(place_blocks_kernel, wheres),
        in_specs=[pl.BlockSpec(memory_space=pltpu.SMEM)] + [ANY] * (number + 3),
        out_specs=[ANY] * 3,
        out_shape=[jax.ShapeDtypeStruct(one.shape, BF16) for one in weights],
        input_output_aliases={number + 1 + i: i for i in range(3)},
        scratch_shapes=[
            pltpu.VMEM((number, rows, LANES), BF16),
            pltpu.VMEM((number, height, d), BF16),
            pltpu.SemaphoreType.DMA((number, 2 + LATE * ff // height)),
        ],
        compiler_params=pltpu.CompilerParams(vmem_limit_bytes=VMEM_BYTES),
        name="place_blocks",
    )(me, *blocks, *weights)


def solution(mesh):
    group = mesh.shape["dp"]
    swap = [(i, i ^ 1) for i in range(group)]
    right = [(i, (i + CORES) % group) for i in range(group)]
    left = [(i, (i - CORES) % group) for i in range(group)]

    def step(x, dy, *arrays):
        weights, m, v = (arrays[i : i + 3] for i in (0, 3, 6))
        layers, d, ff = weights[0].shape
        me = lax.axis_index("dp").reshape(1)
        *sums, columns, rows, own, _ = backward(mesh, *forward(x[0], *weights, 0), dy[0], weights, m, v)

        def send(block, to):
            return lax.ppermute(block, "dp", to)

        from_left, from_right = send(own, right), send(own, left)
        gate, up = place_columns(columns, 1, layers, d, ff)
        first, *states = moments(m, v, sums)
        gate, first, from_left, from_right = lax.optimization_barrier((gate, first, from_left, from_right))
        opposite = send(jnp.where(lax.rem(lax.axis_index("dp"), CORES) == 0, from_left, from_right), [(right, left)[i % CORES][i] for i in range(group)])
        near = {(0, 0): own, (-1, 0): from_left, (1, 0): from_right}
        other = {(hops, 1): send(block, swap) for (hops, _), block in near.items()}
        gate, up = place_columns(columns, 0, layers, d, ff, (gate, up))
        up, rows = lax.optimization_barrier((up, rows))
        down = place_rows(rows, layers, d, ff)
        down, opposite = lax.optimization_barrier((down, opposite))
        last = send(opposite, swap)
        weights = place_blocks(me, {**near, **other}, (gate, up, down))
        weights = place_blocks(me, {(2, 0): opposite, (2, 1): last}, weights)
        return (*weights, first, *states)

    seq, whole, rows = P(("rep", "dp"), None, None), P(None, None, None), P(None, "dp", None)
    return jax.shard_map(
        step,
        mesh=mesh,
        in_specs=(seq, seq, whole, whole, whole) + (rows,) * 6,
        out_specs=(P("rep", None, None),) * 3 + (P("rep", "dp", None),) * 6,
        check_vma=False,
    )
```

```python
import functools

import jax
import jax.numpy as jnp
from jax import lax
from jax.experimental import pallas as pl
from jax.experimental.pallas import tpu as pltpu
from jax.sharding import PartitionSpec as P

F32, BF16 = jnp.float32, jnp.bfloat16
NN, NT = (((1,), (0,)), ((), ())), (((1,), (1,)), ((), ()))
MESH = pl.DeviceIdType.MESH
ANY = pl.BlockSpec(memory_space=pl.ANY)
LANES = 128
CORES = 2
VMEM_BYTES = 67_043_328
COPY_FLOPS = 64
LATE = 2
SIDES = (0, 1), (1, -1)


def dot(a, b, dims=NN):
    return lax.dot_general(a, b, dims, preferred_element_type=F32)


def norm(h):
    wide = h.astype(F32)
    return (wide * lax.rsqrt(jnp.mean(wide**2, -1, keepdims=True) + 1e-6)).astype(BF16)


def strip(start, size):
    return pl.ds(pl.multiple_of(start, size), size)


def head(size):
    return pl.ds(0, size)


def parity(n):
    return lax.rem(n, 2)


def lanes(n):
    return pl.ds(n * LANES, LANES)


def start(copies):
    for copy in copies:
        copy.start()


def wait(copies):
    for copy in copies:
        copy.wait()


def moves(moved):
    return cost(COPY_FLOPS * moved, moved)


def cost(flops, moved):
    return pl.CostEstimate(flops=flops, bytes_accessed=moved, transcendentals=moved)


def forward_kernel(tile, x_ref, wg_ref, wu_ref, wd_ref, a_hbm, h_hbm, a_ref, total, ends, a_sem, end_sem):
    block = pl.program_id(0)
    first, last = block == 0, block == pl.num_programs(0) - 1
    tiles = x_ref.shape[0] // tile

    def keep(t):
        rows = strip(t * tile, tile)
        return pltpu.make_async_copy(a_ref.at[rows], a_hbm.at[0, rows], a_sem.at[t])

    def finish(t):
        rows = strip(t * tile, tile)
        for i, out in enumerate((h_hbm, a_hbm.at[1])):
            yield pltpu.make_async_copy(ends.at[parity(t), i], out.at[rows], end_sem.at[parity(t), i])

    @pl.when(first)
    def _():
        def begin(t, _):
            rows = strip(t * tile, tile)
            a_ref[rows, :] = norm(x_ref[rows, :])
            total[rows, :] = jnp.zeros((tile, total.shape[1]), F32)
            keep(t).start()
            return t

        lax.fori_loop(0, tiles, begin, 0)

    def one(t, _):
        rows = strip(t * tile, tile)
        a = a_ref[rows, :]
        gate, up = dot(a, wg_ref[...]), dot(a, wu_ref[...])
        z = (jax.nn.sigmoid(gate) * gate * up).astype(BF16)
        total[rows, :] += dot(z, wd_ref[...])

        @pl.when(last)
        def _():
            keep(t).wait()
            pl.when(t >= 2)(lambda: wait(finish(t - 2)))
            h = x_ref[rows, :] + total[rows, :].astype(BF16)
            for i, end in enumerate((h, norm(h))):
                ends[parity(t), i] = end
            start(finish(t))

        return t

    lax.fori_loop(0, tiles, one, 0)

    @pl.when(last)
    def _():
        for t in range(tiles - 2, tiles):
            wait(finish(t))


def forward(x, wg, wu, wd, layer, width=768, tile=512):
    tokens, d = x.shape
    ff = wg.shape[2]
    state = jax.ShapeDtypeStruct((tokens, d), BF16)
    columns = pl.BlockSpec((None, d, width), lambda i: (layer, 0, i))
    return pl.pallas_call(
        functools.partial(forward_kernel, tile),
        grid=(ff // width,),
        out_shape=[jax.ShapeDtypeStruct((2, tokens, d), BF16), state],
        in_specs=[pl.BlockSpec(x.shape, lambda i: (0, 0)), columns, columns, pl.BlockSpec((None, width, d), lambda i: (layer, i, 0))],
        out_specs=[ANY] * 2,
        scratch_shapes=[
            pltpu.VMEM(x.shape, BF16),
            pltpu.VMEM(x.shape, F32),
            pltpu.VMEM((2, 2, tile, d), BF16),
            pltpu.SemaphoreType.DMA((tokens // tile,)),
            pltpu.SemaphoreType.DMA((2, 2)),
        ],
        compiler_params=pltpu.CompilerParams(vmem_limit_bytes=VMEM_BYTES),
        cost_estimate=cost(6 * tokens * d * ff, 6 * d * ff),
        name="forward",
    )(x, wg, wu, wd)


class Pool:
    def __init__(self, number, chips, core, chip, bufs, sems, gathered):
        self.number, self.chips, self.core, self.chip = number, chips, core, chip
        self.mine, self.other, self.cross, self.near, self.out1, self.out2, self.sum, self.new = bufs
        self.dma, self.credit, self.out_sem, self.ag_sem, self.own_sem = sems
        self.gathered = gathered
        self.slots, self.lanes, self.turns = self.mine.shape[0], self.cross.shape[0], self.ag_sem.shape[0]

    def index(self, chip, core):
        return lax.rem(chip + self.chips, self.chips) * CORES + core

    def device(self, hops, core=None):
        return {"dp": self.index(self.chip + hops, self.core if core is None else core)}

    def partner(self):
        return self.device(0, 1 - self.core)

    def hop(self, sems, src, dst, to):
        return pltpu.make_async_remote_copy(src_ref=src, dst_ref=dst, send_sem=sems.at[0], recv_sem=sems.at[1], device_id=to, device_id_type=MESH)

    def copies0(self, n, rows):
        slot = lax.rem(n, self.slots)
        src = self.mine.at[slot, 1 - self.core, :, head(rows), :]
        return [self.hop(self.dma.at[slot, 0], src, self.other.at[slot, :, head(rows), :], self.partner())]

    def copies1(self, n, rows):
        slot, sem, half = lax.rem(n, self.lanes), lax.rem(n, self.slots), head(rows // 2)
        return [self.hop(self.dma.at[sem, 1 + side], self.out1.at[slot, side, half], self.cross.at[slot, side, half], self.device(hop)) for side, hop in SIDES]

    def copies2(self, n, rows):
        slot, sem, full = lax.rem(n, self.lanes), lax.rem(n, self.slots), head(rows)
        return [self.hop(self.dma.at[sem, 3 + side], self.out2.at[slot, side, full], self.near.at[slot, side, full], self.device(hop)) for side, hop in SIDES]

    def both(self, n, hops, start, size):
        slot, chip = lax.rem(n, self.slots), lax.rem(self.chip + hops + self.chips, self.chips)
        rows = pl.ds(start, size)
        return self.mine[slot, self.core, chip, rows, :].astype(F32) + self.other[slot, chip, rows, :].astype(F32)

    def give(self, kind, to):
        pl.semaphore_signal(self.credit.at[kind], inc=1, device_id=to, device_id_type=MESH)

    def take(self, when, kinds):
        @pl.when(when)
        def _():
            for kind in kinds:
                pl.semaphore_wait(self.credit.at[kind], 1)

    def event0(self, n, rows):
        self.take(n >= self.slots, (0,))
        start(self.copies0(n, rows))

    def event1(self, n, rows):
        slot, half = lax.rem(n, self.lanes), rows // 2
        wait(self.copies0(n, rows))
        for side, _ in SIDES:
            self.out1[slot, side, head(half)] = self.both(n, 2, side * half, half).astype(BF16)
        self.take(n >= self.lanes, (1, 2))
        start(self.copies1(n, rows))

    def event2(self, n, rows):
        slot, half = lax.rem(n, self.lanes), rows // 2
        wait(self.copies1(n, rows))
        for side, hop in SIDES:
            passed = self.both(n, hop, side * half, half) + self.cross[slot, side, head(half)].astype(F32)
            self.out2[slot, side, pl.ds(side * half, half), :] = passed.astype(BF16)
            self.out2[slot, side, pl.ds(half - side * half, half), :] = self.both(n, hop, half - side * half, half).astype(BF16)

        @pl.when(n + self.lanes < self.number)
        def _():
            for side, hop in SIDES:
                self.give(1 + side, self.device(-hop))

        self.take(n >= self.lanes, (3, 4))
        start(self.copies2(n, rows))

    def total(self, n, start, size):
        total = self.both(n, 0, start, size)
        for side, _ in SIDES:
            total += self.near[lax.rem(n, self.lanes), side, pl.ds(start, size), :].astype(F32)
        return total.astype(BF16).astype(F32)

    def event3(self, n, rows):
        wait(self.copies2(n, rows))

    def after3(self, n):
        pl.when(n + self.slots < self.number)(lambda: self.give(0, self.partner()))

        @pl.when(n + self.lanes < self.number)
        def _():
            for side, hop in SIDES:
                self.give(3 + side, self.device(-hop))

    def block(self, n, hops, core, start, size):
        return self.gathered.at[n, self.index(self.chip + hops, core), pl.ds(start, size), :]

    def sems(self, n, kind):
        return self.ag_sem.at[lax.rem(n, self.turns), kind]

    def gathers1(self, n, rows):
        new, own = self.new.at[head(rows)], self.block(n, 0, self.core, 0, rows)
        copies = [self.hop(self.sems(n, side), new, own, self.device(hop)) for side, hop in SIDES]
        return [*copies, self.hop(self.sems(n, 7), new, own, self.partner()), pltpu.make_async_copy(new, own, self.own_sem)]

    def gathers2(self, n, rows):
        copies, half = [], rows // 2
        for side, hop in SIDES:
            part, full = (self.block(n, -hop, self.core, *which) for which in ((side * half, half), (0, rows)))
            copies.append(self.hop(self.sems(n, 2 + side), part, part, self.device(hop)))
            copies.append(self.hop(self.sems(n, 4 + side), full, full, self.partner()))
        return copies

    def gathers3(self, n, rows):
        opposite = self.block(n, 2, self.core, 0, rows)
        return [self.hop(self.sems(n, 6), opposite, opposite, self.partner())]

    def gather1(self, n, rows):
        start(self.gathers1(n, rows))

    def gather2(self, n, rows):
        wait(self.gathers1(n, rows))
        start(self.gathers2(n, rows))

    def gather3(self, n, rows):
        wait(self.gathers2(n, rows))
        start(self.gathers3(n, rows))

    def gather4(self, n, rows):
        wait(self.gathers3(n, rows))


def moment(m, v, g):
    return 0.9 * m + 0.1 * g, 0.95 * v + 0.05 * g * g


def adam(w, m, v, g):
    m, v = moment(m, v, g)
    w = w.astype(F32)
    return (w - 0.02 * (m * lax.rsqrt(v + 1e-8) + 0.1 * w)).astype(BF16)


def backward_kernel(chips, tile, *refs):
    a_hbm, h_hbm, dy_hbm, wg_hbm, wu_hbm, wd_hbm, mg_hbm, mu_hbm, md_hbm, vg_hbm, vu_hbm, vd_hbm, *refs = refs
    gg_hbm, gu_hbm, gd_hbm, whole_gu, whole_dn, own_hbm, dy0_hbm, *refs = refs
    a_tile, dy_tile, at_ref, dyt_ref, da_ref, wg_ref, wu_ref, wd_ref, z_ref, dgu_ref, m_ref, v_ref, w_ref, *refs = refs
    tile_sem, w_sem, state_sem, own_sem, *pools = refs
    tokens, d = dy_hbm.shape
    layers, _, ff = wg_hbm.shape
    width = chips * LANES
    blocks = ff // width
    pairs = blocks // 2
    rows = d // (CORES * chips)
    lane_blocks = d // LANES
    me = lax.axis_index("dp")
    chip, core = me // CORES, lax.rem(me, CORES)
    tiles = tokens // tile
    steps = layers * blocks
    full, small, small_tile = d, d // 2, tile // 4

    gu = Pool(steps, chips, core, chip, pools[0:8], pools[8:13], whole_gu)
    dn = Pool(layers * (pairs + 1), chips, core, chip, pools[13:21], pools[21:26], whole_dn)

    def layer_of(j):
        return layers - 1 - j // blocks

    def block_of(j):
        j = lax.rem(j, blocks)
        return j // 2 + (pairs + 1) * parity(j)

    def columns(c, j):
        return strip(c * blocks * LANES + block_of(j) * LANES, LANES)

    def is_last(j):
        return lax.rem(j, blocks) == blocks - 1

    def gives_down(j):
        return (j >= 0) & (j < steps) & ((parity(lax.rem(j, blocks)) == 1) | is_last(j))

    def down_of(j):
        return (j // blocks) * (pairs + 1) + lax.rem(j, blocks) // 2

    def for_down(j, act):
        @pl.when(gives_down(j) & ~is_last(j))
        def _():
            act(down_of(j), full)

        @pl.when(gives_down(j) & is_last(j))
        def _():
            act(down_of(j), small)

    def weight_copies(j):
        layer, slot = layer_of(j), parity(j)
        for c in range(chips):
            there, here = columns(c, j), lanes(c)
            yield pltpu.make_async_copy(wg_hbm.at[layer, :, there], wg_ref.at[slot, :, here], w_sem.at[slot, 3 * c])
            yield pltpu.make_async_copy(wu_hbm.at[layer, :, there], wu_ref.at[slot, :, here], w_sem.at[slot, 3 * c + 1])
            yield pltpu.make_async_copy(wd_hbm.at[layer, there, :], wd_ref.at[slot, here, :], w_sem.at[slot, 3 * c + 2])

    def load(src, buf, t, which):
        slot = parity(t)
        return pltpu.make_async_copy(src.at[strip(t * tile, tile), :], buf.at[slot], tile_sem.at[slot, which])

    def start_tile(j, t):
        load(a_hbm.at[layer_of(j)], a_tile, t, 0).start()

        @pl.when(layer_of(j) == layers - 1)
        def _():
            load(dy_hbm, dy_tile, t, 1).start()

        @pl.when(layer_of(j) < layers - 1)
        def _():
            load(dy0_hbm, dy_tile, t, 1).start()

    def wait_tile(t):
        load(dy_hbm, a_tile, t, 0).wait()
        load(dy_hbm, dy_tile, t, 1).wait()

    def gu_parts(n):
        for c in range(chips):
            for u in range(2):
                yield u * chips + c, u, pl.ds((u * chips + c) * rows, rows), columns(c, n)

    def gu_outs(n):
        for i, u, here, there in gu_parts(n):
            yield pltpu.make_async_copy(gu.sum.at[here, :], (gg_hbm, gu_hbm)[u].at[layer_of(n), :, there], gu.out_sem.at[i])

    def gu_state(n):
        layer = layer_of(n)
        for i, u, here, there in gu_parts(n):
            for k, (src, buf) in enumerate((((mg_hbm, mu_hbm)[u], m_ref), ((vg_hbm, vu_hbm)[u], v_ref))):
                yield pltpu.make_async_copy(src.at[layer, :, there], buf.at[here, :], state_sem.at[3 * i + k])
            src = (wg_hbm, wu_hbm)[u].at[layer, strip(me * rows, rows), there]
            yield pltpu.make_async_copy(src, w_ref.at[here, :], state_sem.at[3 * i + 2])

    def dn_parts(n, size):
        step = lax.rem(n, pairs + 1)
        start = step * LANES + core * (LANES // 2) if size == full else pairs * LANES * (1 - core)
        height = size // lane_blocks
        for b in range(lane_blocks):
            yield b, layers - 1 - n // (pairs + 1), start, height, pl.ds(b * height, height), lanes(b)

    def dn_outs(n, size):
        for b, layer, start, height, here, there in dn_parts(n, size):
            at = pl.ds(pl.multiple_of(start, LANES // 2), height)
            yield pltpu.make_async_copy(dn.sum.at[here, :], gd_hbm.at[layer, at, there], dn.out_sem.at[b])

    def own_out(pool, at, size, sem):
        return [pltpu.make_async_copy(pool.new.at[head(size)], own_hbm.at[pl.ds(pl.multiple_of(at, LANES // 2), size)], own_sem.at[sem])]

    def dn_own(n, size):
        return own_out(dn, (n - (layers - 1) * (pairs + 1)) * full, size, 0)

    def gu_own(n):
        return own_out(gu, pairs * full + small + (n - steps + LATE) * full, full, 1)

    def dn_state(n, size):
        for b, layer, start, height, here, there in dn_parts(n, size):
            at = pl.ds(pl.multiple_of(start, LANES // 2), height)
            for k, (src, buf) in enumerate(((md_hbm, m_ref), (vd_hbm, v_ref))):
                yield pltpu.make_async_copy(src.at[layer, at, there], buf.at[here, :], state_sem.at[3 * b + k])
            at = pl.ds(pl.multiple_of(me * (d // 2) + start, LANES // 2), height)
            yield pltpu.make_async_copy(wd_hbm.at[layer, at, there], w_ref.at[here, :], state_sem.at[3 * b + 2])

    some = d // 3

    def gu_new(n, size):
        gu.event3(n, size)
        pl.when(n > 0)(lambda: wait(gu_outs(n - 1)))
        wait(gu_state(n))
        late = n >= steps - LATE
        pl.when(n > steps - LATE)(lambda: wait(gu_own(n - 1)))

        def piece(i, _):
            at = strip(i * some, some)
            g = gu.total(n, i * some, some)
            gu.sum[at, :] = g.astype(BF16)
            gu.new[at, :] = adam(w_ref[at, :], m_ref[at, :], v_ref[at, :], g)
            return i

        lax.fori_loop(0, size // some, piece, 0)
        gu.after3(n)
        start(gu_outs(n))
        pl.when(~late)(lambda: gu.gather1(n, size))
        pl.when(late)(lambda: start(gu_own(n)))

    def dn_new(n, size):
        half, height = LANES // 2, size // lane_blocks
        dn.event3(n, size)
        if size == full:
            begins = lax.rem(n, pairs + 1) == 0
            pl.when((n > 0) & ~begins)(lambda: wait(dn_outs(n - 1, full)))
            pl.when((n > 0) & begins)(lambda: wait(dn_outs(n - 1, small)))
        else:
            wait(dn_outs(n - 1, full))
        wait(dn_state(n, size))
        upper = n < (layers - 1) * (pairs + 1)
        pl.when(n > (layers - 1) * (pairs + 1))(lambda: wait(dn_own(n - 1, full)))

        def finish(at, g):
            dn.sum[at, :] = g.astype(BF16)
            dn.new[at, :] = adam(w_ref[at, :], m_ref[at, :], v_ref[at, :], g)

        if size == full:

            def piece(i, _):
                for start in range(0, some, LANES):
                    finish(strip(i * some + start, LANES), dn.total(n, i * some + start, LANES).T)
                return i

            lax.fori_loop(0, size // some, piece, 0)
        else:
            g = dn.total(n, 0, size).T
            g = jnp.concatenate([g[:half], g[half:]], 1)
            for b in range(lane_blocks):
                finish(pl.ds(b * height, height), g[:, b * LANES : (b + 1) * LANES])
        dn.after3(n)
        start(dn_outs(n, size))
        pl.when(upper)(lambda: dn.gather1(n, size))
        pl.when(~upper)(lambda: start(dn_own(n, size)))

    def turn(buf, slot, into, part):
        for b in range(lane_blocks):
            into[lanes(b), part] = buf[slot, :, b * LANES : (b + 1) * LANES].T

    start_tile(0, 0)
    start(weight_copies(0))
    barrier = pltpu.get_barrier_semaphore()
    peers = (gu.partner(), gu.device(1), gu.device(-1))
    for peer in peers:
        pl.semaphore_signal(barrier, inc=1, device_id=peer, device_id_type=MESH)
    pl.semaphore_wait(barrier, len(peers))

    def keep(t):
        slot = parity(t)
        return pltpu.make_async_copy(dy_tile.at[slot], dy0_hbm.at[strip(t * tile, tile)], tile_sem.at[slot, 2])

    def compute_tile(j, t):
        slot, here = parity(j), parity(t)
        part = strip(t * tile, tile)
        wait_tile(t)
        pl.when(t + 1 < tiles)(lambda: start_tile(j, t + 1))
        a, dy = a_tile[here], dy_tile[here]
        for c in range(0, chips, 2):
            some = pl.ds(c * LANES, 2 * LANES)
            gate = dot(a, wg_ref[slot, :, some])
            up = dot(a, wu_ref[slot, :, some])
            dz = dot(dy, wd_ref[slot, some, :], NT).astype(BF16).astype(F32)
            s = jax.nn.sigmoid(gate)
            act = s * gate
            z_ref[part, some] = (act * up).astype(BF16)
            dgu_ref[1, part, some] = (dz * act).astype(BF16)
            dgu_ref[0, part, some] = (dz * up * (s + act * (1 - s))).astype(BF16)

        @pl.when(j == 0)
        def _():
            turn(a_tile, here, at_ref, part)
            turn(dy_tile, here, dyt_ref, part)
            da_ref[part, :] = jnp.zeros((tile, d), F32)

    def compute_gate_up(j, u):
        slot = lax.rem(j, gu.slots)
        g = dot(at_ref[...], dgu_ref[u]).astype(BF16)
        for c in range(chips):
            at = strip((u * chips + c) * rows, rows)
            for owner in range(CORES * chips):
                gu.mine[slot, owner % CORES, owner // CORES, at, :] = g[owner * rows : (owner + 1) * rows, c * LANES : (c + 1) * LANES]

    def compute_down(j, _):
        slot, owner = lax.rem(down_of(j), dn.slots), parity(lax.rem(j, blocks))

        @pl.when(~is_last(j))
        def _():
            g = dot(dyt_ref[...], z_ref[...]).astype(BF16)
            for c in range(chips):
                dn.mine[slot, owner, c, :, :] = g[:, c * LANES : (c + 1) * LANES]

        @pl.when(is_last(j))
        def _():
            half = LANES // 2
            low = lax.broadcasted_iota(jnp.int32, (small, LANES), 1) < half

            def one(h, _):
                both = dot(dyt_ref[...], z_ref[:, strip(h * 2 * LANES, 2 * LANES)])
                for c in range(2):
                    straight = both[:, c * LANES : (c + 1) * LANES]
                    turned = pltpu.roll(straight, half, 1)
                    dn.mine[slot, 0, 2 * h + c, head(small), :] = jnp.where(low, straight[:small], turned[small:]).astype(BF16)
                    dn.mine[slot, 1, 2 * h + c, head(small), :] = jnp.where(low, turned[:small], straight[small:]).astype(BF16)
                return h

            lax.fori_loop(0, chips // 2, one, 0)

    def compute_da(j, t):
        slot, part = parity(j), strip(t * 2 * tile, 2 * tile)
        middle = lane_blocks // 2 * LANES
        for begin, end in ((0, middle), (middle, d)):
            some = pl.ds(begin, end - begin)
            da_ref[part, some] += dot(dgu_ref[0, part, :], wg_ref[slot, some, :], NT) + dot(dgu_ref[1, part, :], wu_ref[slot, some, :], NT)

    def begin_change(t):
        load(h_hbm, a_tile, t, 0).start()
        load(dy_hbm, dy_tile, t, 1).start()

    def change_layer():
        def one(t, _):
            slot = parity(t)
            wait_tile(t)
            pl.when(t > 0)(lambda: keep(t - 1).wait())
            pl.when(t + 1 < tiles)(lambda: begin_change(t + 1))
            pl.when(t + 1 == tiles)(lambda: start_tile(blocks, 0))

            def piece(i, _):
                here, there = strip(i * small_tile, small_tile), strip(t * tile + i * small_tile, small_tile)
                wide = a_tile[slot, here, :].astype(F32)
                da = da_ref[there, :].astype(BF16).astype(F32)
                scale = lax.rsqrt(jnp.mean(wide * wide, -1, keepdims=True) + 1e-6)
                along = jnp.mean(da * wide, -1, keepdims=True)
                back = (da * scale - wide * (along * scale * scale * scale)).astype(BF16)
                dy_tile[slot, here, :] = dy_tile[slot, here, :] + back
                return 0

            lax.fori_loop(0, tile // small_tile, piece, 0)
            keep(t).start()
            turn(dy_tile, slot, dyt_ref, strip(t * tile, tile))
            return 0

        lax.fori_loop(0, tiles, one, 0)
        keep(tiles - 1).wait()

    def on(j, act):
        pl.when((j >= 0) & (j < steps))(lambda: act(j, full))

    def early(j, act):
        pl.when(j < steps - LATE)(lambda: on(j, act))

    def upper_down(j, act):
        pl.when(j < (layers - 1) * blocks)(lambda: for_down(j, act))

    def gu_load(n, rows):
        start(gu_state(n))

    def dn_load(n, rows):
        start(dn_state(n, rows))

    events = {
        "tile0": [(on, gu_new, 2)],
        "tile1": [(upper_down, dn.gather2, 2), (for_down, dn_load, 1)],
        "tile3": [(upper_down, dn.gather3, 3), (on, gu.event2, 1)],
        "down0": [(for_down, dn.event0)],
        "gate0": [(early, gu.gather3, 3), (for_down, dn.event1)],
        "gate1": [(on, gu.event0), (early, gu.gather4, 3), (early, gu.gather2, 2), (for_down, dn_new, 1)],
        "back0": [(upper_down, dn.gather4, 3), (on, gu.event1), (on, gu_load, 1)],
        "back1": [(for_down, dn.event2)],
    }
    longest = max(sum(ago) for these in events.values() for _, _, *ago in these)

    def step(j, _):
        busy = j < steps
        lower = layer_of(j) > 0
        changes = is_last(j) & lower & busy

        @pl.when(busy)
        def _():
            wait(weight_copies(j))
            pl.when(j + 1 < steps)(lambda: start(weight_copies(j + 1)))

        def parts(name, number, active, compute):
            def one(t, _):
                pl.when(active)(lambda: compute(j, t))
                for at in range(number):

                    @pl.when(t == at)
                    def _():
                        for stream, act, *ago in events.get(f"{name}{at}", ()):
                            stream(j - sum(ago), act)

                return 0

            lax.fori_loop(0, number, one, 0)

        def da_tiles(j, t):
            fetch = [load(a_hbm.at[0], a_tile, 2 * t + i, 0) for i in range(2)]
            pl.when(changes)(lambda: start(fetch))
            compute_da(j, t)

            @pl.when(changes)
            def _():
                for i, one in enumerate(fetch):
                    one.wait()
                    turn(a_tile, i, at_ref, strip((2 * t + i) * tile, tile))
                pl.when(t > 0)(lambda: begin_change(0))

        parts("tile", tiles, busy, compute_tile)
        pl.when(busy & (j + 1 < steps) & ~changes)(lambda: start_tile(j + 1, 0))
        parts("down", 1, busy, compute_down)
        parts("gate", 2, busy, compute_gate_up)
        parts("back", tiles // 2, busy & lower, da_tiles)

        pl.when(changes)(change_layer)

        return 0

    lax.fori_loop(0, steps + longest, step, 0)
    wait(gu_outs(steps - 1))
    wait(dn_outs(dn.number - 1, small))
    wait(dn_own(dn.number - 1, small))
    wait(gu_own(steps - 1))


def backward(mesh, a, h, dy, weights, m, v, tile=512):
    tokens, d = dy.shape
    layers, _, ff = weights[0].shape
    chips = mesh.shape["dp"] // CORES
    width = chips * LANES
    blocks = ff // width
    pairs = blocks // 2
    rows = d // (CORES * chips)
    assert layers == 2 and chips == 4 and blocks % 2 == 1 and blocks * width == ff and d % LANES == 0
    shape = lambda *s: jax.ShapeDtypeStruct(s, BF16)
    devices = CORES * chips
    outs = [
        shape(layers, rows, ff),
        shape(layers, rows, ff),
        shape(layers, ff // devices, d),
        shape(layers * blocks, devices, d, LANES),
        shape((layers - 1) * (pairs + 1), devices, d, LANES),
        shape(pairs * d + d // 2 + LATE * d, LANES),
        shape(tokens, d),
    ]

    def pool(lanes, outputs):
        return [
            pltpu.VMEM((2, CORES, chips, d, LANES), BF16),
            pltpu.VMEM((2, chips, d, LANES), BF16),
            pltpu.VMEM((lanes, 2, d // 2, LANES), BF16),
            pltpu.VMEM((lanes, 2, d, LANES), BF16),
            pltpu.VMEM((lanes, 2, d // 2, LANES), BF16),
            pltpu.VMEM((lanes, 2, d, LANES), BF16),
            pltpu.VMEM((d, LANES), BF16),
            pltpu.VMEM((d, LANES), BF16),
            pltpu.SemaphoreType.DMA((2, 5, 2)),
            pltpu.SemaphoreType.REGULAR((5,)),
            pltpu.SemaphoreType.DMA((outputs,)),
            pltpu.SemaphoreType.DMA((4, 8, 2)),
            pltpu.SemaphoreType.DMA,
        ]

    return pl.pallas_call(
        functools.partial(backward_kernel, chips, tile),
        out_shape=outs,
        in_specs=[ANY] * 12,
        out_specs=[ANY] * len(outs),
        scratch_shapes=[
            pltpu.VMEM((2, tile, d), BF16),
            pltpu.VMEM((2, tile, d), BF16),
            pltpu.VMEM((d, tokens), BF16),
            pltpu.VMEM((d, tokens), BF16),
            pltpu.VMEM((tokens, d), F32),
            pltpu.VMEM((2, d, width), BF16),
            pltpu.VMEM((2, d, width), BF16),
            pltpu.VMEM((2, width, d), BF16),
            pltpu.VMEM((tokens, width), BF16),
            pltpu.VMEM((2, tokens, width), BF16),
            pltpu.VMEM((d, LANES), F32),
            pltpu.VMEM((d, LANES), F32),
            pltpu.VMEM((d, LANES), BF16),
            pltpu.SemaphoreType.DMA((2, 3)),
            pltpu.SemaphoreType.DMA((2, 3 * chips)),
            pltpu.SemaphoreType.DMA((max(6 * chips, 3 * (d // LANES)),)),
            pltpu.SemaphoreType.DMA((2,)),
            *pool(1, 2 * chips),
            *pool(2, d // LANES),
        ],
        compiler_params=pltpu.CompilerParams(collective_id=1, has_side_effects=True, vmem_limit_bytes=VMEM_BYTES),
        cost_estimate=cost(28 * tokens * d * ff, 24 * d * ff),
        name="backward",
    )(a, h, dy, *weights, *m, *v)


class Ring:
    def __init__(self, units, slots, loads, stores, work):
        self.units, self.slots, self.loads, self.stores, self.work = units, slots, loads, stores, work

    def begin(self):
        for unit in range(self.slots):
            for copy in self.loads(unit, unit):
                copy.start()

    def run(self):
        def one(unit, _):
            slot = lax.rem(unit, self.slots)
            for copy in self.loads(unit, slot):
                copy.wait()

            @pl.when(unit >= self.slots)
            def _():
                for copy in self.stores(unit - self.slots, slot):
                    copy.wait()

            self.work(unit, slot)
            for copy in self.stores(unit, slot):
                copy.start()

            @pl.when(unit + self.slots < self.units)
            def _():
                for copy in self.loads(unit + self.slots, slot):
                    copy.start()

            return 0

        lax.fori_loop(0, self.units, one, 0)

    def end(self):
        for unit in range(self.units - self.slots, self.units):
            for copy in self.stores(unit, unit % self.slots):
                copy.wait()


def place_columns_kernel(layer, slots, x_hbm, *refs):
    gate_hbm, up_hbm, c_in, c_out, sem = refs[-5:]
    _, blocks, devices, _, chips, rows, _ = x_hbm.shape
    wide, there, some = blocks * LANES, *c_in.shape[1:3]
    spots = [j // 2 + (blocks // 2 + 1) * (j % 2) for j in range(there)]
    begins = [at for at in spots if at - 1 not in spots]
    ends = [at + 1 for at in spots if at + 1 not in spots]
    spans = list(zip(sorted(begins), sorted(ends)))
    turns = devices // some

    def place(unit):
        return unit // turns, lax.rem(unit, turns) * some

    def loads(unit, slot):
        chip, owners = place(unit)
        return [pltpu.make_async_copy(x_hbm.at[x_hbm.shape[0] - 1 - layer, head(there), pl.ds(owners, some), :, chip], c_in.at[slot], sem.at[slot, 0])]

    def stores(unit, slot):
        chip, owners = place(unit)
        copies = []
        for begin, end in spans:
            size = (end - begin) * LANES
            to = layer, strip(owners * rows, some * rows), pl.ds(pl.multiple_of(chip * wide + begin * LANES, LANES), size)
            for u, out in enumerate((gate_hbm, up_hbm)):
                copies.append(pltpu.make_async_copy(c_out.at[slot, u, :, pl.ds(begin * LANES, size)], out.at[to], sem.at[slot, 1 + len(copies)]))
        return copies

    def work(unit, slot):
        for j, at in enumerate(spots):
            for owner in range(some):
                for u in range(2):
                    c_out[slot, u, pl.ds(owner * rows, rows), lanes(at)] = c_in[slot, j, owner, u]

    ring = Ring(chips * turns, slots, loads, stores, work)
    ring.begin()
    ring.run()
    ring.end()


def place_columns(chunks, layer, layers, d, ff, into=(), slots=4, some=2):
    devices = chunks.shape[1]
    chips, rows = devices // CORES, d // devices
    x = chunks.reshape(layers, -1, devices, 2, chips, rows, LANES)
    there = x.shape[1] - LATE * (layer == 0)
    return pl.pallas_call(
        functools.partial(place_columns_kernel, layer, slots),
        in_specs=[ANY] * (1 + len(into)),
        out_specs=[ANY] * 2,
        input_output_aliases={1 + i: i for i in range(len(into))},
        out_shape=[jax.ShapeDtypeStruct((layers, d, ff), BF16)] * 2,
        scratch_shapes=[
            pltpu.VMEM((slots, there, some, 2, rows, LANES), BF16),
            pltpu.VMEM((slots, 2, some * rows, ff // chips), BF16),
            pltpu.SemaphoreType.DMA((slots, devices)),
        ],
        compiler_params=pltpu.CompilerParams(vmem_limit_bytes=VMEM_BYTES),
        cost_estimate=moves(8 * d * ff),
        name="place_columns",
    )(x, *into)


def moments_kernel(layers, parts, slots, *refs):
    states, news, s_in, g_in, s_out, sem = refs[:9], refs[9:15], refs[15:18], refs[18:21], refs[21:24], refs[24]

    def at(i, unit):
        layer, part = unit // parts, lax.rem(unit, parts)
        _, r, c = states[i].shape
        return (layer, strip(part * (r // parts), r // parts), slice(None)) if i == 2 else (layer, slice(None), strip(part * (c // parts), c // parts))

    def loads(unit, slot):
        copies = []
        for i in range(3):
            for k in range(2):
                copies.append(pltpu.make_async_copy(states[3 * k + i].at[at(i, unit)], s_in[i].at[slot, k], sem.at[slot, 5 * i + k]))
            copies.append(pltpu.make_async_copy(states[6 + i].at[at(i, unit)], g_in[i].at[slot], sem.at[slot, 5 * i + 2]))
        return copies

    def stores(unit, slot):
        return [
            pltpu.make_async_copy(s_out[i].at[slot, k], news[3 * k + i].at[at(i, unit)], sem.at[slot, 5 * i + 3 + k]) for i in range(3) for k in range(2)
        ]

    def work(unit, slot):
        for i in range(3):
            g = g_in[i][slot].astype(F32)
            s_out[i][slot, 0], s_out[i][slot, 1] = moment(s_in[i][slot, 0], s_in[i][slot, 1], g)

    ring = Ring(layers * parts, slots, loads, stores, work)
    ring.begin()
    ring.run()
    ring.end()


def moments(m, v, g, parts=9, slots=4):
    layers = m[0].shape[0]
    shapes = [(one.shape[1], one.shape[2] // parts) for one in m[:2]] + [(m[2].shape[1] // parts, m[2].shape[2])]
    size = sum(one.size for one in m)
    return pl.pallas_call(
        functools.partial(moments_kernel, layers, parts, slots),
        in_specs=[ANY] * 9,
        out_specs=[ANY] * 6,
        out_shape=[jax.ShapeDtypeStruct(one.shape, F32) for one in m] * 2,
        scratch_shapes=[
            *(pltpu.VMEM((slots, 2, *shape), F32) for shape in shapes),
            *(pltpu.VMEM((slots, *shape), BF16) for shape in shapes),
            *(pltpu.VMEM((slots, 2, *shape), F32) for shape in shapes),
            pltpu.SemaphoreType.DMA((slots, 15)),
        ],
        compiler_params=pltpu.CompilerParams(vmem_limit_bytes=VMEM_BYTES),
        cost_estimate=moves(18 * size),
        name="moments",
    )(*m, *v, *g)


def unfold(chunks, out, core):
    pairs, half = chunks.shape[0] - 1, LANES // 2
    for b in range(out.shape[1] // LANES):
        for n in range(pairs):
            out[pl.ds(pl.multiple_of(n * LANES + core * half, half), LANES), lanes(b)] = chunks[n, lanes(b), :]
        out[pl.ds(pl.multiple_of(pairs * LANES * (1 - core), half), half), lanes(b)] = chunks[pairs, pl.ds(b * half, half), :]


def place_rows_kernel(layers, slots, x_hbm, down_hbm, r_in, r_out, sem):
    devices = x_hbm.shape[2]
    pairs = x_hbm.shape[1] - 1
    height, d = r_out.shape[1:]

    def loads(unit, slot):
        layer, device = layers - 2 - unit // devices, lax.rem(unit, devices)
        return [
            pltpu.make_async_copy(x_hbm.at[layer, head(pairs), device], r_in.at[slot, head(pairs)], sem.at[slot, 0]),
            pltpu.make_async_copy(x_hbm.at[layer, pairs, device, head(d // 2)], r_in.at[slot, pairs, head(d // 2)], sem.at[slot, 1]),
        ]

    def stores(unit, slot):
        layer, device = unit // devices + 1, lax.rem(unit, devices)
        return [pltpu.make_async_copy(r_out.at[slot], down_hbm.at[layer, strip(device * height, height)], sem.at[slot, 2])]

    def work(unit, slot):
        unfold(r_in.at[slot], r_out.at[slot], lax.rem(unit, CORES))

    ring = Ring((layers - 1) * devices, slots, loads, stores, work)
    ring.begin()
    ring.run()
    ring.end()


def place_rows(chunks, layers, d, ff, slots=4):
    devices = chunks.shape[1]
    x = chunks.reshape(layers - 1, -1, devices, d, LANES)
    height = ff // devices
    return pl.pallas_call(
        functools.partial(place_rows_kernel, layers, slots),
        in_specs=[ANY],
        out_specs=ANY,
        out_shape=jax.ShapeDtypeStruct((layers, ff, d), BF16),
        scratch_shapes=[
            pltpu.VMEM((slots, x.shape[1], d, LANES), BF16),
            pltpu.VMEM((slots, height, d), BF16),
            pltpu.SemaphoreType.DMA((slots, 3)),
        ],
        compiler_params=pltpu.CompilerParams(vmem_limit_bytes=VMEM_BYTES),
        cost_estimate=moves(4 * d * ff),
        name="place_rows",
    )(x)


def place_blocks_kernel(wheres, me_ref, *refs):
    blocks, (gate_hbm, up_hbm, down_hbm, held, down, sem) = refs[: len(wheres)], refs[-6:]
    layers, d, ff = gate_hbm.shape
    height = down.shape[1]
    devices = ff // height
    chips, rows = devices // CORES, d // devices
    wide = ff // chips
    pairs = wide // LANES // 2
    chip, core = me_ref[0] // CORES, lax.rem(me_ref[0], CORES)

    def fetch(i):
        return pltpu.make_async_copy(blocks[i], held.at[i], sem.at[i, 0])

    def put(i):
        hops, flip = wheres[i]
        side = 1 - core if flip else core
        owner = lax.rem(chip + hops * (1 - 2 * side) + chips, chips) * CORES + side
        copies = [pltpu.make_async_copy(down.at[i], down_hbm.at[0, strip(owner * height, height)], sem.at[i, 1])]
        for n in range(LATE):
            step = 2 * pairs + 1 - LATE + n
            column = (step // 2 + (pairs + 1) * (step % 2)) * LANES
            for u, out in enumerate((gate_hbm, up_hbm)):
                for c in range(chips):
                    here = pl.ds(pairs * d + d // 2 + n * d + (u * chips + c) * rows, rows)
                    to = out.at[0, strip(owner * rows, rows), pl.ds(c * wide + column, LANES)]
                    copies.append(pltpu.make_async_copy(held.at[i, here], to, sem.at[i, 1 + len(copies)]))
        return side, copies

    number = len(wheres)
    for i in range(number):
        fetch(i).start()
    for i in range(number):
        fetch(i).wait()
        side, copies = put(i)
        start(copies[1:])
        for n in range(pairs + 1):
            size_n = d if n < pairs else d // 2
            for b in range(d // LANES):
                part = size_n // (d // LANES)
                at = n * LANES + side * (LANES // 2) if n < pairs else pairs * LANES * (1 - side)
                down[i, pl.ds(pl.multiple_of(at, LANES // 2), part), lanes(b)] = held[i, pl.ds(n * d + b * part, part), :]
        copies[0].start()
    for i in range(number):
        wait(put(i)[1])


def place_blocks(me, blocks, weights):
    wheres, blocks = tuple(blocks), list(blocks.values())
    number, rows = len(blocks), blocks[0].shape[0]
    layers, ff, d = weights[2].shape
    height = rows * LANES // d - LATE * LANES
    return pl.pallas_call(
        functools.partial(place_blocks_kernel, wheres),
        in_specs=[pl.BlockSpec(memory_space=pltpu.SMEM)] + [ANY] * (number + 3),
        out_specs=[ANY] * 3,
        out_shape=[jax.ShapeDtypeStruct(one.shape, BF16) for one in weights],
        input_output_aliases={number + 1 + i: i for i in range(3)},
        scratch_shapes=[
            pltpu.VMEM((number, rows, LANES), BF16),
            pltpu.VMEM((number, height, d), BF16),
            pltpu.SemaphoreType.DMA((number, 2 + LATE * ff // height)),
        ],
        compiler_params=pltpu.CompilerParams(vmem_limit_bytes=VMEM_BYTES),
        name="place_blocks",
    )(me, *blocks, *weights)


def solution(mesh):
    group = mesh.shape["dp"]
    swap = [(i, i ^ 1) for i in range(group)]
    onward = [(i, (i + CORES * (1 - 2 * (i % CORES))) % group) for i in range(group)]
    back = [(to, i) for i, to in onward]

    def step(x, dy, *arrays):
        weights, m, v = (arrays[i : i + 3] for i in (0, 3, 6))
        layers, d, ff = weights[0].shape
        me = lax.axis_index("dp").reshape(1)
        *sums, columns, rows, own, _ = backward(mesh, *forward(x[0], *weights, 0), dy[0], weights, m, v)

        def send(block, to):
            return lax.ppermute(block, "dp", to)

        behind, ahead = send(own, onward), send(own, back)
        gate, up = place_columns(columns, 1, layers, d, ff)
        first, *states = moments(m, v, sums)
        gate, first, behind, ahead = lax.optimization_barrier((gate, first, behind, ahead))
        opposite = send(behind, onward)
        near = {(0, 0): own, (-1, 0): behind, (1, 0): ahead}
        other = {(hops, 1): send(block, swap) for (hops, _), block in near.items()}
        gate, up = place_columns(columns, 0, layers, d, ff, (gate, up))
        up, rows = lax.optimization_barrier((up, rows))
        down = place_rows(rows, layers, d, ff)
        gate, up, down = place_blocks(me, near, (gate, up, down))
        down, opposite = lax.optimization_barrier((down, opposite))
        last = send(opposite, swap)
        weights = place_blocks(me, other, (gate, up, down))
        weights = place_blocks(me, {(2, 0): opposite, (2, 1): last}, weights)
        return (*weights, first, *states)

    seq, whole, rows = P(("rep", "dp"), None, None), P(None, None, None), P(None, "dp", None)
    return jax.shard_map(
        step,
        mesh=mesh,
        in_specs=(seq, seq, whole, whole, whole) + (rows,) * 6,
        out_specs=(P("rep", None, None),) * 3 + (P("rep", "dp", None),) * 6,
        check_vma=False,
    )
```

```python
import functools

import jax
import jax.numpy as jnp
from jax import lax
from jax.experimental import pallas as pl
from jax.experimental.pallas import tpu as pltpu
from jax.sharding import PartitionSpec as P

F32, BF16 = jnp.float32, jnp.bfloat16
NN, NT = (((1,), (0,)), ((), ())), (((1,), (1,)), ((), ()))
MESH = pl.DeviceIdType.MESH
ANY = pl.BlockSpec(memory_space=pl.ANY)
LANES = 128
CORES = 2
VMEM_BYTES = 67_043_328
COPY_FLOPS = 64
LATE = 2
SIDES = (0, 1), (1, -1)


def dot(a, b, dims=NN):
    return lax.dot_general(a, b, dims, preferred_element_type=F32)


def norm(h):
    wide = h.astype(F32)
    return (wide * lax.rsqrt(jnp.mean(wide**2, -1, keepdims=True) + 1e-6)).astype(BF16)


def strip(start, size):
    return pl.ds(pl.multiple_of(start, size), size)


def head(size):
    return pl.ds(0, size)


def parity(n):
    return lax.rem(n, 2)


def lanes(n):
    return pl.ds(n * LANES, LANES)


def start(copies):
    for copy in copies:
        copy.start()


def wait(copies):
    for copy in copies:
        copy.wait()


def moves(moved):
    return cost(COPY_FLOPS * moved, moved)


def cost(flops, moved):
    return pl.CostEstimate(flops=flops, bytes_accessed=moved, transcendentals=moved)


def forward_kernel(tile, x_ref, wg_ref, wu_ref, wd_ref, a_hbm, h_hbm, a_ref, total, ends, a_sem, end_sem):
    block = pl.program_id(0)
    first, last = block == 0, block == pl.num_programs(0) - 1
    tiles = x_ref.shape[0] // tile

    def keep(t):
        rows = strip(t * tile, tile)
        return pltpu.make_async_copy(a_ref.at[rows], a_hbm.at[0, rows], a_sem.at[t])

    def finish(t):
        rows = strip(t * tile, tile)
        for i, out in enumerate((h_hbm, a_hbm.at[1])):
            yield pltpu.make_async_copy(ends.at[parity(t), i], out.at[rows], end_sem.at[parity(t), i])

    @pl.when(first)
    def _():
        def begin(t, _):
            rows = strip(t * tile, tile)
            a_ref[rows, :] = norm(x_ref[rows, :])
            total[rows, :] = jnp.zeros((tile, total.shape[1]), F32)
            keep(t).start()
            return t

        lax.fori_loop(0, tiles, begin, 0)

    def one(t, _):
        rows = strip(t * tile, tile)
        a = a_ref[rows, :]
        gate, up = dot(a, wg_ref[...]), dot(a, wu_ref[...])
        z = (jax.nn.sigmoid(gate) * gate * up).astype(BF16)
        total[rows, :] += dot(z, wd_ref[...])

        @pl.when(last)
        def _():
            keep(t).wait()
            pl.when(t >= 2)(lambda: wait(finish(t - 2)))
            h = x_ref[rows, :] + total[rows, :].astype(BF16)
            for i, end in enumerate((h, norm(h))):
                ends[parity(t), i] = end
            start(finish(t))

        return t

    lax.fori_loop(0, tiles, one, 0)

    @pl.when(last)
    def _():
        for t in range(tiles - 2, tiles):
            wait(finish(t))


def forward(x, wg, wu, wd, layer, width=768, tile=512):
    tokens, d = x.shape
    ff = wg.shape[2]
    state = jax.ShapeDtypeStruct((tokens, d), BF16)
    columns = pl.BlockSpec((None, d, width), lambda i: (layer, 0, i))
    return pl.pallas_call(
        functools.partial(forward_kernel, tile),
        grid=(ff // width,),
        out_shape=[jax.ShapeDtypeStruct((2, tokens, d), BF16), state],
        in_specs=[pl.BlockSpec(x.shape, lambda i: (0, 0)), columns, columns, pl.BlockSpec((None, width, d), lambda i: (layer, i, 0))],
        out_specs=[ANY] * 2,
        scratch_shapes=[
            pltpu.VMEM(x.shape, BF16),
            pltpu.VMEM(x.shape, F32),
            pltpu.VMEM((2, 2, tile, d), BF16),
            pltpu.SemaphoreType.DMA((tokens // tile,)),
            pltpu.SemaphoreType.DMA((2, 2)),
        ],
        compiler_params=pltpu.CompilerParams(vmem_limit_bytes=VMEM_BYTES),
        cost_estimate=cost(6 * tokens * d * ff, 6 * d * ff),
        name="forward",
    )(x, wg, wu, wd)


class Pool:
    def __init__(self, number, chips, core, chip, bufs, sems, gathered):
        self.number, self.chips, self.core, self.chip = number, chips, core, chip
        self.mine, self.other, self.cross, self.near, self.out1, self.out2, self.sum, self.new = bufs
        self.dma, self.credit, self.out_sem, self.ag_sem, self.own_sem = sems
        self.gathered = gathered
        self.slots, self.lanes, self.turns = self.mine.shape[0], self.cross.shape[0], self.ag_sem.shape[0]

    def index(self, chip, core):
        return lax.rem(chip + self.chips, self.chips) * CORES + core

    def device(self, hops, core=None):
        return {"dp": self.index(self.chip + hops, self.core if core is None else core)}

    def partner(self):
        return self.device(0, 1 - self.core)

    def hop(self, sems, src, dst, to):
        return pltpu.make_async_remote_copy(src_ref=src, dst_ref=dst, send_sem=sems.at[0], recv_sem=sems.at[1], device_id=to, device_id_type=MESH)

    def copies0(self, n, rows):
        slot = lax.rem(n, self.slots)
        src = self.mine.at[slot, 1 - self.core, :, head(rows), :]
        return [self.hop(self.dma.at[slot, 0], src, self.other.at[slot, :, head(rows), :], self.partner())]

    def copies1(self, n, rows):
        slot, sem, half = lax.rem(n, self.lanes), lax.rem(n, self.slots), head(rows // 2)
        return [self.hop(self.dma.at[sem, 1 + side], self.out1.at[slot, side, half], self.cross.at[slot, side, half], self.device(hop)) for side, hop in SIDES]

    def copies2(self, n, rows):
        slot, sem, full = lax.rem(n, self.lanes), lax.rem(n, self.slots), head(rows)
        return [self.hop(self.dma.at[sem, 3 + side], self.out2.at[slot, side, full], self.near.at[slot, side, full], self.device(hop)) for side, hop in SIDES]

    def both(self, n, hops, start, size):
        slot, chip = lax.rem(n, self.slots), lax.rem(self.chip + hops + self.chips, self.chips)
        rows = pl.ds(start, size)
        return self.mine[slot, self.core, chip, rows, :].astype(F32) + self.other[slot, chip, rows, :].astype(F32)

    def give(self, kind, to):
        pl.semaphore_signal(self.credit.at[kind], inc=1, device_id=to, device_id_type=MESH)

    def take(self, when, kinds):
        @pl.when(when)
        def _():
            for kind in kinds:
                pl.semaphore_wait(self.credit.at[kind], 1)

    def event0(self, n, rows):
        self.take(n >= self.slots, (0,))
        start(self.copies0(n, rows))

    def event1(self, n, rows):
        slot, half = lax.rem(n, self.lanes), rows // 2
        wait(self.copies0(n, rows))
        for side, _ in SIDES:
            self.out1[slot, side, head(half)] = self.both(n, 2, side * half, half).astype(BF16)
        self.take(n >= self.lanes, (1, 2))
        start(self.copies1(n, rows))

    def event2(self, n, rows):
        slot, half = lax.rem(n, self.lanes), rows // 2
        wait(self.copies1(n, rows))
        for side, hop in SIDES:
            passed = self.both(n, hop, side * half, half) + self.cross[slot, side, head(half)].astype(F32)
            self.out2[slot, side, pl.ds(side * half, half), :] = passed.astype(BF16)
            self.out2[slot, side, pl.ds(half - side * half, half), :] = self.both(n, hop, half - side * half, half).astype(BF16)

        @pl.when(n + self.lanes < self.number)
        def _():
            for side, hop in SIDES:
                self.give(1 + side, self.device(-hop))

        self.take(n >= self.lanes, (3, 4))
        start(self.copies2(n, rows))

    def total(self, n, start, size):
        total = self.both(n, 0, start, size)
        for side, _ in SIDES:
            total += self.near[lax.rem(n, self.lanes), side, pl.ds(start, size), :].astype(F32)
        return total.astype(BF16).astype(F32)

    def event3(self, n, rows):
        wait(self.copies2(n, rows))

    def after3(self, n):
        pl.when(n + self.slots < self.number)(lambda: self.give(0, self.partner()))

        @pl.when(n + self.lanes < self.number)
        def _():
            for side, hop in SIDES:
                self.give(3 + side, self.device(-hop))

    def block(self, n, hops, core, start, size):
        return self.gathered.at[n, self.index(self.chip + hops, core), pl.ds(start, size), :]

    def sems(self, n, kind):
        return self.ag_sem.at[lax.rem(n, self.turns), kind]

    def gathers1(self, n, rows):
        new, own = self.new.at[head(rows)], self.block(n, 0, self.core, 0, rows)
        copies = [self.hop(self.sems(n, side), new, own, self.device(hop)) for side, hop in SIDES]
        return [*copies, self.hop(self.sems(n, 7), new, own, self.partner()), pltpu.make_async_copy(new, own, self.own_sem)]

    def gathers2(self, n, rows):
        copies, half = [], rows // 2
        for side, hop in SIDES:
            part, full = (self.block(n, -hop, self.core, *which) for which in ((side * half, half), (0, rows)))
            copies.append(self.hop(self.sems(n, 2 + side), part, part, self.device(hop)))
            copies.append(self.hop(self.sems(n, 4 + side), full, full, self.partner()))
        return copies

    def gathers3(self, n, rows):
        opposite = self.block(n, 2, self.core, 0, rows)
        return [self.hop(self.sems(n, 6), opposite, opposite, self.partner())]

    def gather1(self, n, rows):
        start(self.gathers1(n, rows))

    def gather2(self, n, rows):
        wait(self.gathers1(n, rows))
        start(self.gathers2(n, rows))

    def gather3(self, n, rows):
        wait(self.gathers2(n, rows))
        start(self.gathers3(n, rows))

    def gather4(self, n, rows):
        wait(self.gathers3(n, rows))


def moment(m, v, g):
    return 0.9 * m + 0.1 * g, 0.95 * v + 0.05 * g * g


def adam(w, m, v, g):
    m, v = moment(m, v, g)
    w = w.astype(F32)
    return (w - 0.02 * (m * lax.rsqrt(v + 1e-8) + 0.1 * w)).astype(BF16)


def backward_kernel(chips, tile, *refs):
    a_hbm, h_hbm, dy_hbm, wg_hbm, wu_hbm, wd_hbm, mg_hbm, mu_hbm, md_hbm, vg_hbm, vu_hbm, vd_hbm, *refs = refs
    gg_hbm, gu_hbm, gd_hbm, whole_gu, whole_dn, own_hbm, dy0_hbm, *refs = refs
    a_tile, dy_tile, at_ref, dyt_ref, da_ref, wg_ref, wu_ref, wd_ref, z_ref, dgu_ref, m_ref, v_ref, w_ref, *refs = refs
    tile_sem, w_sem, state_sem, own_sem, *pools = refs
    tokens, d = dy_hbm.shape
    layers, _, ff = wg_hbm.shape
    width = chips * LANES
    blocks = ff // width
    pairs = blocks // 2
    rows = d // (CORES * chips)
    lane_blocks = d // LANES
    me = lax.axis_index("dp")
    chip, core = me // CORES, lax.rem(me, CORES)
    tiles = tokens // tile
    steps = layers * blocks
    full, small, small_tile = d, d // 2, tile // 4

    gu = Pool(steps, chips, core, chip, pools[0:8], pools[8:13], whole_gu)
    dn = Pool(layers * (pairs + 1), chips, core, chip, pools[13:21], pools[21:26], whole_dn)

    def layer_of(j):
        return layers - 1 - j // blocks

    def block_of(j):
        j = lax.rem(j, blocks)
        return j // 2 + (pairs + 1) * parity(j)

    def columns(c, j):
        return strip(c * blocks * LANES + block_of(j) * LANES, LANES)

    def is_last(j):
        return lax.rem(j, blocks) == blocks - 1

    def gives_down(j):
        return (j >= 0) & (j < steps) & ((parity(lax.rem(j, blocks)) == 1) | is_last(j))

    def down_of(j):
        return (j // blocks) * (pairs + 1) + lax.rem(j, blocks) // 2

    def for_down(j, act):
        @pl.when(gives_down(j) & ~is_last(j))
        def _():
            act(down_of(j), full)

        @pl.when(gives_down(j) & is_last(j))
        def _():
            act(down_of(j), small)

    def weight_copies(j):
        layer, slot = layer_of(j), parity(j)
        for c in range(chips):
            there, here = columns(c, j), lanes(c)
            yield pltpu.make_async_copy(wg_hbm.at[layer, :, there], wg_ref.at[slot, :, here], w_sem.at[slot, 3 * c])
            yield pltpu.make_async_copy(wu_hbm.at[layer, :, there], wu_ref.at[slot, :, here], w_sem.at[slot, 3 * c + 1])
            yield pltpu.make_async_copy(wd_hbm.at[layer, there, :], wd_ref.at[slot, here, :], w_sem.at[slot, 3 * c + 2])

    def load(src, buf, t, which):
        slot = parity(t)
        return pltpu.make_async_copy(src.at[strip(t * tile, tile), :], buf.at[slot], tile_sem.at[slot, which])

    def start_tile(j, t):
        load(a_hbm.at[layer_of(j)], a_tile, t, 0).start()

        @pl.when(layer_of(j) == layers - 1)
        def _():
            load(dy_hbm, dy_tile, t, 1).start()

        @pl.when(layer_of(j) < layers - 1)
        def _():
            load(dy0_hbm, dy_tile, t, 1).start()

    def wait_tile(t):
        load(dy_hbm, a_tile, t, 0).wait()
        load(dy_hbm, dy_tile, t, 1).wait()

    def gu_parts(n):
        for c in range(chips):
            for u in range(2):
                yield u * chips + c, u, pl.ds((u * chips + c) * rows, rows), columns(c, n)

    def gu_outs(n):
        for i, u, here, there in gu_parts(n):
            yield pltpu.make_async_copy(gu.sum.at[here, :], (gg_hbm, gu_hbm)[u].at[layer_of(n), :, there], gu.out_sem.at[i])

    def gu_state(n):
        layer = layer_of(n)
        for i, u, here, there in gu_parts(n):
            for k, (src, buf) in enumerate((((mg_hbm, mu_hbm)[u], m_ref), ((vg_hbm, vu_hbm)[u], v_ref))):
                yield pltpu.make_async_copy(src.at[layer, :, there], buf.at[here, :], state_sem.at[3 * i + k])
            src = (wg_hbm, wu_hbm)[u].at[layer, strip(me * rows, rows), there]
            yield pltpu.make_async_copy(src, w_ref.at[here, :], state_sem.at[3 * i + 2])

    def dn_parts(n, size):
        step = lax.rem(n, pairs + 1)
        start = step * LANES + core * (LANES // 2) if size == full else pairs * LANES * (1 - core)
        height = size // lane_blocks
        for b in range(lane_blocks):
            yield b, layers - 1 - n // (pairs + 1), start, height, pl.ds(b * height, height), lanes(b)

    def dn_outs(n, size):
        for b, layer, start, height, here, there in dn_parts(n, size):
            at = pl.ds(pl.multiple_of(start, LANES // 2), height)
            yield pltpu.make_async_copy(dn.sum.at[here, :], gd_hbm.at[layer, at, there], dn.out_sem.at[b])

    def own_out(pool, at, size, sem):
        return [pltpu.make_async_copy(pool.new.at[head(size)], own_hbm.at[pl.ds(pl.multiple_of(at, LANES // 2), size)], own_sem.at[sem])]

    def dn_own(n, size):
        return own_out(dn, (n - (layers - 1) * (pairs + 1)) * full, size, 0)

    def gu_own(n):
        return own_out(gu, pairs * full + small + (n - steps + LATE) * full, full, 1)

    def dn_state(n, size):
        for b, layer, start, height, here, there in dn_parts(n, size):
            at = pl.ds(pl.multiple_of(start, LANES // 2), height)
            for k, (src, buf) in enumerate(((md_hbm, m_ref), (vd_hbm, v_ref))):
                yield pltpu.make_async_copy(src.at[layer, at, there], buf.at[here, :], state_sem.at[3 * b + k])
            at = pl.ds(pl.multiple_of(me * (d // 2) + start, LANES // 2), height)
            yield pltpu.make_async_copy(wd_hbm.at[layer, at, there], w_ref.at[here, :], state_sem.at[3 * b + 2])

    some = d // 3

    def gu_new(n, size):
        gu.event3(n, size)
        pl.when(n > 0)(lambda: wait(gu_outs(n - 1)))
        wait(gu_state(n))
        late = n >= steps - LATE
        pl.when(n > steps - LATE)(lambda: wait(gu_own(n - 1)))

        def piece(i, _):
            at = strip(i * some, some)
            g = gu.total(n, i * some, some)
            gu.sum[at, :] = g.astype(BF16)
            gu.new[at, :] = adam(w_ref[at, :], m_ref[at, :], v_ref[at, :], g)
            return i

        lax.fori_loop(0, size // some, piece, 0)
        gu.after3(n)
        start(gu_outs(n))
        pl.when(~late)(lambda: gu.gather1(n, size))
        pl.when(late)(lambda: start(gu_own(n)))

    def dn_new(n, size):
        half, height = LANES // 2, size // lane_blocks
        dn.event3(n, size)
        if size == full:
            begins = lax.rem(n, pairs + 1) == 0
            pl.when((n > 0) & ~begins)(lambda: wait(dn_outs(n - 1, full)))
            pl.when((n > 0) & begins)(lambda: wait(dn_outs(n - 1, small)))
        else:
            wait(dn_outs(n - 1, full))
        wait(dn_state(n, size))
        upper = n < (layers - 1) * (pairs + 1)
        pl.when(n > (layers - 1) * (pairs + 1))(lambda: wait(dn_own(n - 1, full)))

        def finish(at, g):
            dn.sum[at, :] = g.astype(BF16)
            dn.new[at, :] = adam(w_ref[at, :], m_ref[at, :], v_ref[at, :], g)

        if size == full:

            def piece(i, _):
                for start in range(0, some, LANES):
                    finish(strip(i * some + start, LANES), dn.total(n, i * some + start, LANES).T)
                return i

            lax.fori_loop(0, size // some, piece, 0)
        else:
            g = dn.total(n, 0, size).T
            g = jnp.concatenate([g[:half], g[half:]], 1)
            for b in range(lane_blocks):
                finish(pl.ds(b * height, height), g[:, b * LANES : (b + 1) * LANES])
        dn.after3(n)
        start(dn_outs(n, size))
        pl.when(upper)(lambda: dn.gather1(n, size))
        pl.when(~upper)(lambda: start(dn_own(n, size)))

    def turn(buf, slot, into, part):
        for b in range(lane_blocks):
            into[lanes(b), part] = buf[slot, :, b * LANES : (b + 1) * LANES].T

    start_tile(0, 0)
    start(weight_copies(0))
    barrier = pltpu.get_barrier_semaphore()
    peers = (gu.partner(), gu.device(1), gu.device(-1))
    for peer in peers:
        pl.semaphore_signal(barrier, inc=1, device_id=peer, device_id_type=MESH)
    pl.semaphore_wait(barrier, len(peers))

    def keep(t):
        slot = parity(t)
        return pltpu.make_async_copy(dy_tile.at[slot], dy0_hbm.at[strip(t * tile, tile)], tile_sem.at[slot, 2])

    def compute_tile(j, t):
        slot, here = parity(j), parity(t)
        part = strip(t * tile, tile)
        wait_tile(t)
        pl.when(t + 1 < tiles)(lambda: start_tile(j, t + 1))
        a, dy = a_tile[here], dy_tile[here]
        for c in range(0, chips, 2):
            some = pl.ds(c * LANES, 2 * LANES)
            gate = dot(a, wg_ref[slot, :, some])
            up = dot(a, wu_ref[slot, :, some])
            dz = dot(dy, wd_ref[slot, some, :], NT).astype(BF16).astype(F32)
            s = jax.nn.sigmoid(gate)
            act = s * gate
            z_ref[part, some] = (act * up).astype(BF16)
            dgu_ref[1, part, some] = (dz * act).astype(BF16)
            dgu_ref[0, part, some] = (dz * up * (s + act * (1 - s))).astype(BF16)

        turn(a_tile, here, at_ref, part)
        turn(dy_tile, here, dyt_ref, part)

        @pl.when(j == 0)
        def _():
            da_ref[part, :] = jnp.zeros((tile, d), F32)

    def compute_gate_up(j, u):
        slot = lax.rem(j, gu.slots)
        g = dot(at_ref[...], dgu_ref[u]).astype(BF16)
        for c in range(chips):
            at = strip((u * chips + c) * rows, rows)
            for owner in range(CORES * chips):
                gu.mine[slot, owner % CORES, owner // CORES, at, :] = g[owner * rows : (owner + 1) * rows, c * LANES : (c + 1) * LANES]

    def compute_down(j, _):
        slot, owner = lax.rem(down_of(j), dn.slots), parity(lax.rem(j, blocks))

        @pl.when(~is_last(j))
        def _():
            g = dot(dyt_ref[...], z_ref[...]).astype(BF16)
            for c in range(chips):
                dn.mine[slot, owner, c, :, :] = g[:, c * LANES : (c + 1) * LANES]

        @pl.when(is_last(j))
        def _():
            half = LANES // 2
            low = lax.broadcasted_iota(jnp.int32, (small, LANES), 1) < half

            def one(h, _):
                both = dot(dyt_ref[...], z_ref[:, strip(h * 2 * LANES, 2 * LANES)])
                for c in range(2):
                    straight = both[:, c * LANES : (c + 1) * LANES]
                    turned = pltpu.roll(straight, half, 1)
                    dn.mine[slot, 0, 2 * h + c, head(small), :] = jnp.where(low, straight[:small], turned[small:]).astype(BF16)
                    dn.mine[slot, 1, 2 * h + c, head(small), :] = jnp.where(low, turned[:small], straight[small:]).astype(BF16)
                return h

            lax.fori_loop(0, chips // 2, one, 0)

    def compute_da(j, t):
        slot, part = parity(j), strip(t * 2 * tile, 2 * tile)
        middle = lane_blocks // 2 * LANES
        for begin, end in ((0, middle), (middle, d)):
            some = pl.ds(begin, end - begin)
            da_ref[part, some] += dot(dgu_ref[0, part, :], wg_ref[slot, some, :], NT) + dot(dgu_ref[1, part, :], wu_ref[slot, some, :], NT)

    def begin_change(t):
        load(h_hbm, a_tile, t, 0).start()
        load(dy_hbm, dy_tile, t, 1).start()

    def change_layer():
        def one(t, _):
            slot = parity(t)
            wait_tile(t)
            pl.when(t > 0)(lambda: keep(t - 1).wait())
            pl.when(t + 1 < tiles)(lambda: begin_change(t + 1))
            pl.when(t + 1 == tiles)(lambda: start_tile(blocks, 0))

            def piece(i, _):
                here, there = strip(i * small_tile, small_tile), strip(t * tile + i * small_tile, small_tile)
                wide = a_tile[slot, here, :].astype(F32)
                da = da_ref[there, :].astype(BF16).astype(F32)
                scale = lax.rsqrt(jnp.mean(wide * wide, -1, keepdims=True) + 1e-6)
                along = jnp.mean(da * wide, -1, keepdims=True)
                back = (da * scale - wide * (along * scale * scale * scale)).astype(BF16)
                dy_tile[slot, here, :] = dy_tile[slot, here, :] + back
                return 0

            lax.fori_loop(0, tile // small_tile, piece, 0)
            keep(t).start()
            return 0

        lax.fori_loop(0, tiles, one, 0)
        keep(tiles - 1).wait()

    def on(j, act):
        pl.when((j >= 0) & (j < steps))(lambda: act(j, full))

    def early(j, act):
        pl.when(j < steps - LATE)(lambda: on(j, act))

    def upper_down(j, act):
        pl.when(j < (layers - 1) * blocks)(lambda: for_down(j, act))

    def gu_load(n, rows):
        start(gu_state(n))

    def dn_load(n, rows):
        start(dn_state(n, rows))

    events = {
        "tile0": [(on, gu_new, 2)],
        "tile1": [(upper_down, dn.gather2, 2), (for_down, dn_load, 1)],
        "tile3": [(upper_down, dn.gather3, 3), (on, gu.event2, 1)],
        "down0": [(for_down, dn.event0)],
        "gate0": [(early, gu.gather3, 3), (for_down, dn.event1)],
        "gate1": [(on, gu.event0), (early, gu.gather4, 3), (early, gu.gather2, 2), (for_down, dn_new, 1)],
        "back0": [(upper_down, dn.gather4, 3), (on, gu.event1), (on, gu_load, 1)],
        "back1": [(for_down, dn.event2)],
    }
    longest = max(sum(ago) for these in events.values() for _, _, *ago in these)

    def step(j, _):
        busy = j < steps
        lower = layer_of(j) > 0
        changes = is_last(j) & lower & busy

        @pl.when(busy)
        def _():
            wait(weight_copies(j))
            pl.when(j + 1 < steps)(lambda: start(weight_copies(j + 1)))

        def parts(name, number, active, compute):
            def one(t, _):
                pl.when(active)(lambda: compute(j, t))
                for at in range(number):

                    @pl.when(t == at)
                    def _():
                        for stream, act, *ago in events.get(f"{name}{at}", ()):
                            stream(j - sum(ago), act)

                return 0

            lax.fori_loop(0, number, one, 0)

        def da_halves(j, t):
            pl.when(changes & (t == 0))(lambda: begin_change(0))
            compute_da(j, t)

        parts("tile", tiles, busy, compute_tile)
        pl.when(busy & (j + 1 < steps) & ~changes)(lambda: start_tile(j + 1, 0))
        parts("down", 1, busy, compute_down)
        parts("gate", 2, busy, compute_gate_up)
        parts("back", tiles // 2, busy & lower, da_halves)

        pl.when(changes)(change_layer)

        return 0

    lax.fori_loop(0, steps + longest, step, 0)
    wait(gu_outs(steps - 1))
    wait(dn_outs(dn.number - 1, small))
    wait(dn_own(dn.number - 1, small))
    wait(gu_own(steps - 1))


def backward(mesh, a, h, dy, weights, m, v, tile=512):
    tokens, d = dy.shape
    layers, _, ff = weights[0].shape
    chips = mesh.shape["dp"] // CORES
    width = chips * LANES
    blocks = ff // width
    pairs = blocks // 2
    rows = d // (CORES * chips)
    assert layers == 2 and chips == 4 and blocks % 2 == 1 and blocks * width == ff and d % LANES == 0
    shape = lambda *s: jax.ShapeDtypeStruct(s, BF16)
    devices = CORES * chips
    outs = [
        shape(layers, rows, ff),
        shape(layers, rows, ff),
        shape(layers, ff // devices, d),
        shape(layers * blocks, devices, d, LANES),
        shape((layers - 1) * (pairs + 1), devices, d, LANES),
        shape(pairs * d + d // 2 + LATE * d, LANES),
        shape(tokens, d),
    ]

    def pool(lanes, outputs):
        return [
            pltpu.VMEM((2, CORES, chips, d, LANES), BF16),
            pltpu.VMEM((2, chips, d, LANES), BF16),
            pltpu.VMEM((lanes, 2, d // 2, LANES), BF16),
            pltpu.VMEM((lanes, 2, d, LANES), BF16),
            pltpu.VMEM((lanes, 2, d // 2, LANES), BF16),
            pltpu.VMEM((lanes, 2, d, LANES), BF16),
            pltpu.VMEM((d, LANES), BF16),
            pltpu.VMEM((d, LANES), BF16),
            pltpu.SemaphoreType.DMA((2, 5, 2)),
            pltpu.SemaphoreType.REGULAR((5,)),
            pltpu.SemaphoreType.DMA((outputs,)),
            pltpu.SemaphoreType.DMA((4, 8, 2)),
            pltpu.SemaphoreType.DMA,
        ]

    return pl.pallas_call(
        functools.partial(backward_kernel, chips, tile),
        out_shape=outs,
        in_specs=[ANY] * 12,
        out_specs=[ANY] * len(outs),
        scratch_shapes=[
            pltpu.VMEM((2, tile, d), BF16),
            pltpu.VMEM((2, tile, d), BF16),
            pltpu.VMEM((d, tokens), BF16),
            pltpu.VMEM((d, tokens), BF16),
            pltpu.VMEM((tokens, d), F32),
            pltpu.VMEM((2, d, width), BF16),
            pltpu.VMEM((2, d, width), BF16),
            pltpu.VMEM((2, width, d), BF16),
            pltpu.VMEM((tokens, width), BF16),
            pltpu.VMEM((2, tokens, width), BF16),
            pltpu.VMEM((d, LANES), F32),
            pltpu.VMEM((d, LANES), F32),
            pltpu.VMEM((d, LANES), BF16),
            pltpu.SemaphoreType.DMA((2, 3)),
            pltpu.SemaphoreType.DMA((2, 3 * chips)),
            pltpu.SemaphoreType.DMA((max(6 * chips, 3 * (d // LANES)),)),
            pltpu.SemaphoreType.DMA((2,)),
            *pool(1, 2 * chips),
            *pool(2, d // LANES),
        ],
        compiler_params=pltpu.CompilerParams(collective_id=1, has_side_effects=True, vmem_limit_bytes=VMEM_BYTES),
        cost_estimate=cost(28 * tokens * d * ff, 24 * d * ff),
        name="backward",
    )(a, h, dy, *weights, *m, *v)


class Ring:
    def __init__(self, units, slots, loads, stores, work):
        self.units, self.slots, self.loads, self.stores, self.work = units, slots, loads, stores, work

    def begin(self):
        for unit in range(self.slots):
            for copy in self.loads(unit, unit):
                copy.start()

    def run(self):
        def one(unit, _):
            slot = lax.rem(unit, self.slots)
            for copy in self.loads(unit, slot):
                copy.wait()

            @pl.when(unit >= self.slots)
            def _():
                for copy in self.stores(unit - self.slots, slot):
                    copy.wait()

            self.work(unit, slot)
            for copy in self.stores(unit, slot):
                copy.start()

            @pl.when(unit + self.slots < self.units)
            def _():
                for copy in self.loads(unit + self.slots, slot):
                    copy.start()

            return 0

        lax.fori_loop(0, self.units, one, 0)

    def end(self):
        for unit in range(self.units - self.slots, self.units):
            for copy in self.stores(unit, unit % self.slots):
                copy.wait()


def place_columns_kernel(layer, slots, x_hbm, *refs):
    gate_hbm, up_hbm, c_in, c_out, sem = refs[-5:]
    _, blocks, devices, _, chips, rows, _ = x_hbm.shape
    wide, there, some = blocks * LANES, *c_in.shape[1:3]
    spots = [j // 2 + (blocks // 2 + 1) * (j % 2) for j in range(there)]
    begins = [at for at in spots if at - 1 not in spots]
    ends = [at + 1 for at in spots if at + 1 not in spots]
    spans = list(zip(sorted(begins), sorted(ends)))
    turns = devices // some

    def place(unit):
        return unit // turns, lax.rem(unit, turns) * some

    def loads(unit, slot):
        chip, owners = place(unit)
        return [pltpu.make_async_copy(x_hbm.at[x_hbm.shape[0] - 1 - layer, head(there), pl.ds(owners, some), :, chip], c_in.at[slot], sem.at[slot, 0])]

    def stores(unit, slot):
        chip, owners = place(unit)
        copies = []
        for begin, end in spans:
            size = (end - begin) * LANES
            to = layer, strip(owners * rows, some * rows), pl.ds(pl.multiple_of(chip * wide + begin * LANES, LANES), size)
            for u, out in enumerate((gate_hbm, up_hbm)):
                copies.append(pltpu.make_async_copy(c_out.at[slot, u, :, pl.ds(begin * LANES, size)], out.at[to], sem.at[slot, 1 + len(copies)]))
        return copies

    def work(unit, slot):
        for j, at in enumerate(spots):
            for owner in range(some):
                for u in range(2):
                    c_out[slot, u, pl.ds(owner * rows, rows), lanes(at)] = c_in[slot, j, owner, u]

    ring = Ring(chips * turns, slots, loads, stores, work)
    ring.begin()
    ring.run()
    ring.end()


def place_columns(chunks, layer, layers, d, ff, into=(), slots=4, some=2):
    devices = chunks.shape[1]
    chips, rows = devices // CORES, d // devices
    x = chunks.reshape(layers, -1, devices, 2, chips, rows, LANES)
    there = x.shape[1] - LATE * (layer == 0)
    return pl.pallas_call(
        functools.partial(place_columns_kernel, layer, slots),
        in_specs=[ANY] * (1 + len(into)),
        out_specs=[ANY] * 2,
        input_output_aliases={1 + i: i for i in range(len(into))},
        out_shape=[jax.ShapeDtypeStruct((layers, d, ff), BF16)] * 2,
        scratch_shapes=[
            pltpu.VMEM((slots, there, some, 2, rows, LANES), BF16),
            pltpu.VMEM((slots, 2, some * rows, ff // chips), BF16),
            pltpu.SemaphoreType.DMA((slots, devices)),
        ],
        compiler_params=pltpu.CompilerParams(vmem_limit_bytes=VMEM_BYTES),
        cost_estimate=moves(8 * d * ff),
        name="place_columns",
    )(x, *into)


def moments_kernel(layers, parts, slots, *refs):
    states, news, s_in, g_in, s_out, sem = refs[:9], refs[9:15], refs[15:18], refs[18:21], refs[21:24], refs[24]

    def at(i, unit):
        layer, part = unit // parts, lax.rem(unit, parts)
        _, r, c = states[i].shape
        return (layer, strip(part * (r // parts), r // parts), slice(None)) if i == 2 else (layer, slice(None), strip(part * (c // parts), c // parts))

    def loads(unit, slot):
        copies = []
        for i in range(3):
            for k in range(2):
                copies.append(pltpu.make_async_copy(states[3 * k + i].at[at(i, unit)], s_in[i].at[slot, k], sem.at[slot, 5 * i + k]))
            copies.append(pltpu.make_async_copy(states[6 + i].at[at(i, unit)], g_in[i].at[slot], sem.at[slot, 5 * i + 2]))
        return copies

    def stores(unit, slot):
        return [
            pltpu.make_async_copy(s_out[i].at[slot, k], news[3 * k + i].at[at(i, unit)], sem.at[slot, 5 * i + 3 + k]) for i in range(3) for k in range(2)
        ]

    def work(unit, slot):
        for i in range(3):
            g = g_in[i][slot].astype(F32)
            s_out[i][slot, 0], s_out[i][slot, 1] = moment(s_in[i][slot, 0], s_in[i][slot, 1], g)

    ring = Ring(layers * parts, slots, loads, stores, work)
    ring.begin()
    ring.run()
    ring.end()


def moments(m, v, g, parts=9, slots=4):
    layers = m[0].shape[0]
    shapes = [(one.shape[1], one.shape[2] // parts) for one in m[:2]] + [(m[2].shape[1] // parts, m[2].shape[2])]
    size = sum(one.size for one in m)
    return pl.pallas_call(
        functools.partial(moments_kernel, layers, parts, slots),
        in_specs=[ANY] * 9,
        out_specs=[ANY] * 6,
        out_shape=[jax.ShapeDtypeStruct(one.shape, F32) for one in m] * 2,
        scratch_shapes=[
            *(pltpu.VMEM((slots, 2, *shape), F32) for shape in shapes),
            *(pltpu.VMEM((slots, *shape), BF16) for shape in shapes),
            *(pltpu.VMEM((slots, 2, *shape), F32) for shape in shapes),
            pltpu.SemaphoreType.DMA((slots, 15)),
        ],
        compiler_params=pltpu.CompilerParams(vmem_limit_bytes=VMEM_BYTES),
        cost_estimate=moves(18 * size),
        name="moments",
    )(*m, *v, *g)


def unfold(chunks, out, core):
    pairs, half = chunks.shape[0] - 1, LANES // 2
    for b in range(out.shape[1] // LANES):
        for n in range(pairs):
            out[pl.ds(pl.multiple_of(n * LANES + core * half, half), LANES), lanes(b)] = chunks[n, lanes(b), :]
        out[pl.ds(pl.multiple_of(pairs * LANES * (1 - core), half), half), lanes(b)] = chunks[pairs, pl.ds(b * half, half), :]


def place_rows_kernel(layers, slots, x_hbm, down_hbm, r_in, r_out, sem):
    devices = x_hbm.shape[2]
    pairs = x_hbm.shape[1] - 1
    height, d = r_out.shape[1:]

    def loads(unit, slot):
        layer, device = layers - 2 - unit // devices, lax.rem(unit, devices)
        return [
            pltpu.make_async_copy(x_hbm.at[layer, head(pairs), device], r_in.at[slot, head(pairs)], sem.at[slot, 0]),
            pltpu.make_async_copy(x_hbm.at[layer, pairs, device, head(d // 2)], r_in.at[slot, pairs, head(d // 2)], sem.at[slot, 1]),
        ]

    def stores(unit, slot):
        layer, device = unit // devices + 1, lax.rem(unit, devices)
        return [pltpu.make_async_copy(r_out.at[slot], down_hbm.at[layer, strip(device * height, height)], sem.at[slot, 2])]

    def work(unit, slot):
        unfold(r_in.at[slot], r_out.at[slot], lax.rem(unit, CORES))

    ring = Ring((layers - 1) * devices, slots, loads, stores, work)
    ring.begin()
    ring.run()
    ring.end()


def place_rows(chunks, layers, d, ff, slots=4):
    devices = chunks.shape[1]
    x = chunks.reshape(layers - 1, -1, devices, d, LANES)
    height = ff // devices
    return pl.pallas_call(
        functools.partial(place_rows_kernel, layers, slots),
        in_specs=[ANY],
        out_specs=ANY,
        out_shape=jax.ShapeDtypeStruct((layers, ff, d), BF16),
        scratch_shapes=[
            pltpu.VMEM((slots, x.shape[1], d, LANES), BF16),
            pltpu.VMEM((slots, height, d), BF16),
            pltpu.SemaphoreType.DMA((slots, 3)),
        ],
        compiler_params=pltpu.CompilerParams(vmem_limit_bytes=VMEM_BYTES),
        cost_estimate=moves(4 * d * ff),
        name="place_rows",
    )(x)


def place_blocks_kernel(wheres, me_ref, *refs):
    blocks, (gate_hbm, up_hbm, down_hbm, held, down, sem) = refs[: len(wheres)], refs[-6:]
    layers, d, ff = gate_hbm.shape
    height = down.shape[1]
    devices = ff // height
    chips, rows = devices // CORES, d // devices
    wide = ff // chips
    pairs = wide // LANES // 2
    chip, core = me_ref[0] // CORES, lax.rem(me_ref[0], CORES)

    def fetch(i):
        return pltpu.make_async_copy(blocks[i], held.at[i], sem.at[i, 0])

    def put(i):
        hops, flip = wheres[i]
        side = 1 - core if flip else core
        owner = lax.rem(chip + hops * (1 - 2 * side) + chips, chips) * CORES + side
        copies = [pltpu.make_async_copy(down.at[i], down_hbm.at[0, strip(owner * height, height)], sem.at[i, 1])]
        for n in range(LATE):
            step = 2 * pairs + 1 - LATE + n
            column = (step // 2 + (pairs + 1) * (step % 2)) * LANES
            for u, out in enumerate((gate_hbm, up_hbm)):
                for c in range(chips):
                    here = pl.ds(pairs * d + d // 2 + n * d + (u * chips + c) * rows, rows)
                    to = out.at[0, strip(owner * rows, rows), pl.ds(c * wide + column, LANES)]
                    copies.append(pltpu.make_async_copy(held.at[i, here], to, sem.at[i, 1 + len(copies)]))
        return side, copies

    number = len(wheres)
    for i in range(number):
        fetch(i).start()
    for i in range(number):
        fetch(i).wait()
        side, copies = put(i)
        start(copies[1:])
        for n in range(pairs + 1):
            size_n = d if n < pairs else d // 2
            for b in range(d // LANES):
                part = size_n // (d // LANES)
                at = n * LANES + side * (LANES // 2) if n < pairs else pairs * LANES * (1 - side)
                down[i, pl.ds(pl.multiple_of(at, LANES // 2), part), lanes(b)] = held[i, pl.ds(n * d + b * part, part), :]
        copies[0].start()
    for i in range(number):
        wait(put(i)[1])


def place_blocks(me, blocks, weights):
    wheres, blocks = tuple(blocks), list(blocks.values())
    number, rows = len(blocks), blocks[0].shape[0]
    layers, ff, d = weights[2].shape
    height = rows * LANES // d - LATE * LANES
    return pl.pallas_call(
        functools.partial(place_blocks_kernel, wheres),
        in_specs=[pl.BlockSpec(memory_space=pltpu.SMEM)] + [ANY] * (number + 3),
        out_specs=[ANY] * 3,
        out_shape=[jax.ShapeDtypeStruct(one.shape, BF16) for one in weights],
        input_output_aliases={number + 1 + i: i for i in range(3)},
        scratch_shapes=[
            pltpu.VMEM((number, rows, LANES), BF16),
            pltpu.VMEM((number, height, d), BF16),
            pltpu.SemaphoreType.DMA((number, 2 + LATE * ff // height)),
        ],
        compiler_params=pltpu.CompilerParams(vmem_limit_bytes=VMEM_BYTES),
        name="place_blocks",
    )(me, *blocks, *weights)


def solution(mesh):
    group = mesh.shape["dp"]
    swap = [(i, i ^ 1) for i in range(group)]
    onward = [(i, (i + CORES * (1 - 2 * (i % CORES))) % group) for i in range(group)]
    back = [(to, i) for i, to in onward]

    def step(x, dy, *arrays):
        weights, m, v = (arrays[i : i + 3] for i in (0, 3, 6))
        layers, d, ff = weights[0].shape
        me = lax.axis_index("dp").reshape(1)
        *sums, columns, rows, own, _ = backward(mesh, *forward(x[0], *weights, 0), dy[0], weights, m, v)

        def send(block, to):
            return lax.ppermute(block, "dp", to)

        behind, ahead = send(own, onward), send(own, back)
        gate, up = place_columns(columns, 1, layers, d, ff)
        first, *states = moments(m, v, sums)
        gate, first, behind, ahead = lax.optimization_barrier((gate, first, behind, ahead))
        opposite = send(behind, onward)
        near = {(0, 0): own, (-1, 0): behind, (1, 0): ahead}
        other = {(hops, 1): send(block, swap) for (hops, _), block in near.items()}
        gate, up = place_columns(columns, 0, layers, d, ff, (gate, up))
        up, rows = lax.optimization_barrier((up, rows))
        down = place_rows(rows, layers, d, ff)
        gate, up, down = place_blocks(me, near, (gate, up, down))
        down, opposite = lax.optimization_barrier((down, opposite))
        last = send(opposite, swap)
        weights = place_blocks(me, other, (gate, up, down))
        weights = place_blocks(me, {(2, 0): opposite, (2, 1): last}, weights)
        return (*weights, first, *states)

    seq, whole, rows = P(("rep", "dp"), None, None), P(None, None, None), P(None, "dp", None)
    return jax.shard_map(
        step,
        mesh=mesh,
        in_specs=(seq, seq, whole, whole, whole) + (rows,) * 6,
        out_specs=(P("rep", None, None),) * 3 + (P("rep", "dp", None),) * 6,
        check_vma=False,
    )
```

```python
import functools

import jax
import jax.numpy as jnp
from jax import lax
from jax.experimental import pallas as pl
from jax.experimental.pallas import tpu as pltpu
from jax.sharding import PartitionSpec as P

F32, BF16 = jnp.float32, jnp.bfloat16
NN, NT = (((1,), (0,)), ((), ())), (((1,), (1,)), ((), ()))
MESH = pl.DeviceIdType.MESH
ANY = pl.BlockSpec(memory_space=pl.ANY)
LANES = 128
CORES = 2
VMEM_BYTES = 67_043_328
COPY_FLOPS = 64
LATE = 2
SIDES = (0, 1), (1, -1)


def dot(a, b, dims=NN):
    return lax.dot_general(a, b, dims, preferred_element_type=F32)


def norm(h):
    wide = h.astype(F32)
    return (wide * lax.rsqrt(jnp.mean(wide**2, -1, keepdims=True) + 1e-6)).astype(BF16)


def strip(start, size):
    return pl.ds(pl.multiple_of(start, size), size)


def head(size):
    return pl.ds(0, size)


def parity(n):
    return lax.rem(n, 2)


def lanes(n):
    return pl.ds(n * LANES, LANES)


def start(copies):
    for copy in copies:
        copy.start()


def wait(copies):
    for copy in copies:
        copy.wait()


def moves(moved):
    return cost(COPY_FLOPS * moved, moved)


def cost(flops, moved):
    return pl.CostEstimate(flops=flops, bytes_accessed=moved, transcendentals=moved)


def forward_kernel(tile, x_ref, wg_ref, wu_ref, wd_ref, a_hbm, h_hbm, a_ref, total, ends, a_sem, end_sem):
    block = pl.program_id(0)
    first, last = block == 0, block == pl.num_programs(0) - 1
    tiles = x_ref.shape[0] // tile

    def keep(t):
        rows = strip(t * tile, tile)
        return pltpu.make_async_copy(a_ref.at[rows], a_hbm.at[0, rows], a_sem.at[t])

    def finish(t):
        rows = strip(t * tile, tile)
        for i, out in enumerate((h_hbm, a_hbm.at[1])):
            yield pltpu.make_async_copy(ends.at[parity(t), i], out.at[rows], end_sem.at[parity(t), i])

    @pl.when(first)
    def _():
        def begin(t, _):
            rows = strip(t * tile, tile)
            a_ref[rows, :] = norm(x_ref[rows, :])
            total[rows, :] = jnp.zeros((tile, total.shape[1]), F32)
            keep(t).start()
            return t

        lax.fori_loop(0, tiles, begin, 0)

    def one(t, _):
        rows = strip(t * tile, tile)
        a = a_ref[rows, :]
        gate, up = dot(a, wg_ref[...]), dot(a, wu_ref[...])
        z = (jax.nn.sigmoid(gate) * gate * up).astype(BF16)
        total[rows, :] += dot(z, wd_ref[...])

        @pl.when(last)
        def _():
            keep(t).wait()
            pl.when(t >= 2)(lambda: wait(finish(t - 2)))
            h = x_ref[rows, :] + total[rows, :].astype(BF16)
            for i, end in enumerate((h, norm(h))):
                ends[parity(t), i] = end
            start(finish(t))

        return t

    lax.fori_loop(0, tiles, one, 0)

    @pl.when(last)
    def _():
        for t in range(tiles - 2, tiles):
            wait(finish(t))


def forward(x, wg, wu, wd, layer, width=768, tile=512):
    tokens, d = x.shape
    ff = wg.shape[2]
    state = jax.ShapeDtypeStruct((tokens, d), BF16)
    columns = pl.BlockSpec((None, d, width), lambda i: (layer, 0, i))
    return pl.pallas_call(
        functools.partial(forward_kernel, tile),
        grid=(ff // width,),
        out_shape=[jax.ShapeDtypeStruct((2, tokens, d), BF16), state],
        in_specs=[pl.BlockSpec(x.shape, lambda i: (0, 0)), columns, columns, pl.BlockSpec((None, width, d), lambda i: (layer, i, 0))],
        out_specs=[ANY] * 2,
        scratch_shapes=[
            pltpu.VMEM(x.shape, BF16),
            pltpu.VMEM(x.shape, F32),
            pltpu.VMEM((2, 2, tile, d), BF16),
            pltpu.SemaphoreType.DMA((tokens // tile,)),
            pltpu.SemaphoreType.DMA((2, 2)),
        ],
        compiler_params=pltpu.CompilerParams(vmem_limit_bytes=VMEM_BYTES),
        cost_estimate=cost(6 * tokens * d * ff, 6 * d * ff),
        name="forward",
    )(x, wg, wu, wd)


class Pool:
    def __init__(self, number, chips, core, chip, bufs, sems, gathered):
        self.number, self.chips, self.core, self.chip = number, chips, core, chip
        self.mine, self.other, self.cross, self.near, self.out1, self.out2, self.sum, self.new = bufs
        self.dma, self.credit, self.out_sem, self.ag_sem, self.own_sem = sems
        self.gathered = gathered
        self.slots, self.lanes, self.turns = self.mine.shape[0], self.cross.shape[0], self.ag_sem.shape[0]

    def index(self, chip, core):
        return lax.rem(chip + self.chips, self.chips) * CORES + core

    def device(self, hops, core=None):
        return {"dp": self.index(self.chip + hops, self.core if core is None else core)}

    def partner(self):
        return self.device(0, 1 - self.core)

    def hop(self, sems, src, dst, to):
        return pltpu.make_async_remote_copy(src_ref=src, dst_ref=dst, send_sem=sems.at[0], recv_sem=sems.at[1], device_id=to, device_id_type=MESH)

    def copies0(self, n, rows):
        slot = lax.rem(n, self.slots)
        src = self.mine.at[slot, 1 - self.core, :, head(rows), :]
        return [self.hop(self.dma.at[slot, 0], src, self.other.at[slot, :, head(rows), :], self.partner())]

    def copies1(self, n, rows):
        slot, sem, half = lax.rem(n, self.lanes), lax.rem(n, self.slots), head(rows // 2)
        return [self.hop(self.dma.at[sem, 1 + side], self.out1.at[slot, side, half], self.cross.at[slot, side, half], self.device(hop)) for side, hop in SIDES]

    def copies2(self, n, rows):
        slot, sem, full = lax.rem(n, self.lanes), lax.rem(n, self.slots), head(rows)
        return [self.hop(self.dma.at[sem, 3 + side], self.out2.at[slot, side, full], self.near.at[slot, side, full], self.device(hop)) for side, hop in SIDES]

    def both(self, n, hops, start, size):
        slot, chip = lax.rem(n, self.slots), lax.rem(self.chip + hops + self.chips, self.chips)
        rows = pl.ds(start, size)
        return self.mine[slot, self.core, chip, rows, :].astype(F32) + self.other[slot, chip, rows, :].astype(F32)

    def give(self, kind, to):
        pl.semaphore_signal(self.credit.at[kind], inc=1, device_id=to, device_id_type=MESH)

    def take(self, when, kinds):
        @pl.when(when)
        def _():
            for kind in kinds:
                pl.semaphore_wait(self.credit.at[kind], 1)

    def event0(self, n, rows):
        self.take(n >= self.slots, (0,))
        start(self.copies0(n, rows))

    def event1(self, n, rows):
        slot, half = lax.rem(n, self.lanes), rows // 2
        wait(self.copies0(n, rows))
        for side, _ in SIDES:
            self.out1[slot, side, head(half)] = self.both(n, 2, side * half, half).astype(BF16)
        self.take(n >= self.lanes, (1, 2))
        start(self.copies1(n, rows))

    def event2(self, n, rows):
        slot, half = lax.rem(n, self.lanes), rows // 2
        wait(self.copies1(n, rows))
        for side, hop in SIDES:
            passed = self.both(n, hop, side * half, half) + self.cross[slot, side, head(half)].astype(F32)
            self.out2[slot, side, pl.ds(side * half, half), :] = passed.astype(BF16)
            self.out2[slot, side, pl.ds(half - side * half, half), :] = self.both(n, hop, half - side * half, half).astype(BF16)

        @pl.when(n + self.lanes < self.number)
        def _():
            for side, hop in SIDES:
                self.give(1 + side, self.device(-hop))

        self.take(n >= self.lanes, (3, 4))
        start(self.copies2(n, rows))

    def total(self, n, start, size):
        total = self.both(n, 0, start, size)
        for side, _ in SIDES:
            total += self.near[lax.rem(n, self.lanes), side, pl.ds(start, size), :].astype(F32)
        return total.astype(BF16).astype(F32)

    def event3(self, n, rows):
        wait(self.copies2(n, rows))

    def after3(self, n):
        pl.when(n + self.slots < self.number)(lambda: self.give(0, self.partner()))

        @pl.when(n + self.lanes < self.number)
        def _():
            for side, hop in SIDES:
                self.give(3 + side, self.device(-hop))

    def block(self, n, hops, core, start, size):
        return self.gathered.at[n, self.index(self.chip + hops, core), pl.ds(start, size), :]

    def sems(self, n, kind):
        return self.ag_sem.at[lax.rem(n, self.turns), kind]

    def gathers1(self, n, rows):
        new, own = self.new.at[head(rows)], self.block(n, 0, self.core, 0, rows)
        copies = [self.hop(self.sems(n, side), new, own, self.device(hop)) for side, hop in SIDES]
        return [*copies, self.hop(self.sems(n, 7), new, own, self.partner()), pltpu.make_async_copy(new, own, self.own_sem)]

    def gathers2(self, n, rows):
        copies, half = [], rows // 2
        for side, hop in SIDES:
            part, full = (self.block(n, -hop, self.core, *which) for which in ((side * half, half), (0, rows)))
            copies.append(self.hop(self.sems(n, 2 + side), part, part, self.device(hop)))
            copies.append(self.hop(self.sems(n, 4 + side), full, full, self.partner()))
        return copies

    def gathers3(self, n, rows):
        opposite = self.block(n, 2, self.core, 0, rows)
        return [self.hop(self.sems(n, 6), opposite, opposite, self.partner())]

    def gather1(self, n, rows):
        start(self.gathers1(n, rows))

    def gather2(self, n, rows):
        wait(self.gathers1(n, rows))
        start(self.gathers2(n, rows))

    def gather3(self, n, rows):
        wait(self.gathers2(n, rows))
        start(self.gathers3(n, rows))

    def gather4(self, n, rows):
        wait(self.gathers3(n, rows))


def moment(m, v, g):
    return 0.9 * m + 0.1 * g, 0.95 * v + 0.05 * g * g


def adam(w, m, v, g):
    m, v = moment(m, v, g)
    w = w.astype(F32)
    return (w - 0.02 * (m * lax.rsqrt(v + 1e-8) + 0.1 * w)).astype(BF16)


def backward_kernel(chips, tile, *refs):
    a_hbm, h_hbm, dy_hbm, wg_hbm, wu_hbm, wd_hbm, mg_hbm, mu_hbm, md_hbm, vg_hbm, vu_hbm, vd_hbm, *refs = refs
    gg_hbm, gu_hbm, gd_hbm, whole_gu, whole_dn, own_hbm, dy0_hbm, *refs = refs
    a_tile, dy_tile, at_ref, dyt_ref, da_ref, wg_ref, wu_ref, wd_ref, z_ref, dgu_ref, m_ref, v_ref, w_ref, *refs = refs
    tile_sem, w_sem, state_sem, own_sem, *pools = refs
    tokens, d = dy_hbm.shape
    layers, _, ff = wg_hbm.shape
    width = chips * LANES
    blocks = ff // width
    pairs = blocks // 2
    rows = d // (CORES * chips)
    lane_blocks = d // LANES
    me = lax.axis_index("dp")
    chip, core = me // CORES, lax.rem(me, CORES)
    tiles = tokens // tile
    steps = layers * blocks
    full, small, small_tile = d, d // 2, tile // 4

    gu = Pool(steps, chips, core, chip, pools[0:8], pools[8:13], whole_gu)
    dn = Pool(layers * (pairs + 1), chips, core, chip, pools[13:21], pools[21:26], whole_dn)

    def layer_of(j):
        return layers - 1 - j // blocks

    def block_of(j):
        j = lax.rem(j, blocks)
        return j // 2 + (pairs + 1) * parity(j)

    def columns(c, j):
        return strip(c * blocks * LANES + block_of(j) * LANES, LANES)

    def is_last(j):
        return lax.rem(j, blocks) == blocks - 1

    def gives_down(j):
        return (j >= 0) & (j < steps) & ((parity(lax.rem(j, blocks)) == 1) | is_last(j))

    def down_of(j):
        return (j // blocks) * (pairs + 1) + lax.rem(j, blocks) // 2

    def for_down(j, act):
        @pl.when(gives_down(j) & ~is_last(j))
        def _():
            act(down_of(j), full)

        @pl.when(gives_down(j) & is_last(j))
        def _():
            act(down_of(j), small)

    def weight_copies(j):
        layer, slot = layer_of(j), parity(j)
        for c in range(chips):
            there, here = columns(c, j), lanes(c)
            yield pltpu.make_async_copy(wg_hbm.at[layer, :, there], wg_ref.at[slot, :, here], w_sem.at[slot, 3 * c])
            yield pltpu.make_async_copy(wu_hbm.at[layer, :, there], wu_ref.at[slot, :, here], w_sem.at[slot, 3 * c + 1])
            yield pltpu.make_async_copy(wd_hbm.at[layer, there, :], wd_ref.at[slot, here, :], w_sem.at[slot, 3 * c + 2])

    def load(src, buf, t, which):
        slot = parity(t)
        return pltpu.make_async_copy(src.at[strip(t * tile, tile), :], buf.at[slot], tile_sem.at[slot, which])

    def start_tile(j, t):
        load(a_hbm.at[layer_of(j)], a_tile, t, 0).start()

        @pl.when(layer_of(j) == layers - 1)
        def _():
            load(dy_hbm, dy_tile, t, 1).start()

        @pl.when(layer_of(j) < layers - 1)
        def _():
            load(dy0_hbm, dy_tile, t, 1).start()

    def wait_tile(t):
        load(dy_hbm, a_tile, t, 0).wait()
        load(dy_hbm, dy_tile, t, 1).wait()

    def gu_parts(n):
        for c in range(chips):
            for u in range(2):
                yield u * chips + c, u, pl.ds((u * chips + c) * rows, rows), columns(c, n)

    def gu_outs(n):
        for i, u, here, there in gu_parts(n):
            yield pltpu.make_async_copy(gu.sum.at[here, :], (gg_hbm, gu_hbm)[u].at[layer_of(n), :, there], gu.out_sem.at[i])

    def gu_state(n):
        layer = layer_of(n)
        for i, u, here, there in gu_parts(n):
            for k, (src, buf) in enumerate((((mg_hbm, mu_hbm)[u], m_ref), ((vg_hbm, vu_hbm)[u], v_ref))):
                yield pltpu.make_async_copy(src.at[layer, :, there], buf.at[here, :], state_sem.at[3 * i + k])
            src = (wg_hbm, wu_hbm)[u].at[layer, strip(me * rows, rows), there]
            yield pltpu.make_async_copy(src, w_ref.at[here, :], state_sem.at[3 * i + 2])

    def dn_parts(n, size):
        step = lax.rem(n, pairs + 1)
        start = step * LANES + core * (LANES // 2) if size == full else pairs * LANES * (1 - core)
        height = size // lane_blocks
        for b in range(lane_blocks):
            yield b, layers - 1 - n // (pairs + 1), start, height, pl.ds(b * height, height), lanes(b)

    def dn_outs(n, size):
        for b, layer, start, height, here, there in dn_parts(n, size):
            at = pl.ds(pl.multiple_of(start, LANES // 2), height)
            yield pltpu.make_async_copy(dn.sum.at[here, :], gd_hbm.at[layer, at, there], dn.out_sem.at[b])

    def own_out(pool, at, size, sem):
        return [pltpu.make_async_copy(pool.new.at[head(size)], own_hbm.at[pl.ds(pl.multiple_of(at, LANES // 2), size)], own_sem.at[sem])]

    def dn_own(n, size):
        return own_out(dn, (n - (layers - 1) * (pairs + 1)) * full, size, 0)

    def gu_own(n):
        return own_out(gu, pairs * full + small + (n - steps + LATE) * full, full, 1)

    def dn_state(n, size):
        for b, layer, start, height, here, there in dn_parts(n, size):
            at = pl.ds(pl.multiple_of(start, LANES // 2), height)
            for k, (src, buf) in enumerate(((md_hbm, m_ref), (vd_hbm, v_ref))):
                yield pltpu.make_async_copy(src.at[layer, at, there], buf.at[here, :], state_sem.at[3 * b + k])
            at = pl.ds(pl.multiple_of(me * (d // 2) + start, LANES // 2), height)
            yield pltpu.make_async_copy(wd_hbm.at[layer, at, there], w_ref.at[here, :], state_sem.at[3 * b + 2])

    some = d // 3

    def gu_new(n, size):
        gu.event3(n, size)
        pl.when(n > 0)(lambda: wait(gu_outs(n - 1)))
        wait(gu_state(n))
        late = n >= steps - LATE
        pl.when(n > steps - LATE)(lambda: wait(gu_own(n - 1)))

        def piece(i, _):
            at = strip(i * some, some)
            g = gu.total(n, i * some, some)
            gu.sum[at, :] = g.astype(BF16)
            gu.new[at, :] = adam(w_ref[at, :], m_ref[at, :], v_ref[at, :], g)
            return i

        lax.fori_loop(0, size // some, piece, 0)
        gu.after3(n)
        start(gu_outs(n))
        pl.when(~late)(lambda: gu.gather1(n, size))
        pl.when(late)(lambda: start(gu_own(n)))

    def dn_new(n, size):
        half, height = LANES // 2, size // lane_blocks
        dn.event3(n, size)
        if size == full:
            begins = lax.rem(n, pairs + 1) == 0
            pl.when((n > 0) & ~begins)(lambda: wait(dn_outs(n - 1, full)))
            pl.when((n > 0) & begins)(lambda: wait(dn_outs(n - 1, small)))
        else:
            wait(dn_outs(n - 1, full))
        wait(dn_state(n, size))
        upper = n < (layers - 1) * (pairs + 1)
        pl.when(n > (layers - 1) * (pairs + 1))(lambda: wait(dn_own(n - 1, full)))

        def finish(at, g):
            dn.sum[at, :] = g.astype(BF16)
            dn.new[at, :] = adam(w_ref[at, :], m_ref[at, :], v_ref[at, :], g)

        if size == full:

            def piece(i, _):
                for start in range(0, some, LANES):
                    finish(strip(i * some + start, LANES), dn.total(n, i * some + start, LANES).T)
                return i

            lax.fori_loop(0, size // some, piece, 0)
        else:
            g = dn.total(n, 0, size).T
            g = jnp.concatenate([g[:half], g[half:]], 1)
            for b in range(lane_blocks):
                finish(pl.ds(b * height, height), g[:, b * LANES : (b + 1) * LANES])
        dn.after3(n)
        start(dn_outs(n, size))
        pl.when(upper)(lambda: dn.gather1(n, size))
        pl.when(~upper)(lambda: start(dn_own(n, size)))

    def turn(buf, slot, into, part):
        for b in range(lane_blocks):
            into[lanes(b), part] = buf[slot, :, b * LANES : (b + 1) * LANES].T

    start_tile(0, 0)
    start(weight_copies(0))
    barrier = pltpu.get_barrier_semaphore()
    peers = (gu.partner(), gu.device(1), gu.device(-1))
    for peer in peers:
        pl.semaphore_signal(barrier, inc=1, device_id=peer, device_id_type=MESH)
    pl.semaphore_wait(barrier, len(peers))

    def keep(t):
        slot = parity(t)
        return pltpu.make_async_copy(dy_tile.at[slot], dy0_hbm.at[strip(t * tile, tile)], tile_sem.at[slot, 2])

    def compute_tile(j, t):
        slot, here = parity(j), parity(t)
        part = strip(t * tile, tile)
        wait_tile(t)
        pl.when(t + 1 < tiles)(lambda: start_tile(j, t + 1))
        a, dy = a_tile[here], dy_tile[here]
        for c in range(0, chips, 2):
            some = pl.ds(c * LANES, 2 * LANES)
            gate = dot(a, wg_ref[slot, :, some])
            up = dot(a, wu_ref[slot, :, some])
            dz = dot(dy, wd_ref[slot, some, :], NT).astype(BF16).astype(F32)
            s = jax.nn.sigmoid(gate)
            act = s * gate
            z_ref[part, some] = (act * up).astype(BF16)
            dgu_ref[1, part, some] = (dz * act).astype(BF16)
            dgu_ref[0, part, some] = (dz * up * (s + act * (1 - s))).astype(BF16)

        turn(a_tile, here, at_ref, part)
        turn(dy_tile, here, dyt_ref, part)

        @pl.when(j == 0)
        def _():
            da_ref[part, :] = jnp.zeros((tile, d), F32)

    def compute_gate_up(j, u):
        slot = lax.rem(j, gu.slots)
        g = dot(at_ref[...], dgu_ref[u]).astype(BF16)
        for c in range(chips):
            at = strip((u * chips + c) * rows, rows)
            for owner in range(CORES * chips):
                gu.mine[slot, owner % CORES, owner // CORES, at, :] = g[owner * rows : (owner + 1) * rows, c * LANES : (c + 1) * LANES]

    def compute_down(j, _):
        slot, owner = lax.rem(down_of(j), dn.slots), parity(lax.rem(j, blocks))

        @pl.when(~is_last(j))
        def _():
            g = dot(dyt_ref[...], z_ref[...]).astype(BF16)
            for c in range(chips):
                dn.mine[slot, owner, c, :, :] = g[:, c * LANES : (c + 1) * LANES]

        @pl.when(is_last(j))
        def _():
            half = LANES // 2
            low = lax.broadcasted_iota(jnp.int32, (small, LANES), 1) < half

            def one(h, _):
                both = dot(dyt_ref[...], z_ref[:, strip(h * 2 * LANES, 2 * LANES)])
                for c in range(2):
                    straight = both[:, c * LANES : (c + 1) * LANES]
                    turned = pltpu.roll(straight, half, 1)
                    dn.mine[slot, 0, 2 * h + c, head(small), :] = jnp.where(low, straight[:small], turned[small:]).astype(BF16)
                    dn.mine[slot, 1, 2 * h + c, head(small), :] = jnp.where(low, turned[:small], straight[small:]).astype(BF16)
                return h

            lax.fori_loop(0, chips // 2, one, 0)

    def compute_da(j, t):
        slot, part = parity(j), strip(t * 2 * tile, 2 * tile)
        middle = lane_blocks // 2 * LANES
        for begin, end in ((0, middle), (middle, d)):
            some = pl.ds(begin, end - begin)
            da_ref[part, some] += dot(dgu_ref[0, part, :], wg_ref[slot, some, :], NT) + dot(dgu_ref[1, part, :], wu_ref[slot, some, :], NT)

    def begin_change(t):
        load(h_hbm, a_tile, t, 0).start()
        load(dy_hbm, dy_tile, t, 1).start()

    def change_layer():
        def one(t, _):
            slot = parity(t)
            wait_tile(t)
            pl.when(t > 0)(lambda: keep(t - 1).wait())
            pl.when(t + 1 < tiles)(lambda: begin_change(t + 1))
            pl.when(t + 1 == tiles)(lambda: start_tile(blocks, 0))

            def piece(i, _):
                here, there = strip(i * small_tile, small_tile), strip(t * tile + i * small_tile, small_tile)
                wide = a_tile[slot, here, :].astype(F32)
                da = da_ref[there, :].astype(BF16).astype(F32)
                scale = lax.rsqrt(jnp.mean(wide * wide, -1, keepdims=True) + 1e-6)
                along = jnp.mean(da * wide, -1, keepdims=True)
                back = (da * scale - wide * (along * scale * scale * scale)).astype(BF16)
                dy_tile[slot, here, :] = dy_tile[slot, here, :] + back
                return 0

            lax.fori_loop(0, tile // small_tile, piece, 0)
            keep(t).start()
            return 0

        lax.fori_loop(0, tiles, one, 0)
        keep(tiles - 1).wait()

    def on(j, act):
        pl.when((j >= 0) & (j < steps))(lambda: act(j, full))

    def early(j, act):
        pl.when(j < steps - LATE)(lambda: on(j, act))

    def upper_down(j, act):
        pl.when(j < (layers - 1) * blocks)(lambda: for_down(j, act))

    def gu_load(n, rows):
        start(gu_state(n))

    def dn_load(n, rows):
        start(dn_state(n, rows))

    events = {
        "tile0": [(on, gu_new, 2)],
        "tile1": [(upper_down, dn.gather2, 2), (for_down, dn_load, 1)],
        "tile3": [(upper_down, dn.gather3, 3), (on, gu.event2, 1)],
        "down0": [(for_down, dn.event0)],
        "gate0": [(early, gu.gather3, 3), (for_down, dn.event1)],
        "gate1": [(on, gu.event0), (early, gu.gather4, 3), (early, gu.gather2, 2), (for_down, dn_new, 1)],
        "back0": [(upper_down, dn.gather4, 3), (on, gu.event1), (on, gu_load, 1)],
        "back1": [(for_down, dn.event2)],
    }
    longest = max(sum(ago) for these in events.values() for _, _, *ago in these)

    def step(j, _):
        busy = j < steps
        lower = layer_of(j) > 0
        changes = is_last(j) & lower & busy

        @pl.when(busy)
        def _():
            wait(weight_copies(j))
            pl.when(j + 1 < steps)(lambda: start(weight_copies(j + 1)))

        def parts(name, number, active, compute):
            def one(t, _):
                pl.when(active)(lambda: compute(j, t))
                for at in range(number):

                    @pl.when(t == at)
                    def _():
                        for stream, act, *ago in events.get(f"{name}{at}", ()):
                            stream(j - sum(ago), act)

                return 0

            lax.fori_loop(0, number, one, 0)

        def da_halves(j, t):
            pl.when(changes & (t == 0))(lambda: begin_change(0))
            compute_da(j, t)

        parts("tile", tiles, busy, compute_tile)
        pl.when(busy & (j + 1 < steps) & ~changes)(lambda: start_tile(j + 1, 0))
        parts("down", 1, busy, compute_down)
        parts("gate", 2, busy, compute_gate_up)
        parts("back", tiles // 2, busy & lower, da_halves)

        pl.when(changes)(change_layer)

        return 0

    lax.fori_loop(0, steps + longest, step, 0)
    wait(gu_outs(steps - 1))
    wait(dn_outs(dn.number - 1, small))
    wait(dn_own(dn.number - 1, small))
    wait(gu_own(steps - 1))


def backward(mesh, a, h, dy, weights, m, v, tile=512):
    tokens, d = dy.shape
    layers, _, ff = weights[0].shape
    chips = mesh.shape["dp"] // CORES
    width = chips * LANES
    blocks = ff // width
    pairs = blocks // 2
    rows = d // (CORES * chips)
    assert layers == 2 and chips == 4 and blocks % 2 == 1 and blocks * width == ff and d % LANES == 0
    shape = lambda *s: jax.ShapeDtypeStruct(s, BF16)
    devices = CORES * chips
    outs = [
        shape(layers, rows, ff),
        shape(layers, rows, ff),
        shape(layers, ff // devices, d),
        shape(layers * blocks, devices, d, LANES),
        shape((layers - 1) * (pairs + 1), devices, d, LANES),
        shape(pairs * d + d // 2 + LATE * d, LANES),
        shape(tokens, d),
    ]

    def pool(lanes, outputs):
        return [
            pltpu.VMEM((2, CORES, chips, d, LANES), BF16),
            pltpu.VMEM((2, chips, d, LANES), BF16),
            pltpu.VMEM((lanes, 2, d // 2, LANES), BF16),
            pltpu.VMEM((lanes, 2, d, LANES), BF16),
            pltpu.VMEM((lanes, 2, d // 2, LANES), BF16),
            pltpu.VMEM((lanes, 2, d, LANES), BF16),
            pltpu.VMEM((d, LANES), BF16),
            pltpu.VMEM((d, LANES), BF16),
            pltpu.SemaphoreType.DMA((2, 5, 2)),
            pltpu.SemaphoreType.REGULAR((5,)),
            pltpu.SemaphoreType.DMA((outputs,)),
            pltpu.SemaphoreType.DMA((4, 8, 2)),
            pltpu.SemaphoreType.DMA,
        ]

    return pl.pallas_call(
        functools.partial(backward_kernel, chips, tile),
        out_shape=outs,
        in_specs=[ANY] * 12,
        out_specs=[ANY] * len(outs),
        scratch_shapes=[
            pltpu.VMEM((2, tile, d), BF16),
            pltpu.VMEM((2, tile, d), BF16),
            pltpu.VMEM((d, tokens), BF16),
            pltpu.VMEM((d, tokens), BF16),
            pltpu.VMEM((tokens, d), F32),
            pltpu.VMEM((2, d, width), BF16),
            pltpu.VMEM((2, d, width), BF16),
            pltpu.VMEM((2, width, d), BF16),
            pltpu.VMEM((tokens, width), BF16),
            pltpu.VMEM((2, tokens, width), BF16),
            pltpu.VMEM((d, LANES), F32),
            pltpu.VMEM((d, LANES), F32),
            pltpu.VMEM((d, LANES), BF16),
            pltpu.SemaphoreType.DMA((2, 3)),
            pltpu.SemaphoreType.DMA((2, 3 * chips)),
            pltpu.SemaphoreType.DMA((max(6 * chips, 3 * (d // LANES)),)),
            pltpu.SemaphoreType.DMA((2,)),
            *pool(1, 2 * chips),
            *pool(2, d // LANES),
        ],
        compiler_params=pltpu.CompilerParams(collective_id=1, has_side_effects=True, vmem_limit_bytes=VMEM_BYTES),
        cost_estimate=cost(28 * tokens * d * ff, 24 * d * ff),
        name="backward",
    )(a, h, dy, *weights, *m, *v)


class Ring:
    def __init__(self, units, slots, loads, stores, work):
        self.units, self.slots, self.loads, self.stores, self.work = units, slots, loads, stores, work

    def begin(self):
        for unit in range(self.slots):
            for copy in self.loads(unit, unit):
                copy.start()

    def run(self):
        def one(unit, _):
            slot = lax.rem(unit, self.slots)
            for copy in self.loads(unit, slot):
                copy.wait()

            @pl.when(unit >= self.slots)
            def _():
                for copy in self.stores(unit - self.slots, slot):
                    copy.wait()

            self.work(unit, slot)
            for copy in self.stores(unit, slot):
                copy.start()

            @pl.when(unit + self.slots < self.units)
            def _():
                for copy in self.loads(unit + self.slots, slot):
                    copy.start()

            return 0

        lax.fori_loop(0, self.units, one, 0)

    def end(self):
        for unit in range(self.units - self.slots, self.units):
            for copy in self.stores(unit, unit % self.slots):
                copy.wait()


def place_columns_kernel(layer, slots, x_hbm, *refs):
    gate_hbm, up_hbm, c_in, c_out, sem = refs[-5:]
    _, blocks, devices, _, chips, rows, _ = x_hbm.shape
    wide, there, some = blocks * LANES, *c_in.shape[1:3]
    spots = [j // 2 + (blocks // 2 + 1) * (j % 2) for j in range(there)]
    begins = [at for at in spots if at - 1 not in spots]
    ends = [at + 1 for at in spots if at + 1 not in spots]
    spans = list(zip(sorted(begins), sorted(ends)))
    turns = devices // some

    def place(unit):
        return unit // turns, lax.rem(unit, turns) * some

    def loads(unit, slot):
        chip, owners = place(unit)
        return [pltpu.make_async_copy(x_hbm.at[x_hbm.shape[0] - 1 - layer, head(there), pl.ds(owners, some), :, chip], c_in.at[slot], sem.at[slot, 0])]

    def stores(unit, slot):
        chip, owners = place(unit)
        copies = []
        for begin, end in spans:
            size = (end - begin) * LANES
            to = layer, strip(owners * rows, some * rows), pl.ds(pl.multiple_of(chip * wide + begin * LANES, LANES), size)
            for u, out in enumerate((gate_hbm, up_hbm)):
                copies.append(pltpu.make_async_copy(c_out.at[slot, u, :, pl.ds(begin * LANES, size)], out.at[to], sem.at[slot, 1 + len(copies)]))
        return copies

    def work(unit, slot):
        for j, at in enumerate(spots):
            for owner in range(some):
                for u in range(2):
                    c_out[slot, u, pl.ds(owner * rows, rows), lanes(at)] = c_in[slot, j, owner, u]

    ring = Ring(chips * turns, slots, loads, stores, work)
    ring.begin()
    ring.run()
    ring.end()


def place_columns(chunks, layer, layers, d, ff, into=(), slots=3, some=4):
    devices = chunks.shape[1]
    chips, rows = devices // CORES, d // devices
    x = chunks.reshape(layers, -1, devices, 2, chips, rows, LANES)
    there = x.shape[1] - LATE * (layer == 0)
    return pl.pallas_call(
        functools.partial(place_columns_kernel, layer, slots),
        in_specs=[ANY] * (1 + len(into)),
        out_specs=[ANY] * 2,
        input_output_aliases={1 + i: i for i in range(len(into))},
        out_shape=[jax.ShapeDtypeStruct((layers, d, ff), BF16)] * 2,
        scratch_shapes=[
            pltpu.VMEM((slots, there, some, 2, rows, LANES), BF16),
            pltpu.VMEM((slots, 2, some * rows, ff // chips), BF16),
            pltpu.SemaphoreType.DMA((slots, devices)),
        ],
        compiler_params=pltpu.CompilerParams(vmem_limit_bytes=VMEM_BYTES),
        cost_estimate=moves(8 * d * ff),
        name="place_columns",
    )(x, *into)


def moments_kernel(layers, parts, slots, *refs):
    states, news, s_in, g_in, s_out, sem = refs[:9], refs[9:15], refs[15:18], refs[18:21], refs[21:24], refs[24]

    def at(i, unit):
        layer, part = unit // parts, lax.rem(unit, parts)
        _, r, c = states[i].shape
        return (layer, strip(part * (r // parts), r // parts), slice(None)) if i == 2 else (layer, slice(None), strip(part * (c // parts), c // parts))

    def loads(unit, slot):
        copies = []
        for i in range(3):
            for k in range(2):
                copies.append(pltpu.make_async_copy(states[3 * k + i].at[at(i, unit)], s_in[i].at[slot, k], sem.at[slot, 5 * i + k]))
            copies.append(pltpu.make_async_copy(states[6 + i].at[at(i, unit)], g_in[i].at[slot], sem.at[slot, 5 * i + 2]))
        return copies

    def stores(unit, slot):
        return [
            pltpu.make_async_copy(s_out[i].at[slot, k], news[3 * k + i].at[at(i, unit)], sem.at[slot, 5 * i + 3 + k]) for i in range(3) for k in range(2)
        ]

    def work(unit, slot):
        for i in range(3):
            g = g_in[i][slot].astype(F32)
            s_out[i][slot, 0], s_out[i][slot, 1] = moment(s_in[i][slot, 0], s_in[i][slot, 1], g)

    ring = Ring(layers * parts, slots, loads, stores, work)
    ring.begin()
    ring.run()
    ring.end()


def moments(m, v, g, parts=9, slots=4):
    layers = m[0].shape[0]
    shapes = [(one.shape[1], one.shape[2] // parts) for one in m[:2]] + [(m[2].shape[1] // parts, m[2].shape[2])]
    size = sum(one.size for one in m)
    return pl.pallas_call(
        functools.partial(moments_kernel, layers, parts, slots),
        in_specs=[ANY] * 9,
        out_specs=[ANY] * 6,
        out_shape=[jax.ShapeDtypeStruct(one.shape, F32) for one in m] * 2,
        scratch_shapes=[
            *(pltpu.VMEM((slots, 2, *shape), F32) for shape in shapes),
            *(pltpu.VMEM((slots, *shape), BF16) for shape in shapes),
            *(pltpu.VMEM((slots, 2, *shape), F32) for shape in shapes),
            pltpu.SemaphoreType.DMA((slots, 15)),
        ],
        compiler_params=pltpu.CompilerParams(vmem_limit_bytes=VMEM_BYTES),
        cost_estimate=moves(18 * size),
        name="moments",
    )(*m, *v, *g)


def unfold(chunks, out, core):
    pairs, half = chunks.shape[0] - 1, LANES // 2
    for b in range(out.shape[1] // LANES):
        for n in range(pairs):
            out[pl.ds(pl.multiple_of(n * LANES + core * half, half), LANES), lanes(b)] = chunks[n, lanes(b), :]
        out[pl.ds(pl.multiple_of(pairs * LANES * (1 - core), half), half), lanes(b)] = chunks[pairs, pl.ds(b * half, half), :]


def place_rows_kernel(layers, slots, x_hbm, down_hbm, r_in, r_out, sem):
    devices = x_hbm.shape[2]
    pairs = x_hbm.shape[1] - 1
    height, d = r_out.shape[1:]

    def loads(unit, slot):
        layer, device = layers - 2 - unit // devices, lax.rem(unit, devices)
        return [
            pltpu.make_async_copy(x_hbm.at[layer, head(pairs), device], r_in.at[slot, head(pairs)], sem.at[slot, 0]),
            pltpu.make_async_copy(x_hbm.at[layer, pairs, device, head(d // 2)], r_in.at[slot, pairs, head(d // 2)], sem.at[slot, 1]),
        ]

    def stores(unit, slot):
        layer, device = unit // devices + 1, lax.rem(unit, devices)
        return [pltpu.make_async_copy(r_out.at[slot], down_hbm.at[layer, strip(device * height, height)], sem.at[slot, 2])]

    def work(unit, slot):
        unfold(r_in.at[slot], r_out.at[slot], lax.rem(unit, CORES))

    ring = Ring((layers - 1) * devices, slots, loads, stores, work)
    ring.begin()
    ring.run()
    ring.end()


def place_rows(chunks, layers, d, ff, slots=4):
    devices = chunks.shape[1]
    x = chunks.reshape(layers - 1, -1, devices, d, LANES)
    height = ff // devices
    return pl.pallas_call(
        functools.partial(place_rows_kernel, layers, slots),
        in_specs=[ANY],
        out_specs=ANY,
        out_shape=jax.ShapeDtypeStruct((layers, ff, d), BF16),
        scratch_shapes=[
            pltpu.VMEM((slots, x.shape[1], d, LANES), BF16),
            pltpu.VMEM((slots, height, d), BF16),
            pltpu.SemaphoreType.DMA((slots, 3)),
        ],
        compiler_params=pltpu.CompilerParams(vmem_limit_bytes=VMEM_BYTES),
        cost_estimate=moves(4 * d * ff),
        name="place_rows",
    )(x)


def place_blocks_kernel(wheres, me_ref, *refs):
    blocks, (gate_hbm, up_hbm, down_hbm, held, down, sem) = refs[: len(wheres)], refs[-6:]
    layers, d, ff = gate_hbm.shape
    height = down.shape[1]
    devices = ff // height
    chips, rows = devices // CORES, d // devices
    wide = ff // chips
    pairs = wide // LANES // 2
    chip, core = me_ref[0] // CORES, lax.rem(me_ref[0], CORES)

    def fetch(i):
        return pltpu.make_async_copy(blocks[i], held.at[i], sem.at[i, 0])

    def put(i):
        hops, flip = wheres[i]
        side = 1 - core if flip else core
        owner = lax.rem(chip + hops * (1 - 2 * side) + chips, chips) * CORES + side
        copies = [pltpu.make_async_copy(down.at[i], down_hbm.at[0, strip(owner * height, height)], sem.at[i, 1])]
        for n in range(LATE):
            step = 2 * pairs + 1 - LATE + n
            column = (step // 2 + (pairs + 1) * (step % 2)) * LANES
            for u, out in enumerate((gate_hbm, up_hbm)):
                for c in range(chips):
                    here = pl.ds(pairs * d + d // 2 + n * d + (u * chips + c) * rows, rows)
                    to = out.at[0, strip(owner * rows, rows), pl.ds(c * wide + column, LANES)]
                    copies.append(pltpu.make_async_copy(held.at[i, here], to, sem.at[i, 1 + len(copies)]))
        return side, copies

    number = len(wheres)
    for i in range(number):
        fetch(i).start()
    for i in range(number):
        fetch(i).wait()
        side, copies = put(i)
        start(copies[1:])
        for n in range(pairs + 1):
            size_n = d if n < pairs else d // 2
            for b in range(d // LANES):
                part = size_n // (d // LANES)
                at = n * LANES + side * (LANES // 2) if n < pairs else pairs * LANES * (1 - side)
                down[i, pl.ds(pl.multiple_of(at, LANES // 2), part), lanes(b)] = held[i, pl.ds(n * d + b * part, part), :]
        copies[0].start()
    for i in range(number):
        wait(put(i)[1])


def place_blocks(me, blocks, weights):
    wheres, blocks = tuple(blocks), list(blocks.values())
    number, rows = len(blocks), blocks[0].shape[0]
    layers, ff, d = weights[2].shape
    height = rows * LANES // d - LATE * LANES
    return pl.pallas_call(
        functools.partial(place_blocks_kernel, wheres),
        in_specs=[pl.BlockSpec(memory_space=pltpu.SMEM)] + [ANY] * (number + 3),
        out_specs=[ANY] * 3,
        out_shape=[jax.ShapeDtypeStruct(one.shape, BF16) for one in weights],
        input_output_aliases={number + 1 + i: i for i in range(3)},
        scratch_shapes=[
            pltpu.VMEM((number, rows, LANES), BF16),
            pltpu.VMEM((number, height, d), BF16),
            pltpu.SemaphoreType.DMA((number, 2 + LATE * ff // height)),
        ],
        compiler_params=pltpu.CompilerParams(vmem_limit_bytes=VMEM_BYTES),
        name="place_blocks",
    )(me, *blocks, *weights)


def solution(mesh):
    group = mesh.shape["dp"]
    swap = [(i, i ^ 1) for i in range(group)]
    onward = [(i, (i + CORES * (1 - 2 * (i % CORES))) % group) for i in range(group)]
    back = [(to, i) for i, to in onward]

    def step(x, dy, *arrays):
        weights, m, v = (arrays[i : i + 3] for i in (0, 3, 6))
        layers, d, ff = weights[0].shape
        me = lax.axis_index("dp").reshape(1)
        *sums, columns, rows, own, _ = backward(mesh, *forward(x[0], *weights, 0), dy[0], weights, m, v)

        def send(block, to):
            return lax.ppermute(block, "dp", to)

        behind, ahead = send(own, onward), send(own, back)
        gate, up = place_columns(columns, 1, layers, d, ff)
        first, *states = moments(m, v, sums)
        gate, first, behind, ahead = lax.optimization_barrier((gate, first, behind, ahead))
        opposite = send(behind, onward)
        near = {(0, 0): own, (-1, 0): behind, (1, 0): ahead}
        other = {(hops, 1): send(block, swap) for (hops, _), block in near.items()}
        gate, up = place_columns(columns, 0, layers, d, ff, (gate, up))
        up, rows = lax.optimization_barrier((up, rows))
        down = place_rows(rows, layers, d, ff)
        gate, up, down = place_blocks(me, near, (gate, up, down))
        down, opposite = lax.optimization_barrier((down, opposite))
        last = send(opposite, swap)
        weights = place_blocks(me, {**other, (2, 0): opposite}, (gate, up, down))
        weights = place_blocks(me, {(2, 1): last}, weights)
        return (*weights, first, *states)

    seq, whole, rows = P(("rep", "dp"), None, None), P(None, None, None), P(None, "dp", None)
    return jax.shard_map(
        step,
        mesh=mesh,
        in_specs=(seq, seq, whole, whole, whole) + (rows,) * 6,
        out_specs=(P("rep", None, None),) * 3 + (P("rep", "dp", None),) * 6,
        check_vma=False,
    )
```
